8 devices in a mesh: x: 2 (over z, y), yz: 4 (over x, core).
Axes of the slice: x: 2, y: 2, z: 1, core: 2. Of those that a mesh axis runs over, the one named last changes fastest.
Arguments:
- x_in: bfloat16 [192, 2560], P(None, ('x', 'yz'))
- ln_scale: float32 [2560], P(('x', 'yz'))
- w_gate_up: bfloat16 [2560, 2, 10240], P('x', None, 'yz')
- w_attn: bfloat16 [2560, 2720], P('x', 'yz')
- w_down: bfloat16 [10240, 2560], P('yz', 'x')
- w_out: bfloat16 [2560, 2560], P('yz', 'x')
- k_cache: bfloat16 [192, 4096, 80], P(('x', 'yz'))
- v_cache: bfloat16 [192, 4096, 80], P(('x', 'yz'))
- lengths: int32 [192], P(('x', 'yz'))
- positions: int32 [192], P(('x', 'yz'))
Outputs:
- output 1: bfloat16 [192, 2560], P(None, ('x', 'yz'))
- output 2: bfloat16 [192, 4096, 80], P(('x', 'yz'))
- output 3: bfloat16 [192, 4096, 80], P(('x', 'yz'))
All inputs are finite; a program needn't handle non-finite values.
Results may differ from the reference program's by a relative error of at most 0.00361131.
Values are sent between devices in bfloat16 or wider.
A program may use at most 1 GiB of HBM per device.

```python
import math
import jax
import jax.numpy as jnp
from jax import lax

D = 2560
FF = 10240
HEADS = 32
HEAD = 80
BATCH = 192
SEQ = 4096

LN_EPS = 1e-6
ROPE_BASE = 10000.0


def setup_inputs(seed: int = 0) -> dict:
    key_list = jax.random.split(jax.random.key(seed), 12)
    q_width = HEADS * HEAD
    key_scale = math.sqrt(math.log(SEQ / 16.0))
    x_in = jax.random.normal(key_list[0], (BATCH, D), jnp.float32)
    ln_scale = jax.random.uniform(key_list[1], (D,), jnp.float32, 0.5, 1.5)
    w_gate_up = jax.random.normal(key_list[2], (D, 2, FF), jnp.float32) * D ** -0.5
    w_attn = jax.random.normal(key_list[3], (D, q_width + 2 * HEAD), jnp.float32) * D ** -0.5
    w_down = jax.random.normal(key_list[4], (FF, D), jnp.float32) * FF ** -0.5
    w_out = jax.random.normal(key_list[5], (q_width, D), jnp.float32) * q_width ** -0.5
    k_cache = jax.random.normal(key_list[6], (BATCH, SEQ, HEAD), jnp.float32) * key_scale
    v_cache = jax.random.normal(key_list[7], (BATCH, SEQ, HEAD), jnp.float32) * 2.0
    len_keys = jax.random.split(key_list[8], 3)
    lengths = jax.random.randint(len_keys[0], (BATCH,), SEQ // 8, SEQ, jnp.int32)
    long_row = jax.random.randint(len_keys[1], (), 0, BATCH, jnp.int32)
    short_row = (long_row + 1 + jax.random.randint(len_keys[2], (), 0, BATCH - 1, jnp.int32)) % BATCH
    lengths = lengths.at[long_row].set(SEQ - 1).at[short_row].set(SEQ // 8)
    positions = jax.random.randint(key_list[9], (BATCH,), 0, 2 * SEQ, jnp.int32)
    return {
        'x_in': x_in.astype(jnp.bfloat16),
        'ln_scale': ln_scale,
        'w_gate_up': w_gate_up.astype(jnp.bfloat16),
        'w_attn': w_attn.astype(jnp.bfloat16),
        'w_down': w_down.astype(jnp.bfloat16),
        'w_out': w_out.astype(jnp.bfloat16),
        'k_cache': k_cache.astype(jnp.bfloat16),
        'v_cache': v_cache.astype(jnp.bfloat16),
        'lengths': lengths,
        'positions': positions,
    }


def rotary(values, positions):
    half_dim = values.shape[-1] // 2
    inv_freq = ROPE_BASE ** (-jnp.arange(half_dim, dtype=jnp.float32) / half_dim)
    angles = positions.astype(jnp.float32)[:, None, None] * inv_freq
    cos_part = jnp.cos(angles)
    sin_part = jnp.sin(angles)
    lo_half = values[..., :half_dim]
    hi_half = values[..., half_dim:]
    return jnp.concatenate([lo_half * cos_part - hi_half * sin_part, hi_half * cos_part + lo_half * sin_part], axis=-1)


def reference(x_in, ln_scale, w_gate_up, w_attn, w_down, w_out, k_cache, v_cache, lengths, positions):
    q_width = HEADS * HEAD
    x_float = x_in.astype(jnp.float32)
    mean_val = jnp.sum(x_float, axis=1, keepdims=True) / D
    var_val = jnp.sum(x_float * x_float, axis=1, keepdims=True) / D - mean_val * mean_val
    normed = ((x_float - mean_val) * lax.rsqrt(var_val + LN_EPS) * ln_scale).astype(jnp.bfloat16)
    gate_up = jnp.dot(normed, w_gate_up.reshape(D, 2 * FF), preferred_element_type=jnp.float32)
    gate_up = gate_up.astype(jnp.bfloat16).reshape(BATCH, 2, FF)
    hidden = (jax.nn.silu(gate_up[:, 0].astype(jnp.float32)) * gate_up[:, 1].astype(jnp.float32)).astype(jnp.bfloat16)
    proj_all = jnp.dot(normed, w_attn, preferred_element_type=jnp.float32).astype(jnp.bfloat16)
    q_raw = proj_all[:, :q_width].reshape(BATCH, HEADS, HEAD)
    k_tok = proj_all[:, q_width:q_width + HEAD]
    v_tok = proj_all[:, q_width + HEAD:]
    q_rot = rotary(q_raw.astype(jnp.float32), positions).astype(jnp.bfloat16)
    k_rot = rotary(k_tok[:, None, :].astype(jnp.float32), positions)[:, 0].astype(jnp.bfloat16)
    slot_ids = jnp.arange(SEQ)
    new_slot = (slot_ids[None, :] == lengths[:, None])[:, :, None]
    k_new = jnp.where(new_slot, k_rot[:, None, :], k_cache)
    v_new = jnp.where(new_slot, v_tok[:, None, :], v_cache)

    def row_attention(row_args):
        q_row, k_row, v_row, row_len = row_args
        scores = jnp.dot(q_row, k_row.T, preferred_element_type=jnp.float32) * HEAD ** -0.5
        scores = jnp.where(slot_ids[None, :] <= row_len, scores, -1e30)
        prob_row = jax.nn.softmax(scores, axis=-1).astype(jnp.bfloat16)
        return jnp.dot(prob_row, v_row, preferred_element_type=jnp.float32).astype(jnp.bfloat16)

    attn_out = lax.map(row_attention, (q_rot, k_new, v_new, lengths))
    o_flat = attn_out.reshape(BATCH, q_width)
    mixed_sum = jnp.dot(hidden, w_down, preferred_element_type=jnp.float32) + jnp.dot(o_flat, w_out, preferred_element_type=jnp.float32)
    y_out = (x_float + mixed_sum).astype(jnp.bfloat16)
    return (y_out, k_new, v_new)
```

```python
import functools

import jax
import jax.numpy as jnp
from jax import lax
from jax.experimental import pallas as pl
from jax.experimental.pallas import tpu as pltpu
from jax.sharding import PartitionSpec as P

LN_EPS = 1e-6
ROPE_BASE = 10000.0
VMEM_MOST = 64 * 1024 * 1024 - 64 * 1024


def attention_kernel(scale, len_ref, q_ref, cols_ref, k_hbm, v_hbm, o_ref, ko_hbm, vo_hbm, k_buf, v_buf, in_sem, out_sem):
    rows, _, seq_len = k_buf.shape

    def load(which, b):
        src, dst = ((k_hbm, k_buf), (v_hbm, v_buf))[which]
        return pltpu.make_async_copy(src.at[b], dst.at[b], in_sem.at[which, b])

    def save(which, b):
        src, dst = ((k_buf, ko_hbm), (v_buf, vo_hbm))[which]
        return pltpu.make_async_copy(src.at[b], dst.at[b], out_sem.at[which, b])

    for b in range(rows):
        load(0, b).start()
        load(1, b).start()

    lane = lax.broadcasted_iota(jnp.int32, (1, 128), 1)
    slots = lax.broadcasted_iota(jnp.int32, (1, seq_len), 1)

    def row(b, carry):
        length = len_ref[b]
        window = pl.ds(pl.multiple_of((length // 128) * 128, 128), 128)
        here = lane == length % 128
        for which, buf in enumerate((k_buf, v_buf)):
            load(which, b).wait()
            col = jnp.sum(jnp.where(lane == b, cols_ref[which], 0.0), axis=1, keepdims=True)
            tile = buf[b, :, window].astype(jnp.float32)
            buf[b, :, window] = jnp.where(here, col, tile).astype(jnp.bfloat16)
        scores = jnp.dot(q_ref[b], k_buf[b], preferred_element_type=jnp.float32) * scale
        scores = jnp.where(slots <= length, scores, -1e30)
        top = jnp.max(scores, axis=1, keepdims=True)
        weights = jnp.exp(scores - top)
        total = jnp.sum(weights, axis=1, keepdims=True)
        probs = (weights * (1.0 / total)).astype(jnp.bfloat16)
        save(0, b).start()
        save(1, b).start()
        o_ref[b] = lax.dot_general(probs, v_buf[b], (((1,), (1,)), ((), ())), preferred_element_type=jnp.float32).astype(jnp.bfloat16)
        return carry

    lax.fori_loop(0, rows, row, 0)
    for b in range(rows):
        save(0, b).wait()
        save(1, b).wait()


def attend(q_rot, cols, k_cache, v_cache, lengths):
    rows, heads, head_dim = q_rot.shape
    seq_len = k_cache.shape[1]
    k_t = jnp.swapaxes(k_cache, 1, 2)
    v_t = jnp.swapaxes(v_cache, 1, 2)
    cache = jax.ShapeDtypeStruct((rows, head_dim, seq_len), jnp.bfloat16)
    o, k_new, v_new = pl.pallas_call(
        functools.partial(attention_kernel, head_dim ** -0.5),
        out_shape=(jax.ShapeDtypeStruct((rows, heads, head_dim), jnp.bfloat16), cache, cache),
        in_specs=[
            pl.BlockSpec(memory_space=pltpu.SMEM),
            pl.BlockSpec(memory_space=pltpu.VMEM),
            pl.BlockSpec(memory_space=pltpu.VMEM),
            pl.BlockSpec(memory_space=pl.ANY),
            pl.BlockSpec(memory_space=pl.ANY),
        ],
        out_specs=(pl.BlockSpec(memory_space=pltpu.VMEM), pl.BlockSpec(memory_space=pl.ANY), pl.BlockSpec(memory_space=pl.ANY)),
        scratch_shapes=[
            pltpu.VMEM((rows, head_dim, seq_len), jnp.bfloat16),
            pltpu.VMEM((rows, head_dim, seq_len), jnp.bfloat16),
            pltpu.SemaphoreType.DMA((2, rows)),
            pltpu.SemaphoreType.DMA((2, rows)),
        ],
        compiler_params=pltpu.CompilerParams(vmem_limit_bytes=48 * 1024 * 1024),
        cost_estimate=pl.CostEstimate(
            flops=4 * rows * heads * head_dim * seq_len,
            bytes_accessed=8 * rows * head_dim * seq_len,
            transcendentals=rows * heads * seq_len,
        ),
        name='attend',
    )(lengths, q_rot, cols, k_t, v_t)
    return o, jnp.swapaxes(k_new, 1, 2), jnp.swapaxes(v_new, 1, 2)


def rotary(values, positions):
    half_dim = values.shape[-1] // 2
    inv_freq = ROPE_BASE ** (-jnp.arange(half_dim, dtype=jnp.float32) / half_dim)
    angles = positions.astype(jnp.float32)[:, None, None] * inv_freq
    cos_part = jnp.cos(angles)
    sin_part = jnp.sin(angles)
    lo_half = values[..., :half_dim]
    hi_half = values[..., half_dim:]
    return jnp.concatenate([lo_half * cos_part - hi_half * sin_part, hi_half * cos_part + lo_half * sin_part], axis=-1)


def solution(mesh):
    x_size = mesh.shape['x']
    yz_size = mesh.shape['yz']
    all_axes = ('x', 'yz')

    def local_step(x_in, ln_scale, w_gate_up, w_attn, w_down, w_out, k_cache, v_cache, lengths, positions):
        local_rows, seq_len, head_dim = k_cache.shape
        q_width = w_out.shape[0] * yz_size
        num_heads = q_width // head_dim
        d_model = x_in.shape[1] * x_size * yz_size
        x_float = x_in.astype(jnp.float32)
        ln_sums = jnp.stack([jnp.sum(x_float, axis=1), jnp.sum(x_float * x_float, axis=1)], axis=1)
        ln_sums = lax.psum(ln_sums, all_axes)
        mean_val = ln_sums[:, 0:1] / d_model
        var_val = ln_sums[:, 1:2] / d_model - mean_val * mean_val
        normed = ((x_float - mean_val) * lax.rsqrt(var_val + LN_EPS) * ln_scale).astype(jnp.bfloat16)
        h_rows = lax.all_gather(normed, 'yz', axis=1, tiled=True)
        gu_part = jnp.einsum('bd,dgf->bgf', h_rows, w_gate_up, preferred_element_type=jnp.float32)
        gate_up = lax.psum_scatter(gu_part, 'x', scatter_dimension=2, tiled=True).astype(jnp.bfloat16)
        hidden = (jax.nn.silu(gate_up[:, 0].astype(jnp.float32)) * gate_up[:, 1].astype(jnp.float32)).astype(jnp.bfloat16)
        hidden_rows = lax.all_gather(hidden, 'x', axis=1, tiled=True)
        proj_part = jnp.dot(h_rows, w_attn, preferred_element_type=jnp.float32)
        proj_rows = lax.psum_scatter(proj_part, 'x', scatter_dimension=0, tiled=True).astype(jnp.bfloat16)
        proj_local = lax.all_to_all(proj_rows, 'yz', 0, 1, tiled=True)
        q_raw = proj_local[:, :q_width].reshape(local_rows, num_heads, head_dim)
        k_tok = proj_local[:, q_width:q_width + head_dim]
        v_tok = proj_local[:, q_width + head_dim:]
        q_rot = rotary(q_raw.astype(jnp.float32), positions).astype(jnp.bfloat16)
        k_rot = rotary(k_tok[:, None, :].astype(jnp.float32), positions)[:, 0].astype(jnp.bfloat16)
        cols = jnp.stack([k_rot, v_tok]).astype(jnp.float32).transpose(0, 2, 1)
        cols = jnp.pad(cols, ((0, 0), (0, 0), (0, 128 - local_rows)))
        attn_out, k_new, v_new = attend(q_rot, cols, k_cache, v_cache, lengths)
        attn_out = attn_out.reshape(local_rows, q_width)
        o_rows = lax.all_to_all(attn_out, 'yz', 1, 0, tiled=True)
        o_all = lax.all_gather(o_rows, 'x', axis=0, tiled=True)
        mixed_sum = jnp.dot(hidden_rows, w_down, preferred_element_type=jnp.float32) + jnp.dot(o_all, w_out, preferred_element_type=jnp.float32)
        mixed_sum = lax.psum_scatter(mixed_sum, 'yz', scatter_dimension=1, tiled=True)
        y_out = (x_float + mixed_sum).astype(jnp.bfloat16)
        return y_out, k_new, v_new

    row_spec = P(None, all_axes)
    vec_spec = P(all_axes)
    cache_spec = P(all_axes, None, None)
    return jax.shard_map(
        local_step,
        mesh=mesh,
        in_specs=(row_spec, vec_spec, P('x', None, 'yz'), P('x', 'yz'), P('yz', 'x'), P('yz', 'x'), cache_spec, cache_spec, vec_spec, vec_spec),
        out_specs=(row_spec, cache_spec, cache_spec),
        check_vma=False,
    )
```

```python
import functools

import jax
import jax.numpy as jnp
from jax import lax
from jax.experimental import pallas as pl
from jax.experimental.pallas import tpu as pltpu
from jax.sharding import PartitionSpec as P

LN_EPS = 1e-6
ROPE_BASE = 10000.0
MESH = pl.DeviceIdType.MESH


def attention_kernel(scale, len_ref, q_ref, cols_ref, k_hbm, v_hbm, o_ref, ko_hbm, vo_hbm, k_buf, v_buf, in_sem, out_sem):
    rows, _, seq_len = k_buf.shape

    def load(which, b):
        src, dst = ((k_hbm, k_buf), (v_hbm, v_buf))[which]
        return pltpu.make_async_copy(src.at[b], dst.at[b], in_sem.at[which, b])

    def save(which, b):
        src, dst = ((k_buf, ko_hbm), (v_buf, vo_hbm))[which]
        return pltpu.make_async_copy(src.at[b], dst.at[b], out_sem.at[which, b])

    for b in range(rows):
        load(0, b).start()
        load(1, b).start()

    lane = lax.broadcasted_iota(jnp.int32, (1, 128), 1)
    slots = lax.broadcasted_iota(jnp.int32, (1, seq_len), 1)

    def row(b, carry):
        length = len_ref[b]
        window = pl.ds(pl.multiple_of((length // 128) * 128, 128), 128)
        here = lane == length % 128
        for which, buf in enumerate((k_buf, v_buf)):
            load(which, b).wait()
            col = jnp.sum(jnp.where(lane == b, cols_ref[which], 0.0), axis=1, keepdims=True)
            tile = buf[b, :, window].astype(jnp.float32)
            buf[b, :, window] = jnp.where(here, col, tile).astype(jnp.bfloat16)
        scores = jnp.dot(q_ref[b], k_buf[b], preferred_element_type=jnp.float32) * scale
        scores = jnp.where(slots <= length, scores, -1e30)
        top = jnp.max(scores, axis=1, keepdims=True)
        weights = jnp.exp(scores - top)
        total = jnp.sum(weights, axis=1, keepdims=True)
        probs = (weights * (1.0 / total)).astype(jnp.bfloat16)
        save(0, b).start()
        save(1, b).start()
        o_ref[b] = lax.dot_general(probs, v_buf[b], (((1,), (1,)), ((), ())), preferred_element_type=jnp.float32).astype(jnp.bfloat16)
        return carry

    lax.fori_loop(0, rows, row, 0)
    for b in range(rows):
        save(0, b).wait()
        save(1, b).wait()


def attend(q_rot, cols, k_cache, v_cache, lengths):
    rows, heads, head_dim = q_rot.shape
    seq_len = k_cache.shape[1]
    k_t = jnp.swapaxes(k_cache, 1, 2)
    v_t = jnp.swapaxes(v_cache, 1, 2)
    cache = jax.ShapeDtypeStruct((rows, head_dim, seq_len), jnp.bfloat16)
    o, k_new, v_new = pl.pallas_call(
        functools.partial(attention_kernel, head_dim ** -0.5),
        out_shape=(jax.ShapeDtypeStruct((rows, heads, head_dim), jnp.bfloat16), cache, cache),
        in_specs=[
            pl.BlockSpec(memory_space=pltpu.SMEM),
            pl.BlockSpec(memory_space=pltpu.VMEM),
            pl.BlockSpec(memory_space=pltpu.VMEM),
            pl.BlockSpec(memory_space=pl.ANY),
            pl.BlockSpec(memory_space=pl.ANY),
        ],
        out_specs=(pl.BlockSpec(memory_space=pltpu.VMEM), pl.BlockSpec(memory_space=pl.ANY), pl.BlockSpec(memory_space=pl.ANY)),
        scratch_shapes=[
            pltpu.VMEM((rows, head_dim, seq_len), jnp.bfloat16),
            pltpu.VMEM((rows, head_dim, seq_len), jnp.bfloat16),
            pltpu.SemaphoreType.DMA((2, rows)),
            pltpu.SemaphoreType.DMA((2, rows)),
        ],
        compiler_params=pltpu.CompilerParams(vmem_limit_bytes=48 * 1024 * 1024),
        cost_estimate=pl.CostEstimate(
            flops=4 * rows * heads * head_dim * seq_len,
            bytes_accessed=8 * rows * head_dim * seq_len,
            transcendentals=rows * heads * seq_len,
        ),
        name='attend',
    )(lengths, q_rot, cols, k_t, v_t)
    return o, jnp.swapaxes(k_new, 1, 2), jnp.swapaxes(v_new, 1, 2)


def start_barrier(me_x, me_yz):
    barrier = pltpu.get_barrier_semaphore()
    for dx in range(2):
        for k in range(4):
            if dx or k:
                peer = (lax.rem(me_x + dx, 2), lax.rem(me_yz + k, 4))
                pl.semaphore_signal(barrier, inc=1, device_id=peer, device_id_type=MESH)
    pl.semaphore_wait(barrier, 7)


def spread(rows, cols, first):
    i = lax.broadcasted_iota(jnp.int32, (rows, cols), 0)
    c = lax.broadcasted_iota(jnp.int32, (rows, cols), 1)
    return jnp.where(c == 2 * i + first, 1.0, 0.0).astype(jnp.bfloat16)


def head_kernel(
    d_model, x_hbm, scale_hbm, wg_hbm, wa_hbm, z_ref, send_hbm, own_hbm,
    xg, sg, stats, h_buf, hx, hc, wg, wa, z_send, z_own, z_recv, zb, zg, gp,
    in_sem, wg_sem, x_send, x_recv, s_send, s_recv, t_send, t_recv, z_sems, a_send, a_recv, out_sem,
):
    me_x = lax.axis_index('x')
    me_yz = lax.axis_index('yz')
    rows, chunk = xg.shape[1:]
    half = rows // 2
    pieces = wg_sem.shape[0]
    depth = wg.shape[0] // pieces
    ff = wg.shape[2]
    x_in = pltpu.make_async_copy(x_hbm, xg.at[me_yz], in_sem.at[0])
    scale_in = pltpu.make_async_copy(scale_hbm, sg.at[me_yz], in_sem.at[1])
    wa_in = pltpu.make_async_copy(wa_hbm, wa, in_sem.at[2])
    wg_in = [
        pltpu.make_async_copy(wg_hbm.at[pl.ds(depth * i, depth)], wg.at[pl.ds(depth * i, depth)], wg_sem.at[i]) for i in range(pieces)
    ]
    x_in.start()
    scale_in.start()
    wa_in.start()
    for copy in wg_in:
        copy.start()
    start_barrier(me_x, me_yz)

    def to_peer(src, dst, sems, i, k, dx=0):
        return pltpu.make_async_remote_copy(
            src_ref=src, dst_ref=dst, send_sem=sems[0].at[i], recv_sem=sems[1].at[i],
            device_id=(lax.rem(me_x + dx, 2), lax.rem(me_yz + k, 4)), device_id_type=MESH,
        )

    x_in.wait()
    x_out = [to_peer(xg.at[me_yz], xg.at[me_yz], (x_send, x_recv), k, k) for k in (1, 2, 3)]
    for copy in x_out:
        copy.start()
    scale_in.wait()
    s_out = [to_peer(sg.at[me_yz], sg.at[me_yz], (s_send, s_recv), k, k) for k in (1, 2, 3)]
    for copy in s_out:
        copy.start()
    lane = lax.broadcasted_iota(jnp.int32, (8, 128), 1)
    mine = xg[me_yz].astype(jnp.float32)
    sum_1 = jnp.sum(mine, axis=1, keepdims=True)
    sum_2 = jnp.sum(mine * mine, axis=1, keepdims=True)
    tile = jnp.zeros((8, 128), jnp.float32)
    for j in range(rows // 8):
        tile = jnp.where(lane == j, sum_1[8 * j:8 * j + 8], tile)
        tile = jnp.where(lane == 32 + j, sum_2[8 * j:8 * j + 8], tile)
    me = me_x * 4 + me_yz
    stats[me] = tile
    t_out = [
        to_peer(stats.at[me], stats.at[me], (t_send, t_recv), 4 * dx + k, k, dx) for dx in range(2) for k in range(4) if dx or k
    ]
    for copy in t_out:
        copy.start()
    for copy in t_out:
        copy.wait()
    total = stats[0]
    for i in range(1, 8):
        total = total + stats[i]
    mean_t = total / d_model
    var_t = pltpu.roll(total, 96, 1) / d_model - mean_t * mean_t
    rstd_t = lax.rsqrt(var_t + LN_EPS)
    mean = jnp.concatenate([mean_t[:, j:j + 1] for j in range(rows // 8)], axis=0)
    rstd = jnp.concatenate([rstd_t[:, j:j + 1] for j in range(rows // 8)], axis=0)
    for copy in s_out:
        copy.wait()
    for copy in x_out:
        copy.wait()
    for s in range(4):
        h_buf[s] = ((xg[s].astype(jnp.float32) - mean) * rstd * sg[s]).astype(jnp.bfloat16)

    wide, thin = spread(128, 256, 0), spread(64, 128, 0)
    wide_u, thin_u = spread(128, 256, 1), spread(64, 128, 1)
    i = lax.broadcasted_iota(jnp.int32, (256, 128), 0)
    c = lax.broadcasted_iota(jnp.int32, (256, 128), 1)
    gather = jnp.where(i == 2 * c, 1.0, 0.0).astype(jnp.bfloat16)

    def start_of(part):
        first = lax.rem(me_x + 1 - part, 2)
        return pl.ds(pl.multiple_of(first * half, 32), half)

    def spread_half(part, g):
        out = pl.ds((2 * part + g) * half, half)
        a, b = ((wide, thin), (wide_u, thin_u))[g]
        for s in range(4):
            base = 2 * chunk * s
            part_rows = start_of(part)
            for t in range(2):
                piece = h_buf[s, part_rows, 128 * t:128 * t + 128]
                hx[out, base + 256 * t:base + 256 * t + 256] = jnp.dot(piece, a, preferred_element_type=jnp.float32).astype(jnp.bfloat16)
            piece = h_buf[s, part_rows, 256:320]
            hx[out, base + 512:base + 640] = jnp.dot(piece, b, preferred_element_type=jnp.float32).astype(jnp.bfloat16)

    def project(part):
        spread_half(part, 0)
        src = pl.ds(2 * part * half, half)
        for t in range(4 * chunk // 128):
            hc[:, 128 * t:128 * t + 128] = jnp.dot(hx[src, 256 * t:256 * t + 256], gather, preferred_element_type=jnp.float32).astype(jnp.bfloat16)
        z = lax.dot_general(hc[...], wa[...], (((1,), (1,)), ((), ())), preferred_element_type=jnp.float32)
        return z.reshape(z_send.shape)

    wa_in.wait()
    z_send[...] = project(0)
    z_copy = pltpu.make_async_remote_copy(
        src_ref=z_send, dst_ref=z_recv, send_sem=z_sems.at[0], recv_sem=z_sems.at[1],
        device_id=(lax.rem(me_x + 1, 2), me_yz), device_id_type=MESH,
    )
    z_copy.start()
    z_own[...] = project(1)
    spread_half(0, 1)
    spread_half(1, 1)
    for copy in wg_in:
        copy.wait()
    flat = wg.reshape(wg.shape[0] * 2, ff)

    def columns(c, carry):
        at = pl.ds(pl.multiple_of(c * 256, 256), 256)
        up = pl.ds(pl.multiple_of(ff + c * 256, 256), 256)
        out = jnp.dot(hx[...], flat[:, at], preferred_element_type=jnp.float32)
        gp[0, :, at] = out[:half]
        gp[0, :, up] = out[half:2 * half]
        gp[1, :, at] = out[2 * half:3 * half]
        gp[1, :, up] = out[3 * half:]
        return carry

    lax.fori_loop(0, ff // 256, columns, 0)
    save = [pltpu.make_async_copy(gp.at[0], send_hbm, out_sem.at[0]), pltpu.make_async_copy(gp.at[1], own_hbm, out_sem.at[1])]
    for copy in save:
        copy.start()
    z_copy.wait()
    zb[...] = (z_own[...] + z_recv[...]).astype(jnp.bfloat16)
    a_out = [
        to_peer(zb.at[lax.rem(me_yz + k, 4)], zg.at[me_yz], (a_send, a_recv), k, k) for k in (1, 2, 3)
    ]
    for copy in a_out:
        copy.start()
    zg[me_yz] = zb[me_yz]
    for copy in a_out:
        copy.wait()
    z_ref[...] = zg[...]
    for copy in save:
        copy.wait()


def head(x_in, ln_scale, w_gate_up, w_attn, d_model):
    rows, chunk = x_in.shape
    depth, _, ff = w_gate_up.shape
    z_cols = w_attn.shape[1]
    owned = rows // 8
    half = rows // 2
    part = jax.ShapeDtypeStruct((half, 2 * ff), jnp.float32)
    any_spec = pl.BlockSpec(memory_space=pl.ANY)
    dma = pltpu.SemaphoreType.DMA
    return pl.pallas_call(
        functools.partial(head_kernel, d_model),
        out_shape=(jax.ShapeDtypeStruct((4, owned, z_cols), jnp.bfloat16), part, part),
        in_specs=[any_spec] * 4,
        out_specs=(pl.BlockSpec(memory_space=pltpu.VMEM), any_spec, any_spec),
        scratch_shapes=[
            pltpu.VMEM((4, rows, chunk), jnp.bfloat16),
            pltpu.VMEM((4, 1, chunk), jnp.float32),
            pltpu.VMEM((8, 8, 128), jnp.float32),
            pltpu.VMEM((4, rows, chunk), jnp.bfloat16),
            pltpu.VMEM((2 * rows, 2 * depth), jnp.bfloat16),
            pltpu.VMEM((half, depth), jnp.bfloat16),
            pltpu.VMEM((depth, 2, ff), jnp.bfloat16),
            pltpu.VMEM((z_cols, depth), jnp.bfloat16),
            pltpu.VMEM((4, owned, z_cols), jnp.float32),
            pltpu.VMEM((4, owned, z_cols), jnp.float32),
            pltpu.VMEM((4, owned, z_cols), jnp.float32),
            pltpu.VMEM((4, owned, z_cols), jnp.bfloat16),
            pltpu.VMEM((4, owned, z_cols), jnp.bfloat16),
            pltpu.VMEM((2, half, 2 * ff), jnp.float32),
            dma((3,)), dma((8,)), dma((4,)), dma((4,)), dma((4,)), dma((4,)), dma((8,)), dma((8,)), dma((2,)), dma((4,)), dma((4,)), dma((2,)),
        ],
        compiler_params=pltpu.CompilerParams(collective_id=0, has_side_effects=True, vmem_limit_bytes=48 * 1024 * 1024),
        cost_estimate=pl.CostEstimate(flops=4 * rows * depth * 2 * ff, bytes_accessed=4 * depth * ff, transcendentals=0),
        name='head',
    )(x_in, ln_scale.reshape(1, chunk), w_gate_up, w_attn.T)


def tail_kernel(
    x_hbm, own_hbm, peer_hbm, o_hbm, wd_hbm, wo_hbm, y_ref,
    xv, g_own, g_peer, ov, oa, of, hb, wd, wo, out_part, y_send, y_recv,
    in_sem, g_sem, o_send, o_recv, h_send, h_recv, y_ssem, y_rsem,
):
    me_x = lax.axis_index('x')
    me_yz = lax.axis_index('yz')
    groups, _, span, ff = hb.shape
    rows, chunk = xv.shape
    half = rows // 2
    owned = ov.shape[1]
    g_in = []
    for i in range(groups):
        at = pl.ds(span * i, span)
        g_in.append((
            pltpu.make_async_copy(own_hbm.at[at], g_own.at[at], g_sem.at[0, i]),
            pltpu.make_async_copy(peer_hbm.at[at], g_peer.at[at], g_sem.at[1, i]),
        ))
    o_in = pltpu.make_async_copy(o_hbm, ov, in_sem.at[0])
    wo_in = pltpu.make_async_copy(wo_hbm, wo, in_sem.at[1])
    wd_in = pltpu.make_async_copy(wd_hbm, wd, in_sem.at[2])
    x_in = pltpu.make_async_copy(x_hbm, xv, in_sem.at[3])
    o_in.start()
    for pair in g_in:
        pair[0].start()
        pair[1].start()
    wo_in.start()
    wd_in.start()
    x_in.start()
    start_barrier(me_x, me_yz)
    me = me_x * 4 + me_yz
    o_in.wait()
    o_out = []
    for dx in range(2):
        for k in range(4):
            if dx or k:
                there = lax.rem(me_yz + k, 4)
                o_out.append(pltpu.make_async_remote_copy(
                    src_ref=ov.at[there], dst_ref=oa.at[me], send_sem=o_send.at[4 * dx + k], recv_sem=o_recv.at[4 * dx + k],
                    device_id=(lax.rem(me_x + dx, 2), there), device_id_type=MESH,
                ))
    for copy in o_out:
        copy.start()
    oa[me] = ov[me_yz]

    h_out = []
    for i in range(groups):
        at = pl.ds(span * i, span)
        g_in[i][0].wait()
        g_in[i][1].wait()
        both = (g_own[at] + g_peer[at]).astype(jnp.bfloat16).astype(jnp.float32)
        hb[i, me_x] = (jax.nn.silu(both[:, :ff]) * both[:, ff:]).astype(jnp.bfloat16)
        copy = pltpu.make_async_remote_copy(
            src_ref=hb.at[i, me_x], dst_ref=hb.at[i, me_x], send_sem=h_send.at[i], recv_sem=h_recv.at[i],
            device_id=(lax.rem(me_x + 1, 2), me_yz), device_id_type=MESH,
        )
        copy.start()
        h_out.append(copy)

    for copy in o_out:
        copy.wait()
    for e in range(8):
        of[owned * e:owned * e + owned] = oa[e].astype(jnp.float32)
    wo_in.wait()
    out_part[...] = jnp.dot(of[...].astype(jnp.bfloat16), wo[...], preferred_element_type=jnp.float32)
    wd_in.wait()
    x_in.wait()

    y_out = []

    def finish(i):
        for copy in y_out[i]:
            copy.wait()
        total = y_send[i, me_yz]
        for k in (1, 2, 3):
            total = total + y_recv[i, lax.rem(me_yz + k, 4)]
        for e in range(2):
            at = pl.ds(half * e + span * i, span)
            y_ref[at, :] = (xv[at, :].astype(jnp.float32) + total[span * e:span * e + span]).astype(jnp.bfloat16)

    for i in range(groups):
        h_out[i].wait()
        part = jnp.dot(hb[i].reshape(2 * span, ff), wd[...], preferred_element_type=jnp.float32)
        part = part + jnp.concatenate([out_part[span * i:span * i + span], out_part[half + span * i:half + span * i + span]], axis=0)
        for j in range(4):
            moved = part if j == 0 else pltpu.roll(part, (4 - j) * chunk, 1)
            y_send[i, j] = moved[:, :chunk]
        sends = []
        for k in (1, 2, 3):
            there = lax.rem(me_yz + k, 4)
            sends.append(pltpu.make_async_remote_copy(
                src_ref=y_send.at[i, there], dst_ref=y_recv.at[i, me_yz], send_sem=y_ssem.at[i, k], recv_sem=y_rsem.at[i, k],
                device_id=(me_x, there), device_id_type=MESH,
            ))
        for copy in sends:
            copy.start()
        y_out.append(sends)
        if i:
            finish(i - 1)
    finish(groups - 1)


def tail(x_in, g_own, g_peer, o_blocks, w_down, w_out):
    rows, chunk = x_in.shape
    half = rows // 2
    span = 16
    groups = half // span
    ff, cols = w_down.shape
    owned = o_blocks.shape[1]
    o_width = w_out.shape[0]
    any_spec = pl.BlockSpec(memory_space=pl.ANY)
    dma = pltpu.SemaphoreType.DMA
    return pl.pallas_call(
        tail_kernel,
        out_shape=jax.ShapeDtypeStruct((rows, chunk), jnp.bfloat16),
        in_specs=[any_spec] * 6,
        out_specs=pl.BlockSpec(memory_space=pltpu.VMEM),
        scratch_shapes=[
            pltpu.VMEM((rows, chunk), jnp.bfloat16),
            pltpu.VMEM((half, 2 * ff), jnp.float32),
            pltpu.VMEM((half, 2 * ff), jnp.float32),
            pltpu.VMEM((4, owned, o_width), jnp.bfloat16),
            pltpu.VMEM((8, owned, o_width), jnp.bfloat16),
            pltpu.VMEM((rows, o_width), jnp.float32),
            pltpu.VMEM((groups, 2, span, ff), jnp.bfloat16),
            pltpu.VMEM((ff, cols), jnp.bfloat16),
            pltpu.VMEM((o_width, cols), jnp.bfloat16),
            pltpu.VMEM((rows, cols), jnp.float32),
            pltpu.VMEM((groups, 4, 2 * span, chunk), jnp.float32),
            pltpu.VMEM((groups, 4, 2 * span, chunk), jnp.float32),
            dma((4,)), dma((2, groups)), dma((8,)), dma((8,)), dma((groups,)), dma((groups,)), dma((groups, 4)), dma((groups, 4)),
        ],
        compiler_params=pltpu.CompilerParams(collective_id=1, has_side_effects=True, vmem_limit_bytes=48 * 1024 * 1024),
        cost_estimate=pl.CostEstimate(flops=2 * rows * (ff + o_width) * cols, bytes_accessed=2 * (ff + o_width) * cols, transcendentals=half * ff),
        name='tail',
    )(x_in, g_own, g_peer, o_blocks, w_down, w_out)


def rotary(values, positions):
    half_dim = values.shape[-1] // 2
    inv_freq = ROPE_BASE ** (-jnp.arange(half_dim, dtype=jnp.float32) / half_dim)
    angles = positions.astype(jnp.float32)[:, None, None] * inv_freq
    cos_part = jnp.cos(angles)
    sin_part = jnp.sin(angles)
    lo_half = values[..., :half_dim]
    hi_half = values[..., half_dim:]
    return jnp.concatenate([lo_half * cos_part - hi_half * sin_part, hi_half * cos_part + lo_half * sin_part], axis=-1)


def solution(mesh):
    x_size = mesh.shape['x']
    yz_size = mesh.shape['yz']
    all_axes = ('x', 'yz')

    def local_step(x_in, ln_scale, w_gate_up, w_attn, w_down, w_out, k_cache, v_cache, lengths, positions):
        local_rows, seq_len, head_dim = k_cache.shape
        q_width = w_out.shape[0] * yz_size
        num_heads = q_width // head_dim
        d_model = x_in.shape[1] * x_size * yz_size
        z_blocks, g_send, g_own = head(x_in, ln_scale, w_gate_up, w_attn, d_model)
        g_peer = lax.ppermute(g_send, 'x', [(0, 1), (1, 0)])
        proj_local = z_blocks.transpose(1, 0, 2).reshape(local_rows, -1)
        q_raw = proj_local[:, :q_width].reshape(local_rows, num_heads, head_dim)
        k_tok = proj_local[:, q_width:q_width + head_dim]
        v_tok = proj_local[:, q_width + head_dim:]
        q_rot = rotary(q_raw.astype(jnp.float32), positions).astype(jnp.bfloat16)
        k_rot = rotary(k_tok[:, None, :].astype(jnp.float32), positions)[:, 0].astype(jnp.bfloat16)
        cols = jnp.stack([k_rot, v_tok]).astype(jnp.float32).transpose(0, 2, 1)
        cols = jnp.pad(cols, ((0, 0), (0, 0), (0, 128 - local_rows)))
        attn_out, k_new, v_new = attend(q_rot, cols, k_cache, v_cache, lengths)
        o_blocks = attn_out.reshape(local_rows, yz_size, q_width // yz_size).transpose(1, 0, 2)
        y_out = tail(x_in, g_own, g_peer, o_blocks, w_down, w_out)
        return y_out, k_new, v_new

    row_spec = P(None, all_axes)
    vec_spec = P(all_axes)
    cache_spec = P(all_axes, None, None)
    return jax.shard_map(
        local_step,
        mesh=mesh,
        in_specs=(row_spec, vec_spec, P('x', None, 'yz'), P('x', 'yz'), P('yz', 'x'), P('yz', 'x'), cache_spec, cache_spec, vec_spec, vec_spec),
        out_specs=(row_spec, cache_spec, cache_spec),
        check_vma=False,
    )
```

```python
import functools

import jax
import jax.numpy as jnp
from jax import lax
from jax.experimental import pallas as pl
from jax.experimental.pallas import tpu as pltpu
from jax.sharding import PartitionSpec as P

LN_EPS = 1e-6
ROPE_BASE = 10000.0
MESH = pl.DeviceIdType.MESH
VMEM_MOST = 64 * 1024 * 1024 - 64 * 1024
EARLY = 2
ROWS_A = 64


def attention_kernel(scale, len_ref, q_ref, cols_ref, k_hbm, v_hbm, o_ref, ko_hbm, vo_hbm, k_buf, v_buf, in_sem, out_sem):
    rows, _, seq_len = k_buf.shape

    def load(which, b):
        src, dst = ((k_hbm, k_buf), (v_hbm, v_buf))[which]
        return pltpu.make_async_copy(src.at[b], dst.at[b], in_sem.at[which, b])

    def save(which, b):
        src, dst = ((k_buf, ko_hbm), (v_buf, vo_hbm))[which]
        return pltpu.make_async_copy(src.at[b], dst.at[b], out_sem.at[which, b])

    for b in range(rows):
        load(0, b).start()
        load(1, b).start()

    lane = lax.broadcasted_iota(jnp.int32, (1, 128), 1)
    slots = lax.broadcasted_iota(jnp.int32, (1, seq_len), 1)

    def row(b, carry):
        length = len_ref[b]
        window = pl.ds(pl.multiple_of((length // 128) * 128, 128), 128)
        here = lane == length % 128
        for which, buf in enumerate((k_buf, v_buf)):
            load(which, b).wait()
            col = jnp.sum(jnp.where(lane == b, cols_ref[which], 0.0), axis=1, keepdims=True)
            tile = buf[b, :, window].astype(jnp.float32)
            buf[b, :, window] = jnp.where(here, col, tile).astype(jnp.bfloat16)
        scores = jnp.dot(q_ref[b], k_buf[b], preferred_element_type=jnp.float32) * scale
        scores = jnp.where(slots <= length, scores, -1e30)
        top = jnp.max(scores, axis=1, keepdims=True)
        weights = jnp.exp(scores - top)
        total = jnp.sum(weights, axis=1, keepdims=True)
        probs = (weights * (1.0 / total)).astype(jnp.bfloat16)
        save(0, b).start()
        save(1, b).start()
        o_ref[b] = lax.dot_general(probs, v_buf[b], (((1,), (1,)), ((), ())), preferred_element_type=jnp.float32).astype(jnp.bfloat16)
        return carry

    lax.fori_loop(0, rows, row, 0)
    for b in range(rows):
        save(0, b).wait()
        save(1, b).wait()


def attend(q_rot, cols, k_cache, v_cache, lengths):
    rows, heads, head_dim = q_rot.shape
    seq_len = k_cache.shape[1]
    k_t = jnp.swapaxes(k_cache, 1, 2)
    v_t = jnp.swapaxes(v_cache, 1, 2)
    cache = jax.ShapeDtypeStruct((rows, head_dim, seq_len), jnp.bfloat16)
    o, k_new, v_new = pl.pallas_call(
        functools.partial(attention_kernel, head_dim ** -0.5),
        out_shape=(jax.ShapeDtypeStruct((rows, heads, head_dim), jnp.bfloat16), cache, cache),
        in_specs=[
            pl.BlockSpec(memory_space=pltpu.SMEM),
            pl.BlockSpec(memory_space=pltpu.VMEM),
            pl.BlockSpec(memory_space=pltpu.VMEM),
            pl.BlockSpec(memory_space=pl.ANY),
            pl.BlockSpec(memory_space=pl.ANY),
        ],
        out_specs=(pl.BlockSpec(memory_space=pltpu.VMEM), pl.BlockSpec(memory_space=pl.ANY), pl.BlockSpec(memory_space=pl.ANY)),
        scratch_shapes=[
            pltpu.VMEM((rows, head_dim, seq_len), jnp.bfloat16),
            pltpu.VMEM((rows, head_dim, seq_len), jnp.bfloat16),
            pltpu.SemaphoreType.DMA((2, rows)),
            pltpu.SemaphoreType.DMA((2, rows)),
        ],
        compiler_params=pltpu.CompilerParams(vmem_limit_bytes=48 * 1024 * 1024),
        cost_estimate=pl.CostEstimate(
            flops=4 * rows * heads * head_dim * seq_len,
            bytes_accessed=8 * rows * head_dim * seq_len,
            transcendentals=rows * heads * seq_len,
        ),
        name='attend',
    )(lengths, q_rot, cols, k_t, v_t)
    return o, jnp.swapaxes(k_new, 1, 2), jnp.swapaxes(v_new, 1, 2)


def start_barrier(me_x, me_yz):
    barrier = pltpu.get_barrier_semaphore()
    for dx in range(2):
        for k in range(4):
            if dx or k:
                peer = (lax.rem(me_x + dx, 2), lax.rem(me_yz + k, 4))
                pl.semaphore_signal(barrier, inc=1, device_id=peer, device_id_type=MESH)
    pl.semaphore_wait(barrier, 7)


def spread(rows, cols, first):
    i = lax.broadcasted_iota(jnp.int32, (rows, cols), 0)
    c = lax.broadcasted_iota(jnp.int32, (rows, cols), 1)
    return jnp.where(c == 2 * i + first, 1.0, 0.0).astype(jnp.bfloat16)


def head_kernel(
    d_model, early, x_hbm, scale_hbm, wg_hbm, wa_hbm, z_ref, first_hbm, send_a_hbm, send_b_hbm, own_hbm,
    xg, sg, stats, h_buf, hx, hc, wg, wa, z_send, z_own, z_recv, zb, zg, g_first, g_got, g_rest, g_own,
    in_sem, wg_sem, x_send, x_recv, s_send, s_recv, t_send, t_recv, z_sems, a_send, a_recv, f_send, f_recv, out_sem,
):
    me_x = lax.axis_index('x')
    me_yz = lax.axis_index('yz')
    half, chunk = xg.shape[2:]
    rows = 2 * half
    pieces = wg_sem.shape[0]
    depth = wg.shape[0] // pieces
    ff = wg.shape[2]
    wide_cols = 256
    other_x = lax.rem(me_x + 1, 2)
    across = lax.rem(me_yz + 2, 4)
    core = lax.rem(me_yz, 2)
    partner = me_yz + 1 - 2 * core
    order = (other_x, me_x)
    x_in = [
        pltpu.make_async_copy(x_hbm.at[pl.ds(pl.multiple_of(order[p] * half, 32), half)], xg.at[me_yz, order[p]], in_sem.at[p]) for p in range(2)
    ]
    scale_in = pltpu.make_async_copy(scale_hbm, sg.at[me_yz], in_sem.at[2])
    wa_in = pltpu.make_async_copy(wa_hbm, wa, in_sem.at[3])
    wg_in = [
        pltpu.make_async_copy(wg_hbm.at[pl.ds(depth * i, depth)], wg.at[pl.ds(depth * i, depth)], wg_sem.at[i]) for i in range(pieces)
    ]
    for copy in (*x_in, scale_in, wa_in, *wg_in):
        copy.start()
    start_barrier(me_x, me_yz)

    def remote(src, dst, send, recv, to_x, to_yz):
        return pltpu.make_async_remote_copy(
            src_ref=src, dst_ref=dst, send_sem=send, recv_sem=recv, device_id=(to_x, to_yz), device_id_type=MESH,
        )

    def x_copy(kind, p):
        owner = across if kind == 2 else me_yz
        at = xg.at[owner, order[p]]
        return remote(at, at, x_send.at[kind, p], x_recv.at[kind, p], me_x, across if kind == 1 else partner)

    for p in range(2):
        x_in[p].wait()
        x_copy(1, p).start()
        x_copy(0, p).start()
    scale_in.wait()
    s_out = [remote(sg.at[me_yz], sg.at[me_yz], s_send.at[k], s_recv.at[k], me_x, lax.rem(me_yz + k, 4)) for k in (1, 2, 3)]
    for copy in s_out:
        copy.start()
    lane = lax.broadcasted_iota(jnp.int32, (8, 128), 1)
    tile = jnp.zeros((8, 128), jnp.float32)
    for e in range(2):
        mine = xg[me_yz, e].astype(jnp.float32)
        sum_1 = jnp.sum(mine, axis=1, keepdims=True)
        sum_2 = jnp.sum(mine * mine, axis=1, keepdims=True)
        for j in range(half // 8):
            col = e * (half // 8) + j
            tile = jnp.where(lane == col, sum_1[8 * j:8 * j + 8], tile)
            tile = jnp.where(lane == 32 + col, sum_2[8 * j:8 * j + 8], tile)
    me = me_x * 4 + me_yz
    stats[me] = tile
    t_out = [
        remote(stats.at[me], stats.at[me], t_send.at[4 * dx + k], t_recv.at[4 * dx + k], lax.rem(me_x + dx, 2), lax.rem(me_yz + k, 4))
        for dx in range(2) for k in range(4) if dx or k
    ]
    for copy in t_out:
        copy.start()
    wide, thin = spread(128, 256, 0), spread(64, 128, 0)
    wide_u, thin_u = spread(128, 256, 1), spread(64, 128, 1)
    i = lax.broadcasted_iota(jnp.int32, (256, 128), 0)
    c = lax.broadcasted_iota(jnp.int32, (256, 128), 1)
    gather = jnp.where(i == 2 * c, 1.0, 0.0).astype(jnp.bfloat16)
    for copy in t_out:
        copy.wait()
    total = stats[0]
    for i in range(1, 8):
        total = total + stats[i]
    mean_t = total / d_model
    var_t = pltpu.roll(total, 96, 1) / d_model - mean_t * mean_t
    rstd_t = lax.rsqrt(var_t + LN_EPS)
    for copy in s_out:
        copy.wait()

    def normalize(p):
        shift = lax.rem(128 - order[p] * (half // 8), 128)
        mean_p = pltpu.roll(mean_t, shift, 1)
        rstd_p = pltpu.roll(rstd_t, shift, 1)
        mean = jnp.concatenate([mean_p[:, j:j + 1] for j in range(half // 8)], axis=0)
        rstd = jnp.concatenate([rstd_p[:, j:j + 1] for j in range(half // 8)], axis=0)
        x_copy(1, p).wait()
        x_copy(2, p).start()
        x_copy(0, p).wait()
        x_copy(2, p).wait()
        for s in range(4):
            h_buf[s] = ((xg[s, order[p]].astype(jnp.float32) - mean) * rstd * sg[s]).astype(jnp.bfloat16)

    def spread_half(part, g):
        out = pl.ds((2 * part + g) * half, half)
        a, b = ((wide, thin), (wide_u, thin_u))[g]
        for s in range(4):
            base = 2 * chunk * s
            for t in range(2):
                piece = h_buf[s, :, 128 * t:128 * t + 128]
                hx[out, base + 256 * t:base + 256 * t + 256] = jnp.dot(piece, a, preferred_element_type=jnp.float32).astype(jnp.bfloat16)
            piece = h_buf[s, :, 256:320]
            hx[out, base + 512:base + 640] = jnp.dot(piece, b, preferred_element_type=jnp.float32).astype(jnp.bfloat16)

    def project(part):
        src = pl.ds(2 * part * half, half)
        for t in range(4 * chunk // 128):
            hc[:, 128 * t:128 * t + 128] = jnp.dot(hx[src, 256 * t:256 * t + 256], gather, preferred_element_type=jnp.float32).astype(jnp.bfloat16)
        z = lax.dot_general(hc[...], wa[...], (((1,), (1,)), ((), ())), preferred_element_type=jnp.float32)
        return z.reshape(z_send.shape)

    normalize(0)
    spread_half(0, 0)
    wa_in.wait()
    z_send[...] = project(0)
    z_copy = remote(z_send, z_recv, z_sems.at[0], z_sems.at[1], other_x, me_yz)
    z_copy.start()
    spread_half(0, 1)
    normalize(1)
    spread_half(1, 0)
    spread_half(1, 1)
    for copy in wg_in:
        copy.wait()

    def columns(c):
        at = pl.ds(pl.multiple_of(c * wide_cols, wide_cols), wide_cols)
        block = wg[:, :, at].reshape(2 * wg.shape[0], wide_cols)
        out = jnp.dot(hx[...], block, preferred_element_type=jnp.float32)
        up = pl.ds(pl.multiple_of(ff + c * wide_cols, wide_cols), wide_cols)
        g_own[:, at] = out[2 * half:3 * half]
        g_own[:, up] = out[3 * half:]
        return out

    first = []
    for c in range(early):
        out = columns(c)
        g_first[c, :, :wide_cols] = out[:half]
        g_first[c, :, wide_cols:] = out[half:2 * half]
        first.append(remote(g_first.at[c], g_got.at[c], f_send.at[c], f_recv.at[c], other_x, me_yz))
        first[-1].start()

    def rest(c, carry):
        out = columns(c)
        at = (c - early) * wide_cols
        g_rest[:, pl.ds(pl.multiple_of(at, wide_cols), wide_cols)] = out[:half]
        g_rest[:, pl.ds(pl.multiple_of(ff - early * wide_cols + at, wide_cols), wide_cols)] = out[half:2 * half]
        return carry

    lax.fori_loop(early, ff // wide_cols, rest, 0)
    rows_a = send_a_hbm.shape[0]
    save = [
        pltpu.make_async_copy(g_rest.at[pl.ds(0, rows_a)], send_a_hbm, out_sem.at[0]),
        pltpu.make_async_copy(g_rest.at[pl.ds(rows_a, half - rows_a)], send_b_hbm, out_sem.at[1]),
        pltpu.make_async_copy(g_own, own_hbm, out_sem.at[2]),
    ]
    for copy in save:
        copy.start()
    z_own[...] = project(1)
    z_copy.wait()
    zb[...] = (z_own[...] + z_recv[...]).astype(jnp.bfloat16)
    a_out = [remote(zb.at[lax.rem(me_yz + k, 4)], zg.at[me_yz], a_send.at[k], a_recv.at[k], me_x, lax.rem(me_yz + k, 4)) for k in (1, 2, 3)]
    for copy in a_out:
        copy.start()
    zg[me_yz] = zb[me_yz]
    for copy in a_out:
        copy.wait()
    z_ref[...] = zg[...]
    for copy in first:
        copy.wait()
    keep = pltpu.make_async_copy(g_got, first_hbm, out_sem.at[3])
    keep.start()
    keep.wait()
    for copy in save:
        copy.wait()


def head(x_in, ln_scale, w_gate_up, w_attn, d_model, early, rows_a):
    rows, chunk = x_in.shape
    depth, _, ff = w_gate_up.shape
    z_cols = w_attn.shape[1]
    owned = rows // 8
    half = rows // 2
    width = 2 * (ff - 256 * early)
    any_spec = pl.BlockSpec(memory_space=pl.ANY)
    dma = pltpu.SemaphoreType.DMA
    f32, bf16 = jnp.float32, jnp.bfloat16
    return pl.pallas_call(
        functools.partial(head_kernel, d_model, early),
        out_shape=(
            jax.ShapeDtypeStruct((4, owned, z_cols), bf16),
            jax.ShapeDtypeStruct((early, half, 512), f32),
            jax.ShapeDtypeStruct((rows_a, width), f32),
            jax.ShapeDtypeStruct((half - rows_a, width), f32),
            jax.ShapeDtypeStruct((half, 2 * ff), f32),
        ),
        in_specs=[any_spec] * 4,
        out_specs=(pl.BlockSpec(memory_space=pltpu.VMEM), *[any_spec] * 4),
        scratch_shapes=[
            pltpu.VMEM((4, 2, half, chunk), bf16),
            pltpu.VMEM((4, 1, chunk), f32),
            pltpu.VMEM((8, 8, 128), f32),
            pltpu.VMEM((4, half, chunk), bf16),
            pltpu.VMEM((2 * rows, 2 * depth), bf16),
            pltpu.VMEM((half, depth), bf16),
            pltpu.VMEM((depth, 2, ff), bf16),
            pltpu.VMEM((z_cols, depth), bf16),
            pltpu.VMEM((4, owned, z_cols), f32),
            pltpu.VMEM((4, owned, z_cols), f32),
            pltpu.VMEM((4, owned, z_cols), f32),
            pltpu.VMEM((4, owned, z_cols), bf16),
            pltpu.VMEM((4, owned, z_cols), bf16),
            pltpu.VMEM((early, half, 512), f32),
            pltpu.VMEM((early, half, 512), f32),
            pltpu.VMEM((half, width), f32),
            pltpu.VMEM((half, 2 * ff), f32),
            dma((4,)), dma((8,)), dma((3, 2)), dma((3, 2)), dma((4,)), dma((4,)), dma((8,)), dma((8,)), dma((2,)), dma((4,)), dma((4,)),
            dma((early,)), dma((early,)), dma((4,)),
        ],
        compiler_params=pltpu.CompilerParams(collective_id=0, has_side_effects=True, vmem_limit_bytes=VMEM_MOST),
        cost_estimate=pl.CostEstimate(flops=4 * rows * depth * 2 * ff, bytes_accessed=4 * depth * ff, transcendentals=0),
        name='head',
    )(x_in, ln_scale.reshape(1, chunk), w_gate_up, w_attn.T)


def tail_kernel(
    x_hbm, first_hbm, peer_hbm, late_hbm, own_hbm, o_hbm, wd_hbm, wo_hbm, y_ref,
    xv, g_first, g_peer, g_late, g_got, g_own, ov, oa, of, hb, wd, wo, out_part, y_send, y_pair, y_over, y_recv,
    in_sem, g_sem, b_send, b_recv, o_send, o_recv, h_send, h_recv, p_send, p_recv, y_ssem, y_rsem,
):
    me_x = lax.axis_index('x')
    me_yz = lax.axis_index('yz')
    groups, _, span, ff = hb.shape
    rows, chunk = xv.shape
    half = rows // 2
    owned = ov.shape[1]
    early, _, wide = g_first.shape
    wide = wide // 2
    groups_a = g_peer.shape[0] // span
    core = lax.rem(me_yz, 2)
    col = me_yz // 2
    partner = me_yz + 1 - 2 * core
    across = lax.rem(me_yz + 2, 4)
    other_x = lax.rem(me_x + 1, 2)

    def rows_of(i):
        return pl.ds(span * i, span)

    late_in = pltpu.make_async_copy(late_hbm, g_late, in_sem.at[4])
    o_in = pltpu.make_async_copy(o_hbm, ov, in_sem.at[0])
    first_in = pltpu.make_async_copy(first_hbm, g_first, in_sem.at[5])
    own_in = [pltpu.make_async_copy(own_hbm.at[rows_of(i)], g_own.at[rows_of(i)], g_sem.at[0, i]) for i in range(groups)]
    peer_in = [pltpu.make_async_copy(peer_hbm.at[rows_of(i)], g_peer.at[rows_of(i)], g_sem.at[1, i]) for i in range(groups_a)]
    wo_in = pltpu.make_async_copy(wo_hbm, wo, in_sem.at[1])
    wd_in = pltpu.make_async_copy(wd_hbm, wd, in_sem.at[2])
    x_in = pltpu.make_async_copy(x_hbm, xv, in_sem.at[3])
    for copy in (o_in, late_in, first_in):
        copy.start()
    for i in range(groups):
        own_in[i].start()
        if i < groups_a:
            peer_in[i].start()
    for copy in (wo_in, wd_in, x_in):
        copy.start()
    start_barrier(me_x, me_yz)
    me = me_x * 4 + me_yz

    def remote(src, dst, send, recv, to_x, to_yz):
        return pltpu.make_async_remote_copy(
            src_ref=src, dst_ref=dst, send_sem=send, recv_sem=recv, device_id=(to_x, to_yz), device_id_type=MESH,
        )

    o_in.wait()
    o_out = []
    for dx in range(2):
        for k in range(4):
            if dx or k:
                there = lax.rem(me_yz + k, 4)
                o_out.append(remote(ov.at[there], oa.at[me], o_send.at[4 * dx + k], o_recv.at[4 * dx + k], lax.rem(me_x + dx, 2), there))
    for copy in o_out:
        copy.start()
    late_in.wait()
    b_out = [
        remote(g_late.at[rows_of(i)], g_got.at[rows_of(i)], b_send.at[i], b_recv.at[i], other_x, me_yz) for i in range(groups - groups_a)
    ]
    for copy in b_out:
        copy.start()
    oa[me] = ov[me_yz]
    first_in.wait()

    h_out = []

    def activate(i):
        own_in[i].wait()
        at = rows_of(i)
        if i < groups_a:
            peer_in[i].wait()
            got, got_at = g_peer, at
        else:
            b_out[i - groups_a].wait()
            got, got_at = g_got, rows_of(i - groups_a)

        def act(gate, up):
            gate = gate.astype(jnp.bfloat16).astype(jnp.float32)
            up = up.astype(jnp.bfloat16).astype(jnp.float32)
            return (jax.nn.silu(gate) * up).astype(jnp.bfloat16)

        for c in range(early):
            cols = slice(wide * c, wide * c + wide)
            up_cols = slice(ff + wide * c, ff + wide * c + wide)
            hb[i, me_x, :, cols] = act(g_own[at, cols] + g_first[c, at, :wide], g_own[at, up_cols] + g_first[c, at, wide:])
        done = early * wide
        hb[i, me_x, :, done:] = act(g_own[at, done:ff] + got[got_at, :ff - done], g_own[at, ff + done:] + got[got_at, ff - done:])
        copy = remote(hb.at[i, me_x], hb.at[i, me_x], h_send.at[i], h_recv.at[i], other_x, me_yz)
        copy.start()
        h_out.append(copy)

    for i in range(groups_a):
        activate(i)
    for copy in o_out:
        copy.wait()
    for e in range(8):
        of[owned * e:owned * e + owned] = oa[e].astype(jnp.float32)
    wo_in.wait()
    out_part[...] = jnp.dot(of[...].astype(jnp.bfloat16), wo[...], preferred_element_type=jnp.float32)
    for i in range(groups_a, groups):
        activate(i)
    wd_in.wait()
    x_in.wait()

    pair = []
    over = []

    def product(i):
        h_out[i].wait()
        part = jnp.dot(hb[i].reshape(2 * span, ff), wd[...], preferred_element_type=jnp.float32)
        part = part + jnp.concatenate([out_part[span * i:span * i + span], out_part[half + span * i:half + span * i + span]], axis=0)
        for j in range(4):
            moved = part if j == 0 else pltpu.roll(part, (4 - j) * chunk, 1)
            y_send[i, j] = moved[:, :chunk]
        pair.append([
            remote(y_send.at[i, 2 * e + 1 - core], y_pair.at[i, e], p_send.at[i, e], p_recv.at[i, e], me_x, partner) for e in range(2)
        ])
        for copy in pair[i]:
            copy.start()

    def cross(i):
        for copy in pair[i]:
            copy.wait()
        y_over[i] = y_send[i, across] + y_pair[i, 1 - col]
        over.append(remote(y_over.at[i], y_recv.at[i], y_ssem.at[i], y_rsem.at[i], me_x, across))
        over[i].start()

    def finish(i):
        over[i].wait()
        total = y_send[i, me_yz] + y_pair[i, col] + y_recv[i]
        for e in range(2):
            at = pl.ds(half * e + span * i, span)
            y_ref[at, :] = (xv[at, :].astype(jnp.float32) + total[span * e:span * e + span]).astype(jnp.bfloat16)

    for i in range(groups):
        product(i)
        if i >= 1:
            cross(i - 1)
        if i >= 2:
            finish(i - 2)
    cross(groups - 1)
    finish(groups - 2)
    finish(groups - 1)


def tail(x_in, g_first, g_peer, g_late, g_own, o_blocks, w_down, w_out):
    rows, chunk = x_in.shape
    half = rows // 2
    span = 16
    groups = half // span
    ff, cols = w_down.shape
    owned = o_blocks.shape[1]
    o_width = w_out.shape[0]
    any_spec = pl.BlockSpec(memory_space=pl.ANY)
    dma = pltpu.SemaphoreType.DMA
    f32, bf16 = jnp.float32, jnp.bfloat16
    late_groups = g_late.shape[0] // span
    return pl.pallas_call(
        tail_kernel,
        out_shape=jax.ShapeDtypeStruct((rows, chunk), bf16),
        in_specs=[any_spec] * 8,
        out_specs=pl.BlockSpec(memory_space=pltpu.VMEM),
        scratch_shapes=[
            pltpu.VMEM((rows, chunk), bf16),
            pltpu.VMEM(g_first.shape, f32),
            pltpu.VMEM(g_peer.shape, f32),
            pltpu.VMEM(g_late.shape, f32),
            pltpu.VMEM(g_late.shape, f32),
            pltpu.VMEM((half, 2 * ff), f32),
            pltpu.VMEM((4, owned, o_width), bf16),
            pltpu.VMEM((8, owned, o_width), bf16),
            pltpu.VMEM((rows, o_width), f32),
            pltpu.VMEM((groups, 2, span, ff), bf16),
            pltpu.VMEM((ff, cols), bf16),
            pltpu.VMEM((o_width, cols), bf16),
            pltpu.VMEM((rows, cols), f32),
            pltpu.VMEM((groups, 4, 2 * span, chunk), f32),
            pltpu.VMEM((groups, 2, 2 * span, chunk), f32),
            pltpu.VMEM((groups, 2 * span, chunk), f32),
            pltpu.VMEM((groups, 2 * span, chunk), f32),
            dma((6,)), dma((2, groups)), dma((late_groups,)), dma((late_groups,)), dma((8,)), dma((8,)), dma((groups,)), dma((groups,)),
            dma((groups, 2)), dma((groups, 2)), dma((groups,)), dma((groups,)),
        ],
        compiler_params=pltpu.CompilerParams(collective_id=1, has_side_effects=True, vmem_limit_bytes=VMEM_MOST),
        cost_estimate=pl.CostEstimate(flops=2 * rows * (ff + o_width) * cols, bytes_accessed=2 * (ff + o_width) * cols, transcendentals=half * ff),
        name='tail',
    )(x_in, g_first, g_peer, g_late, g_own, o_blocks, w_down, w_out)


def rotary(values, positions):
    half_dim = values.shape[-1] // 2
    inv_freq = ROPE_BASE ** (-jnp.arange(half_dim, dtype=jnp.float32) / half_dim)
    angles = positions.astype(jnp.float32)[:, None, None] * inv_freq
    cos_part = jnp.cos(angles)
    sin_part = jnp.sin(angles)
    lo_half = values[..., :half_dim]
    hi_half = values[..., half_dim:]
    return jnp.concatenate([lo_half * cos_part - hi_half * sin_part, hi_half * cos_part + lo_half * sin_part], axis=-1)


def solution(mesh):
    x_size = mesh.shape['x']
    yz_size = mesh.shape['yz']
    all_axes = ('x', 'yz')

    def local_step(x_in, ln_scale, w_gate_up, w_attn, w_down, w_out, k_cache, v_cache, lengths, positions):
        local_rows, seq_len, head_dim = k_cache.shape
        q_width = w_out.shape[0] * yz_size
        num_heads = q_width // head_dim
        d_model = x_in.shape[1] * x_size * yz_size
        z_blocks, g_first, g_send, g_late, g_own = head(x_in, ln_scale, w_gate_up, w_attn, d_model, EARLY, ROWS_A)
        g_peer = lax.ppermute(g_send, 'x', [(0, 1), (1, 0)])
        proj_local = z_blocks.transpose(1, 0, 2).reshape(local_rows, -1)
        q_raw = proj_local[:, :q_width].reshape(local_rows, num_heads, head_dim)
        k_tok = proj_local[:, q_width:q_width + head_dim]
        v_tok = proj_local[:, q_width + head_dim:]
        q_rot = rotary(q_raw.astype(jnp.float32), positions).astype(jnp.bfloat16)
        k_rot = rotary(k_tok[:, None, :].astype(jnp.float32), positions)[:, 0].astype(jnp.bfloat16)
        cols = jnp.stack([k_rot, v_tok]).astype(jnp.float32).transpose(0, 2, 1)
        cols = jnp.pad(cols, ((0, 0), (0, 0), (0, 128 - local_rows)))
        attn_out, k_new, v_new = attend(q_rot, cols, k_cache, v_cache, lengths)
        o_blocks = attn_out.reshape(local_rows, yz_size, q_width // yz_size).transpose(1, 0, 2)
        y_out = tail(x_in, g_first, g_peer, g_late, g_own, o_blocks, w_down, w_out)
        return y_out, k_new, v_new

    row_spec = P(None, all_axes)
    vec_spec = P(all_axes)
    cache_spec = P(all_axes, None, None)
    return jax.shard_map(
        local_step,
        mesh=mesh,
        in_specs=(row_spec, vec_spec, P('x', None, 'yz'), P('x', 'yz'), P('yz', 'x'), P('yz', 'x'), cache_spec, cache_spec, vec_spec, vec_spec),
        out_specs=(row_spec, cache_spec, cache_spec),
        check_vma=False,
    )
```

```python
import functools

import jax
import jax.numpy as jnp
from jax import lax
from jax.experimental import pallas as pl
from jax.experimental.pallas import tpu as pltpu
from jax.sharding import PartitionSpec as P

LN_EPS = 1e-6
ROPE_BASE = 10000.0
MESH = pl.DeviceIdType.MESH
VMEM_MOST = 64 * 1024 * 1024 - 64 * 1024
EARLY = 2
ROWS_A = 80


def attention_kernel(scale, len_ref, q_ref, cols_ref, k_hbm, v_hbm, o_ref, ko_hbm, vo_hbm, k_buf, v_buf, in_sem, out_sem):
    rows, _, seq_len = k_buf.shape

    def load(which, b):
        src, dst = ((k_hbm, k_buf), (v_hbm, v_buf))[which]
        return pltpu.make_async_copy(src.at[b], dst.at[b], in_sem.at[which, b])

    def save(which, b):
        src, dst = ((k_buf, ko_hbm), (v_buf, vo_hbm))[which]
        return pltpu.make_async_copy(src.at[b], dst.at[b], out_sem.at[which, b])

    for b in range(rows):
        load(0, b).start()
        load(1, b).start()

    lane = lax.broadcasted_iota(jnp.int32, (1, 128), 1)
    slots = lax.broadcasted_iota(jnp.int32, (1, seq_len), 1)

    def row(b, carry):
        length = len_ref[b]
        window = pl.ds(pl.multiple_of((length // 128) * 128, 128), 128)
        here = lane == length % 128
        for which, buf in enumerate((k_buf, v_buf)):
            load(which, b).wait()
            col = jnp.sum(jnp.where(lane == b, cols_ref[which], 0.0), axis=1, keepdims=True)
            tile = buf[b, :, window].astype(jnp.float32)
            buf[b, :, window] = jnp.where(here, col, tile).astype(jnp.bfloat16)
        scores = jnp.dot(q_ref[b], k_buf[b], preferred_element_type=jnp.float32) * scale
        scores = jnp.where(slots <= length, scores, -1e30)
        top = jnp.max(scores, axis=1, keepdims=True)
        weights = jnp.exp(scores - top)
        total = jnp.sum(weights, axis=1, keepdims=True)
        probs = (weights * (1.0 / total)).astype(jnp.bfloat16)
        save(0, b).start()
        save(1, b).start()
        o_ref[b] = lax.dot_general(probs, v_buf[b], (((1,), (1,)), ((), ())), preferred_element_type=jnp.float32).astype(jnp.bfloat16)
        return carry

    lax.fori_loop(0, rows, row, 0)
    for b in range(rows):
        save(0, b).wait()
        save(1, b).wait()


def attend(q_rot, cols, k_cache, v_cache, lengths):
    rows, heads, head_dim = q_rot.shape
    seq_len = k_cache.shape[1]
    k_t = jnp.swapaxes(k_cache, 1, 2)
    v_t = jnp.swapaxes(v_cache, 1, 2)
    cache = jax.ShapeDtypeStruct((rows, head_dim, seq_len), jnp.bfloat16)
    o, k_new, v_new = pl.pallas_call(
        functools.partial(attention_kernel, head_dim ** -0.5),
        out_shape=(jax.ShapeDtypeStruct((rows, heads, head_dim), jnp.bfloat16), cache, cache),
        in_specs=[
            pl.BlockSpec(memory_space=pltpu.SMEM),
            pl.BlockSpec(memory_space=pltpu.VMEM),
            pl.BlockSpec(memory_space=pltpu.VMEM),
            pl.BlockSpec(memory_space=pl.ANY),
            pl.BlockSpec(memory_space=pl.ANY),
        ],
        out_specs=(pl.BlockSpec(memory_space=pltpu.VMEM), pl.BlockSpec(memory_space=pl.ANY), pl.BlockSpec(memory_space=pl.ANY)),
        scratch_shapes=[
            pltpu.VMEM((rows, head_dim, seq_len), jnp.bfloat16),
            pltpu.VMEM((rows, head_dim, seq_len), jnp.bfloat16),
            pltpu.SemaphoreType.DMA((2, rows)),
            pltpu.SemaphoreType.DMA((2, rows)),
        ],
        compiler_params=pltpu.CompilerParams(vmem_limit_bytes=48 * 1024 * 1024),
        cost_estimate=pl.CostEstimate(
            flops=4 * rows * heads * head_dim * seq_len,
            bytes_accessed=8 * rows * head_dim * seq_len,
            transcendentals=rows * heads * seq_len,
        ),
        name='attend',
    )(lengths, q_rot, cols, k_t, v_t)
    return o, jnp.swapaxes(k_new, 1, 2), jnp.swapaxes(v_new, 1, 2)


def start_barrier(me_x, me_yz):
    barrier = pltpu.get_barrier_semaphore()
    for dx in range(2):
        for k in range(4):
            if dx or k:
                peer = (lax.rem(me_x + dx, 2), lax.rem(me_yz + k, 4))
                pl.semaphore_signal(barrier, inc=1, device_id=peer, device_id_type=MESH)
    pl.semaphore_wait(barrier, 7)


def spread(rows, cols, first):
    i = lax.broadcasted_iota(jnp.int32, (rows, cols), 0)
    c = lax.broadcasted_iota(jnp.int32, (rows, cols), 1)
    return jnp.where(c == 2 * i + first, 1.0, 0.0).astype(jnp.bfloat16)


def head_kernel(
    d_model, early, x_hbm, scale_hbm, wg_hbm, wa_hbm, z_ref, first_hbm, send_a_hbm, send_b_hbm, own_hbm,
    xg, sg, stats, h_buf, hx, hc, wg, wa, z_send, z_own, z_recv, zb, zg, g_first, g_got, g_rest, g_own,
    in_sem, wg_sem, x_send, x_recv, s_send, s_recv, t_send, t_recv, z_sems, a_send, a_recv, f_send, f_recv, out_sem,
):
    me_x = lax.axis_index('x')
    me_yz = lax.axis_index('yz')
    half, chunk = xg.shape[2:]
    rows = 2 * half
    pieces = wg_sem.shape[0]
    depth = wg.shape[0] // pieces
    ff = wg.shape[2]
    wide_cols = 256
    other_x = lax.rem(me_x + 1, 2)
    across = lax.rem(me_yz + 2, 4)
    core = lax.rem(me_yz, 2)
    partner = me_yz + 1 - 2 * core
    order = (other_x, me_x)
    x_in = [
        pltpu.make_async_copy(x_hbm.at[pl.ds(pl.multiple_of(order[p] * half, 32), half)], xg.at[me_yz, order[p]], in_sem.at[p]) for p in range(2)
    ]
    scale_in = pltpu.make_async_copy(scale_hbm, sg.at[me_yz], in_sem.at[2])
    wa_in = pltpu.make_async_copy(wa_hbm, wa, in_sem.at[3])
    wg_in = [
        pltpu.make_async_copy(wg_hbm.at[pl.ds(depth * i, depth)], wg.at[pl.ds(depth * i, depth)], wg_sem.at[i]) for i in range(pieces)
    ]
    for copy in (*x_in, scale_in, wa_in, *wg_in):
        copy.start()
    start_barrier(me_x, me_yz)

    def remote(src, dst, send, recv, to_x, to_yz):
        return pltpu.make_async_remote_copy(
            src_ref=src, dst_ref=dst, send_sem=send, recv_sem=recv, device_id=(to_x, to_yz), device_id_type=MESH,
        )

    def x_copy(kind, p):
        owner = across if kind == 2 else me_yz
        at = xg.at[owner, order[p]]
        return remote(at, at, x_send.at[kind, p], x_recv.at[kind, p], me_x, across if kind == 1 else partner)

    for p in range(2):
        x_in[p].wait()
    lane = lax.broadcasted_iota(jnp.int32, (8, 128), 1)
    tile = jnp.zeros((8, 128), jnp.float32)
    for e in range(2):
        mine = xg[me_yz, e].astype(jnp.float32)
        sum_1 = jnp.sum(mine, axis=1, keepdims=True)
        sum_2 = jnp.sum(mine * mine, axis=1, keepdims=True)
        for j in range(half // 8):
            col = e * (half // 8) + j
            tile = jnp.where(lane == col, sum_1[8 * j:8 * j + 8], tile)
            tile = jnp.where(lane == 32 + col, sum_2[8 * j:8 * j + 8], tile)
    me = me_x * 4 + me_yz
    stats[me] = tile
    t_out = [
        remote(stats.at[me], stats.at[me], t_send.at[4 * dx + k], t_recv.at[4 * dx + k], lax.rem(me_x + dx, 2), lax.rem(me_yz + k, 4))
        for dx in range(2) for k in range(4) if dx or k
    ]
    for copy in t_out:
        copy.start()
    scale_in.wait()
    s_out = [remote(sg.at[me_yz], sg.at[me_yz], s_send.at[k], s_recv.at[k], me_x, lax.rem(me_yz + k, 4)) for k in (1, 2, 3)]
    for copy in s_out:
        copy.start()
    for p in range(2):
        x_copy(1, p).start()
        x_copy(0, p).start()
    wide, thin = spread(128, 256, 0), spread(64, 128, 0)
    wide_u, thin_u = spread(128, 256, 1), spread(64, 128, 1)
    i = lax.broadcasted_iota(jnp.int32, (256, 128), 0)
    c = lax.broadcasted_iota(jnp.int32, (256, 128), 1)
    gather = jnp.where(i == 2 * c, 1.0, 0.0).astype(jnp.bfloat16)
    for copy in t_out:
        copy.wait()
    total = stats[0]
    for i in range(1, 8):
        total = total + stats[i]
    mean_t = total / d_model
    var_t = pltpu.roll(total, 96, 1) / d_model - mean_t * mean_t
    rstd_t = lax.rsqrt(var_t + LN_EPS)
    for copy in s_out:
        copy.wait()

    def normalize(p):
        shift = lax.rem(128 - order[p] * (half // 8), 128)
        mean_p = pltpu.roll(mean_t, shift, 1)
        rstd_p = pltpu.roll(rstd_t, shift, 1)
        mean = jnp.concatenate([mean_p[:, j:j + 1] for j in range(half // 8)], axis=0)
        rstd = jnp.concatenate([rstd_p[:, j:j + 1] for j in range(half // 8)], axis=0)
        x_copy(1, p).wait()
        x_copy(2, p).start()
        x_copy(0, p).wait()
        x_copy(2, p).wait()
        for s in range(4):
            h_buf[s] = ((xg[s, order[p]].astype(jnp.float32) - mean) * rstd * sg[s]).astype(jnp.bfloat16)

    def spread_half(part, g):
        out = pl.ds((2 * part + g) * half, half)
        a, b = ((wide, thin), (wide_u, thin_u))[g]
        for s in range(4):
            base = 2 * chunk * s
            for t in range(2):
                piece = h_buf[s, :, 128 * t:128 * t + 128]
                hx[out, base + 256 * t:base + 256 * t + 256] = jnp.dot(piece, a, preferred_element_type=jnp.float32).astype(jnp.bfloat16)
            piece = h_buf[s, :, 256:320]
            hx[out, base + 512:base + 640] = jnp.dot(piece, b, preferred_element_type=jnp.float32).astype(jnp.bfloat16)

    def project(part):
        src = pl.ds(2 * part * half, half)
        for t in range(4 * chunk // 128):
            hc[:, 128 * t:128 * t + 128] = jnp.dot(hx[src, 256 * t:256 * t + 256], gather, preferred_element_type=jnp.float32).astype(jnp.bfloat16)
        z = lax.dot_general(hc[...], wa[...], (((1,), (1,)), ((), ())), preferred_element_type=jnp.float32)
        return z.reshape(z_send.shape)

    normalize(0)
    spread_half(0, 0)
    wa_in.wait()
    z_send[...] = project(0)
    z_copy = remote(z_send, z_recv, z_sems.at[0], z_sems.at[1], other_x, me_yz)
    z_copy.start()
    spread_half(0, 1)
    normalize(1)
    spread_half(1, 0)
    spread_half(1, 1)
    for copy in wg_in:
        copy.wait()

    def columns(c):
        at = pl.ds(pl.multiple_of(c * wide_cols, wide_cols), wide_cols)
        block = wg[:, :, at].reshape(2 * wg.shape[0], wide_cols)
        out = jnp.dot(hx[...], block, preferred_element_type=jnp.float32)
        up = pl.ds(pl.multiple_of(ff + c * wide_cols, wide_cols), wide_cols)
        g_own[:, at] = out[2 * half:3 * half]
        g_own[:, up] = out[3 * half:]
        return out

    first = []
    for c in range(early):
        out = columns(c)
        g_first[c, :, :wide_cols] = out[:half]
        g_first[c, :, wide_cols:] = out[half:2 * half]
        first.append(remote(g_first.at[c], g_got.at[c], f_send.at[c], f_recv.at[c], other_x, me_yz))
        first[-1].start()

    def rest(c, carry):
        out = columns(c)
        at = (c - early) * wide_cols
        g_rest[:, pl.ds(pl.multiple_of(at, wide_cols), wide_cols)] = out[:half]
        g_rest[:, pl.ds(pl.multiple_of(ff - early * wide_cols + at, wide_cols), wide_cols)] = out[half:2 * half]
        return carry

    lax.fori_loop(early, ff // wide_cols, rest, 0)
    rows_a = send_a_hbm.shape[0]
    save = [
        pltpu.make_async_copy(g_rest.at[pl.ds(0, rows_a)], send_a_hbm, out_sem.at[0]),
        pltpu.make_async_copy(g_rest.at[pl.ds(rows_a, half - rows_a)], send_b_hbm, out_sem.at[1]),
        pltpu.make_async_copy(g_own, own_hbm, out_sem.at[2]),
    ]
    for copy in save:
        copy.start()
    z_own[...] = project(1)
    z_copy.wait()
    zb[...] = (z_own[...] + z_recv[...]).astype(jnp.bfloat16)
    a_out = [remote(zb.at[lax.rem(me_yz + k, 4)], zg.at[me_yz], a_send.at[k], a_recv.at[k], me_x, lax.rem(me_yz + k, 4)) for k in (1, 2, 3)]
    for copy in a_out:
        copy.start()
    zg[me_yz] = zb[me_yz]
    for copy in a_out:
        copy.wait()
    z_ref[...] = zg[...]
    for copy in first:
        copy.wait()
    keep = pltpu.make_async_copy(g_got, first_hbm, out_sem.at[3])
    keep.start()
    keep.wait()
    for copy in save:
        copy.wait()


def head(x_in, ln_scale, w_gate_up, w_attn, d_model, early, rows_a):
    rows, chunk = x_in.shape
    depth, _, ff = w_gate_up.shape
    z_cols = w_attn.shape[1]
    owned = rows // 8
    half = rows // 2
    width = 2 * (ff - 256 * early)
    any_spec = pl.BlockSpec(memory_space=pl.ANY)
    dma = pltpu.SemaphoreType.DMA
    f32, bf16 = jnp.float32, jnp.bfloat16
    return pl.pallas_call(
        functools.partial(head_kernel, d_model, early),
        out_shape=(
            jax.ShapeDtypeStruct((4, owned, z_cols), bf16),
            jax.ShapeDtypeStruct((early, half, 512), f32),
            jax.ShapeDtypeStruct((rows_a, width), f32),
            jax.ShapeDtypeStruct((half - rows_a, width), f32),
            jax.ShapeDtypeStruct((half, 2 * ff), f32),
        ),
        in_specs=[any_spec] * 4,
        out_specs=(pl.BlockSpec(memory_space=pltpu.VMEM), *[any_spec] * 4),
        scratch_shapes=[
            pltpu.VMEM((4, 2, half, chunk), bf16),
            pltpu.VMEM((4, 1, chunk), f32),
            pltpu.VMEM((8, 8, 128), f32),
            pltpu.VMEM((4, half, chunk), bf16),
            pltpu.VMEM((2 * rows, 2 * depth), bf16),
            pltpu.VMEM((half, depth), bf16),
            pltpu.VMEM((depth, 2, ff), bf16),
            pltpu.VMEM((z_cols, depth), bf16),
            pltpu.VMEM((4, owned, z_cols), f32),
            pltpu.VMEM((4, owned, z_cols), f32),
            pltpu.VMEM((4, owned, z_cols), f32),
            pltpu.VMEM((4, owned, z_cols), bf16),
            pltpu.VMEM((4, owned, z_cols), bf16),
            pltpu.VMEM((early, half, 512), f32),
            pltpu.VMEM((early, half, 512), f32),
            pltpu.VMEM((half, width), f32),
            pltpu.VMEM((half, 2 * ff), f32),
            dma((4,)), dma((8,)), dma((3, 2)), dma((3, 2)), dma((4,)), dma((4,)), dma((8,)), dma((8,)), dma((2,)), dma((4,)), dma((4,)),
            dma((early,)), dma((early,)), dma((4,)),
        ],
        compiler_params=pltpu.CompilerParams(collective_id=0, has_side_effects=True, vmem_limit_bytes=VMEM_MOST),
        cost_estimate=pl.CostEstimate(flops=4 * rows * depth * 2 * ff, bytes_accessed=4 * depth * ff, transcendentals=0),
        name='head',
    )(x_in, ln_scale.reshape(1, chunk), w_gate_up, w_attn.T)


def tail_kernel(
    x_hbm, first_hbm, peer_hbm, late_hbm, own_hbm, o_hbm, wd_hbm, wo_hbm, y_ref,
    xv, g_first, g_peer, g_late, g_got, g_own, ov, oa, of, hb, wd, wo, out_part, y_send, y_pair, y_over, y_recv, y_last,
    in_sem, g_sem, b_send, b_recv, o_send, o_recv, h_send, h_recv, p_send, p_recv, y_ssem, y_rsem, l_send, l_recv,
):
    me_x = lax.axis_index('x')
    me_yz = lax.axis_index('yz')
    groups, _, span, ff = hb.shape
    rows, chunk = xv.shape
    half = rows // 2
    owned = ov.shape[1]
    early, _, wide = g_first.shape
    wide = wide // 2
    groups_a = g_peer.shape[0] // span
    core = lax.rem(me_yz, 2)
    col = me_yz // 2
    partner = me_yz + 1 - 2 * core
    across = lax.rem(me_yz + 2, 4)
    other_x = lax.rem(me_x + 1, 2)

    def rows_of(i):
        return pl.ds(span * i, span)

    late_in = pltpu.make_async_copy(late_hbm, g_late, in_sem.at[4])
    o_in = pltpu.make_async_copy(o_hbm, ov, in_sem.at[0])
    first_in = pltpu.make_async_copy(first_hbm, g_first, in_sem.at[5])
    own_in = [pltpu.make_async_copy(own_hbm.at[rows_of(i)], g_own.at[rows_of(i)], g_sem.at[0, i]) for i in range(groups)]
    peer_in = [pltpu.make_async_copy(peer_hbm.at[rows_of(i)], g_peer.at[rows_of(i)], g_sem.at[1, i]) for i in range(groups_a)]
    wo_in = pltpu.make_async_copy(wo_hbm, wo, in_sem.at[1])
    wd_in = pltpu.make_async_copy(wd_hbm, wd, in_sem.at[2])
    x_in = pltpu.make_async_copy(x_hbm, xv, in_sem.at[3])
    for copy in (late_in, o_in, first_in):
        copy.start()
    for i in range(groups):
        own_in[i].start()
        if i < groups_a:
            peer_in[i].start()
    for copy in (wo_in, wd_in, x_in):
        copy.start()
    start_barrier(me_x, me_yz)
    me = me_x * 4 + me_yz

    def remote(src, dst, send, recv, to_x, to_yz):
        return pltpu.make_async_remote_copy(
            src_ref=src, dst_ref=dst, send_sem=send, recv_sem=recv, device_id=(to_x, to_yz), device_id_type=MESH,
        )

    late_in.wait()
    b_out = [
        remote(g_late.at[rows_of(i)], g_got.at[rows_of(i)], b_send.at[i], b_recv.at[i], other_x, me_yz) for i in range(groups - groups_a)
    ]
    for copy in b_out:
        copy.start()
    o_in.wait()
    o_out = []
    for dx in range(2):
        for k in range(4):
            if dx or k:
                there = lax.rem(me_yz + k, 4)
                o_out.append(remote(ov.at[there], oa.at[me], o_send.at[4 * dx + k], o_recv.at[4 * dx + k], lax.rem(me_x + dx, 2), there))
    for copy in o_out:
        copy.start()
    oa[me] = ov[me_yz]
    first_in.wait()

    h_out = []

    def activate(i):
        own_in[i].wait()
        at = rows_of(i)
        if i < groups_a:
            peer_in[i].wait()
            got, got_at = g_peer, at
        else:
            b_out[i - groups_a].wait()
            got, got_at = g_got, rows_of(i - groups_a)

        def act(gate, up):
            gate = gate.astype(jnp.bfloat16).astype(jnp.float32)
            up = up.astype(jnp.bfloat16).astype(jnp.float32)
            return (jax.nn.silu(gate) * up).astype(jnp.bfloat16)

        for c in range(early):
            cols = slice(wide * c, wide * c + wide)
            up_cols = slice(ff + wide * c, ff + wide * c + wide)
            hb[i, me_x, :, cols] = act(g_own[at, cols] + g_first[c, at, :wide], g_own[at, up_cols] + g_first[c, at, wide:])
        done = early * wide
        hb[i, me_x, :, done:] = act(g_own[at, done:ff] + got[got_at, :ff - done], g_own[at, ff + done:] + got[got_at, ff - done:])
        copy = remote(hb.at[i, me_x], hb.at[i, me_x], h_send.at[i], h_recv.at[i], other_x, me_yz)
        copy.start()
        h_out.append(copy)

    for i in range(groups_a):
        activate(i)
    for copy in o_out:
        copy.wait()
    for e in range(8):
        of[owned * e:owned * e + owned] = oa[e].astype(jnp.float32)
    wo_in.wait()
    out_part[...] = jnp.dot(of[...].astype(jnp.bfloat16), wo[...], preferred_element_type=jnp.float32)
    for i in range(groups_a, groups):
        activate(i)
    wd_in.wait()
    x_in.wait()

    pair, over, last = [], [], []

    def product(i):
        h_out[i].wait()
        part = jnp.dot(hb[i].reshape(2 * span, ff), wd[...], preferred_element_type=jnp.float32)
        part = part + jnp.concatenate([out_part[span * i:span * i + span], out_part[half + span * i:half + span * i + span]], axis=0)
        for j in range(4):
            moved = part if j == 0 else pltpu.roll(part, (4 - j) * chunk, 1)
            y_send[i, j] = moved[:, :chunk]
        if i < groups - 1:
            pair.append([
                remote(y_send.at[i, 2 * e + 1 - core], y_pair.at[i, e], p_send.at[i, e], p_recv.at[i, e], me_x, partner) for e in range(2)
            ])
            for copy in pair[i]:
                copy.start()
        else:
            for k in (2, 3, 1):
                there = lax.rem(me_yz + k, 4)
                last.append(remote(y_send.at[i, there], y_last.at[me_yz], l_send.at[k], l_recv.at[k], me_x, there))
                last[-1].start()

    def cross(i):
        for copy in pair[i]:
            copy.wait()
        y_over[i] = y_send[i, across] + y_pair[i, 1 - col]
        over.append(remote(y_over.at[i], y_recv.at[i], y_ssem.at[i], y_rsem.at[i], me_x, across))
        over[i].start()

    def finish(i):
        if i < groups - 1:
            over[i].wait()
            total = y_send[i, me_yz] + y_pair[i, col] + y_recv[i]
        else:
            for copy in last:
                copy.wait()
            total = y_send[i, me_yz]
            for k in (1, 2, 3):
                total = total + y_last[lax.rem(me_yz + k, 4)]
        for e in range(2):
            at = pl.ds(half * e + span * i, span)
            y_ref[at, :] = (xv[at, :].astype(jnp.float32) + total[span * e:span * e + span]).astype(jnp.bfloat16)

    for i in range(groups):
        product(i)
        if i >= 1:
            cross(i - 1)
        if i >= 2:
            finish(i - 2)
    finish(groups - 2)
    finish(groups - 1)


def tail(x_in, g_first, g_peer, g_late, g_own, o_blocks, w_down, w_out):
    rows, chunk = x_in.shape
    half = rows // 2
    span = 16
    groups = half // span
    ff, cols = w_down.shape
    owned = o_blocks.shape[1]
    o_width = w_out.shape[0]
    any_spec = pl.BlockSpec(memory_space=pl.ANY)
    dma = pltpu.SemaphoreType.DMA
    f32, bf16 = jnp.float32, jnp.bfloat16
    late_groups = g_late.shape[0] // span
    return pl.pallas_call(
        tail_kernel,
        out_shape=jax.ShapeDtypeStruct((rows, chunk), bf16),
        in_specs=[any_spec] * 8,
        out_specs=pl.BlockSpec(memory_space=pltpu.VMEM),
        scratch_shapes=[
            pltpu.VMEM((rows, chunk), bf16),
            pltpu.VMEM(g_first.shape, f32),
            pltpu.VMEM(g_peer.shape, f32),
            pltpu.VMEM(g_late.shape, f32),
            pltpu.VMEM(g_late.shape, f32),
            pltpu.VMEM((half, 2 * ff), f32),
            pltpu.VMEM((4, owned, o_width), bf16),
            pltpu.VMEM((8, owned, o_width), bf16),
            pltpu.VMEM((rows, o_width), f32),
            pltpu.VMEM((groups, 2, span, ff), bf16),
            pltpu.VMEM((ff, cols), bf16),
            pltpu.VMEM((o_width, cols), bf16),
            pltpu.VMEM((rows, cols), f32),
            pltpu.VMEM((groups, 4, 2 * span, chunk), f32),
            pltpu.VMEM((groups, 2, 2 * span, chunk), f32),
            pltpu.VMEM((groups, 2 * span, chunk), f32),
            pltpu.VMEM((groups, 2 * span, chunk), f32),
            pltpu.VMEM((4, 2 * span, chunk), f32),
            dma((6,)), dma((2, groups)), dma((late_groups,)), dma((late_groups,)), dma((8,)), dma((8,)), dma((groups,)), dma((groups,)),
            dma((groups, 2)), dma((groups, 2)), dma((groups,)), dma((groups,)), dma((4,)), dma((4,)),
        ],
        compiler_params=pltpu.CompilerParams(collective_id=1, has_side_effects=True, vmem_limit_bytes=VMEM_MOST - 1536 * 1024),
        cost_estimate=pl.CostEstimate(flops=2 * rows * (ff + o_width) * cols, bytes_accessed=2 * (ff + o_width) * cols, transcendentals=half * ff),
        name='tail',
    )(x_in, g_first, g_peer, g_late, g_own, o_blocks, w_down, w_out)


def rotary(values, positions):
    half_dim = values.shape[-1] // 2
    inv_freq = ROPE_BASE ** (-jnp.arange(half_dim, dtype=jnp.float32) / half_dim)
    angles = positions.astype(jnp.float32)[:, None, None] * inv_freq
    cos_part = jnp.cos(angles)
    sin_part = jnp.sin(angles)
    lo_half = values[..., :half_dim]
    hi_half = values[..., half_dim:]
    return jnp.concatenate([lo_half * cos_part - hi_half * sin_part, hi_half * cos_part + lo_half * sin_part], axis=-1)


def solution(mesh):
    x_size = mesh.shape['x']
    yz_size = mesh.shape['yz']
    all_axes = ('x', 'yz')

    def local_step(x_in, ln_scale, w_gate_up, w_attn, w_down, w_out, k_cache, v_cache, lengths, positions):
        local_rows, seq_len, head_dim = k_cache.shape
        q_width = w_out.shape[0] * yz_size
        num_heads = q_width // head_dim
        d_model = x_in.shape[1] * x_size * yz_size
        z_blocks, g_first, g_send, g_late, g_own = head(x_in, ln_scale, w_gate_up, w_attn, d_model, EARLY, ROWS_A)
        g_peer = lax.ppermute(g_send, 'x', [(0, 1), (1, 0)])
        proj_local = z_blocks.transpose(1, 0, 2).reshape(local_rows, -1)
        q_raw = proj_local[:, :q_width].reshape(local_rows, num_heads, head_dim)
        k_tok = proj_local[:, q_width:q_width + head_dim]
        v_tok = proj_local[:, q_width + head_dim:]
        q_rot = rotary(q_raw.astype(jnp.float32), positions).astype(jnp.bfloat16)
        k_rot = rotary(k_tok[:, None, :].astype(jnp.float32), positions)[:, 0].astype(jnp.bfloat16)
        cols = jnp.stack([k_rot, v_tok]).astype(jnp.float32).transpose(0, 2, 1)
        cols = jnp.pad(cols, ((0, 0), (0, 0), (0, 128 - local_rows)))
        attn_out, k_new, v_new = attend(q_rot, cols, k_cache, v_cache, lengths)
        o_blocks = attn_out.reshape(local_rows, yz_size, q_width // yz_size).transpose(1, 0, 2)
        y_out = tail(x_in, g_first, g_peer, g_late, g_own, o_blocks, w_down, w_out)
        return y_out, k_new, v_new

    row_spec = P(None, all_axes)
    vec_spec = P(all_axes)
    cache_spec = P(all_axes, None, None)
    return jax.shard_map(
        local_step,
        mesh=mesh,
        in_specs=(row_spec, vec_spec, P('x', None, 'yz'), P('x', 'yz'), P('yz', 'x'), P('yz', 'x'), cache_spec, cache_spec, vec_spec, vec_spec),
        out_specs=(row_spec, cache_spec, cache_spec),
        check_vma=False,
    )
```

```python
import functools

import jax
import jax.numpy as jnp
from jax import lax
from jax.experimental import pallas as pl
from jax.experimental.pallas import tpu as pltpu
from jax.sharding import PartitionSpec as P

LN_EPS = 1e-6
ROPE_BASE = 10000.0
MESH = pl.DeviceIdType.MESH
VMEM_MOST = 64 * 1024 * 1024 - 64 * 1024
EARLY = 2
ROWS_A = 80


def attention_kernel(scale, len_ref, q_ref, cols_ref, k_hbm, v_hbm, o_ref, ko_hbm, vo_hbm, k_buf, v_buf, in_sem, out_sem):
    rows, _, seq_len = k_buf.shape

    def load(which, b):
        src, dst = ((k_hbm, k_buf), (v_hbm, v_buf))[which]
        return pltpu.make_async_copy(src.at[b], dst.at[b], in_sem.at[which, b])

    def save(which, b):
        src, dst = ((k_buf, ko_hbm), (v_buf, vo_hbm))[which]
        return pltpu.make_async_copy(src.at[b], dst.at[b], out_sem.at[which, b])

    for b in range(rows):
        load(0, b).start()
        load(1, b).start()

    lane = lax.broadcasted_iota(jnp.int32, (1, 128), 1)
    slots = lax.broadcasted_iota(jnp.int32, (1, seq_len), 1)

    def row(b, carry):
        length = len_ref[b]
        window = pl.ds(pl.multiple_of((length // 128) * 128, 128), 128)
        here = lane == length % 128
        for which, buf in enumerate((k_buf, v_buf)):
            load(which, b).wait()
            col = jnp.sum(jnp.where(lane == b, cols_ref[which], 0.0), axis=1, keepdims=True)
            tile = buf[b, :, window].astype(jnp.float32)
            buf[b, :, window] = jnp.where(here, col, tile).astype(jnp.bfloat16)
        scores = jnp.dot(q_ref[b], k_buf[b], preferred_element_type=jnp.float32) * scale
        scores = jnp.where(slots <= length, scores, -1e30)
        top = jnp.max(scores, axis=1, keepdims=True)
        weights = jnp.exp(scores - top)
        total = jnp.sum(weights, axis=1, keepdims=True)
        probs = (weights * (1.0 / total)).astype(jnp.bfloat16)
        save(0, b).start()
        save(1, b).start()
        o_ref[b] = lax.dot_general(probs, v_buf[b], (((1,), (1,)), ((), ())), preferred_element_type=jnp.float32).astype(jnp.bfloat16)
        return carry

    lax.fori_loop(0, rows, row, 0)
    for b in range(rows):
        save(0, b).wait()
        save(1, b).wait()


def attend(q_rot, cols, k_cache, v_cache, lengths):
    rows, heads, head_dim = q_rot.shape
    seq_len = k_cache.shape[1]
    k_t = jnp.swapaxes(k_cache, 1, 2)
    v_t = jnp.swapaxes(v_cache, 1, 2)
    cache = jax.ShapeDtypeStruct((rows, head_dim, seq_len), jnp.bfloat16)
    o, k_new, v_new = pl.pallas_call(
        functools.partial(attention_kernel, head_dim ** -0.5),
        out_shape=(jax.ShapeDtypeStruct((rows, heads, head_dim), jnp.bfloat16), cache, cache),
        in_specs=[
            pl.BlockSpec(memory_space=pltpu.SMEM),
            pl.BlockSpec(memory_space=pltpu.VMEM),
            pl.BlockSpec(memory_space=pltpu.VMEM),
            pl.BlockSpec(memory_space=pl.ANY),
            pl.BlockSpec(memory_space=pl.ANY),
        ],
        out_specs=(pl.BlockSpec(memory_space=pltpu.VMEM), pl.BlockSpec(memory_space=pl.ANY), pl.BlockSpec(memory_space=pl.ANY)),
        scratch_shapes=[
            pltpu.VMEM((rows, head_dim, seq_len), jnp.bfloat16),
            pltpu.VMEM((rows, head_dim, seq_len), jnp.bfloat16),
            pltpu.SemaphoreType.DMA((2, rows)),
            pltpu.SemaphoreType.DMA((2, rows)),
        ],
        compiler_params=pltpu.CompilerParams(vmem_limit_bytes=48 * 1024 * 1024),
        cost_estimate=pl.CostEstimate(
            flops=4 * rows * heads * head_dim * seq_len,
            bytes_accessed=8 * rows * head_dim * seq_len,
            transcendentals=rows * heads * seq_len,
        ),
        name='attend',
    )(lengths, q_rot, cols, k_t, v_t)
    return o, jnp.swapaxes(k_new, 1, 2), jnp.swapaxes(v_new, 1, 2)


def start_barrier(me_x, me_yz):
    barrier = pltpu.get_barrier_semaphore()
    for dx in range(2):
        for k in range(4):
            if dx or k:
                peer = (lax.rem(me_x + dx, 2), lax.rem(me_yz + k, 4))
                pl.semaphore_signal(barrier, inc=1, device_id=peer, device_id_type=MESH)
    return lambda: pl.semaphore_wait(barrier, 7)


def spread(rows, cols, first):
    i = lax.broadcasted_iota(jnp.int32, (rows, cols), 0)
    c = lax.broadcasted_iota(jnp.int32, (rows, cols), 1)
    return jnp.where(c == 2 * i + first, 1.0, 0.0).astype(jnp.bfloat16)


def head_kernel(
    d_model, early, x_hbm, scale_hbm, wg_hbm, wa_hbm, z_hbm, first_hbm, send_a_hbm, send_b_hbm, own_hbm,
    xg, scale_row, sg, stats, h_buf, hx, hc, wg, wa, z_send, z_own, z_recv, zb, zg, g_first, g_rest, g_own,
    in_sem, wg_sem, x_send, x_recv, s_send, s_recv, t_send, t_recv, z_sems, a_send, a_recv, f_send, f_recv, out_sem,
):
    me_x = lax.axis_index('x')
    me_yz = lax.axis_index('yz')
    half, chunk = xg.shape[2:]
    rows = 2 * half
    pieces = wg_sem.shape[0]
    depth = wg.shape[0] // pieces
    ff = wg.shape[2]
    wide_cols = 256
    other_x = lax.rem(me_x + 1, 2)
    across = lax.rem(me_yz + 2, 4)
    core = lax.rem(me_yz, 2)
    partner = me_yz + 1 - 2 * core
    order = (other_x, me_x)
    x_in = [
        pltpu.make_async_copy(x_hbm.at[pl.ds(pl.multiple_of(order[p] * half, 32), half)], xg.at[me_yz, order[p]], in_sem.at[p]) for p in range(2)
    ]
    scale_in = pltpu.make_async_copy(scale_hbm, scale_row, in_sem.at[2])
    wa_in = pltpu.make_async_copy(wa_hbm, wa, in_sem.at[3])
    wg_in = [
        pltpu.make_async_copy(wg_hbm.at[pl.ds(depth * i, depth)], wg.at[pl.ds(depth * i, depth)], wg_sem.at[i]) for i in range(pieces)
    ]
    for copy in (*x_in, scale_in, wa_in, *wg_in):
        copy.start()
    others_ready = start_barrier(me_x, me_yz)

    def remote(src, dst, send, recv, to_x, to_yz):
        return pltpu.make_async_remote_copy(
            src_ref=src, dst_ref=dst, send_sem=send, recv_sem=recv, device_id=(to_x, to_yz), device_id_type=MESH,
        )

    def x_copy(kind, p):
        owner = across if kind == 2 else me_yz
        at = xg.at[owner, order[p]]
        return remote(at, at, x_send.at[kind, p], x_recv.at[kind, p], me_x, across if kind == 1 else partner)

    for p in range(2):
        x_in[p].wait()
    lane = lax.broadcasted_iota(jnp.int32, (8, 128), 1)
    tile = jnp.zeros((8, 128), jnp.float32)
    for e in range(2):
        mine = xg[me_yz, e].astype(jnp.float32)
        sum_1 = jnp.sum(mine, axis=1, keepdims=True)
        sum_2 = jnp.sum(mine * mine, axis=1, keepdims=True)
        for j in range(half // 8):
            col = e * (half // 8) + j
            tile = jnp.where(lane == col, sum_1[8 * j:8 * j + 8], tile)
            tile = jnp.where(lane == 32 + col, sum_2[8 * j:8 * j + 8], tile)
    me = me_x * 4 + me_yz
    stats[me] = tile
    others_ready()
    t_out = [
        remote(stats.at[me], stats.at[me], t_send.at[4 * dx + k], t_recv.at[4 * dx + k], lax.rem(me_x + dx, 2), lax.rem(me_yz + k, 4))
        for dx in range(2) for k in range(4) if dx or k
    ]
    for copy in t_out:
        copy.start()
    scale_in.wait()
    sg[me_yz] = scale_row[...].reshape(1, chunk)
    s_out = [remote(sg.at[me_yz], sg.at[me_yz], s_send.at[k], s_recv.at[k], me_x, lax.rem(me_yz + k, 4)) for k in (1, 2, 3)]
    for copy in s_out:
        copy.start()
    for p in range(2):
        x_copy(1, p).start()
        x_copy(0, p).start()
    wide, thin = spread(128, 256, 0), spread(64, 128, 0)
    wide_u, thin_u = spread(128, 256, 1), spread(64, 128, 1)
    i = lax.broadcasted_iota(jnp.int32, (256, 128), 0)
    c = lax.broadcasted_iota(jnp.int32, (256, 128), 1)
    gather = jnp.where(i == 2 * c, 1.0, 0.0).astype(jnp.bfloat16)
    for copy in t_out:
        copy.wait()
    total = stats[0]
    for i in range(1, 8):
        total = total + stats[i]
    mean_t = total / d_model
    var_t = pltpu.roll(total, 96, 1) / d_model - mean_t * mean_t
    rstd_t = lax.rsqrt(var_t + LN_EPS)
    for copy in s_out:
        copy.wait()

    def normalize(p):
        shift = lax.rem(128 - order[p] * (half // 8), 128)
        mean_p = pltpu.roll(mean_t, shift, 1)
        rstd_p = pltpu.roll(rstd_t, shift, 1)
        mean = jnp.concatenate([mean_p[:, j:j + 1] for j in range(half // 8)], axis=0)
        rstd = jnp.concatenate([rstd_p[:, j:j + 1] for j in range(half // 8)], axis=0)
        x_copy(1, p).wait()
        x_copy(2, p).start()
        x_copy(0, p).wait()
        x_copy(2, p).wait()
        for s in range(4):
            h_buf[s] = ((xg[s, order[p]].astype(jnp.float32) - mean) * rstd * sg[s]).astype(jnp.bfloat16)

    def spread_half(part, g):
        out = pl.ds((2 * part + g) * half, half)
        a, b = ((wide, thin), (wide_u, thin_u))[g]
        for s in range(4):
            base = 2 * chunk * s
            for t in range(2):
                piece = h_buf[s, :, 128 * t:128 * t + 128]
                hx[out, base + 256 * t:base + 256 * t + 256] = jnp.dot(piece, a, preferred_element_type=jnp.float32).astype(jnp.bfloat16)
            piece = h_buf[s, :, 256:320]
            hx[out, base + 512:base + 640] = jnp.dot(piece, b, preferred_element_type=jnp.float32).astype(jnp.bfloat16)

    def project(part):
        src = pl.ds(2 * part * half, half)
        for t in range(4 * chunk // 128):
            hc[:, 128 * t:128 * t + 128] = jnp.dot(hx[src, 256 * t:256 * t + 256], gather, preferred_element_type=jnp.float32).astype(jnp.bfloat16)
        z = lax.dot_general(hc[...], wa[...], (((1,), (1,)), ((), ())), preferred_element_type=jnp.float32)
        return z.reshape(z_send.shape)

    normalize(0)
    spread_half(0, 0)
    wa_in.wait()
    z_send[...] = project(0)
    z_copy = remote(z_send, z_recv, z_sems.at[0], z_sems.at[1], other_x, me_yz)
    z_copy.start()
    spread_half(0, 1)
    normalize(1)
    spread_half(1, 0)
    spread_half(1, 1)
    for copy in wg_in:
        copy.wait()

    def columns(c):
        at = pl.ds(pl.multiple_of(c * wide_cols, wide_cols), wide_cols)
        block = wg[:, :, at].reshape(2 * wg.shape[0], wide_cols)
        out = jnp.dot(hx[...], block, preferred_element_type=jnp.float32)
        up = pl.ds(pl.multiple_of(ff + c * wide_cols, wide_cols), wide_cols)
        g_own[:, at] = out[2 * half:3 * half]
        g_own[:, up] = out[3 * half:]
        return out

    first = []
    for c in range(early):
        out = columns(c)
        g_first[c, :, :wide_cols] = out[:half]
        g_first[c, :, wide_cols:] = out[half:2 * half]
        first.append(remote(g_first.at[c], first_hbm.at[c], f_send.at[c], f_recv.at[c], other_x, me_yz))
        first[-1].start()

    def rest(c, carry):
        out = columns(c)
        at = (c - early) * wide_cols
        g_rest[:, pl.ds(pl.multiple_of(at, wide_cols), wide_cols)] = out[:half]
        g_rest[:, pl.ds(pl.multiple_of(ff - early * wide_cols + at, wide_cols), wide_cols)] = out[half:2 * half]
        return carry

    lax.fori_loop(early, ff // wide_cols, rest, 0)
    rows_a = send_a_hbm.shape[0]
    save = [
        pltpu.make_async_copy(g_rest.at[pl.ds(0, rows_a)], send_a_hbm, out_sem.at[0]),
        pltpu.make_async_copy(g_rest.at[pl.ds(rows_a, half - rows_a)], send_b_hbm, out_sem.at[1]),
        pltpu.make_async_copy(g_own, own_hbm, out_sem.at[2]),
    ]
    for copy in save:
        copy.start()
    z_own[...] = project(1)
    z_copy.wait()
    zb[...] = (z_own[...] + z_recv[...]).astype(jnp.bfloat16)
    a_out = [remote(zb.at[lax.rem(me_yz + k, 4)], zg.at[me_yz], a_send.at[k], a_recv.at[k], me_x, lax.rem(me_yz + k, 4)) for k in (1, 2, 3)]
    for copy in a_out:
        copy.start()
    zg[me_yz] = zb[me_yz]
    for copy in a_out:
        copy.wait()
    save.append(pltpu.make_async_copy(zg, z_hbm, out_sem.at[3]))
    save[-1].start()
    for copy in first:
        copy.wait()
    for copy in save:
        copy.wait()


def head(x_in, ln_scale, w_gate_up, w_attn, d_model, early, rows_a):
    rows, chunk = x_in.shape
    depth, _, ff = w_gate_up.shape
    z_cols = w_attn.shape[1]
    owned = rows // 8
    half = rows // 2
    width = 2 * (ff - 256 * early)
    any_spec = pl.BlockSpec(memory_space=pl.ANY)
    dma = pltpu.SemaphoreType.DMA
    f32, bf16 = jnp.float32, jnp.bfloat16
    return pl.pallas_call(
        functools.partial(head_kernel, d_model, early),
        out_shape=(
            jax.ShapeDtypeStruct((4, owned, z_cols), bf16),
            jax.ShapeDtypeStruct((early, half, 512), f32),
            jax.ShapeDtypeStruct((rows_a, width), f32),
            jax.ShapeDtypeStruct((half - rows_a, width), f32),
            jax.ShapeDtypeStruct((half, 2 * ff), f32),
        ),
        in_specs=[any_spec] * 4,
        out_specs=[any_spec] * 5,
        scratch_shapes=[
            pltpu.VMEM((4, 2, half, chunk), bf16),
            pltpu.VMEM((chunk,), f32),
            pltpu.VMEM((4, 1, chunk), f32),
            pltpu.VMEM((8, 8, 128), f32),
            pltpu.VMEM((4, half, chunk), bf16),
            pltpu.VMEM((2 * rows, 2 * depth), bf16),
            pltpu.VMEM((half, depth), bf16),
            pltpu.VMEM((depth, 2, ff), bf16),
            pltpu.VMEM((z_cols, depth), bf16),
            pltpu.VMEM((4, owned, z_cols), f32),
            pltpu.VMEM((4, owned, z_cols), f32),
            pltpu.VMEM((4, owned, z_cols), f32),
            pltpu.VMEM((4, owned, z_cols), bf16),
            pltpu.VMEM((4, owned, z_cols), bf16),
            pltpu.VMEM((early, half, 512), f32),
            pltpu.VMEM((half, width), f32),
            pltpu.VMEM((half, 2 * ff), f32),
            dma((4,)), dma((8,)), dma((3, 2)), dma((3, 2)), dma((4,)), dma((4,)), dma((8,)), dma((8,)), dma((2,)), dma((4,)), dma((4,)),
            dma((early,)), dma((early,)), dma((4,)),
        ],
        compiler_params=pltpu.CompilerParams(collective_id=0, has_side_effects=True, vmem_limit_bytes=VMEM_MOST),
        cost_estimate=pl.CostEstimate(flops=4 * rows * depth * 2 * ff, bytes_accessed=4 * depth * ff, transcendentals=0),
        name='head',
    )(x_in, ln_scale, w_gate_up, w_attn.T)


def tail_kernel(
    g_first, g_peer, g_late, own_hbm, ov, wd_hbm, wo_hbm, y_ref,
    g_got, g_own, oa, of, hb, wd, wo, out_part, y_send, y_pair, y_over, y_recv, y_last,
    in_sem, own_sem, b_send, b_recv, o_send, o_recv, h_send, h_recv, p_send, p_recv, y_ssem, y_rsem, l_send, l_recv,
):
    me_x = lax.axis_index('x')
    me_yz = lax.axis_index('yz')
    groups, _, span, ff = hb.shape
    rows, chunk = y_ref.shape
    half = rows // 2
    owned = ov.shape[1]
    early, _, wide = g_first.shape
    wide = wide // 2
    groups_a = g_peer.shape[0] // span
    core = lax.rem(me_yz, 2)
    col = me_yz // 2
    partner = me_yz + 1 - 2 * core
    across = lax.rem(me_yz + 2, 4)
    other_x = lax.rem(me_x + 1, 2)

    def rows_of(i):
        return pl.ds(span * i, span)

    own_in = [pltpu.make_async_copy(own_hbm.at[rows_of(i)], g_own.at[rows_of(i)], own_sem.at[i]) for i in range(groups)]
    wo_in = pltpu.make_async_copy(wo_hbm, wo, in_sem.at[1])
    wd_in = pltpu.make_async_copy(wd_hbm, wd, in_sem.at[2])
    for copy in (*own_in, wo_in, wd_in):
        copy.start()
    start_barrier(me_x, me_yz)()
    me = me_x * 4 + me_yz

    def remote(src, dst, send, recv, to_x, to_yz):
        return pltpu.make_async_remote_copy(
            src_ref=src, dst_ref=dst, send_sem=send, recv_sem=recv, device_id=(to_x, to_yz), device_id_type=MESH,
        )

    b_out = [
        remote(g_late.at[rows_of(i)], g_got.at[rows_of(i)], b_send.at[i], b_recv.at[i], other_x, me_yz) for i in range(groups - groups_a)
    ]
    for copy in b_out:
        copy.start()
    o_out = []
    for dx in range(2):
        for k in range(4):
            if dx or k:
                there = lax.rem(me_yz + k, 4)
                o_out.append(remote(ov.at[there], oa.at[me], o_send.at[4 * dx + k], o_recv.at[4 * dx + k], lax.rem(me_x + dx, 2), there))
    for copy in o_out:
        copy.start()
    oa[me] = ov[me_yz]

    h_out = []

    def activate(i):
        own_in[i].wait()
        at = rows_of(i)
        if i < groups_a:
            got, got_at = g_peer, at
        else:
            b_out[i - groups_a].wait()
            got, got_at = g_got, rows_of(i - groups_a)

        def act(gate, up):
            gate = gate.astype(jnp.bfloat16).astype(jnp.float32)
            up = up.astype(jnp.bfloat16).astype(jnp.float32)
            return (jax.nn.silu(gate) * up).astype(jnp.bfloat16)

        for c in range(early):
            cols = slice(wide * c, wide * c + wide)
            up_cols = slice(ff + wide * c, ff + wide * c + wide)
            hb[i, me_x, :, cols] = act(g_own[at, cols] + g_first[c, at, :wide], g_own[at, up_cols] + g_first[c, at, wide:])
        done = early * wide
        hb[i, me_x, :, done:] = act(g_own[at, done:ff] + got[got_at, :ff - done], g_own[at, ff + done:] + got[got_at, ff - done:])
        copy = remote(hb.at[i, me_x], hb.at[i, me_x], h_send.at[i], h_recv.at[i], other_x, me_yz)
        copy.start()
        h_out.append(copy)

    for i in range(groups_a):
        activate(i)
    for copy in o_out:
        copy.wait()
    for e in range(8):
        of[owned * e:owned * e + owned] = oa[e].astype(jnp.float32)
    wo_in.wait()
    out_part[...] = jnp.dot(of[...].astype(jnp.bfloat16), wo[...], preferred_element_type=jnp.float32)
    for i in range(groups_a, groups):
        activate(i)
    wd_in.wait()

    pair, over, last = [], [], []

    def product(i):
        h_out[i].wait()
        part = jnp.dot(hb[i].reshape(2 * span, ff), wd[...], preferred_element_type=jnp.float32)
        part = part + jnp.concatenate([out_part[span * i:span * i + span], out_part[half + span * i:half + span * i + span]], axis=0)
        for j in range(4):
            moved = part if j == 0 else pltpu.roll(part, (4 - j) * chunk, 1)
            y_send[i, j] = moved[:, :chunk]
        if i < groups - 1:
            pair.append([
                remote(y_send.at[i, 2 * e + 1 - core], y_pair.at[i, e], p_send.at[i, e], p_recv.at[i, e], me_x, partner) for e in range(2)
            ])
            for copy in pair[i]:
                copy.start()
        else:
            for k in (2, 3, 1):
                there = lax.rem(me_yz + k, 4)
                last.append(remote(y_send.at[i, there], y_last.at[me_yz], l_send.at[k], l_recv.at[k], me_x, there))
                last[-1].start()

    def cross(i):
        for copy in pair[i]:
            copy.wait()
        y_over[i] = y_send[i, across] + y_pair[i, 1 - col]
        over.append(remote(y_over.at[i], y_recv.at[i], y_ssem.at[i], y_rsem.at[i], me_x, across))
        over[i].start()

    def finish(i):
        if i < groups - 1:
            over[i].wait()
            total = y_send[i, me_yz] + y_pair[i, col] + y_recv[i]
        else:
            for copy in last:
                copy.wait()
            total = y_send[i, me_yz]
            for k in (1, 2, 3):
                total = total + y_last[lax.rem(me_yz + k, 4)]
        for e in range(2):
            at = pl.ds(half * e + span * i, span)
            y_ref[at, :] = total[span * e:span * e + span]

    for i in range(groups):
        product(i)
        if i >= 1:
            cross(i - 1)
        if i >= 2:
            finish(i - 2)
    finish(groups - 2)
    finish(groups - 1)


def tail(g_first, g_peer, g_late, g_own, o_blocks, w_down, w_out):
    half = g_own.shape[0]
    rows = 2 * half
    span = 16
    groups = half // span
    ff, cols = w_down.shape
    chunk = cols // 4
    owned = o_blocks.shape[1]
    o_width = w_out.shape[0]
    any_spec, vmem_spec = pl.BlockSpec(memory_space=pl.ANY), pl.BlockSpec(memory_space=pltpu.VMEM)
    dma = pltpu.SemaphoreType.DMA
    f32, bf16 = jnp.float32, jnp.bfloat16
    late_groups = g_late.shape[0] // span
    return pl.pallas_call(
        tail_kernel,
        out_shape=jax.ShapeDtypeStruct((rows, chunk), f32),
        in_specs=[vmem_spec, vmem_spec, vmem_spec, any_spec, vmem_spec, any_spec, any_spec],
        out_specs=pl.BlockSpec(memory_space=pltpu.VMEM),
        scratch_shapes=[
            pltpu.VMEM(g_late.shape, f32),
            pltpu.VMEM((half, 2 * ff), f32),
            pltpu.VMEM((8, owned, o_width), bf16),
            pltpu.VMEM((rows, o_width), f32),
            pltpu.VMEM((groups, 2, span, ff), bf16),
            pltpu.VMEM((ff, cols), bf16),
            pltpu.VMEM((o_width, cols), bf16),
            pltpu.VMEM((rows, cols), f32),
            pltpu.VMEM((groups, 4, 2 * span, chunk), f32),
            pltpu.VMEM((groups, 2, 2 * span, chunk), f32),
            pltpu.VMEM((groups, 2 * span, chunk), f32),
            pltpu.VMEM((groups, 2 * span, chunk), f32),
            pltpu.VMEM((4, 2 * span, chunk), f32),
            dma((3,)), dma((groups,)), dma((late_groups,)), dma((late_groups,)), dma((8,)), dma((8,)), dma((groups,)), dma((groups,)),
            dma((groups, 2)), dma((groups, 2)), dma((groups,)), dma((groups,)), dma((4,)), dma((4,)),
        ],
        compiler_params=pltpu.CompilerParams(collective_id=1, has_side_effects=True, vmem_limit_bytes=51 * 1024 * 1024),
        cost_estimate=pl.CostEstimate(flops=2 * rows * (ff + o_width) * cols, bytes_accessed=2 * (ff + o_width) * cols, transcendentals=half * ff),
        name='tail',
    )(g_first, g_peer, g_late, g_own, o_blocks, w_down, w_out)


def rotary(values, positions):
    half_dim = values.shape[-1] // 2
    inv_freq = ROPE_BASE ** (-jnp.arange(half_dim, dtype=jnp.float32) / half_dim)
    angles = positions.astype(jnp.float32)[:, None, None] * inv_freq
    cos_part = jnp.cos(angles)
    sin_part = jnp.sin(angles)
    lo_half = values[..., :half_dim]
    hi_half = values[..., half_dim:]
    return jnp.concatenate([lo_half * cos_part - hi_half * sin_part, hi_half * cos_part + lo_half * sin_part], axis=-1)


def solution(mesh):
    x_size = mesh.shape['x']
    yz_size = mesh.shape['yz']
    all_axes = ('x', 'yz')

    def local_step(x_in, ln_scale, w_gate_up, w_attn, w_down, w_out, k_cache, v_cache, lengths, positions):
        local_rows, seq_len, head_dim = k_cache.shape
        q_width = w_out.shape[0] * yz_size
        num_heads = q_width // head_dim
        d_model = x_in.shape[1] * x_size * yz_size
        z_blocks, g_first, g_send, g_late, g_own = head(x_in, ln_scale, w_gate_up, w_attn, d_model, EARLY, ROWS_A)
        g_peer = lax.ppermute(g_send, 'x', [(0, 1), (1, 0)])
        proj_local = z_blocks.transpose(1, 0, 2).reshape(local_rows, -1)
        q_raw = proj_local[:, :q_width].reshape(local_rows, num_heads, head_dim)
        k_tok = proj_local[:, q_width:q_width + head_dim]
        v_tok = proj_local[:, q_width + head_dim:]
        q_rot = rotary(q_raw.astype(jnp.float32), positions).astype(jnp.bfloat16)
        k_rot = rotary(k_tok[:, None, :].astype(jnp.float32), positions)[:, 0].astype(jnp.bfloat16)
        cols = jnp.stack([k_rot, v_tok]).astype(jnp.float32).transpose(0, 2, 1)
        cols = jnp.pad(cols, ((0, 0), (0, 0), (0, 128 - local_rows)))
        attn_out, k_new, v_new = attend(q_rot, cols, k_cache, v_cache, lengths)
        o_blocks = attn_out.reshape(local_rows, yz_size, q_width // yz_size).transpose(1, 0, 2)
        mixed_sum = tail(g_first, g_peer, g_late, g_own, o_blocks, w_down, w_out)
        y_out = (x_in.astype(jnp.float32) + mixed_sum).astype(jnp.bfloat16)
        return y_out, k_new, v_new

    row_spec = P(None, all_axes)
    vec_spec = P(all_axes)
    cache_spec = P(all_axes, None, None)
    return jax.shard_map(
        local_step,
        mesh=mesh,
        in_specs=(row_spec, vec_spec, P('x', None, 'yz'), P('x', 'yz'), P('yz', 'x'), P('yz', 'x'), cache_spec, cache_spec, vec_spec, vec_spec),
        out_specs=(row_spec, cache_spec, cache_spec),
        check_vma=False,
    )
```

```python
import functools

import jax
import jax.numpy as jnp
from jax import lax
from jax.experimental import pallas as pl
from jax.experimental.pallas import tpu as pltpu
from jax.sharding import PartitionSpec as P

LN_EPS = 1e-6
ROPE_BASE = 10000.0
MESH = pl.DeviceIdType.MESH
VMEM_MOST = 64 * 1024 * 1024 - 64 * 1024
EARLY = 2
ROWS_A = 80


def attention_kernel(scale, len_ref, q_ref, cols_ref, k_hbm, v_hbm, o_ref, ko_hbm, vo_hbm, k_buf, v_buf, in_sem, out_sem):
    rows, _, seq_len = k_buf.shape

    def load(which, b):
        src, dst = ((k_hbm, k_buf), (v_hbm, v_buf))[which]
        return pltpu.make_async_copy(src.at[b], dst.at[b], in_sem.at[which, b])

    def save(which, b):
        src, dst = ((k_buf, ko_hbm), (v_buf, vo_hbm))[which]
        return pltpu.make_async_copy(src.at[b], dst.at[b], out_sem.at[which, b])

    for b in range(rows):
        load(0, b).start()
        load(1, b).start()

    lane = lax.broadcasted_iota(jnp.int32, (1, 128), 1)
    slots = lax.broadcasted_iota(jnp.int32, (1, seq_len), 1)

    def row(b, carry):
        length = len_ref[b]
        window = pl.ds(pl.multiple_of((length // 128) * 128, 128), 128)
        here = lane == length % 128
        for which, buf in enumerate((k_buf, v_buf)):
            load(which, b).wait()
            col = jnp.sum(jnp.where(lane == b, cols_ref[which], 0.0), axis=1, keepdims=True)
            tile = buf[b, :, window].astype(jnp.float32)
            buf[b, :, window] = jnp.where(here, col, tile).astype(jnp.bfloat16)
        scores = jnp.dot(q_ref[b], k_buf[b], preferred_element_type=jnp.float32) * scale
        scores = jnp.where(slots <= length, scores, -1e30)
        top = jnp.max(scores, axis=1, keepdims=True)
        weights = jnp.exp(scores - top)
        total = jnp.sum(weights, axis=1, keepdims=True)
        probs = (weights * (1.0 / total)).astype(jnp.bfloat16)
        save(0, b).start()
        save(1, b).start()
        o_ref[b] = lax.dot_general(probs, v_buf[b], (((1,), (1,)), ((), ())), preferred_element_type=jnp.float32).astype(jnp.bfloat16)
        return carry

    lax.fori_loop(0, rows, row, 0)
    for b in range(rows):
        save(0, b).wait()
        save(1, b).wait()


def attend(q_rot, cols, k_cache, v_cache, lengths):
    rows, heads, head_dim = q_rot.shape
    seq_len = k_cache.shape[1]
    k_t = jnp.swapaxes(k_cache, 1, 2)
    v_t = jnp.swapaxes(v_cache, 1, 2)
    cache = jax.ShapeDtypeStruct((rows, head_dim, seq_len), jnp.bfloat16)
    o, k_new, v_new = pl.pallas_call(
        functools.partial(attention_kernel, head_dim ** -0.5),
        out_shape=(jax.ShapeDtypeStruct((rows, heads, head_dim), jnp.bfloat16), cache, cache),
        in_specs=[
            pl.BlockSpec(memory_space=pltpu.SMEM),
            pl.BlockSpec(memory_space=pltpu.VMEM),
            pl.BlockSpec(memory_space=pltpu.VMEM),
            pl.BlockSpec(memory_space=pl.ANY),
            pl.BlockSpec(memory_space=pl.ANY),
        ],
        out_specs=(pl.BlockSpec(memory_space=pltpu.VMEM), pl.BlockSpec(memory_space=pl.ANY), pl.BlockSpec(memory_space=pl.ANY)),
        scratch_shapes=[
            pltpu.VMEM((rows, head_dim, seq_len), jnp.bfloat16),
            pltpu.VMEM((rows, head_dim, seq_len), jnp.bfloat16),
            pltpu.SemaphoreType.DMA((2, rows)),
            pltpu.SemaphoreType.DMA((2, rows)),
        ],
        compiler_params=pltpu.CompilerParams(vmem_limit_bytes=48 * 1024 * 1024),
        cost_estimate=pl.CostEstimate(
            flops=4 * rows * heads * head_dim * seq_len,
            bytes_accessed=8 * rows * head_dim * seq_len,
            transcendentals=rows * heads * seq_len,
        ),
        name='attend',
    )(lengths, q_rot, cols, k_t, v_t)
    return o, jnp.swapaxes(k_new, 1, 2), jnp.swapaxes(v_new, 1, 2)


def start_barrier(me_x, me_yz):
    barrier = pltpu.get_barrier_semaphore()
    for dx in range(2):
        for k in range(4):
            if dx or k:
                peer = (lax.rem(me_x + dx, 2), lax.rem(me_yz + k, 4))
                pl.semaphore_signal(barrier, inc=1, device_id=peer, device_id_type=MESH)
    return lambda: pl.semaphore_wait(barrier, 7)


def spread(rows, cols, first):
    i = lax.broadcasted_iota(jnp.int32, (rows, cols), 0)
    c = lax.broadcasted_iota(jnp.int32, (rows, cols), 1)
    return jnp.where(c == 2 * i + first, 1.0, 0.0).astype(jnp.bfloat16)


def head_kernel(
    d_model, early, x_hbm, scale_hbm, wg_hbm, wa_hbm, z_hbm, first_hbm, send_a_hbm, send_b_hbm, own_hbm,
    xg, scale_row, sg, stats, h_buf, hx, hc, wg, wa, z_send, z_own, z_recv, zb, zg, g_first, g_rest, g_own,
    in_sem, wg_sem, x_send, x_recv, s_send, s_recv, t_send, t_recv, z_sems, a_send, a_recv, f_send, f_recv, out_sem,
):
    me_x = lax.axis_index('x')
    me_yz = lax.axis_index('yz')
    half, chunk = xg.shape[2:]
    rows = 2 * half
    pieces = wg_sem.shape[0]
    depth = wg.shape[0] // pieces
    ff = wg.shape[2]
    wide_cols = 256
    other_x = lax.rem(me_x + 1, 2)
    across = lax.rem(me_yz + 2, 4)
    core = lax.rem(me_yz, 2)
    partner = me_yz + 1 - 2 * core
    order = (other_x, me_x)
    x_in = [
        pltpu.make_async_copy(x_hbm.at[pl.ds(pl.multiple_of(order[p] * half, 32), half)], xg.at[me_yz, order[p]], in_sem.at[p]) for p in range(2)
    ]
    scale_in = pltpu.make_async_copy(scale_hbm, scale_row, in_sem.at[2])
    wa_in = pltpu.make_async_copy(wa_hbm, wa, in_sem.at[3])
    wg_in = [
        pltpu.make_async_copy(wg_hbm.at[pl.ds(depth * i, depth)], wg.at[pl.ds(depth * i, depth)], wg_sem.at[i]) for i in range(pieces)
    ]
    for copy in (*x_in, scale_in, wa_in):
        copy.start()
    others_ready = start_barrier(me_x, me_yz)

    def remote(src, dst, send, recv, to_x, to_yz):
        return pltpu.make_async_remote_copy(
            src_ref=src, dst_ref=dst, send_sem=send, recv_sem=recv, device_id=(to_x, to_yz), device_id_type=MESH,
        )

    def x_copy(kind, p):
        owner = across if kind == 2 else me_yz
        at = xg.at[owner, order[p]]
        return remote(at, at, x_send.at[kind, p], x_recv.at[kind, p], me_x, across if kind == 1 else partner)

    for p in range(2):
        x_in[p].wait()
    lane = lax.broadcasted_iota(jnp.int32, (8, 128), 1)
    tile = jnp.zeros((8, 128), jnp.float32)
    for e in range(2):
        mine = xg[me_yz, e].astype(jnp.float32)
        sum_1 = jnp.sum(mine, axis=1, keepdims=True)
        sum_2 = jnp.sum(mine * mine, axis=1, keepdims=True)
        for j in range(half // 8):
            col = e * (half // 8) + j
            tile = jnp.where(lane == col, sum_1[8 * j:8 * j + 8], tile)
            tile = jnp.where(lane == 32 + col, sum_2[8 * j:8 * j + 8], tile)
    me = me_x * 4 + me_yz
    stats[me] = tile
    others_ready()
    t_out = [
        remote(stats.at[me], stats.at[me], t_send.at[4 * dx + k], t_recv.at[4 * dx + k], lax.rem(me_x + dx, 2), lax.rem(me_yz + k, 4))
        for dx in range(2) for k in range(4) if dx or k
    ]
    for copy in t_out:
        copy.start()
    scale_in.wait()
    sg[me_yz] = scale_row[...].reshape(1, chunk)
    s_out = [remote(sg.at[me_yz], sg.at[me_yz], s_send.at[k], s_recv.at[k], me_x, lax.rem(me_yz + k, 4)) for k in (1, 2, 3)]
    for copy in s_out:
        copy.start()
    for p in range(2):
        x_copy(1, p).start()
        x_copy(0, p).start()
    for copy in wg_in:
        copy.start()
    wide, thin = spread(128, 256, 0), spread(64, 128, 0)
    wide_u, thin_u = spread(128, 256, 1), spread(64, 128, 1)
    i = lax.broadcasted_iota(jnp.int32, (256, 128), 0)
    c = lax.broadcasted_iota(jnp.int32, (256, 128), 1)
    gather = jnp.where(i == 2 * c, 1.0, 0.0).astype(jnp.bfloat16)
    for copy in t_out:
        copy.wait()
    total = stats[0]
    for i in range(1, 8):
        total = total + stats[i]
    mean_t = total / d_model
    var_t = pltpu.roll(total, 96, 1) / d_model - mean_t * mean_t
    rstd_t = lax.rsqrt(var_t + LN_EPS)
    for copy in s_out:
        copy.wait()

    def normalize(p):
        shift = lax.rem(128 - order[p] * (half // 8), 128)
        mean_p = pltpu.roll(mean_t, shift, 1)
        rstd_p = pltpu.roll(rstd_t, shift, 1)
        mean = jnp.concatenate([mean_p[:, j:j + 1] for j in range(half // 8)], axis=0)
        rstd = jnp.concatenate([rstd_p[:, j:j + 1] for j in range(half // 8)], axis=0)
        x_copy(1, p).wait()
        x_copy(2, p).start()
        x_copy(0, p).wait()
        x_copy(2, p).wait()
        for s in range(4):
            h_buf[s] = ((xg[s, order[p]].astype(jnp.float32) - mean) * rstd * sg[s]).astype(jnp.bfloat16)

    def spread_half(part, g):
        out = pl.ds((2 * part + g) * half, half)
        a, b = ((wide, thin), (wide_u, thin_u))[g]
        for s in range(4):
            base = 2 * chunk * s
            for t in range(2):
                piece = h_buf[s, :, 128 * t:128 * t + 128]
                hx[out, base + 256 * t:base + 256 * t + 256] = jnp.dot(piece, a, preferred_element_type=jnp.float32).astype(jnp.bfloat16)
            piece = h_buf[s, :, 256:320]
            hx[out, base + 512:base + 640] = jnp.dot(piece, b, preferred_element_type=jnp.float32).astype(jnp.bfloat16)

    def project(part):
        src = pl.ds(2 * part * half, half)
        for t in range(4 * chunk // 128):
            hc[:, 128 * t:128 * t + 128] = jnp.dot(hx[src, 256 * t:256 * t + 256], gather, preferred_element_type=jnp.float32).astype(jnp.bfloat16)
        z = lax.dot_general(hc[...], wa[...], (((1,), (1,)), ((), ())), preferred_element_type=jnp.float32)
        return z.reshape(z_send.shape)

    normalize(0)
    spread_half(0, 0)
    wa_in.wait()
    z_send[...] = project(0)
    z_copy = remote(z_send, z_recv, z_sems.at[0], z_sems.at[1], other_x, me_yz)
    z_copy.start()
    spread_half(0, 1)
    normalize(1)
    spread_half(1, 0)
    spread_half(1, 1)
    for copy in wg_in:
        copy.wait()

    def columns(c):
        at = pl.ds(pl.multiple_of(c * wide_cols, wide_cols), wide_cols)
        block = wg[:, :, at].reshape(2 * wg.shape[0], wide_cols)
        out = jnp.dot(hx[...], block, preferred_element_type=jnp.float32)
        up = pl.ds(pl.multiple_of(ff + c * wide_cols, wide_cols), wide_cols)
        g_own[:, at] = out[2 * half:3 * half]
        g_own[:, up] = out[3 * half:]
        return out

    first = []
    for c in range(early):
        out = columns(c)
        g_first[c, :, :wide_cols] = out[:half]
        g_first[c, :, wide_cols:] = out[half:2 * half]
        first.append(remote(g_first.at[c], first_hbm.at[c], f_send.at[c], f_recv.at[c], other_x, me_yz))
        first[-1].start()

    def rest(c, carry):
        out = columns(c)
        at = (c - early) * wide_cols
        g_rest[:, pl.ds(pl.multiple_of(at, wide_cols), wide_cols)] = out[:half]
        g_rest[:, pl.ds(pl.multiple_of(ff - early * wide_cols + at, wide_cols), wide_cols)] = out[half:2 * half]
        return carry

    lax.fori_loop(early, ff // wide_cols, rest, 0)
    rows_a = send_a_hbm.shape[0]
    save = [
        pltpu.make_async_copy(g_rest.at[pl.ds(0, rows_a)], send_a_hbm, out_sem.at[0]),
        pltpu.make_async_copy(g_rest.at[pl.ds(rows_a, half - rows_a)], send_b_hbm, out_sem.at[1]),
        pltpu.make_async_copy(g_own, own_hbm, out_sem.at[2]),
    ]
    for copy in save:
        copy.start()
    z_own[...] = project(1)
    z_copy.wait()
    zb[...] = (z_own[...] + z_recv[...]).astype(jnp.bfloat16)
    a_out = [remote(zb.at[lax.rem(me_yz + k, 4)], zg.at[me_yz], a_send.at[k], a_recv.at[k], me_x, lax.rem(me_yz + k, 4)) for k in (1, 2, 3)]
    for copy in a_out:
        copy.start()
    zg[me_yz] = zb[me_yz]
    for copy in a_out:
        copy.wait()
    save.append(pltpu.make_async_copy(zg, z_hbm, out_sem.at[3]))
    save[-1].start()
    for copy in first:
        copy.wait()
    for copy in save:
        copy.wait()


def head(x_in, ln_scale, w_gate_up, w_attn, d_model, early, rows_a):
    rows, chunk = x_in.shape
    depth, _, ff = w_gate_up.shape
    z_cols = w_attn.shape[1]
    owned = rows // 8
    half = rows // 2
    width = 2 * (ff - 256 * early)
    any_spec = pl.BlockSpec(memory_space=pl.ANY)
    dma = pltpu.SemaphoreType.DMA
    f32, bf16 = jnp.float32, jnp.bfloat16
    return pl.pallas_call(
        functools.partial(head_kernel, d_model, early),
        out_shape=(
            jax.ShapeDtypeStruct((4, owned, z_cols), bf16),
            jax.ShapeDtypeStruct((early, half, 512), f32),
            jax.ShapeDtypeStruct((rows_a, width), f32),
            jax.ShapeDtypeStruct((half - rows_a, width), f32),
            jax.ShapeDtypeStruct((half, 2 * ff), f32),
        ),
        in_specs=[any_spec] * 4,
        out_specs=[any_spec] * 5,
        scratch_shapes=[
            pltpu.VMEM((4, 2, half, chunk), bf16),
            pltpu.VMEM((chunk,), f32),
            pltpu.VMEM((4, 1, chunk), f32),
            pltpu.VMEM((8, 8, 128), f32),
            pltpu.VMEM((4, half, chunk), bf16),
            pltpu.VMEM((2 * rows, 2 * depth), bf16),
            pltpu.VMEM((half, depth), bf16),
            pltpu.VMEM((depth, 2, ff), bf16),
            pltpu.VMEM((z_cols, depth), bf16),
            pltpu.VMEM((4, owned, z_cols), f32),
            pltpu.VMEM((4, owned, z_cols), f32),
            pltpu.VMEM((4, owned, z_cols), f32),
            pltpu.VMEM((4, owned, z_cols), bf16),
            pltpu.VMEM((4, owned, z_cols), bf16),
            pltpu.VMEM((early, half, 512), f32),
            pltpu.VMEM((half, width), f32),
            pltpu.VMEM((half, 2 * ff), f32),
            dma((4,)), dma((8,)), dma((3, 2)), dma((3, 2)), dma((4,)), dma((4,)), dma((8,)), dma((8,)), dma((2,)), dma((4,)), dma((4,)),
            dma((early,)), dma((early,)), dma((4,)),
        ],
        compiler_params=pltpu.CompilerParams(collective_id=0, has_side_effects=True, vmem_limit_bytes=VMEM_MOST),
        cost_estimate=pl.CostEstimate(flops=4 * rows * depth * 2 * ff, bytes_accessed=4 * depth * ff, transcendentals=0),
        name='head',
    )(x_in, ln_scale, w_gate_up, w_attn.T)


def tail_kernel(
    g_first, g_peer, g_late, own_hbm, ov, wd_hbm, wo_hbm, y_ref,
    g_got, g_own, oa, of, hb, wd, wo, out_part, y_send, y_pair, y_over, y_recv,
    in_sem, own_sem, b_send, b_recv, o_send, o_recv, h_send, h_recv, p_send, p_recv, y_ssem, y_rsem,
):
    me_x = lax.axis_index('x')
    me_yz = lax.axis_index('yz')
    groups, _, span, ff = hb.shape
    rows, chunk = y_ref.shape
    half = rows // 2
    owned = ov.shape[1]
    early, _, wide = g_first.shape
    wide = wide // 2
    groups_a = g_peer.shape[0] // span
    core = lax.rem(me_yz, 2)
    col = me_yz // 2
    partner = me_yz + 1 - 2 * core
    across = lax.rem(me_yz + 2, 4)
    other_x = lax.rem(me_x + 1, 2)

    def rows_of(i):
        return pl.ds(span * i, span)

    own_in = [pltpu.make_async_copy(own_hbm.at[rows_of(i)], g_own.at[rows_of(i)], own_sem.at[i]) for i in range(groups)]
    wo_in = pltpu.make_async_copy(wo_hbm, wo, in_sem.at[1])
    wd_in = pltpu.make_async_copy(wd_hbm, wd, in_sem.at[2])
    for copy in (*own_in, wo_in, wd_in):
        copy.start()
    start_barrier(me_x, me_yz)()
    me = me_x * 4 + me_yz

    def remote(src, dst, send, recv, to_x, to_yz):
        return pltpu.make_async_remote_copy(
            src_ref=src, dst_ref=dst, send_sem=send, recv_sem=recv, device_id=(to_x, to_yz), device_id_type=MESH,
        )

    b_out = [
        remote(g_late.at[rows_of(i)], g_got.at[rows_of(i)], b_send.at[i], b_recv.at[i], other_x, me_yz) for i in range(groups - groups_a)
    ]
    for copy in b_out:
        copy.start()
    o_out = []
    for dx in range(2):
        for k in range(4):
            if dx or k:
                there = lax.rem(me_yz + k, 4)
                o_out.append(remote(ov.at[there], oa.at[me], o_send.at[4 * dx + k], o_recv.at[4 * dx + k], lax.rem(me_x + dx, 2), there))
    for copy in o_out:
        copy.start()
    oa[me] = ov[me_yz]

    h_out = []

    def activate(i):
        own_in[i].wait()
        at = rows_of(i)
        if i < groups_a:
            got, got_at = g_peer, at
        else:
            b_out[i - groups_a].wait()
            got, got_at = g_got, rows_of(i - groups_a)

        def act(gate, up):
            gate = gate.astype(jnp.bfloat16).astype(jnp.float32)
            up = up.astype(jnp.bfloat16).astype(jnp.float32)
            return (jax.nn.silu(gate) * up).astype(jnp.bfloat16)

        for c in range(early):
            cols = slice(wide * c, wide * c + wide)
            up_cols = slice(ff + wide * c, ff + wide * c + wide)
            hb[i, me_x, :, cols] = act(g_own[at, cols] + g_first[c, at, :wide], g_own[at, up_cols] + g_first[c, at, wide:])
        done = early * wide
        hb[i, me_x, :, done:] = act(g_own[at, done:ff] + got[got_at, :ff - done], g_own[at, ff + done:] + got[got_at, ff - done:])
        copy = remote(hb.at[i, me_x], hb.at[i, me_x], h_send.at[i], h_recv.at[i], other_x, me_yz)
        copy.start()
        h_out.append(copy)

    for i in range(groups_a):
        activate(i)
    for copy in o_out:
        copy.wait()
    for e in range(8):
        of[owned * e:owned * e + owned] = oa[e].astype(jnp.float32)
    wo_in.wait()
    out_part[...] = jnp.dot(of[...].astype(jnp.bfloat16), wo[...], preferred_element_type=jnp.float32)
    for i in range(groups_a, groups):
        activate(i)
    wd_in.wait()

    pair, over = [], []

    def product(i):
        h_out[i].wait()
        part = jnp.dot(hb[i].reshape(2 * span, ff), wd[...], preferred_element_type=jnp.float32)
        part = part + jnp.concatenate([out_part[span * i:span * i + span], out_part[half + span * i:half + span * i + span]], axis=0)
        for j in range(4):
            moved = part if j == 0 else pltpu.roll(part, (4 - j) * chunk, 1)
            y_send[i, j] = moved[:, :chunk]
        pair.append([
            remote(y_send.at[i, 2 * e + 1 - core], y_pair.at[i, e], p_send.at[i, e], p_recv.at[i, e], me_x, partner) for e in range(2)
        ])
        for copy in pair[i]:
            copy.start()

    def cross(i):
        for copy in pair[i]:
            copy.wait()
        y_over[i] = y_send[i, across] + y_pair[i, 1 - col]
        over.append(remote(y_over.at[i], y_recv.at[i], y_ssem.at[i], y_rsem.at[i], me_x, across))
        over[i].start()

    def finish(i):
        over[i].wait()
        total = y_send[i, me_yz] + y_pair[i, col] + y_recv[i]
        for e in range(2):
            at = pl.ds(half * e + span * i, span)
            y_ref[at, :] = total[span * e:span * e + span]

    for i in range(groups):
        product(i)
        if i >= 1:
            cross(i - 1)
    for i in range(groups - 3):
        finish(i)
    cross(groups - 1)
    for i in range(groups - 3, groups):
        finish(i)


def tail(g_first, g_peer, g_late, g_own, o_blocks, w_down, w_out):
    half = g_own.shape[0]
    rows = 2 * half
    span = 16
    groups = half // span
    ff, cols = w_down.shape
    chunk = cols // 4
    owned = o_blocks.shape[1]
    o_width = w_out.shape[0]
    any_spec, vmem_spec = pl.BlockSpec(memory_space=pl.ANY), pl.BlockSpec(memory_space=pltpu.VMEM)
    dma = pltpu.SemaphoreType.DMA
    f32, bf16 = jnp.float32, jnp.bfloat16
    late_groups = g_late.shape[0] // span
    return pl.pallas_call(
        tail_kernel,
        out_shape=jax.ShapeDtypeStruct((rows, chunk), f32),
        in_specs=[vmem_spec, vmem_spec, vmem_spec, any_spec, vmem_spec, any_spec, any_spec],
        out_specs=pl.BlockSpec(memory_space=pltpu.VMEM),
        scratch_shapes=[
            pltpu.VMEM(g_late.shape, f32),
            pltpu.VMEM((half, 2 * ff), f32),
            pltpu.VMEM((8, owned, o_width), bf16),
            pltpu.VMEM((rows, o_width), f32),
            pltpu.VMEM((groups, 2, span, ff), bf16),
            pltpu.VMEM((ff, cols), bf16),
            pltpu.VMEM((o_width, cols), bf16),
            pltpu.VMEM((rows, cols), f32),
            pltpu.VMEM((groups, 4, 2 * span, chunk), f32),
            pltpu.VMEM((groups, 2, 2 * span, chunk), f32),
            pltpu.VMEM((groups, 2 * span, chunk), f32),
            pltpu.VMEM((groups, 2 * span, chunk), f32),
            dma((3,)), dma((groups,)), dma((late_groups,)), dma((late_groups,)), dma((8,)), dma((8,)), dma((groups,)), dma((groups,)),
            dma((groups, 2)), dma((groups, 2)), dma((groups,)), dma((groups,)),
        ],
        compiler_params=pltpu.CompilerParams(collective_id=1, has_side_effects=True, vmem_limit_bytes=51 * 1024 * 1024),
        cost_estimate=pl.CostEstimate(flops=2 * rows * (ff + o_width) * cols, bytes_accessed=2 * (ff + o_width) * cols, transcendentals=half * ff),
        name='tail',
    )(g_first, g_peer, g_late, g_own, o_blocks, w_down, w_out)


def rotary(values, positions):
    half_dim = values.shape[-1] // 2
    inv_freq = ROPE_BASE ** (-jnp.arange(half_dim, dtype=jnp.float32) / half_dim)
    angles = positions.astype(jnp.float32)[:, None, None] * inv_freq
    cos_part = jnp.cos(angles)
    sin_part = jnp.sin(angles)
    lo_half = values[..., :half_dim]
    hi_half = values[..., half_dim:]
    return jnp.concatenate([lo_half * cos_part - hi_half * sin_part, hi_half * cos_part + lo_half * sin_part], axis=-1)


def solution(mesh):
    x_size = mesh.shape['x']
    yz_size = mesh.shape['yz']
    all_axes = ('x', 'yz')

    def local_step(x_in, ln_scale, w_gate_up, w_attn, w_down, w_out, k_cache, v_cache, lengths, positions):
        local_rows, seq_len, head_dim = k_cache.shape
        q_width = w_out.shape[0] * yz_size
        num_heads = q_width // head_dim
        d_model = x_in.shape[1] * x_size * yz_size
        z_blocks, g_first, g_send, g_late, g_own = head(x_in, ln_scale, w_gate_up, w_attn, d_model, EARLY, ROWS_A)
        g_peer = lax.ppermute(g_send, 'x', [(0, 1), (1, 0)])
        proj_local = z_blocks.transpose(1, 0, 2).reshape(local_rows, -1)
        q_raw = proj_local[:, :q_width].reshape(local_rows, num_heads, head_dim)
        k_tok = proj_local[:, q_width:q_width + head_dim]
        v_tok = proj_local[:, q_width + head_dim:]
        q_rot = rotary(q_raw.astype(jnp.float32), positions).astype(jnp.bfloat16)
        k_rot = rotary(k_tok[:, None, :].astype(jnp.float32), positions)[:, 0].astype(jnp.bfloat16)
        cols = jnp.stack([k_rot, v_tok]).astype(jnp.float32).transpose(0, 2, 1)
        cols = jnp.pad(cols, ((0, 0), (0, 0), (0, 128 - local_rows)))
        attn_out, k_new, v_new = attend(q_rot, cols, k_cache, v_cache, lengths)
        o_blocks = attn_out.reshape(local_rows, yz_size, q_width // yz_size).transpose(1, 0, 2)
        mixed_sum = tail(g_first, g_peer, g_late, g_own, o_blocks, w_down, w_out)
        y_out = (x_in.astype(jnp.float32) + mixed_sum).astype(jnp.bfloat16)
        return y_out, k_new, v_new

    row_spec = P(None, all_axes)
    vec_spec = P(all_axes)
    cache_spec = P(all_axes, None, None)
    return jax.shard_map(
        local_step,
        mesh=mesh,
        in_specs=(row_spec, vec_spec, P('x', None, 'yz'), P('x', 'yz'), P('yz', 'x'), P('yz', 'x'), cache_spec, cache_spec, vec_spec, vec_spec),
        out_specs=(row_spec, cache_spec, cache_spec),
        check_vma=False,
    )
```

```python
import functools

import jax
import jax.numpy as jnp
from jax import lax
from jax.experimental import pallas as pl
from jax.experimental.pallas import tpu as pltpu
from jax.sharding import PartitionSpec as P

LN_EPS = 1e-6
ROPE_BASE = 10000.0
MESH = pl.DeviceIdType.MESH
VMEM_MOST = 64 * 1024 * 1024 - 64 * 1024
EARLY = 2


def attention_kernel(scale, len_ref, q_ref, cols_ref, k_hbm, v_hbm, o_ref, ko_hbm, vo_hbm, k_buf, v_buf, in_sem, out_sem):
    rows, _, seq_len = k_buf.shape

    def load(which, b):
        src, dst = ((k_hbm, k_buf), (v_hbm, v_buf))[which]
        return pltpu.make_async_copy(src.at[b], dst.at[b], in_sem.at[which, b])

    def save(which, b):
        src, dst = ((k_buf, ko_hbm), (v_buf, vo_hbm))[which]
        return pltpu.make_async_copy(src.at[b], dst.at[b], out_sem.at[which, b])

    for b in range(rows):
        load(0, b).start()
        load(1, b).start()

    lane = lax.broadcasted_iota(jnp.int32, (1, 128), 1)
    slots = lax.broadcasted_iota(jnp.int32, (1, seq_len), 1)

    def row(b, carry):
        length = len_ref[b]
        window = pl.ds(pl.multiple_of((length // 128) * 128, 128), 128)
        here = lane == length % 128
        for which, buf in enumerate((k_buf, v_buf)):
            load(which, b).wait()
            col = jnp.sum(jnp.where(lane == b, cols_ref[which], 0.0), axis=1, keepdims=True)
            tile = buf[b, :, window].astype(jnp.float32)
            buf[b, :, window] = jnp.where(here, col, tile).astype(jnp.bfloat16)
        scores = jnp.dot(q_ref[b], k_buf[b], preferred_element_type=jnp.float32) * scale
        scores = jnp.where(slots <= length, scores, -1e30)
        top = jnp.max(scores, axis=1, keepdims=True)
        weights = jnp.exp(scores - top)
        total = jnp.sum(weights, axis=1, keepdims=True)
        probs = (weights * (1.0 / total)).astype(jnp.bfloat16)
        save(0, b).start()
        save(1, b).start()
        o_ref[b] = lax.dot_general(probs, v_buf[b], (((1,), (1,)), ((), ())), preferred_element_type=jnp.float32).astype(jnp.bfloat16)
        return carry

    lax.fori_loop(0, rows, row, 0)
    for b in range(rows):
        save(0, b).wait()
        save(1, b).wait()


def attend(q_rot, cols, k_cache, v_cache, lengths):
    rows, heads, head_dim = q_rot.shape
    seq_len = k_cache.shape[1]
    k_t = jnp.swapaxes(k_cache, 1, 2)
    v_t = jnp.swapaxes(v_cache, 1, 2)
    cache = jax.ShapeDtypeStruct((rows, head_dim, seq_len), jnp.bfloat16)
    o, k_new, v_new = pl.pallas_call(
        functools.partial(attention_kernel, head_dim ** -0.5),
        out_shape=(jax.ShapeDtypeStruct((rows, heads, head_dim), jnp.bfloat16), cache, cache),
        in_specs=[
            pl.BlockSpec(memory_space=pltpu.SMEM),
            pl.BlockSpec(memory_space=pltpu.VMEM),
            pl.BlockSpec(memory_space=pltpu.VMEM),
            pl.BlockSpec(memory_space=pl.ANY),
            pl.BlockSpec(memory_space=pl.ANY),
        ],
        out_specs=(pl.BlockSpec(memory_space=pltpu.VMEM), pl.BlockSpec(memory_space=pl.ANY), pl.BlockSpec(memory_space=pl.ANY)),
        scratch_shapes=[
            pltpu.VMEM((rows, head_dim, seq_len), jnp.bfloat16),
            pltpu.VMEM((rows, head_dim, seq_len), jnp.bfloat16),
            pltpu.SemaphoreType.DMA((2, rows)),
            pltpu.SemaphoreType.DMA((2, rows)),
        ],
        compiler_params=pltpu.CompilerParams(vmem_limit_bytes=48 * 1024 * 1024),
        cost_estimate=pl.CostEstimate(
            flops=4 * rows * heads * head_dim * seq_len,
            bytes_accessed=8 * rows * head_dim * seq_len,
            transcendentals=rows * heads * seq_len,
        ),
        name='attend',
    )(lengths, q_rot, cols, k_t, v_t)
    return o, jnp.swapaxes(k_new, 1, 2), jnp.swapaxes(v_new, 1, 2)


def start_barrier(me_x, me_yz):
    barrier = pltpu.get_barrier_semaphore()
    for dx in range(2):
        for k in range(4):
            if dx or k:
                peer = (lax.rem(me_x + dx, 2), lax.rem(me_yz + k, 4))
                pl.semaphore_signal(barrier, inc=1, device_id=peer, device_id_type=MESH)
    return lambda: pl.semaphore_wait(barrier, 7)


def spread(rows, cols, first):
    i = lax.broadcasted_iota(jnp.int32, (rows, cols), 0)
    c = lax.broadcasted_iota(jnp.int32, (rows, cols), 1)
    return jnp.where(c == 2 * i + first, 1.0, 0.0).astype(jnp.bfloat16)


def head_kernel(
    d_model, early, x_hbm, scale_hbm, wg_hbm, wa_hbm, z_hbm, first_hbm, send_hbm, own_hbm,
    xg, scale_row, sg, stats, h_buf, hx, hc, wg, wa, z_send, z_own, z_recv, r_send, r_own, r_recv, zb, zg, g_first, g_rest, g_own,
    in_sem, wg_sem, x_send, x_recv, s_send, s_recv, t_send, t_recv, z_sems, a_send, a_recv, f_send, f_recv, out_sem,
):
    me_x = lax.axis_index('x')
    me_yz = lax.axis_index('yz')
    half, chunk = xg.shape[2:]
    rows = 2 * half
    pieces = wg_sem.shape[0]
    depth = wg.shape[0] // pieces
    ff = wg.shape[2]
    wide_cols = 256
    full = z_send.shape[2]
    third = half // 3
    tail_cols = wa.shape[0] - full
    other_x = lax.rem(me_x + 1, 2)
    across = lax.rem(me_yz + 2, 4)
    core = lax.rem(me_yz, 2)
    partner = me_yz + 1 - 2 * core
    order = (other_x, me_x)
    x_in = [
        pltpu.make_async_copy(x_hbm.at[pl.ds(pl.multiple_of(order[p] * half, 32), half)], xg.at[me_yz, order[p]], in_sem.at[p]) for p in range(2)
    ]
    scale_in = pltpu.make_async_copy(scale_hbm, scale_row, in_sem.at[2])
    wa_in = pltpu.make_async_copy(wa_hbm, wa, in_sem.at[3])
    wg_in = [
        pltpu.make_async_copy(wg_hbm.at[pl.ds(depth * i, depth)], wg.at[pl.ds(depth * i, depth)], wg_sem.at[i]) for i in range(pieces)
    ]
    for copy in (*x_in, scale_in, wa_in):
        copy.start()
    others_ready = start_barrier(me_x, me_yz)

    def remote(src, dst, send, recv, to_x, to_yz):
        return pltpu.make_async_remote_copy(
            src_ref=src, dst_ref=dst, send_sem=send, recv_sem=recv, device_id=(to_x, to_yz), device_id_type=MESH,
        )

    def x_copy(kind, p):
        owner = across if kind == 2 else me_yz
        at = xg.at[owner, order[p]]
        return remote(at, at, x_send.at[kind, p], x_recv.at[kind, p], me_x, across if kind == 1 else partner)

    for p in range(2):
        x_in[p].wait()
    lane = lax.broadcasted_iota(jnp.int32, (8, 128), 1)
    tile = jnp.zeros((8, 128), jnp.float32)
    for e in range(2):
        mine = xg[me_yz, e].astype(jnp.float32)
        sum_1 = jnp.sum(mine, axis=1, keepdims=True)
        sum_2 = jnp.sum(mine * mine, axis=1, keepdims=True)
        for j in range(half // 8):
            col = e * (half // 8) + j
            tile = jnp.where(lane == col, sum_1[8 * j:8 * j + 8], tile)
            tile = jnp.where(lane == 32 + col, sum_2[8 * j:8 * j + 8], tile)
    me = me_x * 4 + me_yz
    stats[me] = tile
    others_ready()
    t_out = [
        remote(stats.at[me], stats.at[me], t_send.at[4 * dx + k], t_recv.at[4 * dx + k], lax.rem(me_x + dx, 2), lax.rem(me_yz + k, 4))
        for dx in range(2) for k in range(4) if dx or k
    ]
    for copy in t_out:
        copy.start()
    scale_in.wait()
    sg[me_yz] = scale_row[...].reshape(1, chunk)
    s_out = [remote(sg.at[me_yz], sg.at[me_yz], s_send.at[k], s_recv.at[k], me_x, lax.rem(me_yz + k, 4)) for k in (1, 2, 3)]
    for copy in s_out:
        copy.start()
    for p in range(2):
        x_copy(1, p).start()
        x_copy(0, p).start()
    for copy in wg_in:
        copy.start()
    wide, thin = spread(128, 256, 0), spread(64, 128, 0)
    wide_u, thin_u = spread(128, 256, 1), spread(64, 128, 1)
    i = lax.broadcasted_iota(jnp.int32, (256, 128), 0)
    c = lax.broadcasted_iota(jnp.int32, (256, 128), 1)
    gather = jnp.where(i == 2 * c, 1.0, 0.0).astype(jnp.bfloat16)
    for copy in t_out:
        copy.wait()
    total = stats[0]
    for i in range(1, 8):
        total = total + stats[i]
    mean_t = total / d_model
    var_t = pltpu.roll(total, 96, 1) / d_model - mean_t * mean_t
    rstd_t = lax.rsqrt(var_t + LN_EPS)
    for copy in s_out:
        copy.wait()

    def normalize(p):
        shift = lax.rem(128 - order[p] * (half // 8), 128)
        mean_p = pltpu.roll(mean_t, shift, 1)
        rstd_p = pltpu.roll(rstd_t, shift, 1)
        mean = jnp.concatenate([mean_p[:, j:j + 1] for j in range(half // 8)], axis=0)
        rstd = jnp.concatenate([rstd_p[:, j:j + 1] for j in range(half // 8)], axis=0)
        x_copy(1, p).wait()
        x_copy(2, p).start()
        x_copy(0, p).wait()
        x_copy(2, p).wait()
        for s in range(4):
            h_buf[s] = ((xg[s, order[p]].astype(jnp.float32) - mean) * rstd * sg[s]).astype(jnp.bfloat16)

    def spread_half(part, g):
        out = pl.ds((2 * part + g) * half, half)
        a, b = ((wide, thin), (wide_u, thin_u))[g]
        for s in range(4):
            base = 2 * chunk * s
            for t in range(2):
                piece = h_buf[s, :, 128 * t:128 * t + 128]
                hx[out, base + 256 * t:base + 256 * t + 256] = jnp.dot(piece, a, preferred_element_type=jnp.float32).astype(jnp.bfloat16)
            piece = h_buf[s, :, 256:320]
            hx[out, base + 512:base + 640] = jnp.dot(piece, b, preferred_element_type=jnp.float32).astype(jnp.bfloat16)

    def project(part):
        src = pl.ds(2 * part * half, half)
        for t in range(4 * chunk // 128):
            hc[:, 128 * t:128 * t + 128] = jnp.dot(hx[src, 256 * t:256 * t + 256], gather, preferred_element_type=jnp.float32).astype(jnp.bfloat16)
        contract = (((1,), (1,)), ((), ()))
        z = lax.dot_general(hc[...], wa[:full, :], contract, preferred_element_type=jnp.float32)
        r = lax.dot_general(hc[...], wa[full:, :], contract, preferred_element_type=jnp.float32)
        r = jnp.concatenate([r[third * i:third * i + third] for i in range(3)], axis=1)
        return z.reshape(z_send.shape), r

    normalize(0)
    spread_half(0, 0)
    wa_in.wait()
    z_send[...], r_send[...] = project(0)
    z_out = [remote(z_send, z_recv, z_sems.at[0], z_sems.at[1], other_x, me_yz), remote(r_send, r_recv, z_sems.at[2], z_sems.at[3], other_x, me_yz)]
    for copy in z_out:
        copy.start()
    spread_half(0, 1)
    normalize(1)
    spread_half(1, 0)
    spread_half(1, 1)
    for copy in wg_in:
        copy.wait()

    def columns(c):
        at = pl.ds(pl.multiple_of(c * wide_cols, wide_cols), wide_cols)
        block = wg[:, :, at].reshape(2 * wg.shape[0], wide_cols)
        out = jnp.dot(hx[...], block, preferred_element_type=jnp.float32)
        up = pl.ds(pl.multiple_of(ff + c * wide_cols, wide_cols), wide_cols)
        g_own[:, at] = out[2 * half:3 * half]
        g_own[:, up] = out[3 * half:]
        return out

    first = []
    for c in range(early):
        out = columns(c)
        g_first[c, :, :wide_cols] = out[:half]
        g_first[c, :, wide_cols:] = out[half:2 * half]
        first.append(remote(g_first.at[c], first_hbm.at[c], f_send.at[c], f_recv.at[c], other_x, me_yz))
        first[-1].start()

    def rest(c, carry):
        out = columns(c)
        at = (c - early) * wide_cols
        g_rest[:, pl.ds(pl.multiple_of(at, wide_cols), wide_cols)] = out[:half]
        g_rest[:, pl.ds(pl.multiple_of(ff - early * wide_cols + at, wide_cols), wide_cols)] = out[half:2 * half]
        return carry

    lax.fori_loop(early, ff // wide_cols, rest, 0)
    save = [pltpu.make_async_copy(g_rest, send_hbm, out_sem.at[0]), pltpu.make_async_copy(g_own, own_hbm, out_sem.at[1])]
    for copy in save:
        copy.start()
    z_own[...], r_own[...] = project(1)
    for copy in z_out:
        copy.wait()
    zb[:, :, :full] = (z_own[...] + z_recv[...]).astype(jnp.bfloat16)
    r = r_own[...] + r_recv[...]
    r = jnp.concatenate([r[:, tail_cols * i:tail_cols * i + tail_cols] for i in range(3)], axis=0)
    zb[:, :, full:] = r.reshape(zb.shape[0], zb.shape[1], tail_cols).astype(jnp.bfloat16)
    a_out = [remote(zb.at[lax.rem(me_yz + k, 4)], zg.at[me_yz], a_send.at[k], a_recv.at[k], me_x, lax.rem(me_yz + k, 4)) for k in (1, 2, 3)]
    for copy in a_out:
        copy.start()
    zg[me_yz] = zb[me_yz]
    for copy in a_out:
        copy.wait()
    save.append(pltpu.make_async_copy(zg, z_hbm, out_sem.at[2]))
    save[-1].start()
    for copy in first:
        copy.wait()
    for copy in save:
        copy.wait()


def head(x_in, ln_scale, w_gate_up, w_attn, d_model, early):
    rows, chunk = x_in.shape
    depth, _, ff = w_gate_up.shape
    z_cols = w_attn.shape[1]
    full = z_cols // 128 * 128
    owned = rows // 8
    half = rows // 2
    width = 2 * (ff - 256 * early)
    any_spec = pl.BlockSpec(memory_space=pl.ANY)
    dma = pltpu.SemaphoreType.DMA
    f32, bf16 = jnp.float32, jnp.bfloat16
    return pl.pallas_call(
        functools.partial(head_kernel, d_model, early),
        out_shape=(
            jax.ShapeDtypeStruct((4, owned, z_cols), bf16),
            jax.ShapeDtypeStruct((early, half, 512), f32),
            jax.ShapeDtypeStruct((half, width), f32),
            jax.ShapeDtypeStruct((half, 2 * ff), f32),
        ),
        in_specs=[any_spec] * 4,
        out_specs=[any_spec] * 4,
        scratch_shapes=[
            pltpu.VMEM((4, 2, half, chunk), bf16),
            pltpu.VMEM((chunk,), f32),
            pltpu.VMEM((4, 1, chunk), f32),
            pltpu.VMEM((8, 8, 128), f32),
            pltpu.VMEM((4, half, chunk), bf16),
            pltpu.VMEM((2 * rows, 2 * depth), bf16),
            pltpu.VMEM((half, depth), bf16),
            pltpu.VMEM((depth, 2, ff), bf16),
            pltpu.VMEM((z_cols, depth), bf16),
            *[pltpu.VMEM((4, owned, full), f32)] * 3,
            *[pltpu.VMEM((half // 3, 3 * (z_cols - full)), f32)] * 3,
            pltpu.VMEM((4, owned, z_cols), bf16),
            pltpu.VMEM((4, owned, z_cols), bf16),
            pltpu.VMEM((early, half, 512), f32),
            pltpu.VMEM((half, width), f32),
            pltpu.VMEM((half, 2 * ff), f32),
            dma((4,)), dma((8,)), dma((3, 2)), dma((3, 2)), dma((4,)), dma((4,)), dma((8,)), dma((8,)), dma((4,)), dma((4,)), dma((4,)),
            dma((early,)), dma((early,)), dma((3,)),
        ],
        compiler_params=pltpu.CompilerParams(collective_id=0, has_side_effects=True, vmem_limit_bytes=VMEM_MOST),
        cost_estimate=pl.CostEstimate(flops=4 * rows * depth * 2 * ff, bytes_accessed=4 * depth * ff, transcendentals=0),
        name='head',
    )(x_in, ln_scale, w_gate_up, w_attn.T)


def tail_kernel(
    g_first, g_peer, own_hbm, ov, wd_hbm, wo_hbm, y_ref,
    g_own, oa, of, hb, wd, wo, out_part, y_send, y_pair, y_over, y_recv,
    in_sem, own_sem, o_send, o_recv, h_send, h_recv, p_send, p_recv, y_ssem, y_rsem,
):
    me_x = lax.axis_index('x')
    me_yz = lax.axis_index('yz')
    groups, _, span, ff = hb.shape
    rows, chunk = y_ref.shape
    half = rows // 2
    owned = ov.shape[1]
    early, _, wide = g_first.shape
    wide = wide // 2
    core = lax.rem(me_yz, 2)
    col = me_yz // 2
    partner = me_yz + 1 - 2 * core
    across = lax.rem(me_yz + 2, 4)
    other_x = lax.rem(me_x + 1, 2)

    def rows_of(i):
        return pl.ds(span * i, span)

    own_in = [pltpu.make_async_copy(own_hbm.at[rows_of(i)], g_own.at[rows_of(i)], own_sem.at[i]) for i in range(groups)]
    wo_in = pltpu.make_async_copy(wo_hbm, wo, in_sem.at[1])
    wd_in = pltpu.make_async_copy(wd_hbm, wd, in_sem.at[2])
    for copy in (*own_in, wo_in, wd_in):
        copy.start()
    start_barrier(me_x, me_yz)()
    me = me_x * 4 + me_yz

    def remote(src, dst, send, recv, to_x, to_yz):
        return pltpu.make_async_remote_copy(
            src_ref=src, dst_ref=dst, send_sem=send, recv_sem=recv, device_id=(to_x, to_yz), device_id_type=MESH,
        )

    o_out = []
    for dx in range(2):
        for k in range(4):
            if dx or k:
                there = lax.rem(me_yz + k, 4)
                o_out.append(remote(ov.at[there], oa.at[me], o_send.at[4 * dx + k], o_recv.at[4 * dx + k], lax.rem(me_x + dx, 2), there))
    for copy in o_out:
        copy.start()
    oa[me] = ov[me_yz]

    h_out = []

    def activate(i):
        own_in[i].wait()
        at = rows_of(i)
        def act(gate, up):
            gate = gate.astype(jnp.bfloat16).astype(jnp.float32)
            up = up.astype(jnp.bfloat16).astype(jnp.float32)
            return (jax.nn.silu(gate) * up).astype(jnp.bfloat16)

        for c in range(early):
            cols = slice(wide * c, wide * c + wide)
            up_cols = slice(ff + wide * c, ff + wide * c + wide)
            hb[i, me_x, :, cols] = act(g_own[at, cols] + g_first[c, at, :wide], g_own[at, up_cols] + g_first[c, at, wide:])
        done = early * wide
        hb[i, me_x, :, done:] = act(g_own[at, done:ff] + g_peer[at, :ff - done], g_own[at, ff + done:] + g_peer[at, ff - done:])
        copy = remote(hb.at[i, me_x], hb.at[i, me_x], h_send.at[i], h_recv.at[i], other_x, me_yz)
        copy.start()
        h_out.append(copy)

    for i in range(groups):
        activate(i)
    for copy in o_out:
        copy.wait()
    for e in range(8):
        of[owned * e:owned * e + owned] = oa[e].astype(jnp.float32)
    wo_in.wait()
    out_part[...] = jnp.dot(of[...].astype(jnp.bfloat16), wo[...], preferred_element_type=jnp.float32)
    wd_in.wait()

    pair, over = [], []

    def product(i):
        h_out[i].wait()
        part = jnp.dot(hb[i].reshape(2 * span, ff), wd[...], preferred_element_type=jnp.float32)
        part = part + jnp.concatenate([out_part[span * i:span * i + span], out_part[half + span * i:half + span * i + span]], axis=0)
        for j in range(4):
            moved = part if j == 0 else pltpu.roll(part, (4 - j) * chunk, 1)
            y_send[i, j] = moved[:, :chunk]
        pair.append([
            remote(y_send.at[i, 2 * e + 1 - core], y_pair.at[i, e], p_send.at[i, e], p_recv.at[i, e], me_x, partner) for e in range(2)
        ])
        for copy in pair[i]:
            copy.start()

    def cross(i):
        for copy in pair[i]:
            copy.wait()
        y_over[i] = y_send[i, across] + y_pair[i, 1 - col]
        over.append(remote(y_over.at[i], y_recv.at[i], y_ssem.at[i], y_rsem.at[i], me_x, across))
        over[i].start()

    def finish(i):
        over[i].wait()
        total = y_send[i, me_yz] + y_pair[i, col] + y_recv[i]
        for e in range(2):
            at = pl.ds(half * e + span * i, span)
            y_ref[at, :] = total[span * e:span * e + span]

    for i in range(groups):
        product(i)
        if i >= 1:
            cross(i - 1)
    for i in range(groups - 3):
        finish(i)
    cross(groups - 1)
    for i in range(groups - 3, groups):
        finish(i)


def tail(g_first, g_peer, g_own, o_blocks, w_down, w_out):
    half = g_own.shape[0]
    rows = 2 * half
    span = 16
    groups = half // span
    ff, cols = w_down.shape
    chunk = cols // 4
    owned = o_blocks.shape[1]
    o_width = w_out.shape[0]
    any_spec, vmem_spec = pl.BlockSpec(memory_space=pl.ANY), pl.BlockSpec(memory_space=pltpu.VMEM)
    dma = pltpu.SemaphoreType.DMA
    f32, bf16 = jnp.float32, jnp.bfloat16
    return pl.pallas_call(
        tail_kernel,
        out_shape=jax.ShapeDtypeStruct((rows, chunk), f32),
        in_specs=[vmem_spec, vmem_spec, any_spec, vmem_spec, any_spec, any_spec],
        out_specs=pl.BlockSpec(memory_space=pltpu.VMEM),
        scratch_shapes=[
            pltpu.VMEM((half, 2 * ff), f32),
            pltpu.VMEM((8, owned, o_width), bf16),
            pltpu.VMEM((rows, o_width), f32),
            pltpu.VMEM((groups, 2, span, ff), bf16),
            pltpu.VMEM((ff, cols), bf16),
            pltpu.VMEM((o_width, cols), bf16),
            pltpu.VMEM((rows, cols), f32),
            pltpu.VMEM((groups, 4, 2 * span, chunk), f32),
            pltpu.VMEM((groups, 2, 2 * span, chunk), f32),
            pltpu.VMEM((groups, 2 * span, chunk), f32),
            pltpu.VMEM((groups, 2 * span, chunk), f32),
            dma((3,)), dma((groups,)), dma((8,)), dma((8,)), dma((groups,)), dma((groups,)),
            dma((groups, 2)), dma((groups, 2)), dma((groups,)), dma((groups,)),
        ],
        compiler_params=pltpu.CompilerParams(collective_id=1, has_side_effects=True, vmem_limit_bytes=51 * 1024 * 1024),
        cost_estimate=pl.CostEstimate(flops=2 * rows * (ff + o_width) * cols, bytes_accessed=2 * (ff + o_width) * cols, transcendentals=half * ff),
        name='tail',
    )(g_first, g_peer, g_own, o_blocks, w_down, w_out)


def rotary(values, positions):
    half_dim = values.shape[-1] // 2
    inv_freq = ROPE_BASE ** (-jnp.arange(half_dim, dtype=jnp.float32) / half_dim)
    angles = positions.astype(jnp.float32)[:, None, None] * inv_freq
    cos_part = jnp.cos(angles)
    sin_part = jnp.sin(angles)
    lo_half = values[..., :half_dim]
    hi_half = values[..., half_dim:]
    return jnp.concatenate([lo_half * cos_part - hi_half * sin_part, hi_half * cos_part + lo_half * sin_part], axis=-1)


def solution(mesh):
    x_size = mesh.shape['x']
    yz_size = mesh.shape['yz']
    all_axes = ('x', 'yz')

    def local_step(x_in, ln_scale, w_gate_up, w_attn, w_down, w_out, k_cache, v_cache, lengths, positions):
        local_rows, seq_len, head_dim = k_cache.shape
        q_width = w_out.shape[0] * yz_size
        num_heads = q_width // head_dim
        d_model = x_in.shape[1] * x_size * yz_size
        z_blocks, g_first, g_send, g_own = head(x_in, ln_scale, w_gate_up, w_attn, d_model, EARLY)
        g_peer = lax.ppermute(g_send, 'x', [(0, 1), (1, 0)])
        proj_local = z_blocks.transpose(1, 0, 2).reshape(local_rows, -1)
        q_raw = proj_local[:, :q_width].reshape(local_rows, num_heads, head_dim)
        k_tok = proj_local[:, q_width:q_width + head_dim]
        v_tok = proj_local[:, q_width + head_dim:]
        q_rot = rotary(q_raw.astype(jnp.float32), positions).astype(jnp.bfloat16)
        k_rot = rotary(k_tok[:, None, :].astype(jnp.float32), positions)[:, 0].astype(jnp.bfloat16)
        cols = jnp.stack([k_rot, v_tok]).astype(jnp.float32).transpose(0, 2, 1)
        cols = jnp.pad(cols, ((0, 0), (0, 0), (0, 128 - local_rows)))
        attn_out, k_new, v_new = attend(q_rot, cols, k_cache, v_cache, lengths)
        o_blocks = attn_out.reshape(local_rows, yz_size, q_width // yz_size).transpose(1, 0, 2)
        mixed_sum = tail(g_first, g_peer, g_own, o_blocks, w_down, w_out)
        y_out = (x_in.astype(jnp.float32) + mixed_sum).astype(jnp.bfloat16)
        return y_out, k_new, v_new

    row_spec = P(None, all_axes)
    vec_spec = P(all_axes)
    cache_spec = P(all_axes, None, None)
    return jax.shard_map(
        local_step,
        mesh=mesh,
        in_specs=(row_spec, vec_spec, P('x', None, 'yz'), P('x', 'yz'), P('yz', 'x'), P('yz', 'x'), cache_spec, cache_spec, vec_spec, vec_spec),
        out_specs=(row_spec, cache_spec, cache_spec),
        check_vma=False,
    )
```

```python
import functools

import jax
import jax.numpy as jnp
from jax import lax
from jax.experimental import pallas as pl
from jax.experimental.pallas import tpu as pltpu
from jax.sharding import PartitionSpec as P

LN_EPS = 1e-6
ROPE_BASE = 10000.0
MESH = pl.DeviceIdType.MESH
VMEM_MOST = 64 * 1024 * 1024 - 64 * 1024
EARLY = 2


def attention_kernel(scale, len_ref, q_ref, cols_ref, k_hbm, v_hbm, o_ref, ko_hbm, vo_hbm, k_buf, v_buf, in_sem, out_sem):
    rows, _, seq_len = k_buf.shape

    def load(which, b):
        src, dst = ((k_hbm, k_buf), (v_hbm, v_buf))[which]
        return pltpu.make_async_copy(src.at[b], dst.at[b], in_sem.at[which, b])

    def save(which, b):
        src, dst = ((k_buf, ko_hbm), (v_buf, vo_hbm))[which]
        return pltpu.make_async_copy(src.at[b], dst.at[b], out_sem.at[which, b])

    for b in range(rows):
        load(0, b).start()
        load(1, b).start()

    lane = lax.broadcasted_iota(jnp.int32, (1, 128), 1)
    slots = lax.broadcasted_iota(jnp.int32, (1, seq_len), 1)

    def row(b, carry):
        length = len_ref[b]
        window = pl.ds(pl.multiple_of((length // 128) * 128, 128), 128)
        here = lane == length % 128
        for which, buf in enumerate((k_buf, v_buf)):
            load(which, b).wait()
            col = jnp.sum(jnp.where(lane == b, cols_ref[which], 0.0), axis=1, keepdims=True)
            tile = buf[b, :, window].astype(jnp.float32)
            buf[b, :, window] = jnp.where(here, col, tile).astype(jnp.bfloat16)
        scores = jnp.dot(q_ref[b], k_buf[b], preferred_element_type=jnp.float32) * scale
        scores = jnp.where(slots <= length, scores, -1e30)
        top = jnp.max(scores, axis=1, keepdims=True)
        weights = jnp.exp(scores - top)
        total = jnp.sum(weights, axis=1, keepdims=True)
        probs = (weights * (1.0 / total)).astype(jnp.bfloat16)
        save(0, b).start()
        save(1, b).start()
        o_ref[b] = lax.dot_general(probs, v_buf[b], (((1,), (1,)), ((), ())), preferred_element_type=jnp.float32).astype(jnp.bfloat16)
        return carry

    lax.fori_loop(0, rows, row, 0)
    for b in range(rows):
        save(0, b).wait()
        save(1, b).wait()


def attend(q_rot, cols, k_cache, v_cache, lengths):
    rows, heads, head_dim = q_rot.shape
    seq_len = k_cache.shape[1]
    k_t = jnp.swapaxes(k_cache, 1, 2)
    v_t = jnp.swapaxes(v_cache, 1, 2)
    cache = jax.ShapeDtypeStruct((rows, head_dim, seq_len), jnp.bfloat16)
    o, k_new, v_new = pl.pallas_call(
        functools.partial(attention_kernel, head_dim ** -0.5),
        out_shape=(jax.ShapeDtypeStruct((rows, heads, head_dim), jnp.bfloat16), cache, cache),
        in_specs=[
            pl.BlockSpec(memory_space=pltpu.SMEM),
            pl.BlockSpec(memory_space=pltpu.VMEM),
            pl.BlockSpec(memory_space=pltpu.VMEM),
            pl.BlockSpec(memory_space=pl.ANY),
            pl.BlockSpec(memory_space=pl.ANY),
        ],
        out_specs=(pl.BlockSpec(memory_space=pltpu.VMEM), pl.BlockSpec(memory_space=pl.ANY), pl.BlockSpec(memory_space=pl.ANY)),
        scratch_shapes=[
            pltpu.VMEM((rows, head_dim, seq_len), jnp.bfloat16),
            pltpu.VMEM((rows, head_dim, seq_len), jnp.bfloat16),
            pltpu.SemaphoreType.DMA((2, rows)),
            pltpu.SemaphoreType.DMA((2, rows)),
        ],
        compiler_params=pltpu.CompilerParams(vmem_limit_bytes=48 * 1024 * 1024),
        cost_estimate=pl.CostEstimate(
            flops=4 * rows * heads * head_dim * seq_len,
            bytes_accessed=8 * rows * head_dim * seq_len,
            transcendentals=rows * heads * seq_len,
        ),
        name='attend',
    )(lengths, q_rot, cols, k_t, v_t)
    return o, jnp.swapaxes(k_new, 1, 2), jnp.swapaxes(v_new, 1, 2)


def start_barrier(me_x, me_yz):
    barrier = pltpu.get_barrier_semaphore()
    peers = [(lax.rem(me_x + 1, 2), me_yz)] + [(me_x, lax.rem(me_yz + k, 4)) for k in (1, 2, 3)]
    for peer in peers:
        pl.semaphore_signal(barrier, inc=1, device_id=peer, device_id_type=MESH)
    return lambda: pl.semaphore_wait(barrier, len(peers))


def spread(rows, cols, first):
    i = lax.broadcasted_iota(jnp.int32, (rows, cols), 0)
    c = lax.broadcasted_iota(jnp.int32, (rows, cols), 1)
    return jnp.where(c == 2 * i + first, 1.0, 0.0).astype(jnp.bfloat16)


def head_kernel(
    d_model, early, x_hbm, scale_hbm, wg_hbm, wa_hbm, z_hbm, first_hbm, send_hbm, own_hbm,
    xg, scale_row, sg, stats, h_buf, hx, hc, wg, wa, z_send, z_own, z_recv, r_send, r_own, r_recv, zb, zg, g_first, g_rest, g_own,
    in_sem, wg_sem, x_send, x_recv, s_send, s_recv, t_send, t_recv, z_sems, a_send, a_recv, f_send, f_recv, out_sem,
):
    me_x = lax.axis_index('x')
    me_yz = lax.axis_index('yz')
    half, chunk = xg.shape[2:]
    rows = 2 * half
    pieces = wg_sem.shape[0]
    depth = wg.shape[0] // pieces
    ff = wg.shape[2]
    wide_cols = 256
    full = z_send.shape[2]
    third = half // 3
    tail_cols = wa.shape[0] - full
    other_x = lax.rem(me_x + 1, 2)
    across = lax.rem(me_yz + 2, 4)
    core = lax.rem(me_yz, 2)
    partner = me_yz + 1 - 2 * core
    order = (other_x, me_x)
    x_in = [
        pltpu.make_async_copy(x_hbm.at[pl.ds(pl.multiple_of(order[p] * half, 32), half)], xg.at[me_yz, order[p]], in_sem.at[p]) for p in range(2)
    ]
    scale_in = pltpu.make_async_copy(scale_hbm, scale_row, in_sem.at[2])
    wa_in = pltpu.make_async_copy(wa_hbm, wa, in_sem.at[3])
    wg_in = [
        pltpu.make_async_copy(wg_hbm.at[pl.ds(depth * i, depth)], wg.at[pl.ds(depth * i, depth)], wg_sem.at[i]) for i in range(pieces)
    ]
    for copy in (*x_in, scale_in, wa_in):
        copy.start()
    others_ready = start_barrier(me_x, me_yz)

    def remote(src, dst, send, recv, to_x, to_yz):
        return pltpu.make_async_remote_copy(
            src_ref=src, dst_ref=dst, send_sem=send, recv_sem=recv, device_id=(to_x, to_yz), device_id_type=MESH,
        )

    def x_copy(kind, p):
        owner = across if kind == 2 else me_yz
        at = xg.at[owner, order[p]]
        return remote(at, at, x_send.at[kind, p], x_recv.at[kind, p], me_x, across if kind == 1 else partner)

    for p in range(2):
        x_in[p].wait()
    lane = lax.broadcasted_iota(jnp.int32, (8, 128), 1)
    tile = jnp.zeros((8, 128), jnp.float32)
    for e in range(2):
        mine = xg[me_yz, e].astype(jnp.float32)
        sum_1 = jnp.sum(mine, axis=1, keepdims=True)
        sum_2 = jnp.sum(mine * mine, axis=1, keepdims=True)
        for j in range(half // 8):
            col = e * (half // 8) + j
            tile = jnp.where(lane == col, sum_1[8 * j:8 * j + 8], tile)
            tile = jnp.where(lane == 32 + col, sum_2[8 * j:8 * j + 8], tile)
    stats[me_yz] = tile
    others_ready()
    t_out = [remote(stats.at[me_yz], stats.at[me_yz], t_send.at[k], t_recv.at[k], me_x, lax.rem(me_yz + k, 4)) for k in (1, 2, 3)]
    for copy in t_out:
        copy.start()
    scale_in.wait()
    sg[me_yz] = scale_row[...].reshape(1, chunk)
    s_out = [remote(sg.at[me_yz], sg.at[me_yz], s_send.at[k], s_recv.at[k], me_x, lax.rem(me_yz + k, 4)) for k in (1, 2, 3)]
    for copy in s_out:
        copy.start()
    for p in range(2):
        x_copy(1, p).start()
        x_copy(0, p).start()
    for copy in wg_in:
        copy.start()
    wide, thin = spread(128, 256, 0), spread(64, 128, 0)
    wide_u, thin_u = spread(128, 256, 1), spread(64, 128, 1)
    i = lax.broadcasted_iota(jnp.int32, (256, 128), 0)
    c = lax.broadcasted_iota(jnp.int32, (256, 128), 1)
    gather = jnp.where(i == 2 * c, 1.0, 0.0).astype(jnp.bfloat16)
    for copy in t_out:
        copy.wait()
    stats[4] = stats[0] + stats[1] + stats[2] + stats[3]
    t_over = remote(stats.at[4], stats.at[5], t_send.at[0], t_recv.at[0], other_x, me_yz)
    t_over.start()
    t_over.wait()
    total = stats[4] + stats[5]
    mean_t = total / d_model
    var_t = pltpu.roll(total, 96, 1) / d_model - mean_t * mean_t
    rstd_t = lax.rsqrt(var_t + LN_EPS)
    for copy in s_out:
        copy.wait()

    def normalize(p):
        shift = lax.rem(128 - order[p] * (half // 8), 128)
        mean_p = pltpu.roll(mean_t, shift, 1)
        rstd_p = pltpu.roll(rstd_t, shift, 1)
        mean = jnp.concatenate([mean_p[:, j:j + 1] for j in range(half // 8)], axis=0)
        rstd = jnp.concatenate([rstd_p[:, j:j + 1] for j in range(half // 8)], axis=0)
        x_copy(1, p).wait()
        x_copy(2, p).start()
        x_copy(0, p).wait()
        x_copy(2, p).wait()
        for s in range(4):
            h_buf[s] = ((xg[s, order[p]].astype(jnp.float32) - mean) * rstd * sg[s]).astype(jnp.bfloat16)

    def spread_half(part, g):
        out = pl.ds((2 * part + g) * half, half)
        a, b = ((wide, thin), (wide_u, thin_u))[g]
        for s in range(4):
            base = 2 * chunk * s
            for t in range(2):
                piece = h_buf[s, :, 128 * t:128 * t + 128]
                hx[out, base + 256 * t:base + 256 * t + 256] = jnp.dot(piece, a, preferred_element_type=jnp.float32).astype(jnp.bfloat16)
            piece = h_buf[s, :, 256:320]
            hx[out, base + 512:base + 640] = jnp.dot(piece, b, preferred_element_type=jnp.float32).astype(jnp.bfloat16)

    def project(part):
        src = pl.ds(2 * part * half, half)
        for t in range(4 * chunk // 128):
            hc[:, 128 * t:128 * t + 128] = jnp.dot(hx[src, 256 * t:256 * t + 256], gather, preferred_element_type=jnp.float32).astype(jnp.bfloat16)
        contract = (((1,), (1,)), ((), ()))
        z = lax.dot_general(hc[...], wa[:full, :], contract, preferred_element_type=jnp.float32)
        r = lax.dot_general(hc[...], wa[full:, :], contract, preferred_element_type=jnp.float32)
        r = jnp.concatenate([r[third * i:third * i + third] for i in range(3)], axis=1)
        return z.reshape(z_send.shape), r

    normalize(0)
    spread_half(0, 0)
    wa_in.wait()
    z_send[...], r_send[...] = project(0)
    z_out = [remote(z_send, z_recv, z_sems.at[0], z_sems.at[1], other_x, me_yz), remote(r_send, r_recv, z_sems.at[2], z_sems.at[3], other_x, me_yz)]
    for copy in z_out:
        copy.start()
    spread_half(0, 1)
    normalize(1)
    spread_half(1, 0)
    spread_half(1, 1)
    for copy in wg_in:
        copy.wait()

    def columns(c):
        at = pl.ds(pl.multiple_of(c * wide_cols, wide_cols), wide_cols)
        block = wg[:, :, at].reshape(2 * wg.shape[0], wide_cols)
        out = jnp.dot(hx[...], block, preferred_element_type=jnp.float32)
        up = pl.ds(pl.multiple_of(ff + c * wide_cols, wide_cols), wide_cols)
        g_own[:, at] = out[2 * half:3 * half]
        g_own[:, up] = out[3 * half:]
        return out

    first = []
    for c in range(early):
        out = columns(c)
        g_first[c, :, :wide_cols] = out[:half]
        g_first[c, :, wide_cols:] = out[half:2 * half]
        first.append(remote(g_first.at[c], first_hbm.at[c], f_send.at[c], f_recv.at[c], other_x, me_yz))
        first[-1].start()

    def rest(c, carry):
        out = columns(c)
        at = (c - early) * wide_cols
        g_rest[:, pl.ds(pl.multiple_of(at, wide_cols), wide_cols)] = out[:half]
        g_rest[:, pl.ds(pl.multiple_of(ff - early * wide_cols + at, wide_cols), wide_cols)] = out[half:2 * half]
        return carry

    lax.fori_loop(early, ff // wide_cols, rest, 0)
    save = [pltpu.make_async_copy(g_rest, send_hbm, out_sem.at[0]), pltpu.make_async_copy(g_own, own_hbm, out_sem.at[1])]
    for copy in save:
        copy.start()
    z_own[...], r_own[...] = project(1)
    for copy in z_out:
        copy.wait()
    zb[:, :, :full] = (z_own[...] + z_recv[...]).astype(jnp.bfloat16)
    r = r_own[...] + r_recv[...]
    r = jnp.concatenate([r[:, tail_cols * i:tail_cols * i + tail_cols] for i in range(3)], axis=0)
    zb[:, :, full:] = r.reshape(zb.shape[0], zb.shape[1], tail_cols).astype(jnp.bfloat16)
    a_out = [remote(zb.at[lax.rem(me_yz + k, 4)], zg.at[me_yz], a_send.at[k], a_recv.at[k], me_x, lax.rem(me_yz + k, 4)) for k in (1, 2, 3)]
    for copy in a_out:
        copy.start()
    zg[me_yz] = zb[me_yz]
    for copy in a_out:
        copy.wait()
    save.append(pltpu.make_async_copy(zg, z_hbm, out_sem.at[2]))
    save[-1].start()
    for copy in first:
        copy.wait()
    for copy in save:
        copy.wait()


def head(x_in, ln_scale, w_gate_up, w_attn, d_model, early):
    rows, chunk = x_in.shape
    depth, _, ff = w_gate_up.shape
    z_cols = w_attn.shape[1]
    full = z_cols // 128 * 128
    owned = rows // 8
    half = rows // 2
    width = 2 * (ff - 256 * early)
    any_spec = pl.BlockSpec(memory_space=pl.ANY)
    dma = pltpu.SemaphoreType.DMA
    f32, bf16 = jnp.float32, jnp.bfloat16
    return pl.pallas_call(
        functools.partial(head_kernel, d_model, early),
        out_shape=(
            jax.ShapeDtypeStruct((4, owned, z_cols), bf16),
            jax.ShapeDtypeStruct((early, half, 512), f32),
            jax.ShapeDtypeStruct((half, width), f32),
            jax.ShapeDtypeStruct((half, 2 * ff), f32),
        ),
        in_specs=[any_spec] * 4,
        out_specs=[any_spec] * 4,
        scratch_shapes=[
            pltpu.VMEM((4, 2, half, chunk), bf16),
            pltpu.VMEM((chunk,), f32),
            pltpu.VMEM((4, 1, chunk), f32),
            pltpu.VMEM((6, 8, 128), f32),
            pltpu.VMEM((4, half, chunk), bf16),
            pltpu.VMEM((2 * rows, 2 * depth), bf16),
            pltpu.VMEM((half, depth), bf16),
            pltpu.VMEM((depth, 2, ff), bf16),
            pltpu.VMEM((z_cols, depth), bf16),
            *[pltpu.VMEM((4, owned, full), f32)] * 3,
            *[pltpu.VMEM((half // 3, 3 * (z_cols - full)), f32)] * 3,
            pltpu.VMEM((4, owned, z_cols), bf16),
            pltpu.VMEM((4, owned, z_cols), bf16),
            pltpu.VMEM((early, half, 512), f32),
            pltpu.VMEM((half, width), f32),
            pltpu.VMEM((half, 2 * ff), f32),
            dma((4,)), dma((8,)), dma((3, 2)), dma((3, 2)), dma((4,)), dma((4,)), dma((4,)), dma((4,)), dma((4,)), dma((4,)), dma((4,)),
            dma((early,)), dma((early,)), dma((3,)),
        ],
        compiler_params=pltpu.CompilerParams(collective_id=0, has_side_effects=True, vmem_limit_bytes=VMEM_MOST),
        cost_estimate=pl.CostEstimate(flops=4 * rows * depth * 2 * ff, bytes_accessed=4 * depth * ff, transcendentals=0),
        name='head',
    )(x_in, ln_scale, w_gate_up, w_attn.T)


def tail_kernel(
    g_first, g_peer, own_hbm, ov, wd_hbm, wo_hbm, y_ref,
    g_own, oy, oa, of, hb, wd, wo, out_part, y_send, y_pair, y_over, y_recv,
    in_sem, own_sem, o_send, o_recv, h_send, h_recv, p_send, p_recv, y_ssem, y_rsem,
):
    me_x = lax.axis_index('x')
    me_yz = lax.axis_index('yz')
    groups, _, span, ff = hb.shape
    rows, chunk = y_ref.shape
    half = rows // 2
    owned = ov.shape[1]
    early, _, wide = g_first.shape
    wide = wide // 2
    core = lax.rem(me_yz, 2)
    col = me_yz // 2
    partner = me_yz + 1 - 2 * core
    across = lax.rem(me_yz + 2, 4)
    other_x = lax.rem(me_x + 1, 2)

    own_in = [pltpu.make_async_copy(own_hbm.at[pl.ds(span * i, span)], g_own.at[pl.ds(span * i, span)], own_sem.at[i]) for i in range(groups)]
    wo_in = pltpu.make_async_copy(wo_hbm, wo, in_sem.at[1])
    wd_in = pltpu.make_async_copy(wd_hbm, wd, in_sem.at[2])
    for copy in (*own_in, wo_in, wd_in):
        copy.start()
    start_barrier(me_x, me_yz)()
    me = me_x * 4 + me_yz

    def remote(src, dst, send, recv, to_x, to_yz):
        return pltpu.make_async_remote_copy(
            src_ref=src, dst_ref=dst, send_sem=send, recv_sem=recv, device_id=(to_x, to_yz), device_id_type=MESH,
        )

    other = other_x * 4 + me_yz
    o_over = remote(ov, oy, o_send.at[0], o_recv.at[0], other_x, me_yz)
    o_over.start()
    there = [lax.rem(me_yz + k, 4) for k in range(4)]
    o_out = [remote(ov.at[there[k]], oa.at[me], o_send.at[k], o_recv.at[k], me_x, there[k]) for k in (1, 2, 3)]
    for copy in o_out:
        copy.start()
    oa[me] = ov[me_yz]

    def h_copy(i):
        return remote(hb.at[i, me_x], hb.at[i, me_x], h_send.at[i], h_recv.at[i], other_x, me_yz)

    for copy in own_in:
        copy.wait()

    def activate(i, carry):
        at = pl.ds(pl.multiple_of(span * i, span), span)

        def act(gate, up):
            gate = gate.astype(jnp.bfloat16).astype(jnp.float32)
            up = up.astype(jnp.bfloat16).astype(jnp.float32)
            return (jax.nn.silu(gate) * up).astype(jnp.bfloat16)

        for c in range(early):
            cols = slice(wide * c, wide * c + wide)
            up_cols = slice(ff + wide * c, ff + wide * c + wide)
            hb[i, me_x, :, cols] = act(g_own[at, cols] + g_first[c, at, :wide], g_own[at, up_cols] + g_first[c, at, wide:])
        done = early * wide
        hb[i, me_x, :, done:] = act(g_own[at, done:ff] + g_peer[at, :ff - done], g_own[at, ff + done:] + g_peer[at, ff - done:])
        h_copy(i).start()
        return carry

    lax.fori_loop(0, groups, activate, 0)
    o_over.wait()
    relay = [remote(oy.at[there[k]], oa.at[other], o_send.at[3 + k], o_recv.at[3 + k], me_x, there[k]) for k in (1, 2, 3)]
    for copy in relay:
        copy.start()
    oa[other] = oy[me_yz]
    for copy in (*o_out, *relay):
        copy.wait()
    for e in range(8):
        of[owned * e:owned * e + owned] = oa[e].astype(jnp.float32)
    wo_in.wait()
    out_part[...] = jnp.dot(of[...].astype(jnp.bfloat16), wo[...], preferred_element_type=jnp.float32)
    wd_in.wait()

    def pair_copies(i):
        return [remote(y_send.at[i, 2 * e + 1 - core], y_pair.at[i, e], p_send.at[i, e], p_recv.at[i, e], me_x, partner) for e in range(2)]

    def over_copy(i):
        return remote(y_over.at[i], y_recv.at[i], y_ssem.at[i], y_rsem.at[i], me_x, across)

    def cross(i):
        for copy in pair_copies(i):
            copy.wait()
        y_over[i] = y_send[i, across] + y_pair[i, 1 - col]
        over_copy(i).start()

    def product(i, carry):
        h_copy(i).wait()
        part = jnp.dot(hb[i].reshape(2 * span, ff), wd[...], preferred_element_type=jnp.float32)
        first_at = pl.multiple_of(span * i, span)
        part = part + jnp.concatenate([out_part[pl.ds(first_at, span)], out_part[pl.ds(half + first_at, span)]], axis=0)
        for j in range(4):
            moved = part if j == 0 else pltpu.roll(part, (4 - j) * chunk, 1)
            y_send[i, j] = moved[:, :chunk]
        for copy in pair_copies(i):
            copy.start()

        @pl.when(i > 0)
        def _():
            cross(i - 1)

        return carry

    def finish(i, carry):
        over_copy(i).wait()
        total = y_send[i, me_yz] + y_pair[i, col] + y_recv[i]
        for e in range(2):
            y_ref[pl.ds(pl.multiple_of(half * e + span * i, span), span), :] = total[span * e:span * e + span]
        return carry

    lax.fori_loop(0, groups, product, 0)
    lax.fori_loop(0, groups - 3, finish, 0)
    cross(groups - 1)
    lax.fori_loop(groups - 3, groups, finish, 0)


def tail(g_first, g_peer, g_own, o_blocks, w_down, w_out):
    half = g_own.shape[0]
    rows = 2 * half
    span = 16
    groups = half // span
    ff, cols = w_down.shape
    chunk = cols // 4
    owned = o_blocks.shape[1]
    o_width = w_out.shape[0]
    any_spec, vmem_spec = pl.BlockSpec(memory_space=pl.ANY), pl.BlockSpec(memory_space=pltpu.VMEM)
    dma = pltpu.SemaphoreType.DMA
    f32, bf16 = jnp.float32, jnp.bfloat16
    return pl.pallas_call(
        tail_kernel,
        out_shape=jax.ShapeDtypeStruct((rows, chunk), f32),
        in_specs=[vmem_spec, vmem_spec, any_spec, vmem_spec, any_spec, any_spec],
        out_specs=pl.BlockSpec(memory_space=pltpu.VMEM),
        scratch_shapes=[
            pltpu.VMEM((half, 2 * ff), f32),
            pltpu.VMEM((4, owned, o_width), bf16),
            pltpu.VMEM((8, owned, o_width), bf16),
            pltpu.VMEM((rows, o_width), f32),
            pltpu.VMEM((groups, 2, span, ff), bf16),
            pltpu.VMEM((ff, cols), bf16),
            pltpu.VMEM((o_width, cols), bf16),
            pltpu.VMEM((rows, cols), f32),
            pltpu.VMEM((groups, 4, 2 * span, chunk), f32),
            pltpu.VMEM((groups, 2, 2 * span, chunk), f32),
            pltpu.VMEM((groups, 2 * span, chunk), f32),
            pltpu.VMEM((groups, 2 * span, chunk), f32),
            dma((3,)), dma((groups,)), dma((8,)), dma((8,)), dma((groups,)), dma((groups,)),
            dma((groups, 2)), dma((groups, 2)), dma((groups,)), dma((groups,)),
        ],
        compiler_params=pltpu.CompilerParams(collective_id=1, has_side_effects=True, vmem_limit_bytes=51 * 1024 * 1024),
        cost_estimate=pl.CostEstimate(flops=2 * rows * (ff + o_width) * cols, bytes_accessed=2 * (ff + o_width) * cols, transcendentals=half * ff),
        name='tail',
    )(g_first, g_peer, g_own, o_blocks, w_down, w_out)


def rotary(values, positions):
    half_dim = values.shape[-1] // 2
    inv_freq = ROPE_BASE ** (-jnp.arange(half_dim, dtype=jnp.float32) / half_dim)
    angles = positions.astype(jnp.float32)[:, None, None] * inv_freq
    cos_part = jnp.cos(angles)
    sin_part = jnp.sin(angles)
    lo_half = values[..., :half_dim]
    hi_half = values[..., half_dim:]
    return jnp.concatenate([lo_half * cos_part - hi_half * sin_part, hi_half * cos_part + lo_half * sin_part], axis=-1)


def solution(mesh):
    x_size = mesh.shape['x']
    yz_size = mesh.shape['yz']
    all_axes = ('x', 'yz')

    def local_step(x_in, ln_scale, w_gate_up, w_attn, w_down, w_out, k_cache, v_cache, lengths, positions):
        local_rows, seq_len, head_dim = k_cache.shape
        q_width = w_out.shape[0] * yz_size
        num_heads = q_width // head_dim
        d_model = x_in.shape[1] * x_size * yz_size
        z_blocks, g_first, g_send, g_own = head(x_in, ln_scale, w_gate_up, w_attn, d_model, EARLY)
        g_peer = lax.ppermute(g_send, 'x', [(0, 1), (1, 0)])
        proj_local = z_blocks.transpose(1, 0, 2).reshape(local_rows, -1)
        q_raw = proj_local[:, :q_width].reshape(local_rows, num_heads, head_dim)
        k_tok = proj_local[:, q_width:q_width + head_dim]
        v_tok = proj_local[:, q_width + head_dim:]
        q_rot = rotary(q_raw.astype(jnp.float32), positions).astype(jnp.bfloat16)
        k_rot = rotary(k_tok[:, None, :].astype(jnp.float32), positions)[:, 0].astype(jnp.bfloat16)
        cols = jnp.stack([k_rot, v_tok]).astype(jnp.float32).transpose(0, 2, 1)
        cols = jnp.pad(cols, ((0, 0), (0, 0), (0, 128 - local_rows)))
        attn_out, k_new, v_new = attend(q_rot, cols, k_cache, v_cache, lengths)
        o_blocks = attn_out.reshape(local_rows, yz_size, q_width // yz_size).transpose(1, 0, 2)
        mixed_sum = tail(g_first, g_peer, g_own, o_blocks, w_down, w_out)
        y_out = (x_in.astype(jnp.float32) + mixed_sum).astype(jnp.bfloat16)
        return y_out, k_new, v_new

    row_spec = P(None, all_axes)
    vec_spec = P(all_axes)
    cache_spec = P(all_axes, None, None)
    return jax.shard_map(
        local_step,
        mesh=mesh,
        in_specs=(row_spec, vec_spec, P('x', None, 'yz'), P('x', 'yz'), P('yz', 'x'), P('yz', 'x'), cache_spec, cache_spec, vec_spec, vec_spec),
        out_specs=(row_spec, cache_spec, cache_spec),
        check_vma=False,
    )
```

```python
import functools

import jax
import jax.numpy as jnp
from jax import lax
from jax.experimental import pallas as pl
from jax.experimental.pallas import tpu as pltpu
from jax.sharding import PartitionSpec as P

LN_EPS = 1e-6
ROPE_BASE = 10000.0
MESH = pl.DeviceIdType.MESH
VMEM_MOST = 64 * 1024 * 1024 - 64 * 1024
EARLY = 2


def attention_kernel(scale, len_ref, q_ref, cols_ref, k_hbm, v_hbm, o_ref, ko_hbm, vo_hbm, k_buf, v_buf, in_sem, out_sem):
    rows, _, seq_len = k_buf.shape

    def load(which, b):
        src, dst = ((k_hbm, k_buf), (v_hbm, v_buf))[which]
        return pltpu.make_async_copy(src.at[b], dst.at[b], in_sem.at[which, b])

    def save(which, b):
        src, dst = ((k_buf, ko_hbm), (v_buf, vo_hbm))[which]
        return pltpu.make_async_copy(src.at[b], dst.at[b], out_sem.at[which, b])

    for b in range(rows):
        load(0, b).start()
        load(1, b).start()

    lane = lax.broadcasted_iota(jnp.int32, (1, 128), 1)
    slots = lax.broadcasted_iota(jnp.int32, (1, seq_len), 1)

    def row(b, carry):
        length = len_ref[b]
        window = pl.ds(pl.multiple_of((length // 128) * 128, 128), 128)
        here = lane == length % 128
        for which, buf in enumerate((k_buf, v_buf)):
            load(which, b).wait()
            col = jnp.sum(jnp.where(lane == b, cols_ref[which], 0.0), axis=1, keepdims=True)
            tile = buf[b, :, window].astype(jnp.float32)
            buf[b, :, window] = jnp.where(here, col, tile).astype(jnp.bfloat16)
        scores = jnp.dot(q_ref[b], k_buf[b], preferred_element_type=jnp.float32) * scale
        scores = jnp.where(slots <= length, scores, -1e30)
        top = jnp.max(scores, axis=1, keepdims=True)
        weights = jnp.exp(scores - top)
        total = jnp.sum(weights, axis=1, keepdims=True)
        probs = (weights * (1.0 / total)).astype(jnp.bfloat16)
        save(0, b).start()
        save(1, b).start()
        o_ref[b] = lax.dot_general(probs, v_buf[b], (((1,), (1,)), ((), ())), preferred_element_type=jnp.float32).astype(jnp.bfloat16)
        return carry

    lax.fori_loop(0, rows, row, 0)
    for b in range(rows):
        save(0, b).wait()
        save(1, b).wait()


def attend(q_rot, cols, k_cache, v_cache, lengths):
    rows, heads, head_dim = q_rot.shape
    seq_len = k_cache.shape[1]
    k_t = jnp.swapaxes(k_cache, 1, 2)
    v_t = jnp.swapaxes(v_cache, 1, 2)
    cache = jax.ShapeDtypeStruct((rows, head_dim, seq_len), jnp.bfloat16)
    o, k_new, v_new = pl.pallas_call(
        functools.partial(attention_kernel, head_dim ** -0.5),
        out_shape=(jax.ShapeDtypeStruct((rows, heads, head_dim), jnp.bfloat16), cache, cache),
        in_specs=[
            pl.BlockSpec(memory_space=pltpu.SMEM),
            pl.BlockSpec(memory_space=pltpu.VMEM),
            pl.BlockSpec(memory_space=pltpu.VMEM),
            pl.BlockSpec(memory_space=pl.ANY),
            pl.BlockSpec(memory_space=pl.ANY),
        ],
        out_specs=(pl.BlockSpec(memory_space=pltpu.VMEM), pl.BlockSpec(memory_space=pl.ANY), pl.BlockSpec(memory_space=pl.ANY)),
        scratch_shapes=[
            pltpu.VMEM((rows, head_dim, seq_len), jnp.bfloat16),
            pltpu.VMEM((rows, head_dim, seq_len), jnp.bfloat16),
            pltpu.SemaphoreType.DMA((2, rows)),
            pltpu.SemaphoreType.DMA((2, rows)),
        ],
        compiler_params=pltpu.CompilerParams(vmem_limit_bytes=48 * 1024 * 1024),
        cost_estimate=pl.CostEstimate(
            flops=4 * rows * heads * head_dim * seq_len,
            bytes_accessed=8 * rows * head_dim * seq_len,
            transcendentals=rows * heads * seq_len,
        ),
        name='attend',
    )(lengths, q_rot, cols, k_t, v_t)
    return o, jnp.swapaxes(k_new, 1, 2), jnp.swapaxes(v_new, 1, 2)


def start_barrier(me_x, me_yz, everyone):
    barrier = pltpu.get_barrier_semaphore()
    peers = [(dx, k) for dx in range(2) for k in range(4) if (dx or k) and (everyone or not (dx and k))]
    for dx, k in peers:
        pl.semaphore_signal(barrier, inc=1, device_id=(lax.rem(me_x + dx, 2), lax.rem(me_yz + k, 4)), device_id_type=MESH)
    return lambda: pl.semaphore_wait(barrier, len(peers))


def spread(rows, cols, first):
    i = lax.broadcasted_iota(jnp.int32, (rows, cols), 0)
    c = lax.broadcasted_iota(jnp.int32, (rows, cols), 1)
    return jnp.where(c == 2 * i + first, 1.0, 0.0).astype(jnp.bfloat16)


def head_kernel(
    d_model, early, x_hbm, scale_hbm, wg_hbm, wa_hbm, z_hbm, first_hbm, send_hbm, own_hbm,
    xg, scale_row, sg, stats, h_buf, hx, wg, wa, z_send, z_own, z_recv, r_send, r_own, r_recv, zb, zg, g_first, g_rest, g_own,
    in_sem, wg_sem, x_send, x_recv, s_send, s_recv, t_send, t_recv, z_sems, a_send, a_recv, f_send, f_recv, out_sem,
):
    me_x = lax.axis_index('x')
    me_yz = lax.axis_index('yz')
    half, chunk = xg.shape[2:]
    rows = 2 * half
    pieces = wg_sem.shape[0]
    depth = wg.shape[0] // pieces
    ff = wg.shape[2]
    wide_cols = 256
    full = z_send.shape[2]
    third = half // 3
    tail_cols = wa.shape[0] - full
    other_x = lax.rem(me_x + 1, 2)
    across = lax.rem(me_yz + 2, 4)
    core = lax.rem(me_yz, 2)
    partner = me_yz + 1 - 2 * core
    order = (other_x, me_x)
    x_in = [
        pltpu.make_async_copy(x_hbm.at[pl.ds(pl.multiple_of(order[p] * half, 32), half)], xg.at[me_yz, order[p]], in_sem.at[p]) for p in range(2)
    ]
    scale_in = pltpu.make_async_copy(scale_hbm, scale_row, in_sem.at[2])
    wa_in = pltpu.make_async_copy(wa_hbm, wa, in_sem.at[3])
    wg_in = [
        pltpu.make_async_copy(wg_hbm.at[pl.ds(depth * i, depth)], wg.at[pl.ds(depth * i, depth)], wg_sem.at[i]) for i in range(pieces)
    ]
    for copy in (*x_in, scale_in, wa_in):
        copy.start()
    others_ready = start_barrier(me_x, me_yz, True)

    def remote(src, dst, send, recv, to_x, to_yz):
        return pltpu.make_async_remote_copy(
            src_ref=src, dst_ref=dst, send_sem=send, recv_sem=recv, device_id=(to_x, to_yz), device_id_type=MESH,
        )

    def x_copy(kind, p):
        owner = across if kind == 2 else me_yz
        at = xg.at[owner, order[p]]
        return remote(at, at, x_send.at[kind, p], x_recv.at[kind, p], me_x, across if kind == 1 else partner)

    for p in range(2):
        x_in[p].wait()
    lane = lax.broadcasted_iota(jnp.int32, (8, 128), 1)
    tile = jnp.zeros((8, 128), jnp.float32)
    for e in range(2):
        mine = xg[me_yz, e].astype(jnp.float32)
        sum_1 = jnp.sum(mine, axis=1, keepdims=True)
        sum_2 = jnp.sum(mine * mine, axis=1, keepdims=True)
        for j in range(half // 8):
            col = e * (half // 8) + j
            tile = jnp.where(lane == col, sum_1[8 * j:8 * j + 8], tile)
            tile = jnp.where(lane == 32 + col, sum_2[8 * j:8 * j + 8], tile)
    me = me_x * 4 + me_yz
    stats[me] = tile
    others_ready()
    t_out = [
        remote(stats.at[me], stats.at[me], t_send.at[4 * dx + k], t_recv.at[4 * dx + k], lax.rem(me_x + dx, 2), lax.rem(me_yz + k, 4))
        for dx in range(2) for k in range(4) if dx or k
    ]
    for copy in t_out:
        copy.start()
    scale_in.wait()
    sg[me_yz] = scale_row[...].reshape(1, chunk)
    s_out = [remote(sg.at[me_yz], sg.at[me_yz], s_send.at[k], s_recv.at[k], me_x, lax.rem(me_yz + k, 4)) for k in (1, 2, 3)]
    for copy in s_out:
        copy.start()
    for p in range(2):
        x_copy(1, p).start()
        x_copy(0, p).start()
    for copy in wg_in:
        copy.start()
    wide, thin = spread(128, 256, 0), spread(64, 128, 0)
    wide_u, thin_u = spread(128, 256, 1), spread(64, 128, 1)
    for copy in t_out:
        copy.wait()
    total = stats[0]
    for i in range(1, 8):
        total = total + stats[i]
    mean_t = total / d_model
    var_t = pltpu.roll(total, 96, 1) / d_model - mean_t * mean_t
    rstd_t = lax.rsqrt(var_t + LN_EPS)
    for copy in s_out:
        copy.wait()

    def rows_scale(p):
        shift = lax.rem(128 - order[p] * (half // 8), 128)
        mean_p = pltpu.roll(mean_t, shift, 1)
        rstd_p = pltpu.roll(rstd_t, shift, 1)
        mean = jnp.concatenate([mean_p[:, j:j + 1] for j in range(half // 8)], axis=0)
        rstd = jnp.concatenate([rstd_p[:, j:j + 1] for j in range(half // 8)], axis=0)
        return mean, rstd

    chip = me_yz // 2
    contract = (((1,), (1,)), ((), ()))

    def project_chip(p, which, mean, rstd):
        both = []
        for e in range(2):
            s = 2 * which + e
            h = (xg[s, order[p]].astype(jnp.float32) - mean) * rstd * sg[s]
            h_buf[s] = h.astype(jnp.bfloat16)
            both.append(h)
        h = jnp.concatenate(both, axis=1).astype(jnp.bfloat16)
        at = pl.ds(pl.multiple_of(2 * chunk * which, 128), 2 * chunk)
        z = lax.dot_general(h, wa[:full, at], contract, preferred_element_type=jnp.float32)
        r = lax.dot_general(h, wa[full:, at], contract, preferred_element_type=jnp.float32)
        return z, r

    def project(p):
        mean, rstd = rows_scale(p)
        x_copy(1, p).wait()
        x_copy(2, p).start()
        x_copy(0, p).wait()
        z_near, r_near = project_chip(p, chip, mean, rstd)
        x_copy(2, p).wait()
        z_far, r_far = project_chip(p, 1 - chip, mean, rstd)
        r = r_near + r_far
        r = jnp.concatenate([r[third * i:third * i + third] for i in range(3)], axis=1)
        return (z_near + z_far).reshape(z_send.shape), r

    def spread_half(part, g):
        out = pl.ds((2 * part + g) * half, half)
        a, b = ((wide, thin), (wide_u, thin_u))[g]
        for s in range(4):
            base = 2 * chunk * s
            for t in range(2):
                piece = h_buf[s, :, 128 * t:128 * t + 128]
                hx[out, base + 256 * t:base + 256 * t + 256] = jnp.dot(piece, a, preferred_element_type=jnp.float32).astype(jnp.bfloat16)
            piece = h_buf[s, :, 256:320]
            hx[out, base + 512:base + 640] = jnp.dot(piece, b, preferred_element_type=jnp.float32).astype(jnp.bfloat16)

    wa_in.wait()
    z_send[...], r_send[...] = project(0)
    z_out = [remote(z_send, z_recv, z_sems.at[0], z_sems.at[1], other_x, me_yz), remote(r_send, r_recv, z_sems.at[2], z_sems.at[3], other_x, me_yz)]
    for copy in z_out:
        copy.start()
    spread_half(0, 0)
    spread_half(0, 1)
    z_own[...], r_own[...] = project(1)
    spread_half(1, 0)
    spread_half(1, 1)
    for copy in wg_in:
        copy.wait()

    def columns(c):
        at = pl.ds(pl.multiple_of(c * wide_cols, wide_cols), wide_cols)
        block = wg[:, :, at].reshape(2 * wg.shape[0], wide_cols)
        out = jnp.dot(hx[...], block, preferred_element_type=jnp.float32)
        up = pl.ds(pl.multiple_of(ff + c * wide_cols, wide_cols), wide_cols)
        g_own[:, at] = out[2 * half:3 * half]
        g_own[:, up] = out[3 * half:]
        return out

    first = []
    for c in range(early):
        out = columns(c)
        g_first[c, :, :wide_cols] = out[:half]
        g_first[c, :, wide_cols:] = out[half:2 * half]
        first.append(remote(g_first.at[c], first_hbm.at[c], f_send.at[c], f_recv.at[c], other_x, me_yz))
        first[-1].start()

    def rest(c, carry):
        out = columns(c)
        at = (c - early) * wide_cols
        g_rest[:, pl.ds(pl.multiple_of(at, wide_cols), wide_cols)] = out[:half]
        g_rest[:, pl.ds(pl.multiple_of(ff - early * wide_cols + at, wide_cols), wide_cols)] = out[half:2 * half]
        return carry

    lax.fori_loop(early, ff // wide_cols, rest, 0)
    save = [pltpu.make_async_copy(g_rest, send_hbm, out_sem.at[0]), pltpu.make_async_copy(g_own, own_hbm, out_sem.at[1])]
    for copy in save:
        copy.start()
    for copy in z_out:
        copy.wait()
    zb[:, :, :full] = (z_own[...] + z_recv[...]).astype(jnp.bfloat16)
    r = r_own[...] + r_recv[...]
    r = jnp.concatenate([r[:, tail_cols * i:tail_cols * i + tail_cols] for i in range(3)], axis=0)
    zb[:, :, full:] = r.reshape(zb.shape[0], zb.shape[1], tail_cols).astype(jnp.bfloat16)
    a_out = [remote(zb.at[lax.rem(me_yz + k, 4)], zg.at[me_yz], a_send.at[k], a_recv.at[k], me_x, lax.rem(me_yz + k, 4)) for k in (1, 2, 3)]
    for copy in a_out:
        copy.start()
    zg[me_yz] = zb[me_yz]
    for copy in a_out:
        copy.wait()
    save.append(pltpu.make_async_copy(zg, z_hbm, out_sem.at[2]))
    save[-1].start()
    for copy in first:
        copy.wait()
    for copy in save:
        copy.wait()


def head(x_in, ln_scale, w_gate_up, w_attn, d_model, early):
    rows, chunk = x_in.shape
    depth, _, ff = w_gate_up.shape
    z_cols = w_attn.shape[1]
    full = z_cols // 128 * 128
    owned = rows // 8
    half = rows // 2
    width = 2 * (ff - 256 * early)
    any_spec = pl.BlockSpec(memory_space=pl.ANY)
    dma = pltpu.SemaphoreType.DMA
    f32, bf16 = jnp.float32, jnp.bfloat16
    return pl.pallas_call(
        functools.partial(head_kernel, d_model, early),
        out_shape=(
            jax.ShapeDtypeStruct((4, owned, z_cols), bf16),
            jax.ShapeDtypeStruct((early, half, 512), f32),
            jax.ShapeDtypeStruct((half, width), f32),
            jax.ShapeDtypeStruct((half, 2 * ff), f32),
        ),
        in_specs=[any_spec] * 4,
        out_specs=[any_spec] * 4,
        scratch_shapes=[
            pltpu.VMEM((4, 2, half, chunk), bf16),
            pltpu.VMEM((chunk,), f32),
            pltpu.VMEM((4, 1, chunk), f32),
            pltpu.VMEM((8, 8, 128), f32),
            pltpu.VMEM((4, half, chunk), bf16),
            pltpu.VMEM((2 * rows, 2 * depth), bf16),
            pltpu.VMEM((depth, 2, ff), bf16),
            pltpu.VMEM((z_cols, depth), bf16),
            *[pltpu.VMEM((4, owned, full), f32)] * 3,
            *[pltpu.VMEM((half // 3, 3 * (z_cols - full)), f32)] * 3,
            pltpu.VMEM((4, owned, z_cols), bf16),
            pltpu.VMEM((4, owned, z_cols), bf16),
            pltpu.VMEM((early, half, 512), f32),
            pltpu.VMEM((half, width), f32),
            pltpu.VMEM((half, 2 * ff), f32),
            dma((4,)), dma((8,)), dma((3, 2)), dma((3, 2)), dma((4,)), dma((4,)), dma((8,)), dma((8,)), dma((4,)), dma((4,)), dma((4,)),
            dma((early,)), dma((early,)), dma((3,)),
        ],
        compiler_params=pltpu.CompilerParams(collective_id=0, has_side_effects=True, vmem_limit_bytes=VMEM_MOST),
        cost_estimate=pl.CostEstimate(flops=4 * rows * depth * 2 * ff, bytes_accessed=4 * depth * ff, transcendentals=0),
        name='head',
    )(x_in, ln_scale, w_gate_up, w_attn.T)


def tail_kernel(
    g_first, g_peer, own_hbm, ov, wd_hbm, wo_hbm, y_ref,
    g_own, oy, oa, of, hb, wd, wo, out_part, y_send, y_pair, y_over, y_recv,
    in_sem, own_sem, o_send, o_recv, h_send, h_recv, p_send, p_recv, y_ssem, y_rsem,
):
    me_x = lax.axis_index('x')
    me_yz = lax.axis_index('yz')
    groups, _, span, ff = hb.shape
    rows, chunk = y_ref.shape
    half = rows // 2
    owned = ov.shape[1]
    early, _, wide = g_first.shape
    wide = wide // 2
    core = lax.rem(me_yz, 2)
    col = me_yz // 2
    partner = me_yz + 1 - 2 * core
    across = lax.rem(me_yz + 2, 4)
    other_x = lax.rem(me_x + 1, 2)

    own_in = [pltpu.make_async_copy(own_hbm.at[pl.ds(span * i, span)], g_own.at[pl.ds(span * i, span)], own_sem.at[i]) for i in range(groups)]
    wo_in = pltpu.make_async_copy(wo_hbm, wo, in_sem.at[1])
    wd_in = pltpu.make_async_copy(wd_hbm, wd, in_sem.at[2])
    for copy in (*own_in, wo_in, wd_in):
        copy.start()
    start_barrier(me_x, me_yz, False)()
    me = me_x * 4 + me_yz

    def remote(src, dst, send, recv, to_x, to_yz):
        return pltpu.make_async_remote_copy(
            src_ref=src, dst_ref=dst, send_sem=send, recv_sem=recv, device_id=(to_x, to_yz), device_id_type=MESH,
        )

    other = other_x * 4 + me_yz
    o_over = remote(ov, oy, o_send.at[0], o_recv.at[0], other_x, me_yz)
    o_over.start()
    there = [lax.rem(me_yz + k, 4) for k in range(4)]
    o_out = [remote(ov.at[there[k]], oa.at[me], o_send.at[k], o_recv.at[k], me_x, there[k]) for k in (1, 2, 3)]
    for copy in o_out:
        copy.start()
    oa[me] = ov[me_yz]

    def h_copy(i):
        return remote(hb.at[i, me_x], hb.at[i, me_x], h_send.at[i], h_recv.at[i], other_x, me_yz)

    for copy in own_in:
        copy.wait()

    def activate(i, carry):
        at = pl.ds(pl.multiple_of(span * i, span), span)

        def act(gate, up):
            gate = gate.astype(jnp.bfloat16).astype(jnp.float32)
            up = up.astype(jnp.bfloat16).astype(jnp.float32)
            return (jax.nn.silu(gate) * up).astype(jnp.bfloat16)

        for c in range(early):
            cols = slice(wide * c, wide * c + wide)
            up_cols = slice(ff + wide * c, ff + wide * c + wide)
            hb[i, me_x, :, cols] = act(g_own[at, cols] + g_first[c, at, :wide], g_own[at, up_cols] + g_first[c, at, wide:])
        done = early * wide
        hb[i, me_x, :, done:] = act(g_own[at, done:ff] + g_peer[at, :ff - done], g_own[at, ff + done:] + g_peer[at, ff - done:])
        h_copy(i).start()
        return carry

    lax.fori_loop(0, groups, activate, 0)
    o_over.wait()
    relay = [remote(oy.at[there[k]], oa.at[other], o_send.at[3 + k], o_recv.at[3 + k], me_x, there[k]) for k in (1, 2, 3)]
    for copy in relay:
        copy.start()
    oa[other] = oy[me_yz]
    for copy in (*o_out, *relay):
        copy.wait()
    for e in range(8):
        of[owned * e:owned * e + owned] = oa[e].astype(jnp.float32)
    wo_in.wait()
    out_part[...] = jnp.dot(of[...].astype(jnp.bfloat16), wo[...], preferred_element_type=jnp.float32)
    wd_in.wait()

    def pair_copy(i, which):
        return remote(y_send.at[i, 2 * which + 1 - core], y_pair.at[i, which], p_send.at[i, which], p_recv.at[i, which], me_x, partner)

    def over_copy(i):
        return remote(y_over.at[i], y_recv.at[i], y_ssem.at[i], y_rsem.at[i], me_x, across)

    def cross(i):
        pair_copy(i, 1 - col).wait()
        y_over[i] = y_send[i, across] + y_pair[i, 1 - col]
        over_copy(i).start()

    def product(i, carry):
        h_copy(i).wait()
        first_at = pl.multiple_of(span * i, span)
        for which in (1 - col, col):
            at = pl.ds(pl.multiple_of(2 * chunk * which, 128), 2 * chunk)
            part = jnp.dot(hb[i].reshape(2 * span, ff), wd[:, at], preferred_element_type=jnp.float32)
            part = part + jnp.concatenate([out_part[pl.ds(first_at, span), at], out_part[pl.ds(half + first_at, span), at]], axis=0)
            y_send[i, 2 * which] = part[:, :chunk]
            y_send[i, 2 * which + 1] = pltpu.roll(part, chunk, 1)[:, :chunk]
            pair_copy(i, which).start()

        @pl.when(i > 0)
        def _():
            cross(i - 1)

        return carry

    def finish(i, carry):
        pair_copy(i, col).wait()
        over_copy(i).wait()
        total = y_send[i, me_yz] + y_pair[i, col] + y_recv[i]
        for e in range(2):
            y_ref[pl.ds(pl.multiple_of(half * e + span * i, span), span), :] = total[span * e:span * e + span]
        return carry

    lax.fori_loop(0, groups, product, 0)
    lax.fori_loop(0, groups - 3, finish, 0)
    cross(groups - 1)
    lax.fori_loop(groups - 3, groups, finish, 0)


def tail(g_first, g_peer, g_own, o_blocks, w_down, w_out):
    half = g_own.shape[0]
    rows = 2 * half
    span = 16
    groups = half // span
    ff, cols = w_down.shape
    chunk = cols // 4
    owned = o_blocks.shape[1]
    o_width = w_out.shape[0]
    any_spec, vmem_spec = pl.BlockSpec(memory_space=pl.ANY), pl.BlockSpec(memory_space=pltpu.VMEM)
    dma = pltpu.SemaphoreType.DMA
    f32, bf16 = jnp.float32, jnp.bfloat16
    return pl.pallas_call(
        tail_kernel,
        out_shape=jax.ShapeDtypeStruct((rows, chunk), f32),
        in_specs=[vmem_spec, vmem_spec, any_spec, vmem_spec, any_spec, any_spec],
        out_specs=pl.BlockSpec(memory_space=pltpu.VMEM),
        scratch_shapes=[
            pltpu.VMEM((half, 2 * ff), f32),
            pltpu.VMEM((4, owned, o_width), bf16),
            pltpu.VMEM((8, owned, o_width), bf16),
            pltpu.VMEM((rows, o_width), f32),
            pltpu.VMEM((groups, 2, span, ff), bf16),
            pltpu.VMEM((ff, cols), bf16),
            pltpu.VMEM((o_width, cols), bf16),
            pltpu.VMEM((rows, cols), f32),
            pltpu.VMEM((groups, 4, 2 * span, chunk), f32),
            pltpu.VMEM((groups, 2, 2 * span, chunk), f32),
            pltpu.VMEM((groups, 2 * span, chunk), f32),
            pltpu.VMEM((groups, 2 * span, chunk), f32),
            dma((3,)), dma((groups,)), dma((8,)), dma((8,)), dma((groups,)), dma((groups,)),
            dma((groups, 2)), dma((groups, 2)), dma((groups,)), dma((groups,)),
        ],
        compiler_params=pltpu.CompilerParams(collective_id=1, has_side_effects=True, vmem_limit_bytes=51 * 1024 * 1024),
        cost_estimate=pl.CostEstimate(flops=2 * rows * (ff + o_width) * cols, bytes_accessed=2 * (ff + o_width) * cols, transcendentals=half * ff),
        name='tail',
    )(g_first, g_peer, g_own, o_blocks, w_down, w_out)


def rotary(values, positions):
    half_dim = values.shape[-1] // 2
    inv_freq = ROPE_BASE ** (-jnp.arange(half_dim, dtype=jnp.float32) / half_dim)
    angles = positions.astype(jnp.float32)[:, None, None] * inv_freq
    cos_part = jnp.cos(angles)
    sin_part = jnp.sin(angles)
    lo_half = values[..., :half_dim]
    hi_half = values[..., half_dim:]
    return jnp.concatenate([lo_half * cos_part - hi_half * sin_part, hi_half * cos_part + lo_half * sin_part], axis=-1)


def solution(mesh):
    x_size = mesh.shape['x']
    yz_size = mesh.shape['yz']
    all_axes = ('x', 'yz')

    def local_step(x_in, ln_scale, w_gate_up, w_attn, w_down, w_out, k_cache, v_cache, lengths, positions):
        local_rows, seq_len, head_dim = k_cache.shape
        q_width = w_out.shape[0] * yz_size
        num_heads = q_width // head_dim
        d_model = x_in.shape[1] * x_size * yz_size
        z_blocks, g_first, g_send, g_own = head(x_in, ln_scale, w_gate_up, w_attn, d_model, EARLY)
        g_peer = lax.ppermute(g_send, 'x', [(0, 1), (1, 0)])
        proj_local = z_blocks.transpose(1, 0, 2).reshape(local_rows, -1)
        q_raw = proj_local[:, :q_width].reshape(local_rows, num_heads, head_dim)
        k_tok = proj_local[:, q_width:q_width + head_dim]
        v_tok = proj_local[:, q_width + head_dim:]
        q_rot = rotary(q_raw.astype(jnp.float32), positions).astype(jnp.bfloat16)
        k_rot = rotary(k_tok[:, None, :].astype(jnp.float32), positions)[:, 0].astype(jnp.bfloat16)
        cols = jnp.stack([k_rot, v_tok]).astype(jnp.float32).transpose(0, 2, 1)
        cols = jnp.pad(cols, ((0, 0), (0, 0), (0, 128 - local_rows)))
        attn_out, k_new, v_new = attend(q_rot, cols, k_cache, v_cache, lengths)
        o_blocks = attn_out.reshape(local_rows, yz_size, q_width // yz_size).transpose(1, 0, 2)
        mixed_sum = tail(g_first, g_peer, g_own, o_blocks, w_down, w_out)
        y_out = (x_in.astype(jnp.float32) + mixed_sum).astype(jnp.bfloat16)
        return y_out, k_new, v_new

    row_spec = P(None, all_axes)
    vec_spec = P(all_axes)
    cache_spec = P(all_axes, None, None)
    return jax.shard_map(
        local_step,
        mesh=mesh,
        in_specs=(row_spec, vec_spec, P('x', None, 'yz'), P('x', 'yz'), P('yz', 'x'), P('yz', 'x'), cache_spec, cache_spec, vec_spec, vec_spec),
        out_specs=(row_spec, cache_spec, cache_spec),
        check_vma=False,
    )
```

```python
import functools

import jax
import jax.numpy as jnp
from jax import lax
from jax.experimental import pallas as pl
from jax.experimental.pallas import tpu as pltpu
from jax.sharding import PartitionSpec as P

LN_EPS = 1e-6
ROPE_BASE = 10000.0
MESH = pl.DeviceIdType.MESH
VMEM_MOST = 64 * 1024 * 1024 - 64 * 1024
EARLY = 2


def attention_kernel(scale, len_ref, q_ref, cols_ref, k_hbm, v_hbm, o_ref, ko_hbm, vo_hbm, k_buf, v_buf, in_sem, out_sem):
    rows, _, seq_len = k_buf.shape

    def load(which, b):
        src, dst = ((k_hbm, k_buf), (v_hbm, v_buf))[which]
        return pltpu.make_async_copy(src.at[b], dst.at[b], in_sem.at[which, b])

    def save(which, b):
        src, dst = ((k_buf, ko_hbm), (v_buf, vo_hbm))[which]
        return pltpu.make_async_copy(src.at[b], dst.at[b], out_sem.at[which, b])

    for b in range(rows):
        load(0, b).start()
        load(1, b).start()

    lane = lax.broadcasted_iota(jnp.int32, (1, 128), 1)
    slots = lax.broadcasted_iota(jnp.int32, (1, seq_len), 1)

    def row(b, carry):
        length = len_ref[b]
        window = pl.ds(pl.multiple_of((length // 128) * 128, 128), 128)
        here = lane == length % 128
        for which, buf in enumerate((k_buf, v_buf)):
            load(which, b).wait()
            col = jnp.sum(jnp.where(lane == b, cols_ref[which], 0.0), axis=1, keepdims=True)
            tile = buf[b, :, window].astype(jnp.float32)
            buf[b, :, window] = jnp.where(here, col, tile).astype(jnp.bfloat16)
        scores = jnp.dot(q_ref[b], k_buf[b], preferred_element_type=jnp.float32) * scale
        scores = jnp.where(slots <= length, scores, -1e30)
        top = jnp.max(scores, axis=1, keepdims=True)
        weights = jnp.exp(scores - top)
        total = jnp.sum(weights, axis=1, keepdims=True)
        probs = (weights * (1.0 / total)).astype(jnp.bfloat16)
        save(0, b).start()
        save(1, b).start()
        o_ref[b] = lax.dot_general(probs, v_buf[b], (((1,), (1,)), ((), ())), preferred_element_type=jnp.float32).astype(jnp.bfloat16)
        return carry

    lax.fori_loop(0, rows, row, 0)
    for b in range(rows):
        save(0, b).wait()
        save(1, b).wait()


def attend(q_rot, cols, k_cache, v_cache, lengths):
    rows, heads, head_dim = q_rot.shape
    seq_len = k_cache.shape[1]
    k_t = jnp.swapaxes(k_cache, 1, 2)
    v_t = jnp.swapaxes(v_cache, 1, 2)
    cache = jax.ShapeDtypeStruct((rows, head_dim, seq_len), jnp.bfloat16)
    o, k_new, v_new = pl.pallas_call(
        functools.partial(attention_kernel, head_dim ** -0.5),
        out_shape=(jax.ShapeDtypeStruct((rows, heads, head_dim), jnp.bfloat16), cache, cache),
        in_specs=[
            pl.BlockSpec(memory_space=pltpu.SMEM),
            pl.BlockSpec(memory_space=pltpu.VMEM),
            pl.BlockSpec(memory_space=pltpu.VMEM),
            pl.BlockSpec(memory_space=pl.ANY),
            pl.BlockSpec(memory_space=pl.ANY),
        ],
        out_specs=(pl.BlockSpec(memory_space=pltpu.VMEM), pl.BlockSpec(memory_space=pl.ANY), pl.BlockSpec(memory_space=pl.ANY)),
        scratch_shapes=[
            pltpu.VMEM((rows, head_dim, seq_len), jnp.bfloat16),
            pltpu.VMEM((rows, head_dim, seq_len), jnp.bfloat16),
            pltpu.SemaphoreType.DMA((2, rows)),
            pltpu.SemaphoreType.DMA((2, rows)),
        ],
        compiler_params=pltpu.CompilerParams(vmem_limit_bytes=48 * 1024 * 1024),
        cost_estimate=pl.CostEstimate(
            flops=4 * rows * heads * head_dim * seq_len,
            bytes_accessed=8 * rows * head_dim * seq_len,
            transcendentals=rows * heads * seq_len,
        ),
        name='attend',
    )(lengths, q_rot, cols, k_t, v_t)
    return o, jnp.swapaxes(k_new, 1, 2), jnp.swapaxes(v_new, 1, 2)


def start_barrier(me_x, me_yz, everyone):
    barrier = pltpu.get_barrier_semaphore()
    peers = [(dx, k) for dx in range(2) for k in range(4) if (dx or k) and (everyone or not (dx and k))]
    for dx, k in peers:
        pl.semaphore_signal(barrier, inc=1, device_id=(lax.rem(me_x + dx, 2), lax.rem(me_yz + k, 4)), device_id_type=MESH)
    return lambda: pl.semaphore_wait(barrier, len(peers))


def spread(rows, cols, first):
    i = lax.broadcasted_iota(jnp.int32, (rows, cols), 0)
    c = lax.broadcasted_iota(jnp.int32, (rows, cols), 1)
    return jnp.where(c == 2 * i + first, 1.0, 0.0).astype(jnp.bfloat16)


def head_kernel(
    d_model, early, x_hbm, scale_hbm, wg_hbm, wa_hbm, z_hbm, first_hbm, send_hbm, own_hbm,
    xg, scale_row, sg, stats, h_buf, hx, wg, wa, z_send, z_own, z_recv, r_send, r_own, r_recv, zb, zg, g_first, g_rest, g_own,
    in_sem, wg_sem, x_send, x_recv, s_send, s_recv, t_send, t_recv, z_sems, a_send, a_recv, f_send, f_recv, out_sem,
):
    me_x = lax.axis_index('x')
    me_yz = lax.axis_index('yz')
    half, chunk = xg.shape[2:]
    rows = 2 * half
    pieces = wg_sem.shape[0]
    depth = wg.shape[0] // pieces
    ff = wg.shape[2]
    wide_cols = 256
    full = z_send.shape[2]
    quarter = half // 2
    third = quarter // 3
    tail_cols = wa.shape[0] - full
    other_x = lax.rem(me_x + 1, 2)
    across = lax.rem(me_yz + 2, 4)
    core = lax.rem(me_yz, 2)
    partner = me_yz + 1 - 2 * core
    order = (other_x, me_x)
    x_in = [
        pltpu.make_async_copy(x_hbm.at[pl.ds(pl.multiple_of(order[p] * half, 32), half)], xg.at[me_yz, order[p]], in_sem.at[p]) for p in range(2)
    ]
    scale_in = pltpu.make_async_copy(scale_hbm, scale_row, in_sem.at[2])
    wa_in = pltpu.make_async_copy(wa_hbm, wa, in_sem.at[3])
    wg_in = [
        pltpu.make_async_copy(wg_hbm.at[pl.ds(depth * i, depth)], wg.at[pl.ds(depth * i, depth)], wg_sem.at[i]) for i in range(pieces)
    ]
    for copy in (*x_in, scale_in, wa_in):
        copy.start()
    others_ready = start_barrier(me_x, me_yz, True)

    def remote(src, dst, send, recv, to_x, to_yz):
        return pltpu.make_async_remote_copy(
            src_ref=src, dst_ref=dst, send_sem=send, recv_sem=recv, device_id=(to_x, to_yz), device_id_type=MESH,
        )

    def x_copy(kind, piece):
        owner = across if kind == 2 else me_yz
        at = xg.at[owner, order[piece // 2], pl.ds(quarter * (piece % 2), quarter)]
        return remote(at, at, x_send.at[kind, piece], x_recv.at[kind, piece], me_x, across if kind == 1 else partner)

    for p in range(2):
        x_in[p].wait()
    lane = lax.broadcasted_iota(jnp.int32, (8, 128), 1)
    tile = jnp.zeros((8, 128), jnp.float32)
    for e in range(2):
        mine = xg[me_yz, e].astype(jnp.float32)
        sum_1 = jnp.sum(mine, axis=1, keepdims=True)
        sum_2 = jnp.sum(mine * mine, axis=1, keepdims=True)
        for j in range(half // 8):
            col = e * (half // 8) + j
            tile = jnp.where(lane == col, sum_1[8 * j:8 * j + 8], tile)
            tile = jnp.where(lane == 32 + col, sum_2[8 * j:8 * j + 8], tile)
    me = me_x * 4 + me_yz
    stats[me] = tile
    others_ready()
    t_out = [
        remote(stats.at[me], stats.at[me], t_send.at[4 * dx + k], t_recv.at[4 * dx + k], lax.rem(me_x + dx, 2), lax.rem(me_yz + k, 4))
        for dx in range(2) for k in range(4) if dx or k
    ]
    for copy in t_out:
        copy.start()
    scale_in.wait()
    sg[me_yz] = scale_row[...].reshape(1, chunk)
    s_out = [remote(sg.at[me_yz], sg.at[me_yz], s_send.at[k], s_recv.at[k], me_x, lax.rem(me_yz + k, 4)) for k in (1, 2, 3)]
    for copy in s_out:
        copy.start()
    for piece in range(4):
        x_copy(1, piece).start()
        x_copy(0, piece).start()
    for copy in wg_in:
        copy.start()
    wide, thin = spread(128, 256, 0), spread(64, 128, 0)
    wide_u, thin_u = spread(128, 256, 1), spread(64, 128, 1)
    for copy in t_out:
        copy.wait()
    total = stats[0]
    for i in range(1, 8):
        total = total + stats[i]
    mean_t = total / d_model
    var_t = pltpu.roll(total, 96, 1) / d_model - mean_t * mean_t
    rstd_t = lax.rsqrt(var_t + LN_EPS)
    for copy in s_out:
        copy.wait()

    chip = me_yz // 2
    contract = (((1,), (1,)), ((), ()))

    def pass_on(piece):
        x_copy(1, piece).wait()
        x_copy(2, piece).start()

    def project_chip(piece, which):
        p, q = piece // 2, piece % 2
        blocks = quarter // 8
        shift = lax.rem(256 - order[p] * (half // 8) - q * blocks, 128)
        mean_p = pltpu.roll(mean_t, shift, 1)
        rstd_p = pltpu.roll(rstd_t, shift, 1)
        mean = jnp.concatenate([mean_p[:, j:j + 1] for j in range(blocks)], axis=0)
        rstd = jnp.concatenate([rstd_p[:, j:j + 1] for j in range(blocks)], axis=0)
        here = pl.ds(quarter * q, quarter)
        both = []
        for e in range(2):
            s = 2 * which + e
            h = (xg[s, order[p], here].astype(jnp.float32) - mean) * rstd * sg[s]
            h_buf[s, here] = h.astype(jnp.bfloat16)
            both.append(h)
        h = jnp.concatenate(both, axis=1).astype(jnp.bfloat16)
        at = pl.ds(pl.multiple_of(2 * chunk * which, 128), 2 * chunk)
        z = lax.dot_general(h, wa[:full, at], contract, preferred_element_type=jnp.float32)
        r = lax.dot_general(h, wa[full:, at], contract, preferred_element_type=jnp.float32)
        return z, r

    def near(piece):
        x_copy(0, piece).wait()
        return project_chip(piece, chip)

    def far(piece, z, r, z_ref, r_ref):
        x_copy(2, piece).wait()
        z_far, r_far = project_chip(piece, 1 - chip)
        q = piece % 2
        z_ref[2 * q:2 * q + 2] = (z + z_far).reshape(2, quarter // 2, full)
        r = r + r_far
        r_ref[q] = jnp.concatenate([r[third * i:third * i + third] for i in range(3)], axis=1)

    def z_copies(q):
        at = pl.ds(2 * q, 2)
        return (
            remote(z_send.at[at], z_recv.at[at], z_sems.at[0, q], z_sems.at[1, q], other_x, me_yz),
            remote(r_send.at[q], r_recv.at[q], z_sems.at[2, q], z_sems.at[3, q], other_x, me_yz),
        )

    def spread_half(part, g):
        out = pl.ds((2 * part + g) * half, half)
        a, b = ((wide, thin), (wide_u, thin_u))[g]
        for s in range(4):
            base = 2 * chunk * s
            for t in range(2):
                piece = h_buf[s, :, 128 * t:128 * t + 128]
                hx[out, base + 256 * t:base + 256 * t + 256] = jnp.dot(piece, a, preferred_element_type=jnp.float32).astype(jnp.bfloat16)
            piece = h_buf[s, :, 256:320]
            hx[out, base + 512:base + 640] = jnp.dot(piece, b, preferred_element_type=jnp.float32).astype(jnp.bfloat16)

    wa_in.wait()
    z_out = [*z_copies(0), *z_copies(1)]
    pass_on(0)
    far(0, *near(0), z_send, r_send)
    z_out[0].start()
    z_out[1].start()
    pass_on(1)
    part_1 = near(1)
    pass_on(2)
    far(1, *part_1, z_send, r_send)
    z_out[2].start()
    z_out[3].start()
    pass_on(3)
    spread_half(0, 0)
    spread_half(0, 1)
    for piece in (2, 3):
        far(piece, *near(piece), z_own, r_own)
    spread_half(1, 0)
    spread_half(1, 1)
    for copy in wg_in:
        copy.wait()

    def columns(c):
        at = pl.ds(pl.multiple_of(c * wide_cols, wide_cols), wide_cols)
        block = wg[:, :, at].reshape(2 * wg.shape[0], wide_cols)
        out = jnp.dot(hx[...], block, preferred_element_type=jnp.float32)
        up = pl.ds(pl.multiple_of(ff + c * wide_cols, wide_cols), wide_cols)
        g_own[:, at] = out[2 * half:3 * half]
        g_own[:, up] = out[3 * half:]
        return out

    first = []
    for c in range(early):
        out = columns(c)
        g_first[c, :, :wide_cols] = out[:half]
        g_first[c, :, wide_cols:] = out[half:2 * half]
        first.append(remote(g_first.at[c], first_hbm.at[c], f_send.at[c], f_recv.at[c], other_x, me_yz))
        first[-1].start()

    def rest(c, carry):
        out = columns(c)
        at = (c - early) * wide_cols
        g_rest[:, pl.ds(pl.multiple_of(at, wide_cols), wide_cols)] = out[:half]
        g_rest[:, pl.ds(pl.multiple_of(ff - early * wide_cols + at, wide_cols), wide_cols)] = out[half:2 * half]
        return carry

    lax.fori_loop(early, ff // wide_cols, rest, 0)
    save = [pltpu.make_async_copy(g_rest, send_hbm, out_sem.at[0]), pltpu.make_async_copy(g_own, own_hbm, out_sem.at[1])]
    for copy in save:
        copy.start()
    for copy in z_out:
        copy.wait()
    zb[:, :, :full] = (z_own[...] + z_recv[...]).astype(jnp.bfloat16)
    for q in range(2):
        r = r_own[q] + r_recv[q]
        r = jnp.concatenate([r[:, tail_cols * i:tail_cols * i + tail_cols] for i in range(3)], axis=0)
        zb[2 * q:2 * q + 2, :, full:] = r.reshape(2, quarter // 2, tail_cols).astype(jnp.bfloat16)
    a_out = [remote(zb.at[lax.rem(me_yz + k, 4)], zg.at[me_yz], a_send.at[k], a_recv.at[k], me_x, lax.rem(me_yz + k, 4)) for k in (1, 2, 3)]
    for copy in a_out:
        copy.start()
    zg[me_yz] = zb[me_yz]
    for copy in a_out:
        copy.wait()
    save.append(pltpu.make_async_copy(zg, z_hbm, out_sem.at[2]))
    save[-1].start()
    for copy in first:
        copy.wait()
    for copy in save:
        copy.wait()


def head(x_in, ln_scale, w_gate_up, w_attn, d_model, early):
    rows, chunk = x_in.shape
    depth, _, ff = w_gate_up.shape
    z_cols = w_attn.shape[1]
    full = z_cols // 128 * 128
    owned = rows // 8
    half = rows // 2
    width = 2 * (ff - 256 * early)
    any_spec = pl.BlockSpec(memory_space=pl.ANY)
    dma = pltpu.SemaphoreType.DMA
    f32, bf16 = jnp.float32, jnp.bfloat16
    return pl.pallas_call(
        functools.partial(head_kernel, d_model, early),
        out_shape=(
            jax.ShapeDtypeStruct((4, owned, z_cols), bf16),
            jax.ShapeDtypeStruct((early, half, 512), f32),
            jax.ShapeDtypeStruct((half, width), f32),
            jax.ShapeDtypeStruct((half, 2 * ff), f32),
        ),
        in_specs=[any_spec] * 4,
        out_specs=[any_spec] * 4,
        scratch_shapes=[
            pltpu.VMEM((4, 2, half, chunk), bf16),
            pltpu.VMEM((chunk,), f32),
            pltpu.VMEM((4, 1, chunk), f32),
            pltpu.VMEM((8, 8, 128), f32),
            pltpu.VMEM((4, half, chunk), bf16),
            pltpu.VMEM((2 * rows, 2 * depth), bf16),
            pltpu.VMEM((depth, 2, ff), bf16),
            pltpu.VMEM((z_cols, depth), bf16),
            *[pltpu.VMEM((4, owned, full), f32)] * 3,
            *[pltpu.VMEM((2, half // 6, 3 * (z_cols - full)), f32)] * 3,
            pltpu.VMEM((4, owned, z_cols), bf16),
            pltpu.VMEM((4, owned, z_cols), bf16),
            pltpu.VMEM((early, half, 512), f32),
            pltpu.VMEM((half, width), f32),
            pltpu.VMEM((half, 2 * ff), f32),
            dma((4,)), dma((8,)), dma((3, 4)), dma((3, 4)), dma((4,)), dma((4,)), dma((8,)), dma((8,)), dma((4, 2)), dma((4,)), dma((4,)),
            dma((early,)), dma((early,)), dma((3,)),
        ],
        compiler_params=pltpu.CompilerParams(collective_id=0, has_side_effects=True, vmem_limit_bytes=VMEM_MOST),
        cost_estimate=pl.CostEstimate(flops=4 * rows * depth * 2 * ff, bytes_accessed=4 * depth * ff, transcendentals=0),
        name='head',
    )(x_in, ln_scale, w_gate_up, w_attn.T)


def tail_kernel(
    g_first, g_peer, own_hbm, ov, wd_hbm, wo_hbm, y_ref,
    g_own, oy, oa, of, hb, wd, wo, out_part, y_send, y_pair, y_over, y_recv,
    in_sem, own_sem, o_send, o_recv, h_send, h_recv, p_send, p_recv, y_ssem, y_rsem,
):
    me_x = lax.axis_index('x')
    me_yz = lax.axis_index('yz')
    groups, _, span, ff = hb.shape
    rows, chunk = y_ref.shape
    half = rows // 2
    owned = ov.shape[1]
    early, _, wide = g_first.shape
    wide = wide // 2
    core = lax.rem(me_yz, 2)
    col = me_yz // 2
    partner = me_yz + 1 - 2 * core
    across = lax.rem(me_yz + 2, 4)
    other_x = lax.rem(me_x + 1, 2)

    own_in = [pltpu.make_async_copy(own_hbm.at[pl.ds(span * i, span)], g_own.at[pl.ds(span * i, span)], own_sem.at[i]) for i in range(groups)]
    wo_in = pltpu.make_async_copy(wo_hbm, wo, in_sem.at[1])
    wd_in = pltpu.make_async_copy(wd_hbm, wd, in_sem.at[2])
    for copy in (*own_in, wo_in, wd_in):
        copy.start()
    start_barrier(me_x, me_yz, False)()
    me = me_x * 4 + me_yz

    def remote(src, dst, send, recv, to_x, to_yz):
        return pltpu.make_async_remote_copy(
            src_ref=src, dst_ref=dst, send_sem=send, recv_sem=recv, device_id=(to_x, to_yz), device_id_type=MESH,
        )

    other = other_x * 4 + me_yz
    o_over = remote(ov, oy, o_send.at[0], o_recv.at[0], other_x, me_yz)
    o_over.start()
    there = [lax.rem(me_yz + k, 4) for k in range(4)]
    o_out = [remote(ov.at[there[k]], oa.at[me], o_send.at[k], o_recv.at[k], me_x, there[k]) for k in (1, 2, 3)]
    for copy in o_out:
        copy.start()
    oa[me] = ov[me_yz]

    def h_copy(i):
        return remote(hb.at[i, me_x], hb.at[i, me_x], h_send.at[i], h_recv.at[i], other_x, me_yz)

    for copy in own_in:
        copy.wait()

    def activate(i, carry):
        at = pl.ds(pl.multiple_of(span * i, span), span)

        def act(gate, up):
            gate = gate.astype(jnp.bfloat16).astype(jnp.float32)
            up = up.astype(jnp.bfloat16).astype(jnp.float32)
            return (jax.nn.silu(gate) * up).astype(jnp.bfloat16)

        for c in range(early):
            cols = slice(wide * c, wide * c + wide)
            up_cols = slice(ff + wide * c, ff + wide * c + wide)
            hb[i, me_x, :, cols] = act(g_own[at, cols] + g_first[c, at, :wide], g_own[at, up_cols] + g_first[c, at, wide:])
        done = early * wide
        hb[i, me_x, :, done:] = act(g_own[at, done:ff] + g_peer[at, :ff - done], g_own[at, ff + done:] + g_peer[at, ff - done:])
        h_copy(i).start()
        return carry

    lax.fori_loop(0, groups, activate, 0)
    o_over.wait()
    relay = [remote(oy.at[there[k]], oa.at[other], o_send.at[3 + k], o_recv.at[3 + k], me_x, there[k]) for k in (1, 2, 3)]
    for copy in relay:
        copy.start()
    oa[other] = oy[me_yz]
    for copy in (*o_out, *relay):
        copy.wait()
    for e in range(8):
        of[owned * e:owned * e + owned] = oa[e].astype(jnp.float32)
    wo_in.wait()
    out_part[...] = jnp.dot(of[...].astype(jnp.bfloat16), wo[...], preferred_element_type=jnp.float32)
    wd_in.wait()

    def pair_copy(i, which):
        return remote(y_send.at[i, 2 * which + 1 - core], y_pair.at[i, which], p_send.at[i, which], p_recv.at[i, which], me_x, partner)

    def over_copy(i):
        return remote(y_over.at[i], y_recv.at[i], y_ssem.at[i], y_rsem.at[i], me_x, across)

    def cross(i):
        pair_copy(i, 1 - col).wait()
        y_over[i] = y_send[i, across] + y_pair[i, 1 - col]
        over_copy(i).start()

    def product(i, carry):
        h_copy(i).wait()
        first_at = pl.multiple_of(span * i, span)
        part = jnp.dot(hb[i].reshape(2 * span, ff), wd[...], preferred_element_type=jnp.float32)
        part = part + jnp.concatenate([out_part[pl.ds(first_at, span)], out_part[pl.ds(half + first_at, span)]], axis=0)
        for j in range(4):
            moved = part if j == 0 else pltpu.roll(part, (4 - j) * chunk, 1)
            y_send[i, j] = moved[:, :chunk]
        for which in (1 - col, col):
            pair_copy(i, which).start()

        @pl.when(i > 0)
        def _():
            cross(i - 1)

        return carry

    def finish(i, carry):
        pair_copy(i, col).wait()
        over_copy(i).wait()
        total = y_send[i, me_yz] + y_pair[i, col] + y_recv[i]
        for e in range(2):
            y_ref[pl.ds(pl.multiple_of(half * e + span * i, span), span), :] = total[span * e:span * e + span]
        return carry

    lax.fori_loop(0, groups, product, 0)
    lax.fori_loop(0, groups - 3, finish, 0)
    cross(groups - 1)
    lax.fori_loop(groups - 3, groups, finish, 0)


def tail(g_first, g_peer, g_own, o_blocks, w_down, w_out):
    half = g_own.shape[0]
    rows = 2 * half
    span = 16
    groups = half // span
    ff, cols = w_down.shape
    chunk = cols // 4
    owned = o_blocks.shape[1]
    o_width = w_out.shape[0]
    any_spec, vmem_spec = pl.BlockSpec(memory_space=pl.ANY), pl.BlockSpec(memory_space=pltpu.VMEM)
    dma = pltpu.SemaphoreType.DMA
    f32, bf16 = jnp.float32, jnp.bfloat16
    return pl.pallas_call(
        tail_kernel,
        out_shape=jax.ShapeDtypeStruct((rows, chunk), f32),
        in_specs=[vmem_spec, vmem_spec, any_spec, vmem_spec, any_spec, any_spec],
        out_specs=pl.BlockSpec(memory_space=pltpu.VMEM),
        scratch_shapes=[
            pltpu.VMEM((half, 2 * ff), f32),
            pltpu.VMEM((4, owned, o_width), bf16),
            pltpu.VMEM((8, owned, o_width), bf16),
            pltpu.VMEM((rows, o_width), f32),
            pltpu.VMEM((groups, 2, span, ff), bf16),
            pltpu.VMEM((ff, cols), bf16),
            pltpu.VMEM((o_width, cols), bf16),
            pltpu.VMEM((rows, cols), f32),
            pltpu.VMEM((groups, 4, 2 * span, chunk), f32),
            pltpu.VMEM((groups, 2, 2 * span, chunk), f32),
            pltpu.VMEM((groups, 2 * span, chunk), f32),
            pltpu.VMEM((groups, 2 * span, chunk), f32),
            dma((3,)), dma((groups,)), dma((8,)), dma((8,)), dma((groups,)), dma((groups,)),
            dma((groups, 2)), dma((groups, 2)), dma((groups,)), dma((groups,)),
        ],
        compiler_params=pltpu.CompilerParams(collective_id=1, has_side_effects=True, vmem_limit_bytes=51 * 1024 * 1024),
        cost_estimate=pl.CostEstimate(flops=2 * rows * (ff + o_width) * cols, bytes_accessed=2 * (ff + o_width) * cols, transcendentals=half * ff),
        name='tail',
    )(g_first, g_peer, g_own, o_blocks, w_down, w_out)


def rotary(values, positions):
    half_dim = values.shape[-1] // 2
    inv_freq = ROPE_BASE ** (-jnp.arange(half_dim, dtype=jnp.float32) / half_dim)
    angles = positions.astype(jnp.float32)[:, None, None] * inv_freq
    cos_part = jnp.cos(angles)
    sin_part = jnp.sin(angles)
    lo_half = values[..., :half_dim]
    hi_half = values[..., half_dim:]
    return jnp.concatenate([lo_half * cos_part - hi_half * sin_part, hi_half * cos_part + lo_half * sin_part], axis=-1)


def solution(mesh):
    x_size = mesh.shape['x']
    yz_size = mesh.shape['yz']
    all_axes = ('x', 'yz')

    def local_step(x_in, ln_scale, w_gate_up, w_attn, w_down, w_out, k_cache, v_cache, lengths, positions):
        local_rows, seq_len, head_dim = k_cache.shape
        q_width = w_out.shape[0] * yz_size
        num_heads = q_width // head_dim
        d_model = x_in.shape[1] * x_size * yz_size
        z_blocks, g_first, g_send, g_own = head(x_in, ln_scale, w_gate_up, w_attn, d_model, EARLY)
        g_peer = lax.ppermute(g_send, 'x', [(0, 1), (1, 0)])
        proj_local = z_blocks.transpose(1, 0, 2).reshape(local_rows, -1)
        q_raw = proj_local[:, :q_width].reshape(local_rows, num_heads, head_dim)
        k_tok = proj_local[:, q_width:q_width + head_dim]
        v_tok = proj_local[:, q_width + head_dim:]
        q_rot = rotary(q_raw.astype(jnp.float32), positions).astype(jnp.bfloat16)
        k_rot = rotary(k_tok[:, None, :].astype(jnp.float32), positions)[:, 0].astype(jnp.bfloat16)
        cols = jnp.stack([k_rot, v_tok]).astype(jnp.float32).transpose(0, 2, 1)
        cols = jnp.pad(cols, ((0, 0), (0, 0), (0, 128 - local_rows)))
        attn_out, k_new, v_new = attend(q_rot, cols, k_cache, v_cache, lengths)
        o_blocks = attn_out.reshape(local_rows, yz_size, q_width // yz_size).transpose(1, 0, 2)
        mixed_sum = tail(g_first, g_peer, g_own, o_blocks, w_down, w_out)
        y_out = (x_in.astype(jnp.float32) + mixed_sum).astype(jnp.bfloat16)
        return y_out, k_new, v_new

    row_spec = P(None, all_axes)
    vec_spec = P(all_axes)
    cache_spec = P(all_axes, None, None)
    return jax.shard_map(
        local_step,
        mesh=mesh,
        in_specs=(row_spec, vec_spec, P('x', None, 'yz'), P('x', 'yz'), P('yz', 'x'), P('yz', 'x'), cache_spec, cache_spec, vec_spec, vec_spec),
        out_specs=(row_spec, cache_spec, cache_spec),
        check_vma=False,
    )
```

```python
import functools

import jax
import jax.numpy as jnp
from jax import lax
from jax.experimental import pallas as pl
from jax.experimental.pallas import tpu as pltpu
from jax.sharding import PartitionSpec as P

LN_EPS = 1e-6
ROPE_BASE = 10000.0
MESH = pl.DeviceIdType.MESH
VMEM_MOST = 64 * 1024 * 1024 - 64 * 1024
EARLY = 2


def attention_kernel(scale, len_ref, q_ref, cols_ref, k_hbm, v_hbm, o_ref, ko_hbm, vo_hbm, k_buf, v_buf, in_sem, out_sem):
    rows, _, seq_len = k_buf.shape

    def load(which, b):
        src, dst = ((k_hbm, k_buf), (v_hbm, v_buf))[which]
        return pltpu.make_async_copy(src.at[b], dst.at[b], in_sem.at[which, b])

    def save(which, b):
        src, dst = ((k_buf, ko_hbm), (v_buf, vo_hbm))[which]
        return pltpu.make_async_copy(src.at[b], dst.at[b], out_sem.at[which, b])

    for b in range(rows):
        load(0, b).start()
        load(1, b).start()

    lane = lax.broadcasted_iota(jnp.int32, (1, 128), 1)
    slots = lax.broadcasted_iota(jnp.int32, (1, seq_len), 1)

    def row(b, carry):
        length = len_ref[b]
        window = pl.ds(pl.multiple_of((length // 128) * 128, 128), 128)
        here = lane == length % 128
        for which, buf in enumerate((k_buf, v_buf)):
            load(which, b).wait()
            col = jnp.sum(jnp.where(lane == b, cols_ref[which], 0.0), axis=1, keepdims=True)
            tile = buf[b, :, window].astype(jnp.float32)
            buf[b, :, window] = jnp.where(here, col, tile).astype(jnp.bfloat16)
        scores = jnp.dot(q_ref[b], k_buf[b], preferred_element_type=jnp.float32) * scale
        scores = jnp.where(slots <= length, scores, -1e30)
        top = jnp.max(scores, axis=1, keepdims=True)
        weights = jnp.exp(scores - top)
        total = jnp.sum(weights, axis=1, keepdims=True)
        probs = (weights * (1.0 / total)).astype(jnp.bfloat16)
        save(0, b).start()
        save(1, b).start()
        o_ref[b] = lax.dot_general(probs, v_buf[b], (((1,), (1,)), ((), ())), preferred_element_type=jnp.float32).astype(jnp.bfloat16)
        return carry

    lax.fori_loop(0, rows, row, 0)
    for b in range(rows):
        save(0, b).wait()
        save(1, b).wait()


def attend(q_rot, cols, k_cache, v_cache, lengths):
    rows, heads, head_dim = q_rot.shape
    seq_len = k_cache.shape[1]
    k_t = jnp.swapaxes(k_cache, 1, 2)
    v_t = jnp.swapaxes(v_cache, 1, 2)
    cache = jax.ShapeDtypeStruct((rows, head_dim, seq_len), jnp.bfloat16)
    o, k_new, v_new = pl.pallas_call(
        functools.partial(attention_kernel, head_dim ** -0.5),
        out_shape=(jax.ShapeDtypeStruct((rows, heads, head_dim), jnp.bfloat16), cache, cache),
        in_specs=[
            pl.BlockSpec(memory_space=pltpu.SMEM),
            pl.BlockSpec(memory_space=pltpu.VMEM),
            pl.BlockSpec(memory_space=pltpu.VMEM),
            pl.BlockSpec(memory_space=pl.ANY),
            pl.BlockSpec(memory_space=pl.ANY),
        ],
        out_specs=(pl.BlockSpec(memory_space=pltpu.VMEM), pl.BlockSpec(memory_space=pl.ANY), pl.BlockSpec(memory_space=pl.ANY)),
        scratch_shapes=[
            pltpu.VMEM((rows, head_dim, seq_len), jnp.bfloat16),
            pltpu.VMEM((rows, head_dim, seq_len), jnp.bfloat16),
            pltpu.SemaphoreType.DMA((2, rows)),
            pltpu.SemaphoreType.DMA((2, rows)),
        ],
        compiler_params=pltpu.CompilerParams(vmem_limit_bytes=48 * 1024 * 1024),
        cost_estimate=pl.CostEstimate(
            flops=4 * rows * heads * head_dim * seq_len,
            bytes_accessed=8 * rows * head_dim * seq_len,
            transcendentals=rows * heads * seq_len,
        ),
        name='attend',
    )(lengths, q_rot, cols, k_t, v_t)
    return o, jnp.swapaxes(k_new, 1, 2), jnp.swapaxes(v_new, 1, 2)


def start_barrier(me_x, me_yz, everyone):
    barrier = pltpu.get_barrier_semaphore()
    peers = [(dx, k) for dx in range(2) for k in range(4) if (dx or k) and (everyone or not (dx and k))]
    for dx, k in peers:
        pl.semaphore_signal(barrier, inc=1, device_id=(lax.rem(me_x + dx, 2), lax.rem(me_yz + k, 4)), device_id_type=MESH)
    return lambda: pl.semaphore_wait(barrier, len(peers))


def spread(rows, cols, first):
    i = lax.broadcasted_iota(jnp.int32, (rows, cols), 0)
    c = lax.broadcasted_iota(jnp.int32, (rows, cols), 1)
    return jnp.where(c == 2 * i + first, 1.0, 0.0).astype(jnp.bfloat16)


def head_kernel(
    d_model, early, x_hbm, scale_hbm, wg_hbm, wa_hbm, z_hbm, first_hbm, send_hbm, own_hbm,
    xg, scale_row, sg, stats, h_buf, hx, wg, wa, z_send, z_own, z_recv, r_send, r_own, r_recv, zb, zg, g_first, g_rest, g_own,
    in_sem, wg_sem, x_send, x_recv, s_send, s_recv, t_send, t_recv, z_sems, a_send, a_recv, f_send, f_recv, out_sem,
):
    me_x = lax.axis_index('x')
    me_yz = lax.axis_index('yz')
    half, chunk = xg.shape[2:]
    rows = 2 * half
    pieces = wg_sem.shape[0]
    depth = wg.shape[0] // pieces
    ff = wg.shape[2]
    wide_cols = 256
    full = z_send.shape[2]
    quarter = half // 2
    third = quarter // 3
    tail_cols = wa.shape[0] - full
    other_x = lax.rem(me_x + 1, 2)
    across = lax.rem(me_yz + 2, 4)
    core = lax.rem(me_yz, 2)
    partner = me_yz + 1 - 2 * core
    order = (other_x, me_x)
    x_in = [
        pltpu.make_async_copy(x_hbm.at[pl.ds(pl.multiple_of(order[p] * half, 32), half)], xg.at[me_yz, order[p]], in_sem.at[p]) for p in range(2)
    ]
    scale_in = pltpu.make_async_copy(scale_hbm, scale_row, in_sem.at[2])
    wa_in = pltpu.make_async_copy(wa_hbm, wa, in_sem.at[3])
    wg_in = [
        pltpu.make_async_copy(wg_hbm.at[pl.ds(depth * i, depth)], wg.at[pl.ds(depth * i, depth)], wg_sem.at[i]) for i in range(pieces)
    ]
    for copy in (*x_in, scale_in, wa_in):
        copy.start()
    others_ready = start_barrier(me_x, me_yz, True)

    def remote(src, dst, send, recv, to_x, to_yz):
        return pltpu.make_async_remote_copy(
            src_ref=src, dst_ref=dst, send_sem=send, recv_sem=recv, device_id=(to_x, to_yz), device_id_type=MESH,
        )

    def x_copy(kind, piece):
        owner = across if kind == 2 else me_yz
        at = xg.at[owner, order[piece // 2], pl.ds(quarter * (piece % 2), quarter)]
        return remote(at, at, x_send.at[kind, piece], x_recv.at[kind, piece], me_x, across if kind == 1 else partner)

    for p in range(2):
        x_in[p].wait()
    lane = lax.broadcasted_iota(jnp.int32, (8, 128), 1)
    tile = jnp.zeros((8, 128), jnp.float32)
    for e in range(2):
        mine = xg[me_yz, e].astype(jnp.float32)
        sum_1 = jnp.sum(mine, axis=1, keepdims=True)
        sum_2 = jnp.sum(mine * mine, axis=1, keepdims=True)
        for j in range(half // 8):
            col = e * (half // 8) + j
            tile = jnp.where(lane == col, sum_1[8 * j:8 * j + 8], tile)
            tile = jnp.where(lane == 32 + col, sum_2[8 * j:8 * j + 8], tile)
    me = me_x * 4 + me_yz
    stats[me] = tile
    others_ready()
    t_out = [
        remote(stats.at[me], stats.at[me], t_send.at[4 * dx + k], t_recv.at[4 * dx + k], lax.rem(me_x + dx, 2), lax.rem(me_yz + k, 4))
        for dx in range(2) for k in range(4) if dx or k
    ]
    for copy in t_out:
        copy.start()
    scale_in.wait()
    sg[me_yz] = scale_row[...].reshape(1, chunk)
    s_out = [remote(sg.at[me_yz], sg.at[me_yz], s_send.at[k], s_recv.at[k], me_x, lax.rem(me_yz + k, 4)) for k in (1, 2, 3)]
    for copy in s_out:
        copy.start()
    for piece in range(4):
        x_copy(1, piece).start()
        x_copy(0, piece).start()
    for copy in wg_in:
        copy.start()
    wide, thin = spread(128, 256, 0), spread(64, 128, 0)
    wide_u, thin_u = spread(128, 256, 1), spread(64, 128, 1)
    for copy in t_out:
        copy.wait()
    total = stats[0]
    for i in range(1, 8):
        total = total + stats[i]
    mean_t = total / d_model
    var_t = pltpu.roll(total, 96, 1) / d_model - mean_t * mean_t
    rstd_t = lax.rsqrt(var_t + LN_EPS)
    for copy in s_out:
        copy.wait()

    chip = me_yz // 2
    contract = (((1,), (1,)), ((), ()))

    def pass_on(piece):
        x_copy(1, piece).wait()
        x_copy(2, piece).start()

    def project_chip(piece, which):
        p, q = piece // 2, piece % 2
        blocks = quarter // 8
        shift = lax.rem(256 - order[p] * (half // 8) - q * blocks, 128)
        mean_p = pltpu.roll(mean_t, shift, 1)
        rstd_p = pltpu.roll(rstd_t, shift, 1)
        mean = jnp.concatenate([mean_p[:, j:j + 1] for j in range(blocks)], axis=0)
        rstd = jnp.concatenate([rstd_p[:, j:j + 1] for j in range(blocks)], axis=0)
        here = pl.ds(quarter * q, quarter)
        both = []
        for e in range(2):
            s = 2 * which + e
            h = (xg[s, order[p], here].astype(jnp.float32) - mean) * rstd * sg[s]
            h_buf[s, here] = h.astype(jnp.bfloat16)
            both.append(h)
        h = jnp.concatenate(both, axis=1).astype(jnp.bfloat16)
        at = pl.ds(pl.multiple_of(2 * chunk * which, 128), 2 * chunk)
        z = lax.dot_general(h, wa[:full, at], contract, preferred_element_type=jnp.float32)
        r = lax.dot_general(h, wa[full:, at], contract, preferred_element_type=jnp.float32)
        return z, r

    def near(piece):
        x_copy(0, piece).wait()
        return project_chip(piece, chip)

    def far(piece, z, r, z_ref, r_ref):
        x_copy(2, piece).wait()
        z_far, r_far = project_chip(piece, 1 - chip)
        q = piece % 2
        z_ref[2 * q:2 * q + 2] = (z + z_far).reshape(2, quarter // 2, full)
        r = r + r_far
        r_ref[q] = jnp.concatenate([r[third * i:third * i + third] for i in range(3)], axis=1)

    def z_copies(q):
        at = pl.ds(2 * q, 2)
        return (
            remote(z_send.at[at], z_recv.at[at], z_sems.at[0, q], z_sems.at[1, q], other_x, me_yz),
            remote(r_send.at[q], r_recv.at[q], z_sems.at[2, q], z_sems.at[3, q], other_x, me_yz),
        )

    def spread_half(part, g):
        out = pl.ds((2 * part + g) * half, half)
        a, b = ((wide, thin), (wide_u, thin_u))[g]
        for s in range(4):
            base = 2 * chunk * s
            for t in range(2):
                piece = h_buf[s, :, 128 * t:128 * t + 128]
                hx[out, base + 256 * t:base + 256 * t + 256] = jnp.dot(piece, a, preferred_element_type=jnp.float32).astype(jnp.bfloat16)
            piece = h_buf[s, :, 256:320]
            hx[out, base + 512:base + 640] = jnp.dot(piece, b, preferred_element_type=jnp.float32).astype(jnp.bfloat16)

    wa_in.wait()
    z_out = [*z_copies(0), *z_copies(1)]
    pass_on(0)
    far(0, *near(0), z_send, r_send)
    z_out[0].start()
    z_out[1].start()
    pass_on(1)
    part_1 = near(1)
    pass_on(2)
    far(1, *part_1, z_send, r_send)
    z_out[2].start()
    z_out[3].start()
    pass_on(3)
    spread_half(0, 0)
    spread_half(0, 1)
    for copy in wg_in:
        copy.wait()

    def block(c):
        at = pl.ds(pl.multiple_of(c * wide_cols, wide_cols), wide_cols)
        return wg[:, :, at].reshape(2 * wg.shape[0], wide_cols)

    def keep_own(c, out):
        g_own[:, pl.ds(pl.multiple_of(c * wide_cols, wide_cols), wide_cols)] = out[:half]
        g_own[:, pl.ds(pl.multiple_of(ff + c * wide_cols, wide_cols), wide_cols)] = out[half:]

    first = []
    for c in range(early):
        out = jnp.dot(hx[:rows], block(c), preferred_element_type=jnp.float32)
        g_first[c, :, :wide_cols] = out[:half]
        g_first[c, :, wide_cols:] = out[half:]
        first.append(remote(g_first.at[c], first_hbm.at[c], f_send.at[c], f_recv.at[c], other_x, me_yz))
        first[-1].start()
    for piece in (2, 3):
        far(piece, *near(piece), z_own, r_own)
    spread_half(1, 0)
    spread_half(1, 1)
    for c in range(early):
        keep_own(c, jnp.dot(hx[rows:], block(c), preferred_element_type=jnp.float32))

    def rest(c, carry):
        out = jnp.dot(hx[...], block(c), preferred_element_type=jnp.float32)
        keep_own(c, out[rows:])
        at = (c - early) * wide_cols
        g_rest[:, pl.ds(pl.multiple_of(at, wide_cols), wide_cols)] = out[:half]
        g_rest[:, pl.ds(pl.multiple_of(ff - early * wide_cols + at, wide_cols), wide_cols)] = out[half:2 * half]
        return carry

    lax.fori_loop(early, ff // wide_cols, rest, 0)
    save = [pltpu.make_async_copy(g_rest, send_hbm, out_sem.at[0]), pltpu.make_async_copy(g_own, own_hbm, out_sem.at[1])]
    for copy in save:
        copy.start()
    for copy in z_out:
        copy.wait()
    zb[:, :, :full] = (z_own[...] + z_recv[...]).astype(jnp.bfloat16)
    for q in range(2):
        r = r_own[q] + r_recv[q]
        r = jnp.concatenate([r[:, tail_cols * i:tail_cols * i + tail_cols] for i in range(3)], axis=0)
        zb[2 * q:2 * q + 2, :, full:] = r.reshape(2, quarter // 2, tail_cols).astype(jnp.bfloat16)
    a_out = [remote(zb.at[lax.rem(me_yz + k, 4)], zg.at[me_yz], a_send.at[k], a_recv.at[k], me_x, lax.rem(me_yz + k, 4)) for k in (1, 2, 3)]
    for copy in a_out:
        copy.start()
    zg[me_yz] = zb[me_yz]
    for copy in a_out:
        copy.wait()
    save.append(pltpu.make_async_copy(zg, z_hbm, out_sem.at[2]))
    save[-1].start()
    for copy in first:
        copy.wait()
    for copy in save:
        copy.wait()


def head(x_in, ln_scale, w_gate_up, w_attn, d_model, early):
    rows, chunk = x_in.shape
    depth, _, ff = w_gate_up.shape
    z_cols = w_attn.shape[1]
    full = z_cols // 128 * 128
    owned = rows // 8
    half = rows // 2
    width = 2 * (ff - 256 * early)
    any_spec = pl.BlockSpec(memory_space=pl.ANY)
    dma = pltpu.SemaphoreType.DMA
    f32, bf16 = jnp.float32, jnp.bfloat16
    return pl.pallas_call(
        functools.partial(head_kernel, d_model, early),
        out_shape=(
            jax.ShapeDtypeStruct((4, owned, z_cols), bf16),
            jax.ShapeDtypeStruct((early, half, 512), f32),
            jax.ShapeDtypeStruct((half, width), f32),
            jax.ShapeDtypeStruct((half, 2 * ff), f32),
        ),
        in_specs=[any_spec] * 4,
        out_specs=[any_spec] * 4,
        scratch_shapes=[
            pltpu.VMEM((4, 2, half, chunk), bf16),
            pltpu.VMEM((chunk,), f32),
            pltpu.VMEM((4, 1, chunk), f32),
            pltpu.VMEM((8, 8, 128), f32),
            pltpu.VMEM((4, half, chunk), bf16),
            pltpu.VMEM((2 * rows, 2 * depth), bf16),
            pltpu.VMEM((depth, 2, ff), bf16),
            pltpu.VMEM((z_cols, depth), bf16),
            *[pltpu.VMEM((4, owned, full), f32)] * 3,
            *[pltpu.VMEM((2, half // 6, 3 * (z_cols - full)), f32)] * 3,
            pltpu.VMEM((4, owned, z_cols), bf16),
            pltpu.VMEM((4, owned, z_cols), bf16),
            pltpu.VMEM((early, half, 512), f32),
            pltpu.VMEM((half, width), f32),
            pltpu.VMEM((half, 2 * ff), f32),
            dma((4,)), dma((8,)), dma((3, 4)), dma((3, 4)), dma((4,)), dma((4,)), dma((8,)), dma((8,)), dma((4, 2)), dma((4,)), dma((4,)),
            dma((early,)), dma((early,)), dma((3,)),
        ],
        compiler_params=pltpu.CompilerParams(collective_id=0, has_side_effects=True, vmem_limit_bytes=VMEM_MOST),
        cost_estimate=pl.CostEstimate(flops=4 * rows * depth * 2 * ff, bytes_accessed=4 * depth * ff, transcendentals=0),
        name='head',
    )(x_in, ln_scale, w_gate_up, w_attn.T)


def tail_kernel(
    g_first, g_peer, own_hbm, ov, wd_hbm, wo_hbm, y_ref,
    g_own, oy, oa, of, hb, wd, wo, out_part, y_send, y_pair, y_over, y_recv,
    in_sem, own_sem, o_send, o_recv, h_send, h_recv, p_send, p_recv, y_ssem, y_rsem,
):
    me_x = lax.axis_index('x')
    me_yz = lax.axis_index('yz')
    groups, _, span, ff = hb.shape
    rows, chunk = y_ref.shape
    half = rows // 2
    owned = ov.shape[1]
    early, _, wide = g_first.shape
    wide = wide // 2
    core = lax.rem(me_yz, 2)
    col = me_yz // 2
    partner = me_yz + 1 - 2 * core
    across = lax.rem(me_yz + 2, 4)
    other_x = lax.rem(me_x + 1, 2)

    own_in = [pltpu.make_async_copy(own_hbm.at[pl.ds(span * i, span)], g_own.at[pl.ds(span * i, span)], own_sem.at[i]) for i in range(groups)]
    wo_in = pltpu.make_async_copy(wo_hbm, wo, in_sem.at[1])
    wd_in = pltpu.make_async_copy(wd_hbm, wd, in_sem.at[2])
    for copy in (*own_in, wo_in, wd_in):
        copy.start()
    start_barrier(me_x, me_yz, False)()
    me = me_x * 4 + me_yz

    def remote(src, dst, send, recv, to_x, to_yz):
        return pltpu.make_async_remote_copy(
            src_ref=src, dst_ref=dst, send_sem=send, recv_sem=recv, device_id=(to_x, to_yz), device_id_type=MESH,
        )

    other = other_x * 4 + me_yz
    o_over = remote(ov, oy, o_send.at[0], o_recv.at[0], other_x, me_yz)
    o_over.start()
    there = [lax.rem(me_yz + k, 4) for k in range(4)]
    o_out = [remote(ov.at[there[k]], oa.at[me], o_send.at[k], o_recv.at[k], me_x, there[k]) for k in (1, 2, 3)]
    for copy in o_out:
        copy.start()
    oa[me] = ov[me_yz]

    def h_copy(i):
        return remote(hb.at[i, me_x], hb.at[i, me_x], h_send.at[i], h_recv.at[i], other_x, me_yz)

    for copy in own_in:
        copy.wait()

    def activate(i, carry):
        at = pl.ds(pl.multiple_of(span * i, span), span)

        def act(gate, up):
            gate = gate.astype(jnp.bfloat16).astype(jnp.float32)
            up = up.astype(jnp.bfloat16).astype(jnp.float32)
            return (jax.nn.silu(gate) * up).astype(jnp.bfloat16)

        for c in range(early):
            cols = slice(wide * c, wide * c + wide)
            up_cols = slice(ff + wide * c, ff + wide * c + wide)
            hb[i, me_x, :, cols] = act(g_own[at, cols] + g_first[c, at, :wide], g_own[at, up_cols] + g_first[c, at, wide:])
        done = early * wide
        hb[i, me_x, :, done:] = act(g_own[at, done:ff] + g_peer[at, :ff - done], g_own[at, ff + done:] + g_peer[at, ff - done:])
        h_copy(i).start()
        return carry

    lax.fori_loop(0, groups, activate, 0)
    o_over.wait()
    relay = [remote(oy.at[there[k]], oa.at[other], o_send.at[3 + k], o_recv.at[3 + k], me_x, there[k]) for k in (1, 2, 3)]
    for copy in relay:
        copy.start()
    oa[other] = oy[me_yz]
    for copy in (*o_out, *relay):
        copy.wait()
    for e in range(8):
        of[owned * e:owned * e + owned] = oa[e].astype(jnp.float32)
    wo_in.wait()
    out_part[...] = jnp.dot(of[...].astype(jnp.bfloat16), wo[...], preferred_element_type=jnp.float32)
    wd_in.wait()

    def pair_copy(i, which):
        return remote(y_send.at[i, 2 * which + 1 - core], y_pair.at[i, which], p_send.at[i, which], p_recv.at[i, which], me_x, partner)

    def over_copy(i):
        return remote(y_over.at[i], y_recv.at[i], y_ssem.at[i], y_rsem.at[i], me_x, across)

    def cross(i):
        pair_copy(i, 1 - col).wait()
        y_over[i] = y_send[i, across] + y_pair[i, 1 - col]
        over_copy(i).start()

    def product(i, carry):
        h_copy(i).wait()
        first_at = pl.multiple_of(span * i, span)
        part = jnp.dot(hb[i].reshape(2 * span, ff), wd[...], preferred_element_type=jnp.float32)
        part = part + jnp.concatenate([out_part[pl.ds(first_at, span)], out_part[pl.ds(half + first_at, span)]], axis=0)
        for j in range(4):
            moved = part if j == 0 else pltpu.roll(part, (4 - j) * chunk, 1)
            y_send[i, j] = moved[:, :chunk]
        for which in (1 - col, col):
            pair_copy(i, which).start()

        @pl.when(i > 0)
        def _():
            cross(i - 1)

        return carry

    def finish(i, carry):
        pair_copy(i, col).wait()
        over_copy(i).wait()
        total = y_send[i, me_yz] + y_pair[i, col] + y_recv[i]
        for e in range(2):
            y_ref[pl.ds(pl.multiple_of(half * e + span * i, span), span), :] = total[span * e:span * e + span]
        return carry

    lax.fori_loop(0, groups, product, 0)
    lax.fori_loop(0, groups - 3, finish, 0)
    cross(groups - 1)
    lax.fori_loop(groups - 3, groups, finish, 0)


def tail(g_first, g_peer, g_own, o_blocks, w_down, w_out):
    half = g_own.shape[0]
    rows = 2 * half
    span = 16
    groups = half // span
    ff, cols = w_down.shape
    chunk = cols // 4
    owned = o_blocks.shape[1]
    o_width = w_out.shape[0]
    any_spec, vmem_spec = pl.BlockSpec(memory_space=pl.ANY), pl.BlockSpec(memory_space=pltpu.VMEM)
    dma = pltpu.SemaphoreType.DMA
    f32, bf16 = jnp.float32, jnp.bfloat16
    return pl.pallas_call(
        tail_kernel,
        out_shape=jax.ShapeDtypeStruct((rows, chunk), f32),
        in_specs=[vmem_spec, vmem_spec, any_spec, vmem_spec, any_spec, any_spec],
        out_specs=pl.BlockSpec(memory_space=pltpu.VMEM),
        scratch_shapes=[
            pltpu.VMEM((half, 2 * ff), f32),
            pltpu.VMEM((4, owned, o_width), bf16),
            pltpu.VMEM((8, owned, o_width), bf16),
            pltpu.VMEM((rows, o_width), f32),
            pltpu.VMEM((groups, 2, span, ff), bf16),
            pltpu.VMEM((ff, cols), bf16),
            pltpu.VMEM((o_width, cols), bf16),
            pltpu.VMEM((rows, cols), f32),
            pltpu.VMEM((groups, 4, 2 * span, chunk), f32),
            pltpu.VMEM((groups, 2, 2 * span, chunk), f32),
            pltpu.VMEM((groups, 2 * span, chunk), f32),
            pltpu.VMEM((groups, 2 * span, chunk), f32),
            dma((3,)), dma((groups,)), dma((8,)), dma((8,)), dma((groups,)), dma((groups,)),
            dma((groups, 2)), dma((groups, 2)), dma((groups,)), dma((groups,)),
        ],
        compiler_params=pltpu.CompilerParams(collective_id=1, has_side_effects=True, vmem_limit_bytes=51 * 1024 * 1024),
        cost_estimate=pl.CostEstimate(flops=2 * rows * (ff + o_width) * cols, bytes_accessed=2 * (ff + o_width) * cols, transcendentals=half * ff),
        name='tail',
    )(g_first, g_peer, g_own, o_blocks, w_down, w_out)


def rotary(values, positions):
    half_dim = values.shape[-1] // 2
    inv_freq = ROPE_BASE ** (-jnp.arange(half_dim, dtype=jnp.float32) / half_dim)
    angles = positions.astype(jnp.float32)[:, None, None] * inv_freq
    cos_part = jnp.cos(angles)
    sin_part = jnp.sin(angles)
    lo_half = values[..., :half_dim]
    hi_half = values[..., half_dim:]
    return jnp.concatenate([lo_half * cos_part - hi_half * sin_part, hi_half * cos_part + lo_half * sin_part], axis=-1)


def solution(mesh):
    x_size = mesh.shape['x']
    yz_size = mesh.shape['yz']
    all_axes = ('x', 'yz')

    def local_step(x_in, ln_scale, w_gate_up, w_attn, w_down, w_out, k_cache, v_cache, lengths, positions):
        local_rows, seq_len, head_dim = k_cache.shape
        q_width = w_out.shape[0] * yz_size
        num_heads = q_width // head_dim
        d_model = x_in.shape[1] * x_size * yz_size
        z_blocks, g_first, g_send, g_own = head(x_in, ln_scale, w_gate_up, w_attn, d_model, EARLY)
        g_peer = lax.ppermute(g_send, 'x', [(0, 1), (1, 0)])
        proj_local = z_blocks.transpose(1, 0, 2).reshape(local_rows, -1)
        q_raw = proj_local[:, :q_width].reshape(local_rows, num_heads, head_dim)
        k_tok = proj_local[:, q_width:q_width + head_dim]
        v_tok = proj_local[:, q_width + head_dim:]
        q_rot = rotary(q_raw.astype(jnp.float32), positions).astype(jnp.bfloat16)
        k_rot = rotary(k_tok[:, None, :].astype(jnp.float32), positions)[:, 0].astype(jnp.bfloat16)
        cols = jnp.stack([k_rot, v_tok]).astype(jnp.float32).transpose(0, 2, 1)
        cols = jnp.pad(cols, ((0, 0), (0, 0), (0, 128 - local_rows)))
        attn_out, k_new, v_new = attend(q_rot, cols, k_cache, v_cache, lengths)
        o_blocks = attn_out.reshape(local_rows, yz_size, q_width // yz_size).transpose(1, 0, 2)
        mixed_sum = tail(g_first, g_peer, g_own, o_blocks, w_down, w_out)
        y_out = (x_in.astype(jnp.float32) + mixed_sum).astype(jnp.bfloat16)
        return y_out, k_new, v_new

    row_spec = P(None, all_axes)
    vec_spec = P(all_axes)
    cache_spec = P(all_axes, None, None)
    return jax.shard_map(
        local_step,
        mesh=mesh,
        in_specs=(row_spec, vec_spec, P('x', None, 'yz'), P('x', 'yz'), P('yz', 'x'), P('yz', 'x'), cache_spec, cache_spec, vec_spec, vec_spec),
        out_specs=(row_spec, cache_spec, cache_spec),
        check_vma=False,
    )
```

```python
import functools

import jax
import jax.numpy as jnp
from jax import lax
from jax.experimental import pallas as pl
from jax.experimental.pallas import tpu as pltpu
from jax.sharding import PartitionSpec as P

LN_EPS = 1e-6
ROPE_BASE = 10000.0
MESH = pl.DeviceIdType.MESH
VMEM_MOST = 64 * 1024 * 1024 - 64 * 1024
EARLY = 2


def attention_kernel(scale, len_ref, q_ref, cols_ref, k_hbm, v_hbm, o_ref, ko_hbm, vo_hbm, k_buf, v_buf, in_sem, out_sem):
    rows, _, seq_len = k_buf.shape

    def load(which, b):
        src, dst = ((k_hbm, k_buf), (v_hbm, v_buf))[which]
        return pltpu.make_async_copy(src.at[b], dst.at[b], in_sem.at[which, b])

    def save(which, b):
        src, dst = ((k_buf, ko_hbm), (v_buf, vo_hbm))[which]
        return pltpu.make_async_copy(src.at[b], dst.at[b], out_sem.at[which, b])

    for b in range(rows):
        load(0, b).start()
        load(1, b).start()

    lane = lax.broadcasted_iota(jnp.int32, (1, 128), 1)
    slots = lax.broadcasted_iota(jnp.int32, (1, seq_len), 1)

    def row(b, carry):
        length = len_ref[b]
        window = pl.ds(pl.multiple_of((length // 128) * 128, 128), 128)
        here = lane == length % 128
        for which, buf in enumerate((k_buf, v_buf)):
            load(which, b).wait()
            col = jnp.sum(jnp.where(lane == b, cols_ref[which], 0.0), axis=1, keepdims=True)
            tile = buf[b, :, window].astype(jnp.float32)
            buf[b, :, window] = jnp.where(here, col, tile).astype(jnp.bfloat16)
        scores = jnp.dot(q_ref[b], k_buf[b], preferred_element_type=jnp.float32) * scale
        scores = jnp.where(slots <= length, scores, -1e30)
        top = jnp.max(scores, axis=1, keepdims=True)
        weights = jnp.exp(scores - top)
        total = jnp.sum(weights, axis=1, keepdims=True)
        probs = (weights * (1.0 / total)).astype(jnp.bfloat16)
        save(0, b).start()
        save(1, b).start()
        o_ref[b] = lax.dot_general(probs, v_buf[b], (((1,), (1,)), ((), ())), preferred_element_type=jnp.float32).astype(jnp.bfloat16)
        return carry

    lax.fori_loop(0, rows, row, 0)
    for b in range(rows):
        save(0, b).wait()
        save(1, b).wait()


def attend(q_rot, cols, k_cache, v_cache, lengths):
    rows, heads, head_dim = q_rot.shape
    seq_len = k_cache.shape[1]
    k_t = jnp.swapaxes(k_cache, 1, 2)
    v_t = jnp.swapaxes(v_cache, 1, 2)
    cache = jax.ShapeDtypeStruct((rows, head_dim, seq_len), jnp.bfloat16)
    o, k_new, v_new = pl.pallas_call(
        functools.partial(attention_kernel, head_dim ** -0.5),
        out_shape=(jax.ShapeDtypeStruct((rows, heads, head_dim), jnp.bfloat16), cache, cache),
        in_specs=[
            pl.BlockSpec(memory_space=pltpu.SMEM),
            pl.BlockSpec(memory_space=pltpu.VMEM),
            pl.BlockSpec(memory_space=pltpu.VMEM),
            pl.BlockSpec(memory_space=pl.ANY),
            pl.BlockSpec(memory_space=pl.ANY),
        ],
        out_specs=(pl.BlockSpec(memory_space=pltpu.VMEM), pl.BlockSpec(memory_space=pl.ANY), pl.BlockSpec(memory_space=pl.ANY)),
        scratch_shapes=[
            pltpu.VMEM((rows, head_dim, seq_len), jnp.bfloat16),
            pltpu.VMEM((rows, head_dim, seq_len), jnp.bfloat16),
            pltpu.SemaphoreType.DMA((2, rows)),
            pltpu.SemaphoreType.DMA((2, rows)),
        ],
        compiler_params=pltpu.CompilerParams(vmem_limit_bytes=48 * 1024 * 1024),
        cost_estimate=pl.CostEstimate(
            flops=4 * rows * heads * head_dim * seq_len,
            bytes_accessed=8 * rows * head_dim * seq_len,
            transcendentals=rows * heads * seq_len,
        ),
        name='attend',
    )(lengths, q_rot, cols, k_t, v_t)
    return o, jnp.swapaxes(k_new, 1, 2), jnp.swapaxes(v_new, 1, 2)


def start_barrier(me_x, me_yz, everyone):
    barrier = pltpu.get_barrier_semaphore()
    peers = [(dx, k) for dx in range(2) for k in range(4) if (dx or k) and (everyone or not (dx and k))]
    for dx, k in peers:
        pl.semaphore_signal(barrier, inc=1, device_id=(lax.rem(me_x + dx, 2), lax.rem(me_yz + k, 4)), device_id_type=MESH)
    return lambda: pl.semaphore_wait(barrier, len(peers))


def spread(rows, cols, first):
    i = lax.broadcasted_iota(jnp.int32, (rows, cols), 0)
    c = lax.broadcasted_iota(jnp.int32, (rows, cols), 1)
    return jnp.where(c == 2 * i + first, 1.0, 0.0).astype(jnp.bfloat16)


def head_kernel(
    d_model, early, x_hbm, scale_hbm, wg_hbm, wa_hbm, z_hbm, first_hbm, send_hbm, own_hbm,
    xg, scale_row, sg, stats, h_buf, hx, wg, wa, z_send, z_own, z_recv, r_send, r_own, r_recv, zb, zg, g_first, g_rest, g_own,
    in_sem, wg_sem, x_send, x_recv, s_send, s_recv, t_send, t_recv, z_sems, a_send, a_recv, f_send, f_recv, out_sem,
):
    me_x = lax.axis_index('x')
    me_yz = lax.axis_index('yz')
    half, chunk = xg.shape[2:]
    rows = 2 * half
    pieces = wg_sem.shape[0]
    depth = wg.shape[0] // pieces
    ff = wg.shape[2]
    wide_cols = 256
    full = z_send.shape[2]
    quarter = half // 2
    third = quarter // 3
    tail_cols = wa.shape[0] - full
    other_x = lax.rem(me_x + 1, 2)
    across = lax.rem(me_yz + 2, 4)
    core = lax.rem(me_yz, 2)
    partner = me_yz + 1 - 2 * core
    order = (other_x, me_x)
    x_in = [
        pltpu.make_async_copy(x_hbm.at[pl.ds(pl.multiple_of(order[p] * half, 32), half)], xg.at[me_yz, order[p]], in_sem.at[p]) for p in range(2)
    ]
    scale_in = pltpu.make_async_copy(scale_hbm, scale_row, in_sem.at[2])
    wa_in = pltpu.make_async_copy(wa_hbm, wa, in_sem.at[3])
    wg_in = [
        pltpu.make_async_copy(wg_hbm.at[pl.ds(depth * i, depth)], wg.at[pl.ds(depth * i, depth)], wg_sem.at[i]) for i in range(pieces)
    ]
    for copy in (*x_in, scale_in, wa_in):
        copy.start()
    others_ready = start_barrier(me_x, me_yz, True)

    def remote(src, dst, send, recv, to_x, to_yz):
        return pltpu.make_async_remote_copy(
            src_ref=src, dst_ref=dst, send_sem=send, recv_sem=recv, device_id=(to_x, to_yz), device_id_type=MESH,
        )

    def x_copy(kind, piece):
        owner = across if kind == 2 else me_yz
        at = xg.at[owner, order[piece // 2], pl.ds(quarter * (piece % 2), quarter)]
        return remote(at, at, x_send.at[kind, piece], x_recv.at[kind, piece], me_x, across if kind == 1 else partner)

    for p in range(2):
        x_in[p].wait()
    lane = lax.broadcasted_iota(jnp.int32, (8, 128), 1)
    tile = jnp.zeros((8, 128), jnp.float32)
    for e in range(2):
        mine = xg[me_yz, e].astype(jnp.float32)
        sum_1 = jnp.sum(mine, axis=1, keepdims=True)
        sum_2 = jnp.sum(mine * mine, axis=1, keepdims=True)
        for j in range(half // 8):
            col = e * (half // 8) + j
            tile = jnp.where(lane == col, sum_1[8 * j:8 * j + 8], tile)
            tile = jnp.where(lane == 32 + col, sum_2[8 * j:8 * j + 8], tile)
    me = me_x * 4 + me_yz
    stats[me] = tile
    others_ready()
    t_out = [
        remote(stats.at[me], stats.at[me], t_send.at[4 * dx + k], t_recv.at[4 * dx + k], lax.rem(me_x + dx, 2), lax.rem(me_yz + k, 4))
        for dx in range(2) for k in range(4) if dx or k
    ]
    for copy in t_out:
        copy.start()
    scale_in.wait()
    sg[me_yz] = scale_row[...].reshape(1, chunk)
    s_out = [remote(sg.at[me_yz], sg.at[me_yz], s_send.at[k], s_recv.at[k], me_x, lax.rem(me_yz + k, 4)) for k in (1, 2, 3)]
    for copy in s_out:
        copy.start()
    for piece in range(4):
        x_copy(1, piece).start()
        x_copy(0, piece).start()
    for copy in wg_in:
        copy.start()
    wide, thin = spread(128, 256, 0), spread(64, 128, 0)
    wide_u, thin_u = spread(128, 256, 1), spread(64, 128, 1)
    for copy in t_out:
        copy.wait()
    total = stats[0]
    for i in range(1, 8):
        total = total + stats[i]
    mean_t = total / d_model
    var_t = pltpu.roll(total, 96, 1) / d_model - mean_t * mean_t
    rstd_t = lax.rsqrt(var_t + LN_EPS)
    for copy in s_out:
        copy.wait()

    chip = me_yz // 2
    contract = (((1,), (1,)), ((), ()))

    def pass_on(piece):
        x_copy(1, piece).wait()
        x_copy(2, piece).start()

    def project_chip(piece, which):
        p, q = piece // 2, piece % 2
        blocks = quarter // 8
        shift = lax.rem(256 - order[p] * (half // 8) - q * blocks, 128)
        mean_p = pltpu.roll(mean_t, shift, 1)
        rstd_p = pltpu.roll(rstd_t, shift, 1)
        mean = jnp.concatenate([mean_p[:, j:j + 1] for j in range(blocks)], axis=0)
        rstd = jnp.concatenate([rstd_p[:, j:j + 1] for j in range(blocks)], axis=0)
        here = pl.ds(quarter * q, quarter)
        both = []
        for e in range(2):
            s = 2 * which + e
            h = (xg[s, order[p], here].astype(jnp.float32) - mean) * rstd * sg[s]
            h_buf[s, here] = h.astype(jnp.bfloat16)
            both.append(h)
        h = jnp.concatenate(both, axis=1).astype(jnp.bfloat16)
        at = pl.ds(pl.multiple_of(2 * chunk * which, 128), 2 * chunk)
        z = lax.dot_general(h, wa[:full, at], contract, preferred_element_type=jnp.float32)
        r = lax.dot_general(h, wa[full:, at], contract, preferred_element_type=jnp.float32)
        return z, r

    def near(piece):
        x_copy(0, piece).wait()
        return project_chip(piece, chip)

    def far(piece, z, r, z_ref, r_ref):
        x_copy(2, piece).wait()
        z_far, r_far = project_chip(piece, 1 - chip)
        q = piece % 2
        z_ref[2 * q:2 * q + 2] = (z + z_far).reshape(2, quarter // 2, full)
        r = r + r_far
        r_ref[q] = jnp.concatenate([r[third * i:third * i + third] for i in range(3)], axis=1)

    def z_copies(q):
        at = pl.ds(2 * q, 2)
        return (
            remote(z_send.at[at], z_recv.at[at], z_sems.at[0, q], z_sems.at[1, q], other_x, me_yz),
            remote(r_send.at[q], r_recv.at[q], z_sems.at[2, q], z_sems.at[3, q], other_x, me_yz),
        )

    def spread_half(part, g):
        out = pl.ds((2 * part + g) * half, half)
        a, b = ((wide, thin), (wide_u, thin_u))[g]
        for s in range(4):
            base = 2 * chunk * s
            for t in range(2):
                piece = h_buf[s, :, 128 * t:128 * t + 128]
                hx[out, base + 256 * t:base + 256 * t + 256] = jnp.dot(piece, a, preferred_element_type=jnp.float32).astype(jnp.bfloat16)
            piece = h_buf[s, :, 256:320]
            hx[out, base + 512:base + 640] = jnp.dot(piece, b, preferred_element_type=jnp.float32).astype(jnp.bfloat16)

    wa_in.wait()
    z_out = [*z_copies(0), *z_copies(1)]
    pass_on(0)
    far(0, *near(0), z_send, r_send)
    z_out[0].start()
    z_out[1].start()
    pass_on(1)
    part_1 = near(1)
    pass_on(2)
    far(1, *part_1, z_send, r_send)
    z_out[2].start()
    z_out[3].start()
    pass_on(3)
    spread_half(0, 0)
    spread_half(0, 1)
    for copy in wg_in:
        copy.wait()

    def block(c):
        at = pl.ds(pl.multiple_of(c * wide_cols, wide_cols), wide_cols)
        return wg[:, :, at].reshape(2 * wg.shape[0], wide_cols)

    def keep_own(c, out):
        g_own[:, pl.ds(pl.multiple_of(c * wide_cols, wide_cols), wide_cols)] = out[:half]
        g_own[:, pl.ds(pl.multiple_of(ff + c * wide_cols, wide_cols), wide_cols)] = out[half:]

    first = []
    for c in range(early):
        out = jnp.dot(hx[:rows], block(c), preferred_element_type=jnp.float32)
        g_first[c, :, :wide_cols] = out[:half]
        g_first[c, :, wide_cols:] = out[half:]
        first.append(remote(g_first.at[c], first_hbm.at[c], f_send.at[c], f_recv.at[c], other_x, me_yz))
        first[-1].start()
    for piece in (2, 3):
        far(piece, *near(piece), z_own, r_own)
    spread_half(1, 0)
    spread_half(1, 1)
    for c in range(early):
        keep_own(c, jnp.dot(hx[rows:], block(c), preferred_element_type=jnp.float32))

    def rest(c, carry):
        out = jnp.dot(hx[...], block(c), preferred_element_type=jnp.float32)
        keep_own(c, out[rows:])
        at = (c - early) * wide_cols
        g_rest[:, pl.ds(pl.multiple_of(at, wide_cols), wide_cols)] = out[:half]
        g_rest[:, pl.ds(pl.multiple_of(ff - early * wide_cols + at, wide_cols), wide_cols)] = out[half:2 * half]
        return carry

    middle = early + 4
    lax.fori_loop(early, middle, rest, 0)
    for copy in z_out:
        copy.wait()
    zb[:, :, :full] = (z_own[...] + z_recv[...]).astype(jnp.bfloat16)
    for q in range(2):
        r = r_own[q] + r_recv[q]
        r = jnp.concatenate([r[:, tail_cols * i:tail_cols * i + tail_cols] for i in range(3)], axis=0)
        zb[2 * q:2 * q + 2, :, full:] = r.reshape(2, quarter // 2, tail_cols).astype(jnp.bfloat16)
    a_out = [remote(zb.at[lax.rem(me_yz + k, 4)], zg.at[me_yz], a_send.at[k], a_recv.at[k], me_x, lax.rem(me_yz + k, 4)) for k in (1, 2, 3)]
    for copy in a_out:
        copy.start()
    zg[me_yz] = zb[me_yz]
    lax.fori_loop(middle, ff // wide_cols, rest, 0)
    save = [pltpu.make_async_copy(g_rest, send_hbm, out_sem.at[0]), pltpu.make_async_copy(g_own, own_hbm, out_sem.at[1])]
    for copy in save:
        copy.start()
    for copy in a_out:
        copy.wait()
    save.append(pltpu.make_async_copy(zg, z_hbm, out_sem.at[2]))
    save[-1].start()
    for copy in first:
        copy.wait()
    for copy in save:
        copy.wait()


def head(x_in, ln_scale, w_gate_up, w_attn, d_model, early):
    rows, chunk = x_in.shape
    depth, _, ff = w_gate_up.shape
    z_cols = w_attn.shape[1]
    full = z_cols // 128 * 128
    owned = rows // 8
    half = rows // 2
    width = 2 * (ff - 256 * early)
    any_spec = pl.BlockSpec(memory_space=pl.ANY)
    dma = pltpu.SemaphoreType.DMA
    f32, bf16 = jnp.float32, jnp.bfloat16
    return pl.pallas_call(
        functools.partial(head_kernel, d_model, early),
        out_shape=(
            jax.ShapeDtypeStruct((4, owned, z_cols), bf16),
            jax.ShapeDtypeStruct((early, half, 512), f32),
            jax.ShapeDtypeStruct((half, width), f32),
            jax.ShapeDtypeStruct((half, 2 * ff), f32),
        ),
        in_specs=[any_spec] * 4,
        out_specs=[any_spec] * 4,
        scratch_shapes=[
            pltpu.VMEM((4, 2, half, chunk), bf16),
            pltpu.VMEM((chunk,), f32),
            pltpu.VMEM((4, 1, chunk), f32),
            pltpu.VMEM((8, 8, 128), f32),
            pltpu.VMEM((4, half, chunk), bf16),
            pltpu.VMEM((2 * rows, 2 * depth), bf16),
            pltpu.VMEM((depth, 2, ff), bf16),
            pltpu.VMEM((z_cols, depth), bf16),
            *[pltpu.VMEM((4, owned, full), f32)] * 3,
            *[pltpu.VMEM((2, half // 6, 3 * (z_cols - full)), f32)] * 3,
            pltpu.VMEM((4, owned, z_cols), bf16),
            pltpu.VMEM((4, owned, z_cols), bf16),
            pltpu.VMEM((early, half, 512), f32),
            pltpu.VMEM((half, width), f32),
            pltpu.VMEM((half, 2 * ff), f32),
            dma((4,)), dma((8,)), dma((3, 4)), dma((3, 4)), dma((4,)), dma((4,)), dma((8,)), dma((8,)), dma((4, 2)), dma((4,)), dma((4,)),
            dma((early,)), dma((early,)), dma((3,)),
        ],
        compiler_params=pltpu.CompilerParams(collective_id=0, has_side_effects=True, vmem_limit_bytes=VMEM_MOST),
        cost_estimate=pl.CostEstimate(flops=4 * rows * depth * 2 * ff, bytes_accessed=4 * depth * ff, transcendentals=0),
        name='head',
    )(x_in, ln_scale, w_gate_up, w_attn.T)


def tail_kernel(
    g_first, g_peer, own_hbm, ov, wd_hbm, wo_hbm, y_ref,
    g_own, oy, oa, of, hb, wd, wo, out_part, y_send, y_pair, y_over, y_recv,
    in_sem, own_sem, o_send, o_recv, h_send, h_recv, p_send, p_recv, y_ssem, y_rsem,
):
    me_x = lax.axis_index('x')
    me_yz = lax.axis_index('yz')
    groups, _, span, ff = hb.shape
    rows, chunk = y_ref.shape
    half = rows // 2
    owned = ov.shape[1]
    early, _, wide = g_first.shape
    wide = wide // 2
    core = lax.rem(me_yz, 2)
    col = me_yz // 2
    partner = me_yz + 1 - 2 * core
    across = lax.rem(me_yz + 2, 4)
    other_x = lax.rem(me_x + 1, 2)

    own_in = [pltpu.make_async_copy(own_hbm.at[pl.ds(span * i, span)], g_own.at[pl.ds(span * i, span)], own_sem.at[i]) for i in range(groups)]
    wo_in = pltpu.make_async_copy(wo_hbm, wo, in_sem.at[1])
    wd_in = pltpu.make_async_copy(wd_hbm, wd, in_sem.at[2])
    for copy in (*own_in, wo_in, wd_in):
        copy.start()
    start_barrier(me_x, me_yz, False)()
    me = me_x * 4 + me_yz

    def remote(src, dst, send, recv, to_x, to_yz):
        return pltpu.make_async_remote_copy(
            src_ref=src, dst_ref=dst, send_sem=send, recv_sem=recv, device_id=(to_x, to_yz), device_id_type=MESH,
        )

    other = other_x * 4 + me_yz
    o_over = remote(ov, oy, o_send.at[0], o_recv.at[0], other_x, me_yz)
    o_over.start()
    there = [lax.rem(me_yz + k, 4) for k in range(4)]
    o_out = [remote(ov.at[there[k]], oa.at[me], o_send.at[k], o_recv.at[k], me_x, there[k]) for k in (1, 2, 3)]
    for copy in o_out:
        copy.start()
    oa[me] = ov[me_yz]

    def h_copy(i):
        return remote(hb.at[i, me_x], hb.at[i, me_x], h_send.at[i], h_recv.at[i], other_x, me_yz)

    for copy in own_in:
        copy.wait()

    def activate(i, carry):
        at = pl.ds(pl.multiple_of(span * i, span), span)

        def act(gate, up):
            gate = gate.astype(jnp.bfloat16).astype(jnp.float32)
            up = up.astype(jnp.bfloat16).astype(jnp.float32)
            return (jax.nn.silu(gate) * up).astype(jnp.bfloat16)

        for c in range(early):
            cols = slice(wide * c, wide * c + wide)
            up_cols = slice(ff + wide * c, ff + wide * c + wide)
            hb[i, me_x, :, cols] = act(g_own[at, cols] + g_first[c, at, :wide], g_own[at, up_cols] + g_first[c, at, wide:])
        done = early * wide
        hb[i, me_x, :, done:] = act(g_own[at, done:ff] + g_peer[at, :ff - done], g_own[at, ff + done:] + g_peer[at, ff - done:])
        h_copy(i).start()
        return carry

    lax.fori_loop(0, groups, activate, 0)
    o_over.wait()
    relay = [remote(oy.at[there[k]], oa.at[other], o_send.at[3 + k], o_recv.at[3 + k], me_x, there[k]) for k in (1, 2, 3)]
    for copy in relay:
        copy.start()
    oa[other] = oy[me_yz]
    for copy in (*o_out, *relay):
        copy.wait()
    for e in range(8):
        of[owned * e:owned * e + owned] = oa[e].astype(jnp.float32)
    wo_in.wait()
    out_part[...] = jnp.dot(of[...].astype(jnp.bfloat16), wo[...], preferred_element_type=jnp.float32)
    wd_in.wait()

    def pair_copy(i, which):
        return remote(y_send.at[i, 2 * which + 1 - core], y_pair.at[i, which], p_send.at[i, which], p_recv.at[i, which], me_x, partner)

    def over_copy(i):
        return remote(y_over.at[i], y_recv.at[i], y_ssem.at[i], y_rsem.at[i], me_x, across)

    def cross(i):
        pair_copy(i, 1 - col).wait()
        y_over[i] = y_send[i, across] + y_pair[i, 1 - col]
        over_copy(i).start()

    def product(i, carry):
        h_copy(i).wait()
        first_at = pl.multiple_of(span * i, span)
        part = jnp.dot(hb[i].reshape(2 * span, ff), wd[...], preferred_element_type=jnp.float32)
        part = part + jnp.concatenate([out_part[pl.ds(first_at, span)], out_part[pl.ds(half + first_at, span)]], axis=0)
        for j in range(4):
            moved = part if j == 0 else pltpu.roll(part, (4 - j) * chunk, 1)
            y_send[i, j] = moved[:, :chunk]
        for which in (1 - col, col):
            pair_copy(i, which).start()

        @pl.when(i > 0)
        def _():
            cross(i - 1)

        return carry

    def finish(i, carry):
        pair_copy(i, col).wait()
        over_copy(i).wait()
        total = y_send[i, me_yz] + y_pair[i, col] + y_recv[i]
        for e in range(2):
            y_ref[pl.ds(pl.multiple_of(half * e + span * i, span), span), :] = total[span * e:span * e + span]
        return carry

    lax.fori_loop(0, groups, product, 0)
    lax.fori_loop(0, groups - 3, finish, 0)
    cross(groups - 1)
    lax.fori_loop(groups - 3, groups, finish, 0)


def tail(g_first, g_peer, g_own, o_blocks, w_down, w_out):
    half = g_own.shape[0]
    rows = 2 * half
    span = 16
    groups = half // span
    ff, cols = w_down.shape
    chunk = cols // 4
    owned = o_blocks.shape[1]
    o_width = w_out.shape[0]
    any_spec, vmem_spec = pl.BlockSpec(memory_space=pl.ANY), pl.BlockSpec(memory_space=pltpu.VMEM)
    dma = pltpu.SemaphoreType.DMA
    f32, bf16 = jnp.float32, jnp.bfloat16
    return pl.pallas_call(
        tail_kernel,
        out_shape=jax.ShapeDtypeStruct((rows, chunk), f32),
        in_specs=[vmem_spec, vmem_spec, any_spec, vmem_spec, any_spec, any_spec],
        out_specs=pl.BlockSpec(memory_space=pltpu.VMEM),
        scratch_shapes=[
            pltpu.VMEM((half, 2 * ff), f32),
            pltpu.VMEM((4, owned, o_width), bf16),
            pltpu.VMEM((8, owned, o_width), bf16),
            pltpu.VMEM((rows, o_width), f32),
            pltpu.VMEM((groups, 2, span, ff), bf16),
            pltpu.VMEM((ff, cols), bf16),
            pltpu.VMEM((o_width, cols), bf16),
            pltpu.VMEM((rows, cols), f32),
            pltpu.VMEM((groups, 4, 2 * span, chunk), f32),
            pltpu.VMEM((groups, 2, 2 * span, chunk), f32),
            pltpu.VMEM((groups, 2 * span, chunk), f32),
            pltpu.VMEM((groups, 2 * span, chunk), f32),
            dma((3,)), dma((groups,)), dma((8,)), dma((8,)), dma((groups,)), dma((groups,)),
            dma((groups, 2)), dma((groups, 2)), dma((groups,)), dma((groups,)),
        ],
        compiler_params=pltpu.CompilerParams(collective_id=1, has_side_effects=True, vmem_limit_bytes=51 * 1024 * 1024),
        cost_estimate=pl.CostEstimate(flops=2 * rows * (ff + o_width) * cols, bytes_accessed=2 * (ff + o_width) * cols, transcendentals=half * ff),
        name='tail',
    )(g_first, g_peer, g_own, o_blocks, w_down, w_out)


def rotary(values, positions):
    half_dim = values.shape[-1] // 2
    inv_freq = ROPE_BASE ** (-jnp.arange(half_dim, dtype=jnp.float32) / half_dim)
    angles = positions.astype(jnp.float32)[:, None, None] * inv_freq
    cos_part = jnp.cos(angles)
    sin_part = jnp.sin(angles)
    lo_half = values[..., :half_dim]
    hi_half = values[..., half_dim:]
    return jnp.concatenate([lo_half * cos_part - hi_half * sin_part, hi_half * cos_part + lo_half * sin_part], axis=-1)


def solution(mesh):
    x_size = mesh.shape['x']
    yz_size = mesh.shape['yz']
    all_axes = ('x', 'yz')

    def local_step(x_in, ln_scale, w_gate_up, w_attn, w_down, w_out, k_cache, v_cache, lengths, positions):
        local_rows, seq_len, head_dim = k_cache.shape
        q_width = w_out.shape[0] * yz_size
        num_heads = q_width // head_dim
        d_model = x_in.shape[1] * x_size * yz_size
        z_blocks, g_first, g_send, g_own = head(x_in, ln_scale, w_gate_up, w_attn, d_model, EARLY)
        g_peer = lax.ppermute(g_send, 'x', [(0, 1), (1, 0)])
        proj_local = z_blocks.transpose(1, 0, 2).reshape(local_rows, -1)
        q_raw = proj_local[:, :q_width].reshape(local_rows, num_heads, head_dim)
        k_tok = proj_local[:, q_width:q_width + head_dim]
        v_tok = proj_local[:, q_width + head_dim:]
        q_rot = rotary(q_raw.astype(jnp.float32), positions).astype(jnp.bfloat16)
        k_rot = rotary(k_tok[:, None, :].astype(jnp.float32), positions)[:, 0].astype(jnp.bfloat16)
        cols = jnp.stack([k_rot, v_tok]).astype(jnp.float32).transpose(0, 2, 1)
        cols = jnp.pad(cols, ((0, 0), (0, 0), (0, 128 - local_rows)))
        attn_out, k_new, v_new = attend(q_rot, cols, k_cache, v_cache, lengths)
        o_blocks = attn_out.reshape(local_rows, yz_size, q_width // yz_size).transpose(1, 0, 2)
        mixed_sum = tail(g_first, g_peer, g_own, o_blocks, w_down, w_out)
        y_out = (x_in.astype(jnp.float32) + mixed_sum).astype(jnp.bfloat16)
        return y_out, k_new, v_new

    row_spec = P(None, all_axes)
    vec_spec = P(all_axes)
    cache_spec = P(all_axes, None, None)
    return jax.shard_map(
        local_step,
        mesh=mesh,
        in_specs=(row_spec, vec_spec, P('x', None, 'yz'), P('x', 'yz'), P('yz', 'x'), P('yz', 'x'), cache_spec, cache_spec, vec_spec, vec_spec),
        out_specs=(row_spec, cache_spec, cache_spec),
        check_vma=False,
    )
```

```python
import functools

import jax
import jax.numpy as jnp
from jax import lax
from jax.experimental import pallas as pl
from jax.experimental.pallas import tpu as pltpu
from jax.sharding import PartitionSpec as P

LN_EPS = 1e-6
ROPE_BASE = 10000.0
MESH = pl.DeviceIdType.MESH
VMEM_MOST = 64 * 1024 * 1024 - 64 * 1024
EARLY = 3


def attention_kernel(scale, len_ref, q_ref, cols_ref, k_hbm, v_hbm, o_ref, ko_hbm, vo_hbm, k_buf, v_buf, in_sem, out_sem):
    rows, _, seq_len = k_buf.shape

    def load(which, b):
        src, dst = ((k_hbm, k_buf), (v_hbm, v_buf))[which]
        return pltpu.make_async_copy(src.at[b], dst.at[b], in_sem.at[which, b])

    def save(which, b):
        src, dst = ((k_buf, ko_hbm), (v_buf, vo_hbm))[which]
        return pltpu.make_async_copy(src.at[b], dst.at[b], out_sem.at[which, b])

    for b in range(rows):
        load(0, b).start()
        load(1, b).start()

    lane = lax.broadcasted_iota(jnp.int32, (1, 128), 1)
    slots = lax.broadcasted_iota(jnp.int32, (1, seq_len), 1)

    def row(b, carry):
        length = len_ref[b]
        window = pl.ds(pl.multiple_of((length // 128) * 128, 128), 128)
        here = lane == length % 128
        for which, buf in enumerate((k_buf, v_buf)):
            load(which, b).wait()
            col = jnp.sum(jnp.where(lane == b, cols_ref[which], 0.0), axis=1, keepdims=True)
            tile = buf[b, :, window].astype(jnp.float32)
            buf[b, :, window] = jnp.where(here, col, tile).astype(jnp.bfloat16)
        scores = jnp.dot(q_ref[b], k_buf[b], preferred_element_type=jnp.float32) * scale
        scores = jnp.where(slots <= length, scores, -1e30)
        top = jnp.max(scores, axis=1, keepdims=True)
        weights = jnp.exp(scores - top)
        total = jnp.sum(weights, axis=1, keepdims=True)
        probs = (weights * (1.0 / total)).astype(jnp.bfloat16)
        save(0, b).start()
        save(1, b).start()
        o_ref[b] = lax.dot_general(probs, v_buf[b], (((1,), (1,)), ((), ())), preferred_element_type=jnp.float32).astype(jnp.bfloat16)
        return carry

    lax.fori_loop(0, rows, row, 0)
    for b in range(rows):
        save(0, b).wait()
        save(1, b).wait()


def attend(q_rot, cols, k_cache, v_cache, lengths):
    rows, heads, head_dim = q_rot.shape
    seq_len = k_cache.shape[1]
    k_t = jnp.swapaxes(k_cache, 1, 2)
    v_t = jnp.swapaxes(v_cache, 1, 2)
    cache = jax.ShapeDtypeStruct((rows, head_dim, seq_len), jnp.bfloat16)
    o, k_new, v_new = pl.pallas_call(
        functools.partial(attention_kernel, head_dim ** -0.5),
        out_shape=(jax.ShapeDtypeStruct((rows, heads, head_dim), jnp.bfloat16), cache, cache),
        in_specs=[
            pl.BlockSpec(memory_space=pltpu.SMEM),
            pl.BlockSpec(memory_space=pltpu.VMEM),
            pl.BlockSpec(memory_space=pltpu.VMEM),
            pl.BlockSpec(memory_space=pl.ANY),
            pl.BlockSpec(memory_space=pl.ANY),
        ],
        out_specs=(pl.BlockSpec(memory_space=pltpu.VMEM), pl.BlockSpec(memory_space=pl.ANY), pl.BlockSpec(memory_space=pl.ANY)),
        scratch_shapes=[
            pltpu.VMEM((rows, head_dim, seq_len), jnp.bfloat16),
            pltpu.VMEM((rows, head_dim, seq_len), jnp.bfloat16),
            pltpu.SemaphoreType.DMA((2, rows)),
            pltpu.SemaphoreType.DMA((2, rows)),
        ],
        compiler_params=pltpu.CompilerParams(vmem_limit_bytes=48 * 1024 * 1024),
        cost_estimate=pl.CostEstimate(
            flops=4 * rows * heads * head_dim * seq_len,
            bytes_accessed=8 * rows * head_dim * seq_len,
            transcendentals=rows * heads * seq_len,
        ),
        name='attend',
    )(lengths, q_rot, cols, k_t, v_t)
    return o, jnp.swapaxes(k_new, 1, 2), jnp.swapaxes(v_new, 1, 2)


def start_barrier(me_x, me_yz, everyone):
    barrier = pltpu.get_barrier_semaphore()
    peers = [(dx, k) for dx in range(2) for k in range(4) if (dx or k) and (everyone or not (dx and k))]
    for dx, k in peers:
        pl.semaphore_signal(barrier, inc=1, device_id=(lax.rem(me_x + dx, 2), lax.rem(me_yz + k, 4)), device_id_type=MESH)
    return lambda: pl.semaphore_wait(barrier, len(peers))


def spread(rows, cols, first):
    i = lax.broadcasted_iota(jnp.int32, (rows, cols), 0)
    c = lax.broadcasted_iota(jnp.int32, (rows, cols), 1)
    return jnp.where(c == 2 * i + first, 1.0, 0.0).astype(jnp.bfloat16)


def head_kernel(
    d_model, early, x_hbm, scale_hbm, wg_hbm, wa_hbm, z_hbm, first_hbm, send_hbm, own_hbm,
    xg, scale_row, sg, stats, h_buf, hx, wg, wa, z_send, z_own, z_recv, r_send, r_own, r_recv, zb, zg, g_first, g_rest, g_own,
    in_sem, wg_sem, x_send, x_recv, s_send, s_recv, t_send, t_recv, z_sems, a_send, a_recv, f_send, f_recv, out_sem,
):
    me_x = lax.axis_index('x')
    me_yz = lax.axis_index('yz')
    half, chunk = xg.shape[2:]
    rows = 2 * half
    pieces = wg_sem.shape[0]
    depth = wg.shape[0] // pieces
    ff = wg.shape[2]
    wide_cols = 256
    full = z_send.shape[2]
    quarter = half // 2
    third = quarter // 3
    tail_cols = wa.shape[0] - full
    other_x = lax.rem(me_x + 1, 2)
    across = lax.rem(me_yz + 2, 4)
    core = lax.rem(me_yz, 2)
    partner = me_yz + 1 - 2 * core
    order = (other_x, me_x)
    x_in = [
        pltpu.make_async_copy(x_hbm.at[pl.ds(pl.multiple_of(order[p] * half, 32), half)], xg.at[me_yz, order[p]], in_sem.at[p]) for p in range(2)
    ]
    scale_in = pltpu.make_async_copy(scale_hbm, scale_row, in_sem.at[2])
    wa_in = pltpu.make_async_copy(wa_hbm, wa, in_sem.at[3])
    wg_in = [
        pltpu.make_async_copy(wg_hbm.at[pl.ds(depth * i, depth)], wg.at[pl.ds(depth * i, depth)], wg_sem.at[i]) for i in range(pieces)
    ]
    for copy in (*x_in, scale_in, wa_in):
        copy.start()
    others_ready = start_barrier(me_x, me_yz, True)

    def remote(src, dst, send, recv, to_x, to_yz):
        return pltpu.make_async_remote_copy(
            src_ref=src, dst_ref=dst, send_sem=send, recv_sem=recv, device_id=(to_x, to_yz), device_id_type=MESH,
        )

    def x_copy(kind, piece):
        owner = across if kind == 2 else me_yz
        at = xg.at[owner, order[piece // 2], pl.ds(quarter * (piece % 2), quarter)]
        return remote(at, at, x_send.at[kind, piece], x_recv.at[kind, piece], me_x, across if kind == 1 else partner)

    for p in range(2):
        x_in[p].wait()
    lane = lax.broadcasted_iota(jnp.int32, (8, 128), 1)
    tile = jnp.zeros((8, 128), jnp.float32)
    for e in range(2):
        mine = xg[me_yz, e].astype(jnp.float32)
        sum_1 = jnp.sum(mine, axis=1, keepdims=True)
        sum_2 = jnp.sum(mine * mine, axis=1, keepdims=True)
        for j in range(half // 8):
            col = e * (half // 8) + j
            tile = jnp.where(lane == col, sum_1[8 * j:8 * j + 8], tile)
            tile = jnp.where(lane == 32 + col, sum_2[8 * j:8 * j + 8], tile)
    me = me_x * 4 + me_yz
    stats[me] = tile
    others_ready()
    t_out = [
        remote(stats.at[me], stats.at[me], t_send.at[4 * dx + k], t_recv.at[4 * dx + k], lax.rem(me_x + dx, 2), lax.rem(me_yz + k, 4))
        for dx in range(2) for k in range(4) if dx or k
    ]
    for copy in t_out:
        copy.start()
    scale_in.wait()
    sg[me_yz] = scale_row[...].reshape(1, chunk)
    s_out = [remote(sg.at[me_yz], sg.at[me_yz], s_send.at[k], s_recv.at[k], me_x, lax.rem(me_yz + k, 4)) for k in (1, 2, 3)]
    for copy in s_out:
        copy.start()
    for piece in range(4):
        x_copy(1, piece).start()
        x_copy(0, piece).start()
    for copy in wg_in:
        copy.start()
    wide, thin = spread(128, 256, 0), spread(64, 128, 0)
    wide_u, thin_u = spread(128, 256, 1), spread(64, 128, 1)
    for copy in t_out:
        copy.wait()
    total = stats[0]
    for i in range(1, 8):
        total = total + stats[i]
    mean_t = total / d_model
    var_t = pltpu.roll(total, 96, 1) / d_model - mean_t * mean_t
    rstd_t = lax.rsqrt(var_t + LN_EPS)
    for copy in s_out:
        copy.wait()

    chip = me_yz // 2
    contract = (((1,), (1,)), ((), ()))

    def pass_on(piece):
        x_copy(1, piece).wait()
        x_copy(2, piece).start()

    def project_chip(piece, which):
        p, q = piece // 2, piece % 2
        blocks = quarter // 8
        shift = lax.rem(256 - order[p] * (half // 8) - q * blocks, 128)
        mean_p = pltpu.roll(mean_t, shift, 1)
        rstd_p = pltpu.roll(rstd_t, shift, 1)
        mean = jnp.concatenate([mean_p[:, j:j + 1] for j in range(blocks)], axis=0)
        rstd = jnp.concatenate([rstd_p[:, j:j + 1] for j in range(blocks)], axis=0)
        here = pl.ds(quarter * q, quarter)
        both = []
        for e in range(2):
            s = 2 * which + e
            h = (xg[s, order[p], here].astype(jnp.float32) - mean) * rstd * sg[s]
            h_buf[s, here] = h.astype(jnp.bfloat16)
            both.append(h)
        h = jnp.concatenate(both, axis=1).astype(jnp.bfloat16)
        at = pl.ds(pl.multiple_of(2 * chunk * which, 128), 2 * chunk)
        z = lax.dot_general(h, wa[:full, at], contract, preferred_element_type=jnp.float32)
        r = lax.dot_general(h, wa[full:, at], contract, preferred_element_type=jnp.float32)
        return z, r

    def near(piece):
        x_copy(0, piece).wait()
        return project_chip(piece, chip)

    def far(piece, z, r, z_ref, r_ref):
        x_copy(2, piece).wait()
        z_far, r_far = project_chip(piece, 1 - chip)
        q = piece % 2
        z_ref[2 * q:2 * q + 2] = (z + z_far).reshape(2, quarter // 2, full)
        r = r + r_far
        r_ref[q] = jnp.concatenate([r[third * i:third * i + third] for i in range(3)], axis=1)

    def z_copies(q):
        at = pl.ds(2 * q, 2)
        return (
            remote(z_send.at[at], z_recv.at[at], z_sems.at[0, q], z_sems.at[1, q], other_x, me_yz),
            remote(r_send.at[q], r_recv.at[q], z_sems.at[2, q], z_sems.at[3, q], other_x, me_yz),
        )

    def spread_half(part, g):
        out = pl.ds((2 * part + g) * half, half)
        a, b = ((wide, thin), (wide_u, thin_u))[g]
        for s in range(4):
            base = 2 * chunk * s
            for t in range(2):
                piece = h_buf[s, :, 128 * t:128 * t + 128]
                hx[out, base + 256 * t:base + 256 * t + 256] = jnp.dot(piece, a, preferred_element_type=jnp.float32).astype(jnp.bfloat16)
            piece = h_buf[s, :, 256:320]
            hx[out, base + 512:base + 640] = jnp.dot(piece, b, preferred_element_type=jnp.float32).astype(jnp.bfloat16)

    wa_in.wait()
    z_out = [*z_copies(0), *z_copies(1)]
    pass_on(0)
    far(0, *near(0), z_send, r_send)
    z_out[0].start()
    z_out[1].start()
    pass_on(1)
    part_1 = near(1)
    pass_on(2)
    far(1, *part_1, z_send, r_send)
    z_out[2].start()
    z_out[3].start()
    pass_on(3)
    spread_half(0, 0)
    spread_half(0, 1)
    for copy in wg_in:
        copy.wait()

    def block(c):
        at = pl.ds(pl.multiple_of(c * wide_cols, wide_cols), wide_cols)
        return wg[:, :, at].reshape(2 * wg.shape[0], wide_cols)

    def keep_own(c, out):
        g_own[:, pl.ds(pl.multiple_of(c * wide_cols, wide_cols), wide_cols)] = out[:half]
        g_own[:, pl.ds(pl.multiple_of(ff + c * wide_cols, wide_cols), wide_cols)] = out[half:]

    first = []
    for c in range(early):
        out = jnp.dot(hx[:rows], block(c), preferred_element_type=jnp.float32)
        g_first[c, :, :wide_cols] = out[:half]
        g_first[c, :, wide_cols:] = out[half:]
        first.append(remote(g_first.at[c], first_hbm.at[c], f_send.at[c], f_recv.at[c], other_x, me_yz))
        first[-1].start()
    for piece in (2, 3):
        far(piece, *near(piece), z_own, r_own)
    spread_half(1, 0)
    spread_half(1, 1)
    for c in range(early):
        keep_own(c, jnp.dot(hx[rows:], block(c), preferred_element_type=jnp.float32))

    def rest(c, carry):
        out = jnp.dot(hx[...], block(c), preferred_element_type=jnp.float32)
        keep_own(c, out[rows:])
        at = (c - early) * wide_cols
        g_rest[:, pl.ds(pl.multiple_of(at, wide_cols), wide_cols)] = out[:half]
        g_rest[:, pl.ds(pl.multiple_of(ff - early * wide_cols + at, wide_cols), wide_cols)] = out[half:2 * half]
        return carry

    middle = early + 3
    lax.fori_loop(early, middle, rest, 0)
    for copy in z_out:
        copy.wait()
    zb[:, :, :full] = (z_own[...] + z_recv[...]).astype(jnp.bfloat16)
    for q in range(2):
        r = r_own[q] + r_recv[q]
        r = jnp.concatenate([r[:, tail_cols * i:tail_cols * i + tail_cols] for i in range(3)], axis=0)
        zb[2 * q:2 * q + 2, :, full:] = r.reshape(2, quarter // 2, tail_cols).astype(jnp.bfloat16)
    a_out = [remote(zb.at[lax.rem(me_yz + k, 4)], zg.at[me_yz], a_send.at[k], a_recv.at[k], me_x, lax.rem(me_yz + k, 4)) for k in (1, 2, 3)]
    for copy in a_out:
        copy.start()
    zg[me_yz] = zb[me_yz]
    lax.fori_loop(middle, ff // wide_cols, rest, 0)
    save = [pltpu.make_async_copy(g_rest, send_hbm, out_sem.at[0]), pltpu.make_async_copy(g_own, own_hbm, out_sem.at[1])]
    for copy in save:
        copy.start()
    for copy in a_out:
        copy.wait()
    save.append(pltpu.make_async_copy(zg, z_hbm, out_sem.at[2]))
    save[-1].start()
    for copy in first:
        copy.wait()
    for copy in save:
        copy.wait()


def head(x_in, ln_scale, w_gate_up, w_attn, d_model, early):
    rows, chunk = x_in.shape
    depth, _, ff = w_gate_up.shape
    z_cols = w_attn.shape[1]
    full = z_cols // 128 * 128
    owned = rows // 8
    half = rows // 2
    width = 2 * (ff - 256 * early)
    any_spec = pl.BlockSpec(memory_space=pl.ANY)
    dma = pltpu.SemaphoreType.DMA
    f32, bf16 = jnp.float32, jnp.bfloat16
    return pl.pallas_call(
        functools.partial(head_kernel, d_model, early),
        out_shape=(
            jax.ShapeDtypeStruct((4, owned, z_cols), bf16),
            jax.ShapeDtypeStruct((early, half, 512), f32),
            jax.ShapeDtypeStruct((half, width), f32),
            jax.ShapeDtypeStruct((half, 2 * ff), f32),
        ),
        in_specs=[any_spec] * 4,
        out_specs=[any_spec] * 4,
        scratch_shapes=[
            pltpu.VMEM((4, 2, half, chunk), bf16),
            pltpu.VMEM((chunk,), f32),
            pltpu.VMEM((4, 1, chunk), f32),
            pltpu.VMEM((8, 8, 128), f32),
            pltpu.VMEM((4, half, chunk), bf16),
            pltpu.VMEM((2 * rows, 2 * depth), bf16),
            pltpu.VMEM((depth, 2, ff), bf16),
            pltpu.VMEM((z_cols, depth), bf16),
            *[pltpu.VMEM((4, owned, full), f32)] * 3,
            *[pltpu.VMEM((2, half // 6, 3 * (z_cols - full)), f32)] * 3,
            pltpu.VMEM((4, owned, z_cols), bf16),
            pltpu.VMEM((4, owned, z_cols), bf16),
            pltpu.VMEM((early, half, 512), f32),
            pltpu.VMEM((half, width), f32),
            pltpu.VMEM((half, 2 * ff), f32),
            dma((4,)), dma((8,)), dma((3, 4)), dma((3, 4)), dma((4,)), dma((4,)), dma((8,)), dma((8,)), dma((4, 2)), dma((4,)), dma((4,)),
            dma((early,)), dma((early,)), dma((3,)),
        ],
        compiler_params=pltpu.CompilerParams(collective_id=0, has_side_effects=True, vmem_limit_bytes=VMEM_MOST),
        cost_estimate=pl.CostEstimate(flops=4 * rows * depth * 2 * ff, bytes_accessed=4 * depth * ff, transcendentals=0),
        name='head',
    )(x_in, ln_scale, w_gate_up, w_attn.T)


def tail_kernel(
    g_first, g_peer, own_hbm, ov, wd_hbm, wo_hbm, y_ref,
    g_own, oy, oa, of, hb, wd, wo, out_part, y_send, y_pair, y_over, y_recv,
    in_sem, own_sem, o_send, o_recv, h_send, h_recv, p_send, p_recv, y_ssem, y_rsem,
):
    me_x = lax.axis_index('x')
    me_yz = lax.axis_index('yz')
    groups, _, span, ff = hb.shape
    rows, chunk = y_ref.shape
    half = rows // 2
    owned = ov.shape[1]
    early, _, wide = g_first.shape
    wide = wide // 2
    core = lax.rem(me_yz, 2)
    col = me_yz // 2
    partner = me_yz + 1 - 2 * core
    across = lax.rem(me_yz + 2, 4)
    other_x = lax.rem(me_x + 1, 2)

    own_in = [pltpu.make_async_copy(own_hbm.at[pl.ds(span * i, span)], g_own.at[pl.ds(span * i, span)], own_sem.at[i]) for i in range(groups)]
    wo_in = pltpu.make_async_copy(wo_hbm, wo, in_sem.at[1])
    wd_in = pltpu.make_async_copy(wd_hbm, wd, in_sem.at[2])
    for copy in (*own_in, wo_in, wd_in):
        copy.start()
    start_barrier(me_x, me_yz, False)()
    me = me_x * 4 + me_yz

    def remote(src, dst, send, recv, to_x, to_yz):
        return pltpu.make_async_remote_copy(
            src_ref=src, dst_ref=dst, send_sem=send, recv_sem=recv, device_id=(to_x, to_yz), device_id_type=MESH,
        )

    other = other_x * 4 + me_yz
    o_over = remote(ov, oy, o_send.at[0], o_recv.at[0], other_x, me_yz)
    o_over.start()
    there = [lax.rem(me_yz + k, 4) for k in range(4)]
    o_out = [remote(ov.at[there[k]], oa.at[me], o_send.at[k], o_recv.at[k], me_x, there[k]) for k in (1, 2, 3)]
    for copy in o_out:
        copy.start()
    oa[me] = ov[me_yz]

    def h_copy(i):
        return remote(hb.at[i, me_x], hb.at[i, me_x], h_send.at[i], h_recv.at[i], other_x, me_yz)

    for copy in own_in:
        copy.wait()

    def activate(i, carry):
        at = pl.ds(pl.multiple_of(span * i, span), span)

        def act(gate, up):
            gate = gate.astype(jnp.bfloat16).astype(jnp.float32)
            up = up.astype(jnp.bfloat16).astype(jnp.float32)
            return (jax.nn.silu(gate) * up).astype(jnp.bfloat16)

        for c in range(early):
            cols = slice(wide * c, wide * c + wide)
            up_cols = slice(ff + wide * c, ff + wide * c + wide)
            hb[i, me_x, :, cols] = act(g_own[at, cols] + g_first[c, at, :wide], g_own[at, up_cols] + g_first[c, at, wide:])
        done = early * wide
        hb[i, me_x, :, done:] = act(g_own[at, done:ff] + g_peer[at, :ff - done], g_own[at, ff + done:] + g_peer[at, ff - done:])
        h_copy(i).start()
        return carry

    lax.fori_loop(0, groups, activate, 0)
    o_over.wait()
    relay = [remote(oy.at[there[k]], oa.at[other], o_send.at[3 + k], o_recv.at[3 + k], me_x, there[k]) for k in (1, 2, 3)]
    for copy in relay:
        copy.start()
    oa[other] = oy[me_yz]
    for copy in (*o_out, *relay):
        copy.wait()
    for e in range(8):
        of[owned * e:owned * e + owned] = oa[e].astype(jnp.float32)
    wo_in.wait()
    out_part[...] = jnp.dot(of[...].astype(jnp.bfloat16), wo[...], preferred_element_type=jnp.float32)
    wd_in.wait()

    def pair_copy(i, which):
        return remote(y_send.at[i, 2 * which + 1 - core], y_pair.at[i, which], p_send.at[i, which], p_recv.at[i, which], me_x, partner)

    def over_copy(i):
        return remote(y_over.at[i], y_recv.at[i], y_ssem.at[i], y_rsem.at[i], me_x, across)

    def cross(i):
        pair_copy(i, 1 - col).wait()
        y_over[i] = y_send[i, across] + y_pair[i, 1 - col]
        over_copy(i).start()

    def product(i, carry):
        h_copy(i).wait()
        first_at = pl.multiple_of(span * i, span)
        part = jnp.dot(hb[i].reshape(2 * span, ff), wd[...], preferred_element_type=jnp.float32)
        part = part + jnp.concatenate([out_part[pl.ds(first_at, span)], out_part[pl.ds(half + first_at, span)]], axis=0)
        for j in range(4):
            moved = part if j == 0 else pltpu.roll(part, (4 - j) * chunk, 1)
            y_send[i, j] = moved[:, :chunk]
        for which in (1 - col, col):
            pair_copy(i, which).start()

        @pl.when(i > 0)
        def _():
            cross(i - 1)

        return carry

    def finish(i, carry):
        pair_copy(i, col).wait()
        over_copy(i).wait()
        total = y_send[i, me_yz] + y_pair[i, col] + y_recv[i]
        for e in range(2):
            y_ref[pl.ds(pl.multiple_of(half * e + span * i, span), span), :] = total[span * e:span * e + span]
        return carry

    lax.fori_loop(0, groups, product, 0)
    lax.fori_loop(0, groups - 3, finish, 0)
    cross(groups - 1)
    lax.fori_loop(groups - 3, groups, finish, 0)


def tail(g_first, g_peer, g_own, o_blocks, w_down, w_out):
    half = g_own.shape[0]
    rows = 2 * half
    span = 16
    groups = half // span
    ff, cols = w_down.shape
    chunk = cols // 4
    owned = o_blocks.shape[1]
    o_width = w_out.shape[0]
    any_spec, vmem_spec = pl.BlockSpec(memory_space=pl.ANY), pl.BlockSpec(memory_space=pltpu.VMEM)
    dma = pltpu.SemaphoreType.DMA
    f32, bf16 = jnp.float32, jnp.bfloat16
    return pl.pallas_call(
        tail_kernel,
        out_shape=jax.ShapeDtypeStruct((rows, chunk), f32),
        in_specs=[vmem_spec, vmem_spec, any_spec, vmem_spec, any_spec, any_spec],
        out_specs=pl.BlockSpec(memory_space=pltpu.VMEM),
        scratch_shapes=[
            pltpu.VMEM((half, 2 * ff), f32),
            pltpu.VMEM((4, owned, o_width), bf16),
            pltpu.VMEM((8, owned, o_width), bf16),
            pltpu.VMEM((rows, o_width), f32),
            pltpu.VMEM((groups, 2, span, ff), bf16),
            pltpu.VMEM((ff, cols), bf16),
            pltpu.VMEM((o_width, cols), bf16),
            pltpu.VMEM((rows, cols), f32),
            pltpu.VMEM((groups, 4, 2 * span, chunk), f32),
            pltpu.VMEM((groups, 2, 2 * span, chunk), f32),
            pltpu.VMEM((groups, 2 * span, chunk), f32),
            pltpu.VMEM((groups, 2 * span, chunk), f32),
            dma((3,)), dma((groups,)), dma((8,)), dma((8,)), dma((groups,)), dma((groups,)),
            dma((groups, 2)), dma((groups, 2)), dma((groups,)), dma((groups,)),
        ],
        compiler_params=pltpu.CompilerParams(collective_id=1, has_side_effects=True, vmem_limit_bytes=51 * 1024 * 1024),
        cost_estimate=pl.CostEstimate(flops=2 * rows * (ff + o_width) * cols, bytes_accessed=2 * (ff + o_width) * cols, transcendentals=half * ff),
        name='tail',
    )(g_first, g_peer, g_own, o_blocks, w_down, w_out)


def rotary(values, positions):
    half_dim = values.shape[-1] // 2
    inv_freq = ROPE_BASE ** (-jnp.arange(half_dim, dtype=jnp.float32) / half_dim)
    angles = positions.astype(jnp.float32)[:, None, None] * inv_freq
    cos_part = jnp.cos(angles)
    sin_part = jnp.sin(angles)
    lo_half = values[..., :half_dim]
    hi_half = values[..., half_dim:]
    return jnp.concatenate([lo_half * cos_part - hi_half * sin_part, hi_half * cos_part + lo_half * sin_part], axis=-1)


def solution(mesh):
    x_size = mesh.shape['x']
    yz_size = mesh.shape['yz']
    all_axes = ('x', 'yz')

    def local_step(x_in, ln_scale, w_gate_up, w_attn, w_down, w_out, k_cache, v_cache, lengths, positions):
        local_rows, seq_len, head_dim = k_cache.shape
        q_width = w_out.shape[0] * yz_size
        num_heads = q_width // head_dim
        d_model = x_in.shape[1] * x_size * yz_size
        z_blocks, g_first, g_send, g_own = head(x_in, ln_scale, w_gate_up, w_attn, d_model, EARLY)
        g_peer = lax.ppermute(g_send, 'x', [(0, 1), (1, 0)])
        proj_local = z_blocks.transpose(1, 0, 2).reshape(local_rows, -1)
        q_raw = proj_local[:, :q_width].reshape(local_rows, num_heads, head_dim)
        k_tok = proj_local[:, q_width:q_width + head_dim]
        v_tok = proj_local[:, q_width + head_dim:]
        q_rot = rotary(q_raw.astype(jnp.float32), positions).astype(jnp.bfloat16)
        k_rot = rotary(k_tok[:, None, :].astype(jnp.float32), positions)[:, 0].astype(jnp.bfloat16)
        cols = jnp.stack([k_rot, v_tok]).astype(jnp.float32).transpose(0, 2, 1)
        cols = jnp.pad(cols, ((0, 0), (0, 0), (0, 128 - local_rows)))
        attn_out, k_new, v_new = attend(q_rot, cols, k_cache, v_cache, lengths)
        o_blocks = attn_out.reshape(local_rows, yz_size, q_width // yz_size).transpose(1, 0, 2)
        mixed_sum = tail(g_first, g_peer, g_own, o_blocks, w_down, w_out)
        y_out = (x_in.astype(jnp.float32) + mixed_sum).astype(jnp.bfloat16)
        return y_out, k_new, v_new

    row_spec = P(None, all_axes)
    vec_spec = P(all_axes)
    cache_spec = P(all_axes, None, None)
    return jax.shard_map(
        local_step,
        mesh=mesh,
        in_specs=(row_spec, vec_spec, P('x', None, 'yz'), P('x', 'yz'), P('yz', 'x'), P('yz', 'x'), cache_spec, cache_spec, vec_spec, vec_spec),
        out_specs=(row_spec, cache_spec, cache_spec),
        check_vma=False,
    )
```

```python
import functools

import jax
import jax.numpy as jnp
from jax import lax
from jax.experimental import pallas as pl
from jax.experimental.pallas import tpu as pltpu
from jax.sharding import PartitionSpec as P

LN_EPS = 1e-6
ROPE_BASE = 10000.0
MESH = pl.DeviceIdType.MESH
VMEM_MOST = 64 * 1024 * 1024 - 64 * 1024
EARLY = 2


def attention_kernel(scale, len_ref, q_ref, cols_ref, k_hbm, v_hbm, o_ref, ko_hbm, vo_hbm, k_buf, v_buf, in_sem, out_sem):
    rows, _, seq_len = k_buf.shape

    def load(which, b):
        src, dst = ((k_hbm, k_buf), (v_hbm, v_buf))[which]
        return pltpu.make_async_copy(src.at[b], dst.at[b], in_sem.at[which, b])

    def save(which, b):
        src, dst = ((k_buf, ko_hbm), (v_buf, vo_hbm))[which]
        return pltpu.make_async_copy(src.at[b], dst.at[b], out_sem.at[which, b])

    for b in range(rows):
        load(0, b).start()
        load(1, b).start()

    lane = lax.broadcasted_iota(jnp.int32, (1, 128), 1)
    slots = lax.broadcasted_iota(jnp.int32, (1, seq_len), 1)

    def row(b, carry):
        length = len_ref[b]
        window = pl.ds(pl.multiple_of((length // 128) * 128, 128), 128)
        here = lane == length % 128
        for which, buf in enumerate((k_buf, v_buf)):
            load(which, b).wait()
            col = jnp.sum(jnp.where(lane == b, cols_ref[which], 0.0), axis=1, keepdims=True)
            tile = buf[b, :, window].astype(jnp.float32)
            buf[b, :, window] = jnp.where(here, col, tile).astype(jnp.bfloat16)
        scores = jnp.dot(q_ref[b], k_buf[b], preferred_element_type=jnp.float32) * scale
        scores = jnp.where(slots <= length, scores, -1e30)
        top = jnp.max(scores, axis=1, keepdims=True)
        weights = jnp.exp(scores - top)
        total = jnp.sum(weights, axis=1, keepdims=True)
        probs = (weights * (1.0 / total)).astype(jnp.bfloat16)
        save(0, b).start()
        save(1, b).start()
        o_ref[b] = lax.dot_general(probs, v_buf[b], (((1,), (1,)), ((), ())), preferred_element_type=jnp.float32).astype(jnp.bfloat16)
        return carry

    lax.fori_loop(0, rows, row, 0)
    for b in range(rows):
        save(0, b).wait()
        save(1, b).wait()


def attend(q_rot, cols, k_cache, v_cache, lengths):
    rows, heads, head_dim = q_rot.shape
    seq_len = k_cache.shape[1]
    k_t = jnp.swapaxes(k_cache, 1, 2)
    v_t = jnp.swapaxes(v_cache, 1, 2)
    cache = jax.ShapeDtypeStruct((rows, head_dim, seq_len), jnp.bfloat16)
    o, k_new, v_new = pl.pallas_call(
        functools.partial(attention_kernel, head_dim ** -0.5),
        out_shape=(jax.ShapeDtypeStruct((rows, heads, head_dim), jnp.bfloat16), cache, cache),
        in_specs=[
            pl.BlockSpec(memory_space=pltpu.SMEM),
            pl.BlockSpec(memory_space=pltpu.VMEM),
            pl.BlockSpec(memory_space=pltpu.VMEM),
            pl.BlockSpec(memory_space=pl.ANY),
            pl.BlockSpec(memory_space=pl.ANY),
        ],
        out_specs=(pl.BlockSpec(memory_space=pltpu.VMEM), pl.BlockSpec(memory_space=pl.ANY), pl.BlockSpec(memory_space=pl.ANY)),
        scratch_shapes=[
            pltpu.VMEM((rows, head_dim, seq_len), jnp.bfloat16),
            pltpu.VMEM((rows, head_dim, seq_len), jnp.bfloat16),
            pltpu.SemaphoreType.DMA((2, rows)),
            pltpu.SemaphoreType.DMA((2, rows)),
        ],
        compiler_params=pltpu.CompilerParams(vmem_limit_bytes=48 * 1024 * 1024),
        cost_estimate=pl.CostEstimate(
            flops=4 * rows * heads * head_dim * seq_len,
            bytes_accessed=8 * rows * head_dim * seq_len,
            transcendentals=rows * heads * seq_len,
        ),
        name='attend',
    )(lengths, q_rot, cols, k_t, v_t)
    return o, jnp.swapaxes(k_new, 1, 2), jnp.swapaxes(v_new, 1, 2)


def start_barrier(me_x, me_yz, everyone):
    barrier = pltpu.get_barrier_semaphore()
    peers = [(dx, k) for dx in range(2) for k in range(4) if (dx or k) and (everyone or not (dx and k))]
    for dx, k in peers:
        pl.semaphore_signal(barrier, inc=1, device_id=(lax.rem(me_x + dx, 2), lax.rem(me_yz + k, 4)), device_id_type=MESH)
    return lambda: pl.semaphore_wait(barrier, len(peers))


def spread(rows, cols, first):
    i = lax.broadcasted_iota(jnp.int32, (rows, cols), 0)
    c = lax.broadcasted_iota(jnp.int32, (rows, cols), 1)
    return jnp.where(c == 2 * i + first, 1.0, 0.0).astype(jnp.bfloat16)


def head_kernel(
    d_model, early, x_hbm, scale_hbm, wg_hbm, wa_hbm, z_hbm, first_hbm, send_hbm, own_hbm,
    xg, scale_row, sg, stats, h_buf, hx, wg, wa, z_send, z_own, z_recv, r_send, r_own, r_recv, zb, zg, g_first, g_rest, g_own,
    in_sem, wg_sem, x_send, x_recv, s_send, s_recv, t_send, t_recv, z_sems, a_send, a_recv, f_send, f_recv, out_sem,
):
    me_x = lax.axis_index('x')
    me_yz = lax.axis_index('yz')
    half, chunk = xg.shape[2:]
    rows = 2 * half
    pieces = wg_sem.shape[0]
    depth = wg.shape[0] // pieces
    ff = wg.shape[2]
    wide_cols = 256
    full = z_send.shape[2]
    quarter = half // 2
    third = quarter // 3
    tail_cols = wa.shape[0] - full
    other_x = lax.rem(me_x + 1, 2)
    across = lax.rem(me_yz + 2, 4)
    core = lax.rem(me_yz, 2)
    partner = me_yz + 1 - 2 * core
    order = (other_x, me_x)
    x_in = [
        pltpu.make_async_copy(x_hbm.at[pl.ds(pl.multiple_of(order[p] * half, 32), half)], xg.at[me_yz, order[p]], in_sem.at[p]) for p in range(2)
    ]
    scale_in = pltpu.make_async_copy(scale_hbm, scale_row, in_sem.at[2])
    wa_in = pltpu.make_async_copy(wa_hbm, wa, in_sem.at[3])
    wg_in = [
        pltpu.make_async_copy(wg_hbm.at[pl.ds(depth * i, depth)], wg.at[pl.ds(depth * i, depth)], wg_sem.at[i]) for i in range(pieces)
    ]
    for copy in (*x_in, scale_in, wa_in):
        copy.start()
    others_ready = start_barrier(me_x, me_yz, True)

    def remote(src, dst, send, recv, to_x, to_yz):
        return pltpu.make_async_remote_copy(
            src_ref=src, dst_ref=dst, send_sem=send, recv_sem=recv, device_id=(to_x, to_yz), device_id_type=MESH,
        )

    def x_copy(kind, piece):
        owner = across if kind == 2 else me_yz
        at = xg.at[owner, order[piece // 2], pl.ds(quarter * (piece % 2), quarter)]
        return remote(at, at, x_send.at[kind, piece], x_recv.at[kind, piece], me_x, across if kind == 1 else partner)

    for p in range(2):
        x_in[p].wait()
    lane = lax.broadcasted_iota(jnp.int32, (8, 128), 1)
    tile = jnp.zeros((8, 128), jnp.float32)
    for e in range(2):
        mine = xg[me_yz, e].astype(jnp.float32)
        sum_1 = jnp.sum(mine, axis=1, keepdims=True)
        sum_2 = jnp.sum(mine * mine, axis=1, keepdims=True)
        for j in range(half // 8):
            col = e * (half // 8) + j
            tile = jnp.where(lane == col, sum_1[8 * j:8 * j + 8], tile)
            tile = jnp.where(lane == 32 + col, sum_2[8 * j:8 * j + 8], tile)
    me = me_x * 4 + me_yz
    stats[me] = tile
    others_ready()
    x_copy(1, 0).start()
    x_copy(0, 0).start()
    t_out = [
        remote(stats.at[me], stats.at[me], t_send.at[4 * dx + k], t_recv.at[4 * dx + k], lax.rem(me_x + dx, 2), lax.rem(me_yz + k, 4))
        for dx in range(2) for k in range(4) if dx or k
    ]
    for copy in t_out:
        copy.start()
    scale_in.wait()
    sg[me_yz] = scale_row[...].reshape(1, chunk)
    s_out = [remote(sg.at[me_yz], sg.at[me_yz], s_send.at[k], s_recv.at[k], me_x, lax.rem(me_yz + k, 4)) for k in (1, 2, 3)]
    for copy in s_out:
        copy.start()
    for piece in range(1, 4):
        x_copy(1, piece).start()
        x_copy(0, piece).start()
    for copy in wg_in:
        copy.start()
    wide, thin = spread(128, 256, 0), spread(64, 128, 0)
    wide_u, thin_u = spread(128, 256, 1), spread(64, 128, 1)
    x_copy(1, 0).wait()
    x_copy(2, 0).start()
    for copy in t_out:
        copy.wait()
    total = stats[0]
    for i in range(1, 8):
        total = total + stats[i]
    mean_t = total / d_model
    var_t = pltpu.roll(total, 96, 1) / d_model - mean_t * mean_t
    rstd_t = lax.rsqrt(var_t + LN_EPS)
    for copy in s_out:
        copy.wait()

    chip = me_yz // 2
    contract = (((1,), (1,)), ((), ()))

    def pass_on(piece):
        x_copy(1, piece).wait()
        x_copy(2, piece).start()

    def project_chip(piece, which):
        p, q = piece // 2, piece % 2
        blocks = quarter // 8
        shift = lax.rem(256 - order[p] * (half // 8) - q * blocks, 128)
        mean_p = pltpu.roll(mean_t, shift, 1)
        rstd_p = pltpu.roll(rstd_t, shift, 1)
        mean = jnp.concatenate([mean_p[:, j:j + 1] for j in range(blocks)], axis=0)
        rstd = jnp.concatenate([rstd_p[:, j:j + 1] for j in range(blocks)], axis=0)
        here = pl.ds(quarter * q, quarter)
        both = []
        for e in range(2):
            s = 2 * which + e
            h = (xg[s, order[p], here].astype(jnp.float32) - mean) * rstd * sg[s]
            h_buf[s, here] = h.astype(jnp.bfloat16)
            both.append(h)
        h = jnp.concatenate(both, axis=1).astype(jnp.bfloat16)
        at = pl.ds(pl.multiple_of(2 * chunk * which, 128), 2 * chunk)
        z = lax.dot_general(h, wa[:full, at], contract, preferred_element_type=jnp.float32)
        r = lax.dot_general(h, wa[full:, at], contract, preferred_element_type=jnp.float32)
        return z, r

    def near(piece):
        x_copy(0, piece).wait()
        return project_chip(piece, chip)

    def far(piece, z, r, z_ref, r_ref):
        x_copy(2, piece).wait()
        z_far, r_far = project_chip(piece, 1 - chip)
        q = piece % 2
        z_ref[2 * q:2 * q + 2] = (z + z_far).reshape(2, quarter // 2, full)
        r = r + r_far
        r_ref[q] = jnp.concatenate([r[third * i:third * i + third] for i in range(3)], axis=1)

    def z_copies(q):
        at = pl.ds(2 * q, 2)
        return (
            remote(z_send.at[at], z_recv.at[at], z_sems.at[0, q], z_sems.at[1, q], other_x, me_yz),
            remote(r_send.at[q], r_recv.at[q], z_sems.at[2, q], z_sems.at[3, q], other_x, me_yz),
        )

    def spread_half(part, g):
        out = pl.ds((2 * part + g) * half, half)
        a, b = ((wide, thin), (wide_u, thin_u))[g]
        for s in range(4):
            base = 2 * chunk * s
            for t in range(2):
                piece = h_buf[s, :, 128 * t:128 * t + 128]
                hx[out, base + 256 * t:base + 256 * t + 256] = jnp.dot(piece, a, preferred_element_type=jnp.float32).astype(jnp.bfloat16)
            piece = h_buf[s, :, 256:320]
            hx[out, base + 512:base + 640] = jnp.dot(piece, b, preferred_element_type=jnp.float32).astype(jnp.bfloat16)

    wa_in.wait()
    z_out = [*z_copies(0), *z_copies(1)]
    far(0, *near(0), z_send, r_send)
    z_out[0].start()
    z_out[1].start()
    pass_on(1)
    part_1 = near(1)
    pass_on(2)
    far(1, *part_1, z_send, r_send)
    z_out[2].start()
    z_out[3].start()
    pass_on(3)
    spread_half(0, 0)
    spread_half(0, 1)
    for copy in wg_in:
        copy.wait()

    def block(c):
        at = pl.ds(pl.multiple_of(c * wide_cols, wide_cols), wide_cols)
        return wg[:, :, at].reshape(2 * wg.shape[0], wide_cols)

    def keep_own(c, out):
        g_own[:, pl.ds(pl.multiple_of(c * wide_cols, wide_cols), wide_cols)] = out[:half]
        g_own[:, pl.ds(pl.multiple_of(ff + c * wide_cols, wide_cols), wide_cols)] = out[half:]

    first = []
    for c in range(early):
        out = jnp.dot(hx[:rows], block(c), preferred_element_type=jnp.float32)
        g_first[c, :, :wide_cols] = out[:half]
        g_first[c, :, wide_cols:] = out[half:]
        first.append(remote(g_first.at[c], first_hbm.at[c], f_send.at[c], f_recv.at[c], other_x, me_yz))
        first[-1].start()
    for piece in (2, 3):
        far(piece, *near(piece), z_own, r_own)
    spread_half(1, 0)
    spread_half(1, 1)
    for c in range(early):
        keep_own(c, jnp.dot(hx[rows:], block(c), preferred_element_type=jnp.float32))

    def rest(c, carry):
        out = jnp.dot(hx[...], block(c), preferred_element_type=jnp.float32)
        keep_own(c, out[rows:])
        at = (c - early) * wide_cols
        g_rest[:, pl.ds(pl.multiple_of(at, wide_cols), wide_cols)] = out[:half]
        g_rest[:, pl.ds(pl.multiple_of(ff - early * wide_cols + at, wide_cols), wide_cols)] = out[half:2 * half]
        return carry

    middle = early + 4
    lax.fori_loop(early, middle, rest, 0)
    for copy in z_out:
        copy.wait()
    zb[:, :, :full] = (z_own[...] + z_recv[...]).astype(jnp.bfloat16)
    for q in range(2):
        r = r_own[q] + r_recv[q]
        r = jnp.concatenate([r[:, tail_cols * i:tail_cols * i + tail_cols] for i in range(3)], axis=0)
        zb[2 * q:2 * q + 2, :, full:] = r.reshape(2, quarter // 2, tail_cols).astype(jnp.bfloat16)
    a_out = [remote(zb.at[lax.rem(me_yz + k, 4)], zg.at[me_yz], a_send.at[k], a_recv.at[k], me_x, lax.rem(me_yz + k, 4)) for k in (1, 2, 3)]
    for copy in a_out:
        copy.start()
    zg[me_yz] = zb[me_yz]
    lax.fori_loop(middle, ff // wide_cols, rest, 0)
    save = [pltpu.make_async_copy(g_rest, send_hbm, out_sem.at[0]), pltpu.make_async_copy(g_own, own_hbm, out_sem.at[1])]
    for copy in save:
        copy.start()
    for copy in a_out:
        copy.wait()
    save.append(pltpu.make_async_copy(zg, z_hbm, out_sem.at[2]))
    save[-1].start()
    for copy in first:
        copy.wait()
    for copy in save:
        copy.wait()


def head(x_in, ln_scale, w_gate_up, w_attn, d_model, early):
    rows, chunk = x_in.shape
    depth, _, ff = w_gate_up.shape
    z_cols = w_attn.shape[1]
    full = z_cols // 128 * 128
    owned = rows // 8
    half = rows // 2
    width = 2 * (ff - 256 * early)
    any_spec = pl.BlockSpec(memory_space=pl.ANY)
    dma = pltpu.SemaphoreType.DMA
    f32, bf16 = jnp.float32, jnp.bfloat16
    return pl.pallas_call(
        functools.partial(head_kernel, d_model, early),
        out_shape=(
            jax.ShapeDtypeStruct((4, owned, z_cols), bf16),
            jax.ShapeDtypeStruct((early, half, 512), f32),
            jax.ShapeDtypeStruct((half, width), f32),
            jax.ShapeDtypeStruct((half, 2 * ff), f32),
        ),
        in_specs=[any_spec] * 4,
        out_specs=[any_spec] * 4,
        scratch_shapes=[
            pltpu.VMEM((4, 2, half, chunk), bf16),
            pltpu.VMEM((chunk,), f32),
            pltpu.VMEM((4, 1, chunk), f32),
            pltpu.VMEM((8, 8, 128), f32),
            pltpu.VMEM((4, half, chunk), bf16),
            pltpu.VMEM((2 * rows, 2 * depth), bf16),
            pltpu.VMEM((depth, 2, ff), bf16),
            pltpu.VMEM((z_cols, depth), bf16),
            *[pltpu.VMEM((4, owned, full), f32)] * 3,
            *[pltpu.VMEM((2, half // 6, 3 * (z_cols - full)), f32)] * 3,
            pltpu.VMEM((4, owned, z_cols), bf16),
            pltpu.VMEM((4, owned, z_cols), bf16),
            pltpu.VMEM((early, half, 512), f32),
            pltpu.VMEM((half, width), f32),
            pltpu.VMEM((half, 2 * ff), f32),
            dma((4,)), dma((8,)), dma((3, 4)), dma((3, 4)), dma((4,)), dma((4,)), dma((8,)), dma((8,)), dma((4, 2)), dma((4,)), dma((4,)),
            dma((early,)), dma((early,)), dma((3,)),
        ],
        compiler_params=pltpu.CompilerParams(collective_id=0, has_side_effects=True, vmem_limit_bytes=VMEM_MOST),
        cost_estimate=pl.CostEstimate(flops=4 * rows * depth * 2 * ff, bytes_accessed=4 * depth * ff, transcendentals=0),
        name='head',
    )(x_in, ln_scale, w_gate_up, w_attn.T)


def tail_kernel(
    g_first, g_peer, own_hbm, ov, wd_hbm, wo_hbm, y_ref,
    g_own, oy, oa, of, hb, wd, wo, out_part, y_send, y_pair, y_over, y_recv,
    in_sem, own_sem, o_send, o_recv, h_send, h_recv, p_send, p_recv, y_ssem, y_rsem,
):
    me_x = lax.axis_index('x')
    me_yz = lax.axis_index('yz')
    groups, _, span, ff = hb.shape
    rows, chunk = y_ref.shape
    half = rows // 2
    owned = ov.shape[1]
    early, _, wide = g_first.shape
    wide = wide // 2
    core = lax.rem(me_yz, 2)
    col = me_yz // 2
    partner = me_yz + 1 - 2 * core
    across = lax.rem(me_yz + 2, 4)
    other_x = lax.rem(me_x + 1, 2)

    own_in = [pltpu.make_async_copy(own_hbm.at[pl.ds(span * i, span)], g_own.at[pl.ds(span * i, span)], own_sem.at[i]) for i in range(groups)]
    wo_in = pltpu.make_async_copy(wo_hbm, wo, in_sem.at[1])
    wd_in = pltpu.make_async_copy(wd_hbm, wd, in_sem.at[2])
    for copy in (*own_in, wo_in, wd_in):
        copy.start()
    start_barrier(me_x, me_yz, False)()
    me = me_x * 4 + me_yz

    def remote(src, dst, send, recv, to_x, to_yz):
        return pltpu.make_async_remote_copy(
            src_ref=src, dst_ref=dst, send_sem=send, recv_sem=recv, device_id=(to_x, to_yz), device_id_type=MESH,
        )

    other = other_x * 4 + me_yz
    o_over = remote(ov, oy, o_send.at[0], o_recv.at[0], other_x, me_yz)
    o_over.start()
    there = [lax.rem(me_yz + k, 4) for k in range(4)]
    o_out = [remote(ov.at[there[k]], oa.at[me], o_send.at[k], o_recv.at[k], me_x, there[k]) for k in (1, 2, 3)]
    for copy in o_out:
        copy.start()
    oa[me] = ov[me_yz]

    def h_copy(i):
        return remote(hb.at[i, me_x], hb.at[i, me_x], h_send.at[i], h_recv.at[i], other_x, me_yz)

    for copy in own_in:
        copy.wait()

    def activate(i, carry):
        at = pl.ds(pl.multiple_of(span * i, span), span)

        def act(gate, up):
            gate = gate.astype(jnp.bfloat16).astype(jnp.float32)
            up = up.astype(jnp.bfloat16).astype(jnp.float32)
            return (jax.nn.silu(gate) * up).astype(jnp.bfloat16)

        for c in range(early):
            cols = slice(wide * c, wide * c + wide)
            up_cols = slice(ff + wide * c, ff + wide * c + wide)
            hb[i, me_x, :, cols] = act(g_own[at, cols] + g_first[c, at, :wide], g_own[at, up_cols] + g_first[c, at, wide:])
        done = early * wide
        hb[i, me_x, :, done:] = act(g_own[at, done:ff] + g_peer[at, :ff - done], g_own[at, ff + done:] + g_peer[at, ff - done:])
        h_copy(i).start()
        return carry

    lax.fori_loop(0, groups, activate, 0)
    o_over.wait()
    relay = [remote(oy.at[there[k]], oa.at[other], o_send.at[3 + k], o_recv.at[3 + k], me_x, there[k]) for k in (1, 2, 3)]
    for copy in relay:
        copy.start()
    oa[other] = oy[me_yz]
    for copy in (*o_out, *relay):
        copy.wait()
    for e in range(8):
        of[owned * e:owned * e + owned] = oa[e].astype(jnp.float32)
    wo_in.wait()
    out_part[...] = jnp.dot(of[...].astype(jnp.bfloat16), wo[...], preferred_element_type=jnp.float32)
    wd_in.wait()

    def pair_copy(i, which):
        return remote(y_send.at[i, 2 * which + 1 - core], y_pair.at[i, which], p_send.at[i, which], p_recv.at[i, which], me_x, partner)

    def over_copy(i):
        return remote(y_over.at[i], y_recv.at[i], y_ssem.at[i], y_rsem.at[i], me_x, across)

    def cross(i):
        pair_copy(i, 1 - col).wait()
        y_over[i] = y_send[i, across] + y_pair[i, 1 - col]
        over_copy(i).start()

    def product(i, carry):
        h_copy(i).wait()
        first_at = pl.multiple_of(span * i, span)
        part = jnp.dot(hb[i].reshape(2 * span, ff), wd[...], preferred_element_type=jnp.float32)
        part = part + jnp.concatenate([out_part[pl.ds(first_at, span)], out_part[pl.ds(half + first_at, span)]], axis=0)
        for j in range(4):
            moved = part if j == 0 else pltpu.roll(part, (4 - j) * chunk, 1)
            y_send[i, j] = moved[:, :chunk]
        for which in (1 - col, col):
            pair_copy(i, which).start()

        @pl.when(i > 0)
        def _():
            cross(i - 1)

        return carry

    def finish(i, carry):
        pair_copy(i, col).wait()
        over_copy(i).wait()
        total = y_send[i, me_yz] + y_pair[i, col] + y_recv[i]
        for e in range(2):
            y_ref[pl.ds(pl.multiple_of(half * e + span * i, span), span), :] = total[span * e:span * e + span]
        return carry

    lax.fori_loop(0, groups, product, 0)
    lax.fori_loop(0, groups - 3, finish, 0)
    cross(groups - 1)
    lax.fori_loop(groups - 3, groups, finish, 0)


def tail(g_first, g_peer, g_own, o_blocks, w_down, w_out):
    half = g_own.shape[0]
    rows = 2 * half
    span = 16
    groups = half // span
    ff, cols = w_down.shape
    chunk = cols // 4
    owned = o_blocks.shape[1]
    o_width = w_out.shape[0]
    any_spec, vmem_spec = pl.BlockSpec(memory_space=pl.ANY), pl.BlockSpec(memory_space=pltpu.VMEM)
    dma = pltpu.SemaphoreType.DMA
    f32, bf16 = jnp.float32, jnp.bfloat16
    return pl.pallas_call(
        tail_kernel,
        out_shape=jax.ShapeDtypeStruct((rows, chunk), f32),
        in_specs=[vmem_spec, vmem_spec, any_spec, vmem_spec, any_spec, any_spec],
        out_specs=pl.BlockSpec(memory_space=pltpu.VMEM),
        scratch_shapes=[
            pltpu.VMEM((half, 2 * ff), f32),
            pltpu.VMEM((4, owned, o_width), bf16),
            pltpu.VMEM((8, owned, o_width), bf16),
            pltpu.VMEM((rows, o_width), f32),
            pltpu.VMEM((groups, 2, span, ff), bf16),
            pltpu.VMEM((ff, cols), bf16),
            pltpu.VMEM((o_width, cols), bf16),
            pltpu.VMEM((rows, cols), f32),
            pltpu.VMEM((groups, 4, 2 * span, chunk), f32),
            pltpu.VMEM((groups, 2, 2 * span, chunk), f32),
            pltpu.VMEM((groups, 2 * span, chunk), f32),
            pltpu.VMEM((groups, 2 * span, chunk), f32),
            dma((3,)), dma((groups,)), dma((8,)), dma((8,)), dma((groups,)), dma((groups,)),
            dma((groups, 2)), dma((groups, 2)), dma((groups,)), dma((groups,)),
        ],
        compiler_params=pltpu.CompilerParams(collective_id=1, has_side_effects=True, vmem_limit_bytes=51 * 1024 * 1024),
        cost_estimate=pl.CostEstimate(flops=2 * rows * (ff + o_width) * cols, bytes_accessed=2 * (ff + o_width) * cols, transcendentals=half * ff),
        name='tail',
    )(g_first, g_peer, g_own, o_blocks, w_down, w_out)


def rotary(values, positions):
    half_dim = values.shape[-1] // 2
    inv_freq = ROPE_BASE ** (-jnp.arange(half_dim, dtype=jnp.float32) / half_dim)
    angles = positions.astype(jnp.float32)[:, None, None] * inv_freq
    cos_part = jnp.cos(angles)
    sin_part = jnp.sin(angles)
    lo_half = values[..., :half_dim]
    hi_half = values[..., half_dim:]
    return jnp.concatenate([lo_half * cos_part - hi_half * sin_part, hi_half * cos_part + lo_half * sin_part], axis=-1)


def solution(mesh):
    x_size = mesh.shape['x']
    yz_size = mesh.shape['yz']
    all_axes = ('x', 'yz')

    def local_step(x_in, ln_scale, w_gate_up, w_attn, w_down, w_out, k_cache, v_cache, lengths, positions):
        local_rows, seq_len, head_dim = k_cache.shape
        q_width = w_out.shape[0] * yz_size
        num_heads = q_width // head_dim
        d_model = x_in.shape[1] * x_size * yz_size
        z_blocks, g_first, g_send, g_own = head(x_in, ln_scale, w_gate_up, w_attn, d_model, EARLY)
        g_peer = lax.ppermute(g_send, 'x', [(0, 1), (1, 0)])
        proj_local = z_blocks.transpose(1, 0, 2).reshape(local_rows, -1)
        q_raw = proj_local[:, :q_width].reshape(local_rows, num_heads, head_dim)
        k_tok = proj_local[:, q_width:q_width + head_dim]
        v_tok = proj_local[:, q_width + head_dim:]
        q_rot = rotary(q_raw.astype(jnp.float32), positions).astype(jnp.bfloat16)
        k_rot = rotary(k_tok[:, None, :].astype(jnp.float32), positions)[:, 0].astype(jnp.bfloat16)
        cols = jnp.stack([k_rot, v_tok]).astype(jnp.float32).transpose(0, 2, 1)
        cols = jnp.pad(cols, ((0, 0), (0, 0), (0, 128 - local_rows)))
        attn_out, k_new, v_new = attend(q_rot, cols, k_cache, v_cache, lengths)
        o_blocks = attn_out.reshape(local_rows, yz_size, q_width // yz_size).transpose(1, 0, 2)
        mixed_sum = tail(g_first, g_peer, g_own, o_blocks, w_down, w_out)
        y_out = (x_in.astype(jnp.float32) + mixed_sum).astype(jnp.bfloat16)
        return y_out, k_new, v_new

    row_spec = P(None, all_axes)
    vec_spec = P(all_axes)
    cache_spec = P(all_axes, None, None)
    return jax.shard_map(
        local_step,
        mesh=mesh,
        in_specs=(row_spec, vec_spec, P('x', None, 'yz'), P('x', 'yz'), P('yz', 'x'), P('yz', 'x'), cache_spec, cache_spec, vec_spec, vec_spec),
        out_specs=(row_spec, cache_spec, cache_spec),
        check_vma=False,
    )
```

```python
import functools

import jax
import jax.numpy as jnp
from jax import lax
from jax.experimental import pallas as pl
from jax.experimental.pallas import tpu as pltpu
from jax.sharding import PartitionSpec as P

LN_EPS = 1e-6
ROPE_BASE = 10000.0
MESH = pl.DeviceIdType.MESH
VMEM_MOST = 64 * 1024 * 1024 - 64 * 1024
EARLY = 2


def attention_kernel(scale, len_ref, q_ref, cols_ref, k_hbm, v_hbm, o_ref, ko_hbm, vo_hbm, k_buf, v_buf, in_sem, out_sem):
    rows, _, seq_len = k_buf.shape

    def load(which, b):
        src, dst = ((k_hbm, k_buf), (v_hbm, v_buf))[which]
        return pltpu.make_async_copy(src.at[b], dst.at[b], in_sem.at[which, b])

    def save(which, b):
        src, dst = ((k_buf, ko_hbm), (v_buf, vo_hbm))[which]
        return pltpu.make_async_copy(src.at[b], dst.at[b], out_sem.at[which, b])

    for b in range(rows):
        load(0, b).start()
        load(1, b).start()

    lane = lax.broadcasted_iota(jnp.int32, (1, 128), 1)
    slots = lax.broadcasted_iota(jnp.int32, (1, seq_len), 1)

    def row(b, carry):
        length = len_ref[b]
        window = pl.ds(pl.multiple_of((length // 128) * 128, 128), 128)
        here = lane == length % 128
        for which, buf in enumerate((k_buf, v_buf)):
            load(which, b).wait()
            col = jnp.sum(jnp.where(lane == b, cols_ref[which], 0.0), axis=1, keepdims=True)
            tile = buf[b, :, window].astype(jnp.float32)
            buf[b, :, window] = jnp.where(here, col, tile).astype(jnp.bfloat16)
        scores = jnp.dot(q_ref[b], k_buf[b], preferred_element_type=jnp.float32) * scale
        scores = jnp.where(slots <= length, scores, -1e30)
        top = jnp.max(scores, axis=1, keepdims=True)
        weights = jnp.exp(scores - top)
        total = jnp.sum(weights, axis=1, keepdims=True)
        probs = (weights * (1.0 / total)).astype(jnp.bfloat16)
        save(0, b).start()
        save(1, b).start()
        o_ref[b] = lax.dot_general(probs, v_buf[b], (((1,), (1,)), ((), ())), preferred_element_type=jnp.float32).astype(jnp.bfloat16)
        return carry

    lax.fori_loop(0, rows, row, 0)
    for b in range(rows):
        save(0, b).wait()
        save(1, b).wait()


def attend(q_rot, cols, k_cache, v_cache, lengths):
    rows, heads, head_dim = q_rot.shape
    seq_len = k_cache.shape[1]
    k_t = jnp.swapaxes(k_cache, 1, 2)
    v_t = jnp.swapaxes(v_cache, 1, 2)
    cache = jax.ShapeDtypeStruct((rows, head_dim, seq_len), jnp.bfloat16)
    o, k_new, v_new = pl.pallas_call(
        functools.partial(attention_kernel, head_dim ** -0.5),
        out_shape=(jax.ShapeDtypeStruct((rows, heads, head_dim), jnp.bfloat16), cache, cache),
        in_specs=[
            pl.BlockSpec(memory_space=pltpu.SMEM),
            pl.BlockSpec(memory_space=pltpu.VMEM),
            pl.BlockSpec(memory_space=pltpu.VMEM),
            pl.BlockSpec(memory_space=pl.ANY),
            pl.BlockSpec(memory_space=pl.ANY),
        ],
        out_specs=(pl.BlockSpec(memory_space=pltpu.VMEM), pl.BlockSpec(memory_space=pl.ANY), pl.BlockSpec(memory_space=pl.ANY)),
        scratch_shapes=[
            pltpu.VMEM((rows, head_dim, seq_len), jnp.bfloat16),
            pltpu.VMEM((rows, head_dim, seq_len), jnp.bfloat16),
            pltpu.SemaphoreType.DMA((2, rows)),
            pltpu.SemaphoreType.DMA((2, rows)),
        ],
        compiler_params=pltpu.CompilerParams(vmem_limit_bytes=48 * 1024 * 1024),
        cost_estimate=pl.CostEstimate(
            flops=4 * rows * heads * head_dim * seq_len,
            bytes_accessed=8 * rows * head_dim * seq_len,
            transcendentals=rows * heads * seq_len,
        ),
        name='attend',
    )(lengths, q_rot, cols, k_t, v_t)
    return o, jnp.swapaxes(k_new, 1, 2), jnp.swapaxes(v_new, 1, 2)


def start_barrier(me_x, me_yz, everyone):
    barrier = pltpu.get_barrier_semaphore()
    peers = [(dx, k) for dx in range(2) for k in range(4) if (dx or k) and (everyone or not (dx and k))]
    for dx, k in peers:
        pl.semaphore_signal(barrier, inc=1, device_id=(lax.rem(me_x + dx, 2), lax.rem(me_yz + k, 4)), device_id_type=MESH)
    return lambda: pl.semaphore_wait(barrier, len(peers))


def spread(rows, cols, first):
    i = lax.broadcasted_iota(jnp.int32, (rows, cols), 0)
    c = lax.broadcasted_iota(jnp.int32, (rows, cols), 1)
    return jnp.where(c == 2 * i + first, 1.0, 0.0).astype(jnp.bfloat16)


def head_kernel(
    d_model, early, x_hbm, scale_hbm, wg_hbm, wa_hbm, z_hbm, first_hbm, send_hbm, own_hbm,
    xg, scale_row, sg, stats, h_buf, hx, wg, wa, z_send, z_own, z_recv, r_send, r_own, r_recv, zb, zg, g_first, g_rest, g_own,
    in_sem, wg_sem, x_send, x_recv, s_send, s_recv, t_send, t_recv, z_sems, a_send, a_recv, f_send, f_recv, out_sem,
):
    me_x = lax.axis_index('x')
    me_yz = lax.axis_index('yz')
    half, chunk = xg.shape[2:]
    rows = 2 * half
    pieces = wg_sem.shape[0]
    depth = wg.shape[0] // pieces
    ff = wg.shape[2]
    wide_cols = 256
    full = z_send.shape[2]
    quarter = half // 2
    third = quarter // 3
    tail_cols = wa.shape[0] - full
    other_x = lax.rem(me_x + 1, 2)
    across = lax.rem(me_yz + 2, 4)
    core = lax.rem(me_yz, 2)
    partner = me_yz + 1 - 2 * core
    order = (other_x, me_x)
    x_in = [
        pltpu.make_async_copy(x_hbm.at[pl.ds(pl.multiple_of(order[p] * half, 32), half)], xg.at[me_yz, order[p]], in_sem.at[p]) for p in range(2)
    ]
    scale_in = pltpu.make_async_copy(scale_hbm, scale_row, in_sem.at[2])
    wa_in = pltpu.make_async_copy(wa_hbm, wa, in_sem.at[3])
    wg_in = [
        pltpu.make_async_copy(wg_hbm.at[pl.ds(depth * i, depth)], wg.at[pl.ds(depth * i, depth)], wg_sem.at[i]) for i in range(pieces)
    ]
    for copy in (*x_in, scale_in, wa_in):
        copy.start()
    others_ready = start_barrier(me_x, me_yz, True)

    def remote(src, dst, send, recv, to_x, to_yz):
        return pltpu.make_async_remote_copy(
            src_ref=src, dst_ref=dst, send_sem=send, recv_sem=recv, device_id=(to_x, to_yz), device_id_type=MESH,
        )

    def x_copy(kind, piece):
        owner = across if kind == 2 else me_yz
        at = xg.at[owner, order[piece // 2], pl.ds(quarter * (piece % 2), quarter)]
        return remote(at, at, x_send.at[kind, piece], x_recv.at[kind, piece], me_x, across if kind == 1 else partner)

    for p in range(2):
        x_in[p].wait()
    lane = lax.broadcasted_iota(jnp.int32, (8, 128), 1)
    tile = jnp.zeros((8, 128), jnp.float32)
    for e in range(2):
        mine = xg[me_yz, e].astype(jnp.float32)
        sum_1 = jnp.sum(mine, axis=1, keepdims=True)
        sum_2 = jnp.sum(mine * mine, axis=1, keepdims=True)
        for j in range(half // 8):
            col = e * (half // 8) + j
            tile = jnp.where(lane == col, sum_1[8 * j:8 * j + 8], tile)
            tile = jnp.where(lane == 32 + col, sum_2[8 * j:8 * j + 8], tile)
    me = me_x * 4 + me_yz
    stats[me] = tile
    others_ready()
    x_copy(1, 0).start()
    x_copy(0, 0).start()
    t_out = [
        remote(stats.at[me], stats.at[me], t_send.at[4 * dx + k], t_recv.at[4 * dx + k], lax.rem(me_x + dx, 2), lax.rem(me_yz + k, 4))
        for dx in range(2) for k in range(4) if dx or k
    ]
    for copy in t_out:
        copy.start()
    scale_in.wait()
    sg[me_yz] = scale_row[...].reshape(1, chunk)
    s_out = [remote(sg.at[me_yz], sg.at[me_yz], s_send.at[k], s_recv.at[k], me_x, lax.rem(me_yz + k, 4)) for k in (1, 2, 3)]
    for copy in s_out:
        copy.start()
    for piece in range(1, 4):
        x_copy(1, piece).start()
        x_copy(0, piece).start()
    for copy in wg_in:
        copy.start()
    wide, thin = spread(128, 256, 0), spread(64, 128, 0)
    wide_u, thin_u = spread(128, 256, 1), spread(64, 128, 1)
    x_copy(1, 0).wait()
    x_copy(2, 0).start()
    for copy in t_out:
        copy.wait()
    total = stats[0]
    for i in range(1, 8):
        total = total + stats[i]
    mean_t = total / d_model
    var_t = pltpu.roll(total, 96, 1) / d_model - mean_t * mean_t
    rstd_t = lax.rsqrt(var_t + LN_EPS)
    for copy in s_out:
        copy.wait()

    chip = me_yz // 2
    contract = (((1,), (1,)), ((), ()))

    def pass_on(piece):
        x_copy(1, piece).wait()
        x_copy(2, piece).start()

    def project_chip(piece, which):
        p, q = piece // 2, piece % 2
        blocks = quarter // 8
        shift = lax.rem(256 - order[p] * (half // 8) - q * blocks, 128)
        mean_p = pltpu.roll(mean_t, shift, 1)
        rstd_p = pltpu.roll(rstd_t, shift, 1)
        mean = jnp.concatenate([mean_p[:, j:j + 1] for j in range(blocks)], axis=0)
        rstd = jnp.concatenate([rstd_p[:, j:j + 1] for j in range(blocks)], axis=0)
        here = pl.ds(quarter * q, quarter)
        both = []
        for e in range(2):
            s = 2 * which + e
            h = (xg[s, order[p], here].astype(jnp.float32) - mean) * rstd * sg[s]
            h_buf[s, here] = h.astype(jnp.bfloat16)
            both.append(h)
        h = jnp.concatenate(both, axis=1).astype(jnp.bfloat16)
        at = pl.ds(pl.multiple_of(2 * chunk * which, 128), 2 * chunk)
        z = lax.dot_general(h, wa[:full, at], contract, preferred_element_type=jnp.float32)
        r = lax.dot_general(h, wa[full:, at], contract, preferred_element_type=jnp.float32)
        return z, r

    def near(piece):
        x_copy(0, piece).wait()
        return project_chip(piece, chip)

    def far(piece, z, r, z_ref, r_ref):
        x_copy(2, piece).wait()
        z_far, r_far = project_chip(piece, 1 - chip)
        q = piece % 2
        z_ref[2 * q:2 * q + 2] = (z + z_far).reshape(2, quarter // 2, full)
        r = r + r_far
        r_ref[q] = jnp.concatenate([r[third * i:third * i + third] for i in range(3)], axis=1)

    def z_copies(q):
        at = pl.ds(2 * q, 2)
        return (
            remote(z_send.at[at], z_recv.at[at], z_sems.at[0, q], z_sems.at[1, q], other_x, me_yz),
            remote(r_send.at[q], r_recv.at[q], z_sems.at[2, q], z_sems.at[3, q], other_x, me_yz),
        )

    def spread_half(part, g):
        out = pl.ds((2 * part + g) * half, half)
        a, b = ((wide, thin), (wide_u, thin_u))[g]
        for s in range(4):
            base = 2 * chunk * s
            for t in range(2):
                piece = h_buf[s, :, 128 * t:128 * t + 128]
                hx[out, base + 256 * t:base + 256 * t + 256] = jnp.dot(piece, a, preferred_element_type=jnp.float32).astype(jnp.bfloat16)
            piece = h_buf[s, :, 256:320]
            hx[out, base + 512:base + 640] = jnp.dot(piece, b, preferred_element_type=jnp.float32).astype(jnp.bfloat16)

    wa_in.wait()
    z_out = [*z_copies(0), *z_copies(1)]
    far(0, *near(0), z_send, r_send)
    z_out[0].start()
    z_out[1].start()
    pass_on(1)
    part_1 = near(1)
    pass_on(2)
    far(1, *part_1, z_send, r_send)
    z_out[2].start()
    z_out[3].start()
    pass_on(3)
    spread_half(0, 0)
    spread_half(0, 1)
    for copy in wg_in:
        copy.wait()

    def block(c):
        at = pl.ds(pl.multiple_of(c * wide_cols, wide_cols), wide_cols)
        return wg[:, :, at].reshape(2 * wg.shape[0], wide_cols)

    def keep_own(c, out):
        g_own[:, pl.ds(pl.multiple_of(c * wide_cols, wide_cols), wide_cols)] = out[:half]
        g_own[:, pl.ds(pl.multiple_of(ff + c * wide_cols, wide_cols), wide_cols)] = out[half:]

    first = []
    for c in range(early):
        out = jnp.dot(hx[:rows], block(c), preferred_element_type=jnp.float32)
        g_first[c, :, :wide_cols] = out[:half]
        g_first[c, :, wide_cols:] = out[half:]
        first.append(remote(g_first.at[c], first_hbm.at[c], f_send.at[c], f_recv.at[c], other_x, me_yz))
        first[-1].start()
    for piece in (2, 3):
        far(piece, *near(piece), z_own, r_own)
    spread_half(1, 0)
    spread_half(1, 1)
    for c in range(early):
        keep_own(c, jnp.dot(hx[rows:], block(c), preferred_element_type=jnp.float32))

    def rest(c, carry):
        out = jnp.dot(hx[...], block(c), preferred_element_type=jnp.float32)
        keep_own(c, out[rows:])
        at = (c - early) * wide_cols
        g_rest[:, pl.ds(pl.multiple_of(at, wide_cols), wide_cols)] = out[:half]
        g_rest[:, pl.ds(pl.multiple_of(ff - early * wide_cols + at, wide_cols), wide_cols)] = out[half:2 * half]
        return carry

    middle = early + 4
    lax.fori_loop(early, middle, rest, 0)
    for copy in z_out:
        copy.wait()
    zb[:, :, :full] = (z_own[...] + z_recv[...]).astype(jnp.bfloat16)
    for q in range(2):
        r = r_own[q] + r_recv[q]
        r = jnp.concatenate([r[:, tail_cols * i:tail_cols * i + tail_cols] for i in range(3)], axis=0)
        zb[2 * q:2 * q + 2, :, full:] = r.reshape(2, quarter // 2, tail_cols).astype(jnp.bfloat16)
    a_out = [remote(zb.at[lax.rem(me_yz + k, 4)], zg.at[me_yz], a_send.at[k], a_recv.at[k], me_x, lax.rem(me_yz + k, 4)) for k in (1, 2, 3)]
    for copy in a_out:
        copy.start()
    zg[me_yz] = zb[me_yz]
    lax.fori_loop(middle, ff // wide_cols, rest, 0)
    save = [pltpu.make_async_copy(g_rest, send_hbm, out_sem.at[0]), pltpu.make_async_copy(g_own, own_hbm, out_sem.at[1])]
    for copy in save:
        copy.start()
    for copy in a_out:
        copy.wait()
    save.append(pltpu.make_async_copy(zg, z_hbm, out_sem.at[2]))
    save[-1].start()
    for copy in first:
        copy.wait()
    for copy in save:
        copy.wait()


def head(x_in, ln_scale, w_gate_up, w_attn, d_model, early):
    rows, chunk = x_in.shape
    depth, _, ff = w_gate_up.shape
    z_cols = w_attn.shape[1]
    full = z_cols // 128 * 128
    owned = rows // 8
    half = rows // 2
    width = 2 * (ff - 256 * early)
    any_spec = pl.BlockSpec(memory_space=pl.ANY)
    dma = pltpu.SemaphoreType.DMA
    f32, bf16 = jnp.float32, jnp.bfloat16
    return pl.pallas_call(
        functools.partial(head_kernel, d_model, early),
        out_shape=(
            jax.ShapeDtypeStruct((4, owned, z_cols), bf16),
            jax.ShapeDtypeStruct((early, half, 512), f32),
            jax.ShapeDtypeStruct((half, width), f32),
            jax.ShapeDtypeStruct((half, 2 * ff), f32),
        ),
        in_specs=[any_spec] * 4,
        out_specs=[any_spec] * 4,
        scratch_shapes=[
            pltpu.VMEM((4, 2, half, chunk), bf16),
            pltpu.VMEM((chunk,), f32),
            pltpu.VMEM((4, 1, chunk), f32),
            pltpu.VMEM((8, 8, 128), f32),
            pltpu.VMEM((4, half, chunk), bf16),
            pltpu.VMEM((2 * rows, 2 * depth), bf16),
            pltpu.VMEM((depth, 2, ff), bf16),
            pltpu.VMEM((z_cols, depth), bf16),
            *[pltpu.VMEM((4, owned, full), f32)] * 3,
            *[pltpu.VMEM((2, half // 6, 3 * (z_cols - full)), f32)] * 3,
            pltpu.VMEM((4, owned, z_cols), bf16),
            pltpu.VMEM((4, owned, z_cols), bf16),
            pltpu.VMEM((early, half, 512), f32),
            pltpu.VMEM((half, width), f32),
            pltpu.VMEM((half, 2 * ff), f32),
            dma((4,)), dma((8,)), dma((3, 4)), dma((3, 4)), dma((4,)), dma((4,)), dma((8,)), dma((8,)), dma((4, 2)), dma((4,)), dma((4,)),
            dma((early,)), dma((early,)), dma((3,)),
        ],
        compiler_params=pltpu.CompilerParams(collective_id=0, has_side_effects=True, vmem_limit_bytes=VMEM_MOST),
        cost_estimate=pl.CostEstimate(flops=4 * rows * depth * 2 * ff, bytes_accessed=4 * depth * ff, transcendentals=0),
        name='head',
    )(x_in, ln_scale, w_gate_up, w_attn.T)


def tail_kernel(
    g_first, g_peer, own_hbm, ov, wd_hbm, wo_hbm, y_ref,
    g_own, oy, oa, of, hb, wd, wo, out_part, y_send, y_pair, y_over, y_recv,
    in_sem, own_sem, o_send, o_recv, h_send, h_recv, p_send, p_recv, y_ssem, y_rsem,
):
    me_x = lax.axis_index('x')
    me_yz = lax.axis_index('yz')
    groups, _, span, ff = hb.shape
    rows, chunk = y_ref.shape
    half = rows // 2
    owned = ov.shape[1]
    early, _, wide = g_first.shape
    wide = wide // 2
    core = lax.rem(me_yz, 2)
    col = me_yz // 2
    partner = me_yz + 1 - 2 * core
    across = lax.rem(me_yz + 2, 4)
    other_x = lax.rem(me_x + 1, 2)

    own_in = [pltpu.make_async_copy(own_hbm.at[pl.ds(span * i, span)], g_own.at[pl.ds(span * i, span)], own_sem.at[i]) for i in range(groups)]
    wo_in = pltpu.make_async_copy(wo_hbm, wo, in_sem.at[1])
    wd_in = pltpu.make_async_copy(wd_hbm, wd, in_sem.at[2])
    for copy in (*own_in, wo_in, wd_in):
        copy.start()
    start_barrier(me_x, me_yz, False)()
    me = me_x * 4 + me_yz

    def remote(src, dst, send, recv, to_x, to_yz):
        return pltpu.make_async_remote_copy(
            src_ref=src, dst_ref=dst, send_sem=send, recv_sem=recv, device_id=(to_x, to_yz), device_id_type=MESH,
        )

    other = other_x * 4 + me_yz
    o_over = remote(ov, oy, o_send.at[0], o_recv.at[0], other_x, me_yz)
    o_over.start()
    there = [lax.rem(me_yz + k, 4) for k in range(4)]
    o_out = [remote(ov.at[there[k]], oa.at[me], o_send.at[k], o_recv.at[k], me_x, there[k]) for k in (1, 2, 3)]
    for copy in o_out:
        copy.start()
    oa[me] = ov[me_yz]

    def h_copy(i, part):
        at = hb.at[i, me_x, :, pl.ds(part * (ff // 2), ff // 2)]
        return remote(at, at, h_send.at[i, part], h_recv.at[i, part], other_x, me_yz)

    for copy in own_in:
        copy.wait()

    def activate(i, carry):
        at = pl.ds(pl.multiple_of(span * i, span), span)

        def act(gate, up):
            gate = gate.astype(jnp.bfloat16).astype(jnp.float32)
            up = up.astype(jnp.bfloat16).astype(jnp.float32)
            return (jax.nn.silu(gate) * up).astype(jnp.bfloat16)

        for c in range(early):
            cols = slice(wide * c, wide * c + wide)
            up_cols = slice(ff + wide * c, ff + wide * c + wide)
            hb[i, me_x, :, cols] = act(g_own[at, cols] + g_first[c, at, :wide], g_own[at, up_cols] + g_first[c, at, wide:])
        done = early * wide
        hb[i, me_x, :, done:] = act(g_own[at, done:ff] + g_peer[at, :ff - done], g_own[at, ff + done:] + g_peer[at, ff - done:])
        h_copy(i, 0).start()
        h_copy(i, 1).start()
        return carry

    lax.fori_loop(0, groups, activate, 0)
    o_over.wait()
    relay = [remote(oy.at[there[k]], oa.at[other], o_send.at[3 + k], o_recv.at[3 + k], me_x, there[k]) for k in (1, 2, 3)]
    for copy in relay:
        copy.start()
    oa[other] = oy[me_yz]
    for copy in (*o_out, *relay):
        copy.wait()
    for e in range(8):
        of[owned * e:owned * e + owned] = oa[e].astype(jnp.float32)
    wo_in.wait()
    out_part[...] = jnp.dot(of[...].astype(jnp.bfloat16), wo[...], preferred_element_type=jnp.float32)
    wd_in.wait()

    def pair_copy(i, which):
        return remote(y_send.at[i, 2 * which + 1 - core], y_pair.at[i, which], p_send.at[i, which], p_recv.at[i, which], me_x, partner)

    def over_copy(i):
        return remote(y_over.at[i], y_recv.at[i], y_ssem.at[i], y_rsem.at[i], me_x, across)

    def cross(i):
        pair_copy(i, 1 - col).wait()
        y_over[i] = y_send[i, across] + y_pair[i, 1 - col]
        over_copy(i).start()

    def product(i, carry):
        first_at = pl.multiple_of(span * i, span)
        part = 0.0
        for k in range(2):
            h_copy(i, k).wait()
            cols = slice(k * (ff // 2), (k + 1) * (ff // 2))
            part = part + jnp.dot(hb[i, :, :, cols].reshape(2 * span, ff // 2), wd[cols, :], preferred_element_type=jnp.float32)
        part = part + jnp.concatenate([out_part[pl.ds(first_at, span)], out_part[pl.ds(half + first_at, span)]], axis=0)
        for j in range(4):
            moved = part if j == 0 else pltpu.roll(part, (4 - j) * chunk, 1)
            y_send[i, j] = moved[:, :chunk]
        for which in (1 - col, col):
            pair_copy(i, which).start()

        @pl.when(i > 0)
        def _():
            cross(i - 1)

        return carry

    def finish(i, carry):
        pair_copy(i, col).wait()
        over_copy(i).wait()
        total = y_send[i, me_yz] + y_pair[i, col] + y_recv[i]
        for e in range(2):
            y_ref[pl.ds(pl.multiple_of(half * e + span * i, span), span), :] = total[span * e:span * e + span]
        return carry

    lax.fori_loop(0, groups, product, 0)
    lax.fori_loop(0, groups - 3, finish, 0)
    cross(groups - 1)
    lax.fori_loop(groups - 3, groups, finish, 0)


def tail(g_first, g_peer, g_own, o_blocks, w_down, w_out):
    half = g_own.shape[0]
    rows = 2 * half
    span = 16
    groups = half // span
    ff, cols = w_down.shape
    chunk = cols // 4
    owned = o_blocks.shape[1]
    o_width = w_out.shape[0]
    any_spec, vmem_spec = pl.BlockSpec(memory_space=pl.ANY), pl.BlockSpec(memory_space=pltpu.VMEM)
    dma = pltpu.SemaphoreType.DMA
    f32, bf16 = jnp.float32, jnp.bfloat16
    return pl.pallas_call(
        tail_kernel,
        out_shape=jax.ShapeDtypeStruct((rows, chunk), f32),
        in_specs=[vmem_spec, vmem_spec, any_spec, vmem_spec, any_spec, any_spec],
        out_specs=pl.BlockSpec(memory_space=pltpu.VMEM),
        scratch_shapes=[
            pltpu.VMEM((half, 2 * ff), f32),
            pltpu.VMEM((4, owned, o_width), bf16),
            pltpu.VMEM((8, owned, o_width), bf16),
            pltpu.VMEM((rows, o_width), f32),
            pltpu.VMEM((groups, 2, span, ff), bf16),
            pltpu.VMEM((ff, cols), bf16),
            pltpu.VMEM((o_width, cols), bf16),
            pltpu.VMEM((rows, cols), f32),
            pltpu.VMEM((groups, 4, 2 * span, chunk), f32),
            pltpu.VMEM((groups, 2, 2 * span, chunk), f32),
            pltpu.VMEM((groups, 2 * span, chunk), f32),
            pltpu.VMEM((groups, 2 * span, chunk), f32),
            dma((3,)), dma((groups,)), dma((8,)), dma((8,)), dma((groups, 2)), dma((groups, 2)),
            dma((groups, 2)), dma((groups, 2)), dma((groups,)), dma((groups,)),
        ],
        compiler_params=pltpu.CompilerParams(collective_id=1, has_side_effects=True, vmem_limit_bytes=51 * 1024 * 1024),
        cost_estimate=pl.CostEstimate(flops=2 * rows * (ff + o_width) * cols, bytes_accessed=2 * (ff + o_width) * cols, transcendentals=half * ff),
        name='tail',
    )(g_first, g_peer, g_own, o_blocks, w_down, w_out)


def rotary(values, positions):
    half_dim = values.shape[-1] // 2
    inv_freq = ROPE_BASE ** (-jnp.arange(half_dim, dtype=jnp.float32) / half_dim)
    angles = positions.astype(jnp.float32)[:, None, None] * inv_freq
    cos_part = jnp.cos(angles)
    sin_part = jnp.sin(angles)
    lo_half = values[..., :half_dim]
    hi_half = values[..., half_dim:]
    return jnp.concatenate([lo_half * cos_part - hi_half * sin_part, hi_half * cos_part + lo_half * sin_part], axis=-1)


def solution(mesh):
    x_size = mesh.shape['x']
    yz_size = mesh.shape['yz']
    all_axes = ('x', 'yz')

    def local_step(x_in, ln_scale, w_gate_up, w_attn, w_down, w_out, k_cache, v_cache, lengths, positions):
        local_rows, seq_len, head_dim = k_cache.shape
        q_width = w_out.shape[0] * yz_size
        num_heads = q_width // head_dim
        d_model = x_in.shape[1] * x_size * yz_size
        z_blocks, g_first, g_send, g_own = head(x_in, ln_scale, w_gate_up, w_attn, d_model, EARLY)
        g_peer = lax.ppermute(g_send, 'x', [(0, 1), (1, 0)])
        proj_local = z_blocks.transpose(1, 0, 2).reshape(local_rows, -1)
        q_raw = proj_local[:, :q_width].reshape(local_rows, num_heads, head_dim)
        k_tok = proj_local[:, q_width:q_width + head_dim]
        v_tok = proj_local[:, q_width + head_dim:]
        q_rot = rotary(q_raw.astype(jnp.float32), positions).astype(jnp.bfloat16)
        k_rot = rotary(k_tok[:, None, :].astype(jnp.float32), positions)[:, 0].astype(jnp.bfloat16)
        cols = jnp.stack([k_rot, v_tok]).astype(jnp.float32).transpose(0, 2, 1)
        cols = jnp.pad(cols, ((0, 0), (0, 0), (0, 128 - local_rows)))
        attn_out, k_new, v_new = attend(q_rot, cols, k_cache, v_cache, lengths)
        o_blocks = attn_out.reshape(local_rows, yz_size, q_width // yz_size).transpose(1, 0, 2)
        mixed_sum = tail(g_first, g_peer, g_own, o_blocks, w_down, w_out)
        y_out = (x_in.astype(jnp.float32) + mixed_sum).astype(jnp.bfloat16)
        return y_out, k_new, v_new

    row_spec = P(None, all_axes)
    vec_spec = P(all_axes)
    cache_spec = P(all_axes, None, None)
    return jax.shard_map(
        local_step,
        mesh=mesh,
        in_specs=(row_spec, vec_spec, P('x', None, 'yz'), P('x', 'yz'), P('yz', 'x'), P('yz', 'x'), cache_spec, cache_spec, vec_spec, vec_spec),
        out_specs=(row_spec, cache_spec, cache_spec),
        check_vma=False,
    )
```

```python
import functools

import jax
import jax.numpy as jnp
from jax import lax
from jax.experimental import pallas as pl
from jax.experimental.pallas import tpu as pltpu
from jax.sharding import PartitionSpec as P

LN_EPS = 1e-6
ROPE_BASE = 10000.0
MESH = pl.DeviceIdType.MESH
VMEM_MOST = 64 * 1024 * 1024 - 64 * 1024
EARLY = 2


def attention_kernel(scale, len_ref, q_ref, cols_ref, k_hbm, v_hbm, o_ref, ko_hbm, vo_hbm, k_buf, v_buf, in_sem, out_sem):
    rows, _, seq_len = k_buf.shape

    def load(which, b):
        src, dst = ((k_hbm, k_buf), (v_hbm, v_buf))[which]
        return pltpu.make_async_copy(src.at[b], dst.at[b], in_sem.at[which, b])

    def save(which, b):
        src, dst = ((k_buf, ko_hbm), (v_buf, vo_hbm))[which]
        return pltpu.make_async_copy(src.at[b], dst.at[b], out_sem.at[which, b])

    for b in range(rows):
        load(0, b).start()
        load(1, b).start()

    lane = lax.broadcasted_iota(jnp.int32, (1, 128), 1)
    slots = lax.broadcasted_iota(jnp.int32, (1, seq_len), 1)

    def row(b, carry):
        length = len_ref[b]
        window = pl.ds(pl.multiple_of((length // 128) * 128, 128), 128)
        here = lane == length % 128
        for which, buf in enumerate((k_buf, v_buf)):
            load(which, b).wait()
            col = jnp.sum(jnp.where(lane == b, cols_ref[which], 0.0), axis=1, keepdims=True)
            tile = buf[b, :, window].astype(jnp.float32)
            buf[b, :, window] = jnp.where(here, col, tile).astype(jnp.bfloat16)
        scores = jnp.dot(q_ref[b], k_buf[b], preferred_element_type=jnp.float32) * scale
        scores = jnp.where(slots <= length, scores, -1e30)
        top = jnp.max(scores, axis=1, keepdims=True)
        weights = jnp.exp(scores - top)
        total = jnp.sum(weights, axis=1, keepdims=True)
        probs = (weights * (1.0 / total)).astype(jnp.bfloat16)
        save(0, b).start()
        save(1, b).start()
        o_ref[b] = lax.dot_general(probs, v_buf[b], (((1,), (1,)), ((), ())), preferred_element_type=jnp.float32).astype(jnp.bfloat16)
        return carry

    lax.fori_loop(0, rows, row, 0)
    for b in range(rows):
        save(0, b).wait()
        save(1, b).wait()


def attend(q_rot, cols, k_cache, v_cache, lengths):
    rows, heads, head_dim = q_rot.shape
    seq_len = k_cache.shape[1]
    k_t = jnp.swapaxes(k_cache, 1, 2)
    v_t = jnp.swapaxes(v_cache, 1, 2)
    cache = jax.ShapeDtypeStruct((rows, head_dim, seq_len), jnp.bfloat16)
    o, k_new, v_new = pl.pallas_call(
        functools.partial(attention_kernel, head_dim ** -0.5),
        out_shape=(jax.ShapeDtypeStruct((rows, heads, head_dim), jnp.bfloat16), cache, cache),
        in_specs=[
            pl.BlockSpec(memory_space=pltpu.SMEM),
            pl.BlockSpec(memory_space=pltpu.VMEM),
            pl.BlockSpec(memory_space=pltpu.VMEM),
            pl.BlockSpec(memory_space=pl.ANY),
            pl.BlockSpec(memory_space=pl.ANY),
        ],
        out_specs=(pl.BlockSpec(memory_space=pltpu.VMEM), pl.BlockSpec(memory_space=pl.ANY), pl.BlockSpec(memory_space=pl.ANY)),
        scratch_shapes=[
            pltpu.VMEM((rows, head_dim, seq_len), jnp.bfloat16),
            pltpu.VMEM((rows, head_dim, seq_len), jnp.bfloat16),
            pltpu.SemaphoreType.DMA((2, rows)),
            pltpu.SemaphoreType.DMA((2, rows)),
        ],
        compiler_params=pltpu.CompilerParams(vmem_limit_bytes=48 * 1024 * 1024),
        cost_estimate=pl.CostEstimate(
            flops=4 * rows * heads * head_dim * seq_len,
            bytes_accessed=8 * rows * head_dim * seq_len,
            transcendentals=rows * heads * seq_len,
        ),
        name='attend',
    )(lengths, q_rot, cols, k_t, v_t)
    return o, jnp.swapaxes(k_new, 1, 2), jnp.swapaxes(v_new, 1, 2)


def start_barrier(me_x, me_yz, everyone):
    barrier = pltpu.get_barrier_semaphore()
    peers = [(dx, k) for dx in range(2) for k in range(4) if (dx or k) and (everyone or not (dx and k))]
    for dx, k in peers:
        pl.semaphore_signal(barrier, inc=1, device_id=(lax.rem(me_x + dx, 2), lax.rem(me_yz + k, 4)), device_id_type=MESH)
    return lambda: pl.semaphore_wait(barrier, len(peers))


def spread(rows, cols, first):
    i = lax.broadcasted_iota(jnp.int32, (rows, cols), 0)
    c = lax.broadcasted_iota(jnp.int32, (rows, cols), 1)
    return jnp.where(c == 2 * i + first, 1.0, 0.0).astype(jnp.bfloat16)


def head_kernel(
    d_model, early, x_hbm, scale_hbm, wg_hbm, wa_hbm, z_hbm, first_hbm, send_hbm, own_hbm,
    xg, scale_row, sg, stats, h_buf, hx, wg, wa, z_send, z_own, z_recv, r_send, r_own, r_recv, zb, zg, g_first, g_rest, g_own,
    in_sem, wg_sem, x_send, x_recv, s_send, s_recv, t_send, t_recv, z_sems, a_send, a_recv, f_send, f_recv, out_sem,
):
    me_x = lax.axis_index('x')
    me_yz = lax.axis_index('yz')
    half, chunk = xg.shape[2:]
    rows = 2 * half
    pieces = wg_sem.shape[0]
    depth = wg.shape[0] // pieces
    ff = wg.shape[2]
    wide_cols = 256
    full = z_send.shape[2]
    quarter = half // 2
    third = quarter // 3
    tail_cols = wa.shape[0] - full
    other_x = lax.rem(me_x + 1, 2)
    across = lax.rem(me_yz + 2, 4)
    core = lax.rem(me_yz, 2)
    partner = me_yz + 1 - 2 * core
    order = (other_x, me_x)
    x_in = [
        pltpu.make_async_copy(x_hbm.at[pl.ds(pl.multiple_of(order[p] * half, 32), half)], xg.at[me_yz, order[p]], in_sem.at[p]) for p in range(2)
    ]
    scale_in = pltpu.make_async_copy(scale_hbm, scale_row, in_sem.at[2])
    wa_in = pltpu.make_async_copy(wa_hbm, wa, in_sem.at[3])
    wg_in = [
        pltpu.make_async_copy(wg_hbm.at[pl.ds(depth * i, depth)], wg.at[pl.ds(depth * i, depth)], wg_sem.at[i]) for i in range(pieces)
    ]
    for copy in (*x_in, scale_in, wa_in):
        copy.start()
    others_ready = start_barrier(me_x, me_yz, True)

    def remote(src, dst, send, recv, to_x, to_yz):
        return pltpu.make_async_remote_copy(
            src_ref=src, dst_ref=dst, send_sem=send, recv_sem=recv, device_id=(to_x, to_yz), device_id_type=MESH,
        )

    def x_copy(kind, piece):
        owner = across if kind == 2 else me_yz
        at = xg.at[owner, order[piece // 2], pl.ds(quarter * (piece % 2), quarter)]
        return remote(at, at, x_send.at[kind, piece], x_recv.at[kind, piece], me_x, across if kind == 1 else partner)

    for p in range(2):
        x_in[p].wait()
    lane = lax.broadcasted_iota(jnp.int32, (8, 128), 1)
    tile = jnp.zeros((8, 128), jnp.float32)
    for e in range(2):
        mine = xg[me_yz, e].astype(jnp.float32)
        sum_1 = jnp.sum(mine, axis=1, keepdims=True)
        sum_2 = jnp.sum(mine * mine, axis=1, keepdims=True)
        for j in range(half // 8):
            col = e * (half // 8) + j
            tile = jnp.where(lane == col, sum_1[8 * j:8 * j + 8], tile)
            tile = jnp.where(lane == 32 + col, sum_2[8 * j:8 * j + 8], tile)
    me = me_x * 4 + me_yz
    stats[me] = tile
    others_ready()
    x_copy(1, 0).start()
    x_copy(0, 0).start()
    t_out = [
        remote(stats.at[me], stats.at[me], t_send.at[4 * dx + k], t_recv.at[4 * dx + k], lax.rem(me_x + dx, 2), lax.rem(me_yz + k, 4))
        for dx in range(2) for k in range(4) if dx or k
    ]
    for copy in t_out:
        copy.start()
    scale_in.wait()
    sg[me_yz] = scale_row[...].reshape(1, chunk)
    s_out = [remote(sg.at[me_yz], sg.at[me_yz], s_send.at[k], s_recv.at[k], me_x, lax.rem(me_yz + k, 4)) for k in (1, 2, 3)]
    for copy in s_out:
        copy.start()
    for piece in range(1, 4):
        x_copy(1, piece).start()
        x_copy(0, piece).start()
    for copy in wg_in:
        copy.start()
    wide, thin = spread(128, 256, 0), spread(64, 128, 0)
    wide_u, thin_u = spread(128, 256, 1), spread(64, 128, 1)
    x_copy(1, 0).wait()
    x_copy(2, 0).start()
    for copy in t_out:
        copy.wait()
    total = stats[0]
    for i in range(1, 8):
        total = total + stats[i]
    mean_t = total / d_model
    var_t = pltpu.roll(total, 96, 1) / d_model - mean_t * mean_t
    rstd_t = lax.rsqrt(var_t + LN_EPS)
    for copy in s_out:
        copy.wait()

    chip = me_yz // 2
    contract = (((1,), (1,)), ((), ()))

    def pass_on(piece):
        x_copy(1, piece).wait()
        x_copy(2, piece).start()

    def project_chip(piece, which):
        p, q = piece // 2, piece % 2
        blocks = quarter // 8
        shift = lax.rem(256 - order[p] * (half // 8) - q * blocks, 128)
        mean_p = pltpu.roll(mean_t, shift, 1)
        rstd_p = pltpu.roll(rstd_t, shift, 1)
        mean = jnp.concatenate([mean_p[:, j:j + 1] for j in range(blocks)], axis=0)
        rstd = jnp.concatenate([rstd_p[:, j:j + 1] for j in range(blocks)], axis=0)
        here = pl.ds(quarter * q, quarter)
        both = []
        for e in range(2):
            s = 2 * which + e
            h = (xg[s, order[p], here].astype(jnp.float32) - mean) * rstd * sg[s]
            h_buf[s, here] = h.astype(jnp.bfloat16)
            both.append(h)
        h = jnp.concatenate(both, axis=1).astype(jnp.bfloat16)
        at = pl.ds(pl.multiple_of(2 * chunk * which, 128), 2 * chunk)
        z = lax.dot_general(h, wa[:full, at], contract, preferred_element_type=jnp.float32)
        r = lax.dot_general(h, wa[full:, at], contract, preferred_element_type=jnp.float32)
        return z, r

    def near(piece):
        x_copy(0, piece).wait()
        return project_chip(piece, chip)

    def far(piece, z, r, z_ref, r_ref):
        x_copy(2, piece).wait()
        z_far, r_far = project_chip(piece, 1 - chip)
        q = piece % 2
        z_ref[2 * q:2 * q + 2] = (z + z_far).reshape(2, quarter // 2, full)
        r = r + r_far
        r_ref[q] = jnp.concatenate([r[third * i:third * i + third] for i in range(3)], axis=1)

    def z_copies(q):
        at = pl.ds(2 * q, 2)
        return (
            remote(z_send.at[at], z_recv.at[at], z_sems.at[0, q], z_sems.at[1, q], other_x, me_yz),
            remote(r_send.at[q], r_recv.at[q], z_sems.at[2, q], z_sems.at[3, q], other_x, me_yz),
        )

    def spread_half(part, g):
        out = pl.ds((2 * part + g) * half, half)
        a, b = ((wide, thin), (wide_u, thin_u))[g]
        for s in range(4):
            base = 2 * chunk * s
            for t in range(2):
                piece = h_buf[s, :, 128 * t:128 * t + 128]
                hx[out, base + 256 * t:base + 256 * t + 256] = jnp.dot(piece, a, preferred_element_type=jnp.float32).astype(jnp.bfloat16)
            piece = h_buf[s, :, 256:320]
            hx[out, base + 512:base + 640] = jnp.dot(piece, b, preferred_element_type=jnp.float32).astype(jnp.bfloat16)

    wa_in.wait()
    z_out = [*z_copies(0), *z_copies(1)]
    far(0, *near(0), z_send, r_send)
    z_out[0].start()
    z_out[1].start()
    pass_on(1)
    part_1 = near(1)
    pass_on(2)
    far(1, *part_1, z_send, r_send)
    z_out[2].start()
    z_out[3].start()
    pass_on(3)
    spread_half(0, 0)
    spread_half(0, 1)
    for copy in wg_in:
        copy.wait()

    def block(c):
        at = pl.ds(pl.multiple_of(c * wide_cols, wide_cols), wide_cols)
        return wg[:, :, at].reshape(2 * wg.shape[0], wide_cols)

    def keep_own(c, out):
        g_own[:, pl.ds(pl.multiple_of(c * wide_cols, wide_cols), wide_cols)] = out[:half]
        g_own[:, pl.ds(pl.multiple_of(ff + c * wide_cols, wide_cols), wide_cols)] = out[half:]

    first = []
    for c in range(early):
        out = jnp.dot(hx[:rows], block(c), preferred_element_type=jnp.float32)
        g_first[c, :, :wide_cols] = out[:half]
        g_first[c, :, wide_cols:] = out[half:]
        first.append(remote(g_first.at[c], first_hbm.at[c], f_send.at[c], f_recv.at[c], other_x, me_yz))
        first[-1].start()
    for piece in (2, 3):
        far(piece, *near(piece), z_own, r_own)
    spread_half(1, 0)
    spread_half(1, 1)
    for c in range(early):
        keep_own(c, jnp.dot(hx[rows:], block(c), preferred_element_type=jnp.float32))

    def rest(c, carry):
        out = jnp.dot(hx[...], block(c), preferred_element_type=jnp.float32)
        keep_own(c, out[rows:])
        at = (c - early) * wide_cols
        g_rest[:, pl.ds(pl.multiple_of(at, wide_cols), wide_cols)] = out[:half]
        g_rest[:, pl.ds(pl.multiple_of(ff - early * wide_cols + at, wide_cols), wide_cols)] = out[half:2 * half]
        return carry

    middle = early + 4
    lax.fori_loop(early, middle, rest, 0)
    for copy in z_out:
        copy.wait()
    zb[:, :, :full] = (z_own[...] + z_recv[...]).astype(jnp.bfloat16)
    for q in range(2):
        r = r_own[q] + r_recv[q]
        r = jnp.concatenate([r[:, tail_cols * i:tail_cols * i + tail_cols] for i in range(3)], axis=0)
        zb[2 * q:2 * q + 2, :, full:] = r.reshape(2, quarter // 2, tail_cols).astype(jnp.bfloat16)
    a_out = [remote(zb.at[lax.rem(me_yz + k, 4)], zg.at[me_yz], a_send.at[k], a_recv.at[k], me_x, lax.rem(me_yz + k, 4)) for k in (1, 2, 3)]
    for copy in a_out:
        copy.start()
    zg[me_yz] = zb[me_yz]
    lax.fori_loop(middle, ff // wide_cols, rest, 0)
    save = [pltpu.make_async_copy(g_rest, send_hbm, out_sem.at[0]), pltpu.make_async_copy(g_own, own_hbm, out_sem.at[1])]
    for copy in save:
        copy.start()
    for copy in a_out:
        copy.wait()
    save.append(pltpu.make_async_copy(zg, z_hbm, out_sem.at[2]))
    save[-1].start()
    for copy in first:
        copy.wait()
    for copy in save:
        copy.wait()


def head(x_in, ln_scale, w_gate_up, w_attn, d_model, early):
    rows, chunk = x_in.shape
    depth, _, ff = w_gate_up.shape
    z_cols = w_attn.shape[1]
    full = z_cols // 128 * 128
    owned = rows // 8
    half = rows // 2
    width = 2 * (ff - 256 * early)
    any_spec = pl.BlockSpec(memory_space=pl.ANY)
    dma = pltpu.SemaphoreType.DMA
    f32, bf16 = jnp.float32, jnp.bfloat16
    return pl.pallas_call(
        functools.partial(head_kernel, d_model, early),
        out_shape=(
            jax.ShapeDtypeStruct((4, owned, z_cols), bf16),
            jax.ShapeDtypeStruct((early, half, 512), f32),
            jax.ShapeDtypeStruct((half, width), f32),
            jax.ShapeDtypeStruct((half, 2 * ff), f32),
        ),
        in_specs=[any_spec] * 4,
        out_specs=[any_spec] * 4,
        scratch_shapes=[
            pltpu.VMEM((4, 2, half, chunk), bf16),
            pltpu.VMEM((chunk,), f32),
            pltpu.VMEM((4, 1, chunk), f32),
            pltpu.VMEM((8, 8, 128), f32),
            pltpu.VMEM((4, half, chunk), bf16),
            pltpu.VMEM((2 * rows, 2 * depth), bf16),
            pltpu.VMEM((depth, 2, ff), bf16),
            pltpu.VMEM((z_cols, depth), bf16),
            *[pltpu.VMEM((4, owned, full), f32)] * 3,
            *[pltpu.VMEM((2, half // 6, 3 * (z_cols - full)), f32)] * 3,
            pltpu.VMEM((4, owned, z_cols), bf16),
            pltpu.VMEM((4, owned, z_cols), bf16),
            pltpu.VMEM((early, half, 512), f32),
            pltpu.VMEM((half, width), f32),
            pltpu.VMEM((half, 2 * ff), f32),
            dma((4,)), dma((8,)), dma((3, 4)), dma((3, 4)), dma((4,)), dma((4,)), dma((8,)), dma((8,)), dma((4, 2)), dma((4,)), dma((4,)),
            dma((early,)), dma((early,)), dma((3,)),
        ],
        compiler_params=pltpu.CompilerParams(collective_id=0, has_side_effects=True, vmem_limit_bytes=VMEM_MOST),
        cost_estimate=pl.CostEstimate(flops=4 * rows * depth * 2 * ff, bytes_accessed=4 * depth * ff, transcendentals=0),
        name='head',
    )(x_in, ln_scale, w_gate_up, w_attn.T)


def tail_kernel(
    g_first, g_peer, own_hbm, ov, wd_hbm, wo_hbm, y_ref,
    g_own, oy, oa, of, hb, wd, wo, out_part, y_send, y_pair, y_over, y_recv,
    in_sem, own_sem, o_send, o_recv, h_send, h_recv, p_send, p_recv, y_ssem, y_rsem,
):
    me_x = lax.axis_index('x')
    me_yz = lax.axis_index('yz')
    groups, _, span, ff = hb.shape
    rows, chunk = y_ref.shape
    half = rows // 2
    owned = ov.shape[1]
    early, _, wide = g_first.shape
    wide = wide // 2
    core = lax.rem(me_yz, 2)
    col = me_yz // 2
    partner = me_yz + 1 - 2 * core
    across = lax.rem(me_yz + 2, 4)
    other_x = lax.rem(me_x + 1, 2)

    own_in = [pltpu.make_async_copy(own_hbm.at[pl.ds(span * i, span)], g_own.at[pl.ds(span * i, span)], own_sem.at[i]) for i in range(groups)]
    wo_in = pltpu.make_async_copy(wo_hbm, wo, in_sem.at[1])
    wd_in = pltpu.make_async_copy(wd_hbm, wd, in_sem.at[2])
    for copy in (*own_in, wo_in, wd_in):
        copy.start()
    start_barrier(me_x, me_yz, False)()
    me = me_x * 4 + me_yz

    def remote(src, dst, send, recv, to_x, to_yz):
        return pltpu.make_async_remote_copy(
            src_ref=src, dst_ref=dst, send_sem=send, recv_sem=recv, device_id=(to_x, to_yz), device_id_type=MESH,
        )

    other = other_x * 4 + me_yz
    o_over = remote(ov, oy, o_send.at[0], o_recv.at[0], other_x, me_yz)
    o_over.start()
    there = [lax.rem(me_yz + k, 4) for k in range(4)]
    o_out = [remote(ov.at[there[k]], oa.at[me], o_send.at[k], o_recv.at[k], me_x, there[k]) for k in (1, 2, 3)]
    for copy in o_out:
        copy.start()
    oa[me] = ov[me_yz]

    def h_copy(i):
        return remote(hb.at[i, me_x], hb.at[i, me_x], h_send.at[i], h_recv.at[i], other_x, me_yz)

    for copy in own_in:
        copy.wait()

    def activate(i, carry):
        at = pl.ds(pl.multiple_of(span * i, span), span)

        def act(gate, up):
            gate = gate.astype(jnp.bfloat16).astype(jnp.float32)
            up = up.astype(jnp.bfloat16).astype(jnp.float32)
            return (jax.nn.silu(gate) * up).astype(jnp.bfloat16)

        for c in range(early):
            cols = slice(wide * c, wide * c + wide)
            up_cols = slice(ff + wide * c, ff + wide * c + wide)
            hb[i, me_x, :, cols] = act(g_own[at, cols] + g_first[c, at, :wide], g_own[at, up_cols] + g_first[c, at, wide:])
        done = early * wide
        hb[i, me_x, :, done:] = act(g_own[at, done:ff] + g_peer[at, :ff - done], g_own[at, ff + done:] + g_peer[at, ff - done:])
        h_copy(i).start()
        return carry

    lax.fori_loop(0, groups, activate, 0)
    o_over.wait()
    relay = [remote(oy.at[there[k]], oa.at[other], o_send.at[3 + k], o_recv.at[3 + k], me_x, there[k]) for k in (1, 2, 3)]
    for copy in relay:
        copy.start()
    oa[other] = oy[me_yz]
    for copy in (*o_out, *relay):
        copy.wait()
    for e in range(8):
        of[owned * e:owned * e + owned] = oa[e].astype(jnp.float32)
    wo_in.wait()
    out_part[...] = jnp.dot(of[...].astype(jnp.bfloat16), wo[...], preferred_element_type=jnp.float32)
    wd_in.wait()

    def pair_copy(i, which):
        return remote(y_send.at[i, 2 * which + 1 - core], y_pair.at[i, which], p_send.at[i, which], p_recv.at[i, which], me_x, partner)

    def over_copy(i):
        return remote(y_over.at[i], y_recv.at[i], y_ssem.at[i], y_rsem.at[i], me_x, across)

    def cross(i):
        pair_copy(i, 1 - col).wait()
        y_over[i] = y_send[i, across] + y_pair[i, 1 - col]
        over_copy(i).start()

    def product(i, carry):
        h_copy(i).wait()
        first_at = pl.multiple_of(span * i, span)
        part = jnp.dot(hb[i].reshape(2 * span, ff), wd[...], preferred_element_type=jnp.float32)
        part = part + jnp.concatenate([out_part[pl.ds(first_at, span)], out_part[pl.ds(half + first_at, span)]], axis=0)
        for j in range(4):
            moved = part if j == 0 else pltpu.roll(part, (4 - j) * chunk, 1)
            y_send[i, j] = moved[:, :chunk]
        for which in (1 - col, col):
            pair_copy(i, which).start()

        @pl.when(i > 1)
        def _():
            cross(i - 2)

        return carry

    def finish(i, carry):
        pair_copy(i, col).wait()
        over_copy(i).wait()
        total = y_send[i, me_yz] + y_pair[i, col] + y_recv[i]
        for e in range(2):
            y_ref[pl.ds(pl.multiple_of(half * e + span * i, span), span), :] = total[span * e:span * e + span]
        return carry

    lax.fori_loop(0, groups, product, 0)
    cross(groups - 2)
    lax.fori_loop(0, groups - 3, finish, 0)
    cross(groups - 1)
    lax.fori_loop(groups - 3, groups, finish, 0)


def tail(g_first, g_peer, g_own, o_blocks, w_down, w_out):
    half = g_own.shape[0]
    rows = 2 * half
    span = 16
    groups = half // span
    ff, cols = w_down.shape
    chunk = cols // 4
    owned = o_blocks.shape[1]
    o_width = w_out.shape[0]
    any_spec, vmem_spec = pl.BlockSpec(memory_space=pl.ANY), pl.BlockSpec(memory_space=pltpu.VMEM)
    dma = pltpu.SemaphoreType.DMA
    f32, bf16 = jnp.float32, jnp.bfloat16
    return pl.pallas_call(
        tail_kernel,
        out_shape=jax.ShapeDtypeStruct((rows, chunk), f32),
        in_specs=[vmem_spec, vmem_spec, any_spec, vmem_spec, any_spec, any_spec],
        out_specs=pl.BlockSpec(memory_space=pltpu.VMEM),
        scratch_shapes=[
            pltpu.VMEM((half, 2 * ff), f32),
            pltpu.VMEM((4, owned, o_width), bf16),
            pltpu.VMEM((8, owned, o_width), bf16),
            pltpu.VMEM((rows, o_width), f32),
            pltpu.VMEM((groups, 2, span, ff), bf16),
            pltpu.VMEM((ff, cols), bf16),
            pltpu.VMEM((o_width, cols), bf16),
            pltpu.VMEM((rows, cols), f32),
            pltpu.VMEM((groups, 4, 2 * span, chunk), f32),
            pltpu.VMEM((groups, 2, 2 * span, chunk), f32),
            pltpu.VMEM((groups, 2 * span, chunk), f32),
            pltpu.VMEM((groups, 2 * span, chunk), f32),
            dma((3,)), dma((groups,)), dma((8,)), dma((8,)), dma((groups,)), dma((groups,)),
            dma((groups, 2)), dma((groups, 2)), dma((groups,)), dma((groups,)),
        ],
        compiler_params=pltpu.CompilerParams(collective_id=1, has_side_effects=True, vmem_limit_bytes=51 * 1024 * 1024),
        cost_estimate=pl.CostEstimate(flops=2 * rows * (ff + o_width) * cols, bytes_accessed=2 * (ff + o_width) * cols, transcendentals=half * ff),
        name='tail',
    )(g_first, g_peer, g_own, o_blocks, w_down, w_out)


def rotary(values, positions):
    half_dim = values.shape[-1] // 2
    inv_freq = ROPE_BASE ** (-jnp.arange(half_dim, dtype=jnp.float32) / half_dim)
    angles = positions.astype(jnp.float32)[:, None, None] * inv_freq
    cos_part = jnp.cos(angles)
    sin_part = jnp.sin(angles)
    lo_half = values[..., :half_dim]
    hi_half = values[..., half_dim:]
    return jnp.concatenate([lo_half * cos_part - hi_half * sin_part, hi_half * cos_part + lo_half * sin_part], axis=-1)


def solution(mesh):
    x_size = mesh.shape['x']
    yz_size = mesh.shape['yz']
    all_axes = ('x', 'yz')

    def local_step(x_in, ln_scale, w_gate_up, w_attn, w_down, w_out, k_cache, v_cache, lengths, positions):
        local_rows, seq_len, head_dim = k_cache.shape
        q_width = w_out.shape[0] * yz_size
        num_heads = q_width // head_dim
        d_model = x_in.shape[1] * x_size * yz_size
        z_blocks, g_first, g_send, g_own = head(x_in, ln_scale, w_gate_up, w_attn, d_model, EARLY)
        g_peer = lax.ppermute(g_send, 'x', [(0, 1), (1, 0)])
        proj_local = z_blocks.transpose(1, 0, 2).reshape(local_rows, -1)
        q_raw = proj_local[:, :q_width].reshape(local_rows, num_heads, head_dim)
        k_tok = proj_local[:, q_width:q_width + head_dim]
        v_tok = proj_local[:, q_width + head_dim:]
        q_rot = rotary(q_raw.astype(jnp.float32), positions).astype(jnp.bfloat16)
        k_rot = rotary(k_tok[:, None, :].astype(jnp.float32), positions)[:, 0].astype(jnp.bfloat16)
        cols = jnp.stack([k_rot, v_tok]).astype(jnp.float32).transpose(0, 2, 1)
        cols = jnp.pad(cols, ((0, 0), (0, 0), (0, 128 - local_rows)))
        attn_out, k_new, v_new = attend(q_rot, cols, k_cache, v_cache, lengths)
        o_blocks = attn_out.reshape(local_rows, yz_size, q_width // yz_size).transpose(1, 0, 2)
        mixed_sum = tail(g_first, g_peer, g_own, o_blocks, w_down, w_out)
        y_out = (x_in.astype(jnp.float32) + mixed_sum).astype(jnp.bfloat16)
        return y_out, k_new, v_new

    row_spec = P(None, all_axes)
    vec_spec = P(all_axes)
    cache_spec = P(all_axes, None, None)
    return jax.shard_map(
        local_step,
        mesh=mesh,
        in_specs=(row_spec, vec_spec, P('x', None, 'yz'), P('x', 'yz'), P('yz', 'x'), P('yz', 'x'), cache_spec, cache_spec, vec_spec, vec_spec),
        out_specs=(row_spec, cache_spec, cache_spec),
        check_vma=False,
    )
```
